32 devices in a mesh: dp: 2 (over core), ctx: 4 (over z), fsdp: 4 (over y, x).
Axes of the slice: x: 2, y: 2, z: 4, core: 2. Of those that a mesh axis runs over, the one named last changes fastest.
Arguments:
- tokens: bfloat16 [2, 2, 1024, 1536], P(None, 'dp', ('ctx', 'fsdp')), may hold values from -6 to 6
- cotangent: bfloat16 [2, 2, 1024, 1536], P(None, 'dp', ('ctx', 'fsdp')), may hold values from -6 to 6
- attn_gain: bfloat16 [1536], P(('dp', 'ctx', 'fsdp')), may hold values from 0.5 to 1.5
- w_qkv: bfloat16 [1536, 3072], P(None, ('dp', 'ctx', 'fsdp')), may hold values from -5 to 5
- w_out: bfloat16 [1536, 1536], P(('dp', 'ctx', 'fsdp')), may hold values from -1.5 to 1.5
- mlp_gain: bfloat16 [1536], P(('dp', 'ctx', 'fsdp')), may hold values from 0.5 to 1.5
- w_gate_up: bfloat16 [1536, 8192], P(None, ('dp', 'ctx', 'fsdp')), may hold values from -0.15625 to 0.15625
- w_down: bfloat16 [4096, 1536], P(('dp', 'ctx', 'fsdp')), may hold values from -0.09375 to 0.09375
Outputs:
- block_out: bfloat16 [2, 2, 1024, 1536], P(None, 'dp', ('ctx', 'fsdp'))
- grad_tokens: bfloat16 [2, 2, 1024, 1536], P(None, 'dp', ('ctx', 'fsdp'))
- grad_attn_gain: float32 [1536], P(('dp', 'ctx', 'fsdp'))
- grad_w_qkv: float32 [1536, 3072], P(None, ('dp', 'ctx', 'fsdp'))
- grad_w_out: float32 [1536, 1536], P(('dp', 'ctx', 'fsdp'))
- grad_mlp_gain: float32 [1536], P(('dp', 'ctx', 'fsdp'))
- grad_w_gate_up: float32 [1536, 8192], P(None, ('dp', 'ctx', 'fsdp'))
- grad_w_down: float32 [4096, 1536], P(('dp', 'ctx', 'fsdp'))
The draws below stay inside these ranges and needn't reach their ends.
All inputs are finite; a program needn't handle non-finite values.
Results may differ from the reference program's by a relative error of at most 0.02.
Values may be sent and summed in bfloat16 or wider, within the bound.
A program may use at most 320 MiB of HBM per device.

```python
import jax
import jax.numpy as jnp
from jax import lax

D = 1536
H = 16
KVH = 8
HD = 96
FF = 4096
MB = 2
SEQS = 2
LEN = 1024


def draw_w_qkv(key, part):
    base = jax.random.normal(key, (D, (H + 2 * KVH) * HD), jnp.float32)
    base = jnp.clip(base, -6.0, 6.0) * D ** (-0.5)
    return jnp.clip(base, -5.0, 5.0).astype(jnp.bfloat16)


def level_of(key, shape, pieces, least, top_value):
    def one(position, shards_of):
        heights = jax.random.uniform(jax.random.fold_in(jax.random.fold_in(key, 6), position), (shards_of,), jnp.float32, least / len(pieces), top_value / len(pieces))
        return jnp.repeat(jnp.exp(heights), shape[position] // shards_of).reshape((-1,) + (1,) * (len(shape) - position - 1))

    gain = one(*pieces[0])
    for cut in pieces[1:]:
        gain = gain * one(*cut)
    return gain


def normal_values(own_key, extent, spread, most, split=(), kind=jnp.bfloat16):
    loudness = level_of(own_key, extent, split, -0.22, 0.18) if split else 1.0
    values = jax.random.normal(own_key, extent, jnp.float32) * spread * loudness
    return jnp.minimum(jnp.maximum(values, -most), most).astype(kind)


def setup_inputs(seed: int = 0) -> dict:
    streams_of = jax.random.split(jax.random.key(seed), 9)
    return {
        "tokens": normal_values(streams_of[0], (MB, SEQS, LEN, D), 1.0, 6.0, ((1, 2), (2, 16))),
        "cotangent": normal_values(streams_of[1], (MB, SEQS, LEN, D), 1.0, 6.0, ((1, 2), (2, 16))),
        "attn_gain": jnp.clip(1.0 + 0.1 * jax.random.normal(streams_of[2], (D,), jnp.float32), 0.5, 1.5).astype(jnp.bfloat16),
        "w_qkv": draw_w_qkv(jax.random.fold_in(streams_of[8], 71), 0),
        "w_out": normal_values(streams_of[4], (H * HD, D), 16 ** -0.5, 1.5, ((0, 32),)),
        "mlp_gain": jnp.clip(1.0 + 0.1 * jax.random.normal(streams_of[5], (D,), jnp.float32), 0.5, 1.5).astype(jnp.bfloat16),
        "w_gate_up": normal_values(streams_of[6], (D, 2 * FF), D ** -0.5, 0.15625, ((1, 32),)),
        "w_down": normal_values(streams_of[7], (FF, D), FF ** -0.5, 0.09375, ((0, 32),)),
    }


@jax.custom_vjp
def low(v):
    return lax.optimization_barrier(v.astype(jnp.bfloat16)).astype(jnp.float32)

@jax.custom_vjp
def low_back(v):
    return v

def low_keep(v):
    return (low(v), None)

def low_pass(kept, grad):
    return (grad,)

def back_keep(v):
    return (v, None)

def back_low(kept, grad):
    return (low(grad),)
low.defvjp(low_keep, low_pass)
low_back.defvjp(back_keep, back_low)
EPS = 1e-05
THETA = 100000.0
NEG = -1e+30

def matmul(left, right):
    return jnp.dot(left, right, preferred_element_type=jnp.float32, precision=lax.Precision.HIGHEST)

def rms_norm(values, gain_vec):
    return values * lax.rsqrt(lax.optimization_barrier(jnp.mean(values * values, axis=-1, keepdims=True)) + EPS) * gain_vec

def tables(start, length, width):
    half_width = width // 2
    frequency = THETA ** (-(jnp.arange(half_width, dtype=jnp.float32) * 2.0) / width)
    angles = (start + jnp.arange(length, dtype=jnp.int32)).astype(jnp.float32)[:, None] * frequency[None, :]
    return (jnp.cos(angles), jnp.sin(angles))

def rotate(values, cosine, sine_table):
    half_width = values.shape[-1] // 2
    first_half = values[..., :half_width]
    second_half = values[..., half_width:]
    cos_b = cosine[:, None, :]
    sin_b = sine_table[:, None, :]
    return jnp.concatenate([first_half * cos_b - second_half * sin_b, second_half * cos_b + first_half * sin_b], axis=-1)

def swiglu(both):
    return jax.nn.silu(both[:, :FF]) * both[:, FF:]

def attention(queries, keys, values):
    length = queries.shape[0]
    rows_block = min(512, length)
    groups = H // KVH
    factor = HD ** (-0.5)

    def block(inputs):
        block_q, start = inputs
        grouped = block_q.reshape(rows_block, KVH, groups, HD)
        scores = jnp.einsum('qkgd,tkd->kgqt', grouped, keys, precision=lax.Precision.HIGHEST) * factor
        scores = low_back(scores)
        allowed = jnp.arange(length, dtype=jnp.int32)[None, :] <= (start + jnp.arange(rows_block, dtype=jnp.int32))[:, None]
        scores = jnp.where(allowed, scores, NEG)
        peak = lax.optimization_barrier(jnp.max(scores, axis=-1, keepdims=True))
        weights = jnp.exp(scores - peak)
        probs = weights / lax.optimization_barrier(jnp.sum(weights, axis=-1, keepdims=True))
        mixed = jnp.einsum('kgqt,tkd->qkgd', low(probs), values, precision=lax.Precision.HIGHEST)
        return mixed.reshape(rows_block, H * HD)
    starts = jnp.arange(length // rows_block, dtype=jnp.int32) * rows_block
    blocks = lax.map(jax.checkpoint(block), (queries.reshape(length // rows_block, rows_block, H, HD), starts))
    return blocks.reshape(length, H * HD)

def forward(inputs, gain_one, mix_qkv, mix_out, gain_two, mix_gate_up, mix_down):
    length = inputs.shape[0]
    normed = low(rms_norm(inputs, gain_one))
    mixed = low_back(matmul(normed, mix_qkv))
    cosine, sine_table = tables(0, length, HD)
    queries = low(rotate(mixed[:, :H * HD].reshape(length, H, HD), cosine, sine_table))
    keys = low(rotate(mixed[:, H * HD:(H + KVH) * HD].reshape(length, KVH, HD), cosine, sine_table))
    values = low(mixed[:, (H + KVH) * HD:].reshape(length, KVH, HD))
    attended = low(low_back(attention(queries, keys, values)))
    resid = inputs + low_back(matmul(attended, mix_out))
    normed_two = low(rms_norm(resid, gain_two))
    both = low_back(matmul(normed_two, mix_gate_up))
    acted = low(swiglu(both))
    return resid + low_back(matmul(acted, mix_down))

def reference(tokens, cotangent, attn_gain, w_qkv, w_out, mlp_gain, w_gate_up, w_down):
    weights_all = tuple((item.astype(jnp.float32) for item in (attn_gain, w_qkv, w_out, mlp_gain, w_gate_up, w_down)))
    flat_in = tokens.reshape(MB * SEQS, LEN, D).astype(jnp.float32)
    flat_grad = cotangent.reshape(MB * SEQS, LEN, D).astype(jnp.float32)

    def one_sequence(totals, inputs):
        seq_in, seq_grad = inputs
        result, pull = jax.vjp(forward, seq_in, *weights_all)
        grads = pull(seq_grad)
        totals = tuple((total_one + grad_one for total_one, grad_one in zip(totals, grads[1:])))
        return (totals, (result.astype(jnp.bfloat16), grads[0].astype(jnp.bfloat16)))
    start_totals = tuple((jnp.zeros(item.shape, jnp.float32) for item in weights_all))
    totals, (results, grads_in) = lax.scan(one_sequence, start_totals, (flat_in, flat_grad))
    return (results.reshape(MB, SEQS, LEN, D), grads_in.reshape(MB, SEQS, LEN, D), totals[0], totals[1], totals[2], totals[3], totals[4], totals[5])
```

```python
import jax
import jax.numpy as jnp
from jax import lax
from jax.sharding import PartitionSpec as P

D = 1536
H = 16
KVH = 8
HD = 96
FF = 4096


EPS = 1e-05
THETA = 100000.0
NEG = -1e30


def in_blocks(value, dim, length):
    lengths = value.shape
    pieces = value.reshape(*lengths[:dim], length, lengths[dim] // length, *lengths[dim + 1 :])
    return jnp.moveaxis(pieces, dim, 0)


def sum_at_owner(value, axis, dim):
    pieces = in_blocks(value, dim, lax.axis_size(axis))
    arrived = lax.all_to_all(pieces, axis, split_axis=0, concat_axis=0, tiled=True)
    return arrived.astype(jnp.float32).sum(axis=0)


def side_by_side(arrays, axis, dim, along):
    both = jnp.concatenate(arrays, axis=along)
    whole, at, finished = (sum_at_owner(both, axis, dim), 0, [])
    for a in arrays:
        finished.append(lax.slice_in_dim(whole, at, at + a.shape[along], axis=along))
        at += a.shape[along]
    return tuple(finished)


def rms_norm(values, gain_vec):
    return values * lax.rsqrt(jnp.mean(values * values, axis=-1, keepdims=True) + EPS) * gain_vec


def tables(start, length, width):
    half_width = width // 2
    frequency = THETA ** (-(jnp.arange(half_width, dtype=jnp.float32) * 2.0) / width)
    angles = (start + jnp.arange(length, dtype=jnp.int32)).astype(jnp.float32)[:, None] * frequency[
        None, :
    ]
    return (jnp.cos(angles), jnp.sin(angles))


def rotate(values, cosine, sine_table):
    half_width = values.shape[-1] // 2
    first_half = values[..., :half_width]
    second_half = values[..., half_width:]
    cos_b = cosine[:, None, :]
    sin_b = sine_table[:, None, :]
    return jnp.concatenate(
        [first_half * cos_b - second_half * sin_b, second_half * cos_b + first_half * sin_b],
        axis=-1,
    )


def swiglu(both):
    return jax.nn.silu(both[:, :FF]) * both[:, FF:]


def inner(left, right):
    return lax.dot_general(
        left, right, (((0,), (0,)), ((), ())), preferred_element_type=jnp.float32
    )


def outer(left, right):
    return lax.dot_general(
        left, right, (((1,), (1,)), ((), ())), preferred_element_type=jnp.float32
    )


def unchanged(state):
    return state


def on_device_gathered(tokens, cotangent, attn_gain, w_qkv, w_out, mlp_gain, w_gate_up, w_down):
    tok_count = tokens.shape[2]
    groups = H // KVH
    factor = HD ** (-0.5)
    seq_length = tok_count * lax.axis_size(("ctx", "fsdp"))
    pos_first = lax.axis_index(("ctx", "fsdp")) * tok_count
    positions = pos_first + jnp.arange(tok_count, dtype=jnp.int32)
    pos_last = pos_first + tok_count - 1
    cosine, sine_table = tables(pos_first, tok_count, HD)
    sums = [
        jnp.zeros((D,), jnp.float32),
        jnp.zeros((D, (H + 2 * KVH) * HD), jnp.float32),
        jnp.zeros((H * HD, D), jnp.float32),
        jnp.zeros((D,), jnp.float32),
        jnp.zeros((D, 2 * FF), jnp.float32),
        jnp.zeros((FF, D), jnp.float32),
    ]
    outputs = []
    in_grads = []
    whole = (
        lax.all_gather(attn_gain, ("dp", "ctx", "fsdp"), axis=0, tiled=True),
        lax.all_gather(w_qkv, ("dp", "ctx", "fsdp"), axis=1, tiled=True),
        lax.all_gather(w_out, ("dp", "ctx", "fsdp"), axis=0, tiled=True),
        lax.all_gather(mlp_gain, ("dp", "ctx", "fsdp"), axis=0, tiled=True),
        lax.all_gather(w_gate_up, ("dp", "ctx", "fsdp"), axis=1, tiled=True),
        lax.all_gather(w_down, ("dp", "ctx", "fsdp"), axis=0, tiled=True),
    )
    for step_index in range(tokens.shape[0]):
        gain_one, mix_qkv, mix_out, gain_two, mix_gate_up, mix_down = whole
        inputs = tokens[step_index, 0].astype(jnp.float32)
        normed = rms_norm(inputs, gain_one.astype(jnp.float32)).astype(jnp.bfloat16)
        mixed = jnp.dot(normed, mix_qkv, preferred_element_type=jnp.float32)
        queries = rotate(mixed[:, : H * HD].reshape(tok_count, H, HD), cosine, sine_table).astype(
            jnp.bfloat16
        )
        key_rows = rotate(
            mixed[:, H * HD : (H + KVH) * HD].reshape(tok_count, KVH, HD), cosine, sine_table
        )
        key_rows = key_rows.astype(jnp.bfloat16).reshape(tok_count, KVH * HD)
        value_rows = mixed[:, (H + KVH) * HD :].astype(jnp.bfloat16)
        grouped = queries.reshape(tok_count, KVH, groups, HD)
        start_state = (
            jnp.full((KVH, groups, tok_count), NEG, jnp.float32),
            jnp.zeros((KVH, groups, tok_count), jnp.float32),
            jnp.zeros((KVH, groups, tok_count, HD), jnp.float32),
        )
        piece = (
            lax.all_gather(key_rows, ("ctx", "fsdp"), axis=0, tiled=True),
            lax.all_gather(value_rows, ("ctx", "fsdp"), axis=0, tiled=True),
        )

        def work(state):
            best, total, summed = state
            key_count = piece[0].shape[0]
            keys = piece[0].reshape(key_count, KVH, HD)
            values = piece[1].reshape(key_count, KVH, HD)
            scores = (
                jnp.einsum("qkgd,tkd->kgqt", grouped, keys, preferred_element_type=jnp.float32)
                * factor
            )
            allowed = jnp.arange(key_count, dtype=jnp.int32)[None, :] <= positions[:, None]
            scores = jnp.where(allowed, scores, NEG)
            new_best = jnp.maximum(best, jnp.max(scores, axis=-1))
            weights = jnp.where(allowed, jnp.exp(scores - new_best[..., None]), 0.0)
            total = jnp.sum(weights, axis=-1)
            summed = jnp.einsum(
                "kgqt,tkd->kgqd",
                weights.astype(jnp.bfloat16),
                values,
                preferred_element_type=jnp.float32,
            )
            return (new_best, total, summed)

        best, total, summed = lax.cond(jnp.int32(0) <= pos_last, work, unchanged, start_state)
        head_out = summed / total[..., None]
        log_total = best + jnp.log(total)
        attended = (
            jnp.transpose(head_out, (2, 0, 1, 3)).reshape(tok_count, H * HD).astype(jnp.bfloat16)
        )
        resid = inputs + jnp.dot(attended, mix_out, preferred_element_type=jnp.float32)
        normed_two = rms_norm(resid, gain_two.astype(jnp.float32)).astype(jnp.bfloat16)
        both = jnp.dot(normed_two, mix_gate_up, preferred_element_type=jnp.float32)
        acted = swiglu(both).astype(jnp.bfloat16)
        result = resid + jnp.dot(acted, mix_down, preferred_element_type=jnp.float32)
        outputs.append(result.astype(jnp.bfloat16))
        gain_one, mix_qkv, mix_out, gain_two, mix_gate_up, mix_down = whole
        up_low = cotangent[step_index, 0]
        upstream = up_low.astype(jnp.float32)
        sums[5] = sums[5] + inner(acted, up_low)
        d_act = outer(up_low, mix_down)
        _, pull_glu = jax.vjp(swiglu, both)
        d_both = pull_glu(d_act)[0].astype(jnp.bfloat16)
        sums[4] = sums[4] + inner(normed_two, d_both)
        d_normed_two = outer(d_both, mix_gate_up)
        _, pull_two = jax.vjp(rms_norm, resid, gain_two.astype(jnp.float32))
        d_resid_norm, d_gain_two = pull_two(d_normed_two)
        sums[3] = sums[3] + d_gain_two
        d_resid = upstream + d_resid_norm
        d_resid_low = d_resid.astype(jnp.bfloat16)
        sums[2] = sums[2] + inner(attended, d_resid_low)
        d_attended = outer(d_resid_low, mix_out).astype(jnp.bfloat16)
        d_grouped = d_attended.reshape(tok_count, KVH, groups, HD)
        delta = jnp.einsum("qkgd,kgqd->kgq", d_grouped.astype(jnp.float32), head_out)
        zero_q = jnp.zeros((tok_count, KVH, groups, HD), jnp.float32)
        back_state = (
            zero_q,
            jnp.zeros((seq_length, KVH * HD), jnp.float32),
            jnp.zeros((seq_length, KVH * HD), jnp.float32),
        )
        attend_piece = (
            lax.all_gather(key_rows, ("ctx", "fsdp"), axis=0, tiled=True),
            lax.all_gather(value_rows, ("ctx", "fsdp"), axis=0, tiled=True),
        )

        def attend_work(state):
            key_count = attend_piece[0].shape[0]
            keys = attend_piece[0].reshape(key_count, KVH, HD)
            values = attend_piece[1].reshape(key_count, KVH, HD)
            scores = (
                jnp.einsum("qkgd,tkd->kgqt", grouped, keys, preferred_element_type=jnp.float32)
                * factor
            )
            allowed = jnp.arange(key_count, dtype=jnp.int32)[None, :] <= positions[:, None]
            scores = jnp.where(allowed, scores, NEG)
            probs = jnp.where(allowed, jnp.exp(scores - log_total[..., None]), 0.0)
            d_probs = jnp.einsum(
                "qkgd,tkd->kgqt", d_grouped, values, preferred_element_type=jnp.float32
            )
            d_scores = (probs * (d_probs - delta[..., None])).astype(jnp.bfloat16)
            grad_q = jnp.einsum(
                "kgqt,tkd->qkgd", d_scores, keys, preferred_element_type=jnp.float32
            )
            piece_k = (
                jnp.einsum("kgqt,qkgd->tkd", d_scores, grouped, preferred_element_type=jnp.float32)
                * factor
            )
            piece_v = jnp.einsum(
                "kgqt,qkgd->tkd",
                probs.astype(jnp.bfloat16),
                d_grouped,
                preferred_element_type=jnp.float32,
            )
            grad_k = piece_k.reshape(key_count, KVH * HD)
            grad_v = piece_v.reshape(key_count, KVH * HD)
            return (grad_q, grad_k, grad_v)

        back_result = lax.cond(jnp.int32(0) <= pos_last, attend_work, unchanged, back_state)
        grad_q = back_result[0]
        summed_k, summed_v = side_by_side(
            (back_result[1].astype(jnp.bfloat16), back_result[2].astype(jnp.bfloat16)),
            ("ctx", "fsdp"),
            0,
            1,
        )
        d_q_raw = rotate(grad_q.reshape(tok_count, H, HD) * factor, cosine, -sine_table).reshape(
            tok_count, H * HD
        )
        d_k_raw = rotate(summed_k.reshape(tok_count, KVH, HD), cosine, -sine_table).reshape(
            tok_count, KVH * HD
        )
        d_mixed = jnp.concatenate([d_q_raw, d_k_raw, summed_v], axis=1).astype(jnp.bfloat16)
        sums[1] = sums[1] + inner(normed, d_mixed)
        d_normed = outer(d_mixed, mix_qkv)
        _, pull_one = jax.vjp(rms_norm, inputs, gain_one.astype(jnp.float32))
        d_inputs_norm, d_gain_one = pull_one(d_normed)
        sums[0] = sums[0] + d_gain_one
        in_grads.append((d_resid + d_inputs_norm).astype(jnp.bfloat16))
    grad_gain_one, grad_qkv, grad_out, grad_gain_two, grad_gate_up, grad_down = (
        lax.psum_scatter(sums[0], ("dp", "ctx", "fsdp"), scatter_dimension=0, tiled=True),
        lax.psum_scatter(sums[1], ("dp", "ctx", "fsdp"), scatter_dimension=1, tiled=True),
        lax.psum_scatter(sums[2], ("dp", "ctx", "fsdp"), scatter_dimension=0, tiled=True),
        lax.psum_scatter(sums[3], ("dp", "ctx", "fsdp"), scatter_dimension=0, tiled=True),
        lax.psum_scatter(sums[4], ("dp", "ctx", "fsdp"), scatter_dimension=1, tiled=True),
        lax.psum_scatter(sums[5], ("dp", "ctx", "fsdp"), scatter_dimension=0, tiled=True),
    )
    block_out = jnp.stack(outputs)[:, None]
    grad_tokens = jnp.stack(in_grads)[:, None]
    return (
        block_out,
        grad_tokens,
        grad_gain_one,
        grad_qkv,
        grad_out,
        grad_gain_two,
        grad_gate_up,
        grad_down,
    )


TP = ("dp", "ctx")
ALL = ("dp", "ctx", "fsdp")


def dot(left, right):
    return jnp.dot(left, right, preferred_element_type=jnp.float32)


def qkv_owner(sizes):
    moves = []
    for head in range(H + 2 * KVH):
        if head < H:
            group, slot = head // 2, head % 2
        elif head < H + KVH:
            group, slot = head - H, 2
        else:
            group, slot = head - H - KVH, 3
        moves.append((head, group * sizes["fsdp"] + slot))
    return moves


def hidden_of(device, sizes):
    ctx = sizes["ctx"]
    return (device % ctx) * sizes["dp"] + device // ctx


def down_owner(sizes):
    n, f = sizes["dp"] * sizes["ctx"], sizes["fsdp"]
    return [
        (hidden_of(device, sizes) * f + slot, device * f + slot)
        for device in range(n)
        for slot in range(f)
    ]


def up_owner(sizes):
    n, f = sizes["dp"] * sizes["ctx"], sizes["fsdp"]
    half = n * f // 2
    moves = []
    for device in range(n):
        first = hidden_of(device, sizes) * (f // 2)
        for slot in range(f):
            source = first + slot if slot < f // 2 else half + first + slot - f // 2
            moves.append((source, device * f + slot))
    return moves


def back(moves):
    return [(to, source) for source, to in moves]


def gather_tp(value):
    return lax.all_gather(value, TP, axis=0, tiled=True)


def sum_tp(value):
    return lax.psum_scatter(value.astype(jnp.bfloat16), TP, scatter_dimension=0, tiled=True).astype(
        jnp.float32
    )


def norm_back(values, scale, gain, incoming):
    weighted = incoming * gain
    mean = jnp.mean(weighted * values, axis=-1, keepdims=True)
    return scale * weighted - values * (scale * scale * scale) * mean


def on_device(tokens, cotangent, attn_gain, w_qkv, w_out, mlp_gain, w_gate_up, w_down):
    sizes = {name: lax.axis_size(name) for name in ALL}
    dp, ctx, fs = sizes["dp"], sizes["ctx"], sizes["fsdp"]
    mb, _, span, _ = tokens.shape
    rows = mb * span
    f_index = lax.axis_index("fsdp")
    length = span * ctx * fs
    factor = HD ** (-0.5)
    hidden = FF // (dp * ctx)

    gains = lax.all_gather(jnp.stack([attn_gain, mlp_gain]), ALL, axis=1, tiled=True)
    gain_one = gains[0].astype(jnp.float32)
    gain_two = gains[1].astype(jnp.float32)
    qkv = lax.all_gather(lax.ppermute(w_qkv, ALL, qkv_owner(sizes)), "fsdp", axis=0)
    out_w = lax.all_gather(w_out, "fsdp", axis=0, tiled=True)
    gate_up = lax.all_gather(lax.ppermute(w_gate_up, ALL, up_owner(sizes)), "fsdp", axis=1, tiled=True)
    down = lax.all_gather(lax.ppermute(w_down, ALL, down_owner(sizes)), "fsdp", axis=0, tiled=True)

    x = tokens.reshape(rows, D).astype(jnp.float32)
    dy = cotangent.reshape(rows, D)
    scale_one = lax.rsqrt(jnp.mean(x * x, axis=-1, keepdims=True) + EPS)
    normed = gather_tp((x * scale_one * gain_one).astype(jnp.bfloat16))
    dy_all = gather_tp(dy)

    heads = jnp.stack([dot(normed, qkv[h]) for h in range(4)])
    positions = (
        (jnp.arange(ctx, dtype=jnp.int32)[:, None] * fs + f_index) * span
        + jnp.arange(span, dtype=jnp.int32)[None, :]
    )
    frequency = THETA ** (-(jnp.arange(HD // 2, dtype=jnp.float32) * 2.0) / HD)
    angles = positions.astype(jnp.float32)[:, :, None] * frequency
    cosine = jnp.cos(angles)[None, None, :, None]
    sine = jnp.sin(angles)[None, None, :, None]

    def turn(values, sin_b):
        a, b = values[..., : HD // 2], values[..., HD // 2 :]
        return jnp.concatenate([a * cosine - b * sin_b, b * cosine + a * sin_b], axis=-1)

    heads = heads.reshape(4, dp, ctx, mb, span, HD)
    turned = turn(heads[:3], sine)
    heads = jnp.concatenate([turned, heads[3:]]).astype(jnp.bfloat16)

    def to_units(values):
        count = values.shape[0]
        values = values.transpose(1, 3, 0, 2, 4, 5)
        values = values.reshape(dp * mb, count, ctx, span, HD)
        values = lax.all_to_all(values, "fsdp", split_axis=0, concat_axis=0, tiled=True)
        return values.transpose(1, 2, 0, 3, 4).reshape(count, length, HD)

    def to_rows(values):
        count = values.shape[0]
        values = values.reshape(count, ctx, fs, span, HD).transpose(2, 0, 1, 3, 4)
        values = lax.all_to_all(values, "fsdp", split_axis=0, concat_axis=0, tiled=True)
        values = values.reshape(dp, mb, count, ctx, span, HD).transpose(2, 0, 3, 1, 4, 5)
        return values.reshape(count, dp * ctx * rows, HD)

    unit = to_units(heads)
    q, k, v = unit[:2], unit[2], unit[3]
    scores = jnp.einsum("hqd,kd->hqk", q, k, preferred_element_type=jnp.float32) * factor
    allowed = jnp.arange(length)[None, :] <= jnp.arange(length)[:, None]
    scores = jnp.where(allowed, scores, NEG)
    best = jnp.max(scores, axis=-1, keepdims=True)
    weights = jnp.where(allowed, jnp.exp(scores - best), 0.0)
    probs = weights / jnp.sum(weights, axis=-1, keepdims=True)
    probs_low = probs.astype(jnp.bfloat16)
    att = jnp.einsum("hqk,kd->hqd", probs_low, v, preferred_element_type=jnp.float32)
    attended = to_rows(att.astype(jnp.bfloat16))
    out_heads = out_w.reshape(2, HD, D)
    partial = dot(attended[0], out_heads[0]) + dot(attended[1], out_heads[1])
    resid = x + sum_tp(partial)
    scale_two = lax.rsqrt(jnp.mean(resid * resid, axis=-1, keepdims=True) + EPS)
    normed_two = gather_tp((resid * scale_two * gain_two).astype(jnp.bfloat16))
    gate = dot(normed_two, gate_up[:, :hidden])
    up = dot(normed_two, gate_up[:, hidden:])
    sig = 1.0 / (1.0 + jnp.exp(-gate))
    silu = gate * sig
    act = (silu * up).astype(jnp.bfloat16)
    block_out = (resid + sum_tp(dot(act, down))).astype(jnp.bfloat16)

    grad_down = inner(act, dy_all)
    d_act = outer(dy_all, down)
    d_gate = d_act * up * (sig * (1.0 + gate * (1.0 - sig)))
    d_up = d_act * silu
    d_both = jnp.concatenate([d_gate, d_up], axis=1).astype(jnp.bfloat16)
    grad_gate_up = inner(normed_two, d_both)
    d_two = sum_tp(outer(d_both, gate_up))
    grad_two = jnp.sum(d_two * resid * scale_two, axis=0)
    d_resid = dy.astype(jnp.float32) + norm_back(resid, scale_two, gain_two, d_two)
    d_resid_all = gather_tp(d_resid.astype(jnp.bfloat16))
    grad_out = jnp.concatenate([inner(attended[h], d_resid_all) for h in range(2)], axis=0)
    d_att = jnp.stack([outer(d_resid_all, out_heads[h]) for h in range(2)]).astype(jnp.bfloat16)
    d_unit = to_units(d_att.reshape(2, dp, ctx, mb, span, HD))
    d_probs = jnp.einsum("hqd,kd->hqk", d_unit, v, preferred_element_type=jnp.float32)
    delta = jnp.sum(probs * d_probs, axis=-1, keepdims=True)
    d_scores = (probs * (d_probs - delta)).astype(jnp.bfloat16)
    d_q = jnp.einsum("hqk,kd->hqd", d_scores, k, preferred_element_type=jnp.float32) * factor
    d_k = jnp.einsum("hqk,hqd->kd", d_scores, q, preferred_element_type=jnp.float32) * factor
    d_v = jnp.einsum("hqk,hqd->kd", probs_low, d_unit, preferred_element_type=jnp.float32)
    all_pos = jnp.arange(length, dtype=jnp.float32)[:, None] * frequency
    cos_u, sin_u = jnp.cos(all_pos), jnp.sin(all_pos)

    def unturn(values):
        a, b = values[..., : HD // 2], values[..., HD // 2 :]
        return jnp.concatenate([a * cos_u + b * sin_u, b * cos_u - a * sin_u], axis=-1)

    d_heads = jnp.concatenate([unturn(d_q), unturn(d_k)[None], d_v[None]]).astype(jnp.bfloat16)
    d_mixed = to_rows(d_heads)
    grad_qkv = jnp.stack([inner(normed, d_mixed[h]) for h in range(4)])
    d_normed = sum_tp(sum(outer(d_mixed[h], qkv[h]) for h in range(4)))
    grad_one = jnp.sum(d_normed * x * scale_one, axis=0)
    grad_tokens = (d_resid + norm_back(x, scale_one, gain_one, d_normed)).astype(jnp.bfloat16)

    def reduce_rows(value, dim, moves):
        value = lax.psum_scatter(value.astype(jnp.bfloat16), "fsdp", scatter_dimension=dim, tiled=True)
        if moves is not None:
            value = lax.ppermute(value, ALL, back(moves))
        return value.astype(jnp.float32)

    gain_grads = lax.psum_scatter(jnp.stack([grad_one, grad_two]), ALL, scatter_dimension=1, tiled=True)
    return (
        block_out.reshape(tokens.shape),
        grad_tokens.reshape(tokens.shape),
        gain_grads[0],
        reduce_rows(grad_qkv, 0, qkv_owner(sizes)).reshape(D, HD),
        reduce_rows(grad_out, 0, None),
        gain_grads[1],
        reduce_rows(grad_gate_up, 1, up_owner(sizes)),
        reduce_rows(grad_down, 0, down_owner(sizes)),
    )


def fits(mesh):
    return mesh.shape["dp"] * mesh.shape["ctx"] == KVH and mesh.shape["fsdp"] == 4


def solution(mesh):
    placed = (
        P(None, "dp", ("ctx", "fsdp"), None),
        P(None, "dp", ("ctx", "fsdp"), None),
        P(("dp", "ctx", "fsdp")),
        P(None, ("dp", "ctx", "fsdp")),
        P(("dp", "ctx", "fsdp"), None),
        P(("dp", "ctx", "fsdp")),
        P(None, ("dp", "ctx", "fsdp")),
        P(("dp", "ctx", "fsdp"), None),
    )
    return jax.shard_map(
        on_device if fits(mesh) else on_device_gathered,
        mesh=mesh,
        in_specs=placed,
        out_specs=(
            P(None, "dp", ("ctx", "fsdp"), None),
            P(None, "dp", ("ctx", "fsdp"), None),
            P(("dp", "ctx", "fsdp")),
            P(None, ("dp", "ctx", "fsdp")),
            P(("dp", "ctx", "fsdp"), None),
            P(("dp", "ctx", "fsdp")),
            P(None, ("dp", "ctx", "fsdp")),
            P(("dp", "ctx", "fsdp"), None),
        ),
        check_vma=False,
    )
```

```python
import functools

import jax
import jax.numpy as jnp
from jax import lax
from jax.experimental import pallas as pl
from jax.experimental.pallas import tpu as pltpu
from jax.sharding import PartitionSpec as P

D = 1536
H = 16
KVH = 8
HD = 96
FF = 4096


EPS = 1e-05
THETA = 100000.0
NEG = -1e30


def in_blocks(value, dim, length):
    lengths = value.shape
    pieces = value.reshape(*lengths[:dim], length, lengths[dim] // length, *lengths[dim + 1 :])
    return jnp.moveaxis(pieces, dim, 0)


def sum_at_owner(value, axis, dim):
    pieces = in_blocks(value, dim, lax.axis_size(axis))
    arrived = lax.all_to_all(pieces, axis, split_axis=0, concat_axis=0, tiled=True)
    return arrived.astype(jnp.float32).sum(axis=0)


def side_by_side(arrays, axis, dim, along):
    both = jnp.concatenate(arrays, axis=along)
    whole, at, finished = (sum_at_owner(both, axis, dim), 0, [])
    for a in arrays:
        finished.append(lax.slice_in_dim(whole, at, at + a.shape[along], axis=along))
        at += a.shape[along]
    return tuple(finished)


def rms_norm(values, gain_vec):
    return values * lax.rsqrt(jnp.mean(values * values, axis=-1, keepdims=True) + EPS) * gain_vec


def tables(start, length, width):
    half_width = width // 2
    frequency = THETA ** (-(jnp.arange(half_width, dtype=jnp.float32) * 2.0) / width)
    angles = (start + jnp.arange(length, dtype=jnp.int32)).astype(jnp.float32)[:, None] * frequency[
        None, :
    ]
    return (jnp.cos(angles), jnp.sin(angles))


def rotate(values, cosine, sine_table):
    half_width = values.shape[-1] // 2
    first_half = values[..., :half_width]
    second_half = values[..., half_width:]
    cos_b = cosine[:, None, :]
    sin_b = sine_table[:, None, :]
    return jnp.concatenate(
        [first_half * cos_b - second_half * sin_b, second_half * cos_b + first_half * sin_b],
        axis=-1,
    )


def swiglu(both):
    return jax.nn.silu(both[:, :FF]) * both[:, FF:]


def inner(left, right):
    return lax.dot_general(
        left, right, (((0,), (0,)), ((), ())), preferred_element_type=jnp.float32
    )


def outer(left, right):
    return lax.dot_general(
        left, right, (((1,), (1,)), ((), ())), preferred_element_type=jnp.float32
    )


def unchanged(state):
    return state


def on_device_gathered(tokens, cotangent, attn_gain, w_qkv, w_out, mlp_gain, w_gate_up, w_down):
    tok_count = tokens.shape[2]
    groups = H // KVH
    factor = HD ** (-0.5)
    seq_length = tok_count * lax.axis_size(("ctx", "fsdp"))
    pos_first = lax.axis_index(("ctx", "fsdp")) * tok_count
    positions = pos_first + jnp.arange(tok_count, dtype=jnp.int32)
    pos_last = pos_first + tok_count - 1
    cosine, sine_table = tables(pos_first, tok_count, HD)
    sums = [
        jnp.zeros((D,), jnp.float32),
        jnp.zeros((D, (H + 2 * KVH) * HD), jnp.float32),
        jnp.zeros((H * HD, D), jnp.float32),
        jnp.zeros((D,), jnp.float32),
        jnp.zeros((D, 2 * FF), jnp.float32),
        jnp.zeros((FF, D), jnp.float32),
    ]
    outputs = []
    in_grads = []
    whole = (
        lax.all_gather(attn_gain, ("dp", "ctx", "fsdp"), axis=0, tiled=True),
        lax.all_gather(w_qkv, ("dp", "ctx", "fsdp"), axis=1, tiled=True),
        lax.all_gather(w_out, ("dp", "ctx", "fsdp"), axis=0, tiled=True),
        lax.all_gather(mlp_gain, ("dp", "ctx", "fsdp"), axis=0, tiled=True),
        lax.all_gather(w_gate_up, ("dp", "ctx", "fsdp"), axis=1, tiled=True),
        lax.all_gather(w_down, ("dp", "ctx", "fsdp"), axis=0, tiled=True),
    )
    for step_index in range(tokens.shape[0]):
        gain_one, mix_qkv, mix_out, gain_two, mix_gate_up, mix_down = whole
        inputs = tokens[step_index, 0].astype(jnp.float32)
        normed = rms_norm(inputs, gain_one.astype(jnp.float32)).astype(jnp.bfloat16)
        mixed = jnp.dot(normed, mix_qkv, preferred_element_type=jnp.float32)
        queries = rotate(mixed[:, : H * HD].reshape(tok_count, H, HD), cosine, sine_table).astype(
            jnp.bfloat16
        )
        key_rows = rotate(
            mixed[:, H * HD : (H + KVH) * HD].reshape(tok_count, KVH, HD), cosine, sine_table
        )
        key_rows = key_rows.astype(jnp.bfloat16).reshape(tok_count, KVH * HD)
        value_rows = mixed[:, (H + KVH) * HD :].astype(jnp.bfloat16)
        grouped = queries.reshape(tok_count, KVH, groups, HD)
        start_state = (
            jnp.full((KVH, groups, tok_count), NEG, jnp.float32),
            jnp.zeros((KVH, groups, tok_count), jnp.float32),
            jnp.zeros((KVH, groups, tok_count, HD), jnp.float32),
        )
        piece = (
            lax.all_gather(key_rows, ("ctx", "fsdp"), axis=0, tiled=True),
            lax.all_gather(value_rows, ("ctx", "fsdp"), axis=0, tiled=True),
        )

        def work(state):
            best, total, summed = state
            key_count = piece[0].shape[0]
            keys = piece[0].reshape(key_count, KVH, HD)
            values = piece[1].reshape(key_count, KVH, HD)
            scores = (
                jnp.einsum("qkgd,tkd->kgqt", grouped, keys, preferred_element_type=jnp.float32)
                * factor
            )
            allowed = jnp.arange(key_count, dtype=jnp.int32)[None, :] <= positions[:, None]
            scores = jnp.where(allowed, scores, NEG)
            new_best = jnp.maximum(best, jnp.max(scores, axis=-1))
            weights = jnp.where(allowed, jnp.exp(scores - new_best[..., None]), 0.0)
            total = jnp.sum(weights, axis=-1)
            summed = jnp.einsum(
                "kgqt,tkd->kgqd",
                weights.astype(jnp.bfloat16),
                values,
                preferred_element_type=jnp.float32,
            )
            return (new_best, total, summed)

        best, total, summed = lax.cond(jnp.int32(0) <= pos_last, work, unchanged, start_state)
        head_out = summed / total[..., None]
        log_total = best + jnp.log(total)
        attended = (
            jnp.transpose(head_out, (2, 0, 1, 3)).reshape(tok_count, H * HD).astype(jnp.bfloat16)
        )
        resid = inputs + jnp.dot(attended, mix_out, preferred_element_type=jnp.float32)
        normed_two = rms_norm(resid, gain_two.astype(jnp.float32)).astype(jnp.bfloat16)
        both = jnp.dot(normed_two, mix_gate_up, preferred_element_type=jnp.float32)
        acted = swiglu(both).astype(jnp.bfloat16)
        result = resid + jnp.dot(acted, mix_down, preferred_element_type=jnp.float32)
        outputs.append(result.astype(jnp.bfloat16))
        gain_one, mix_qkv, mix_out, gain_two, mix_gate_up, mix_down = whole
        up_low = cotangent[step_index, 0]
        upstream = up_low.astype(jnp.float32)
        sums[5] = sums[5] + inner(acted, up_low)
        d_act = outer(up_low, mix_down)
        _, pull_glu = jax.vjp(swiglu, both)
        d_both = pull_glu(d_act)[0].astype(jnp.bfloat16)
        sums[4] = sums[4] + inner(normed_two, d_both)
        d_normed_two = outer(d_both, mix_gate_up)
        _, pull_two = jax.vjp(rms_norm, resid, gain_two.astype(jnp.float32))
        d_resid_norm, d_gain_two = pull_two(d_normed_two)
        sums[3] = sums[3] + d_gain_two
        d_resid = upstream + d_resid_norm
        d_resid_low = d_resid.astype(jnp.bfloat16)
        sums[2] = sums[2] + inner(attended, d_resid_low)
        d_attended = outer(d_resid_low, mix_out).astype(jnp.bfloat16)
        d_grouped = d_attended.reshape(tok_count, KVH, groups, HD)
        delta = jnp.einsum("qkgd,kgqd->kgq", d_grouped.astype(jnp.float32), head_out)
        zero_q = jnp.zeros((tok_count, KVH, groups, HD), jnp.float32)
        back_state = (
            zero_q,
            jnp.zeros((seq_length, KVH * HD), jnp.float32),
            jnp.zeros((seq_length, KVH * HD), jnp.float32),
        )
        attend_piece = (
            lax.all_gather(key_rows, ("ctx", "fsdp"), axis=0, tiled=True),
            lax.all_gather(value_rows, ("ctx", "fsdp"), axis=0, tiled=True),
        )

        def attend_work(state):
            key_count = attend_piece[0].shape[0]
            keys = attend_piece[0].reshape(key_count, KVH, HD)
            values = attend_piece[1].reshape(key_count, KVH, HD)
            scores = (
                jnp.einsum("qkgd,tkd->kgqt", grouped, keys, preferred_element_type=jnp.float32)
                * factor
            )
            allowed = jnp.arange(key_count, dtype=jnp.int32)[None, :] <= positions[:, None]
            scores = jnp.where(allowed, scores, NEG)
            probs = jnp.where(allowed, jnp.exp(scores - log_total[..., None]), 0.0)
            d_probs = jnp.einsum(
                "qkgd,tkd->kgqt", d_grouped, values, preferred_element_type=jnp.float32
            )
            d_scores = (probs * (d_probs - delta[..., None])).astype(jnp.bfloat16)
            grad_q = jnp.einsum(
                "kgqt,tkd->qkgd", d_scores, keys, preferred_element_type=jnp.float32
            )
            piece_k = (
                jnp.einsum("kgqt,qkgd->tkd", d_scores, grouped, preferred_element_type=jnp.float32)
                * factor
            )
            piece_v = jnp.einsum(
                "kgqt,qkgd->tkd",
                probs.astype(jnp.bfloat16),
                d_grouped,
                preferred_element_type=jnp.float32,
            )
            grad_k = piece_k.reshape(key_count, KVH * HD)
            grad_v = piece_v.reshape(key_count, KVH * HD)
            return (grad_q, grad_k, grad_v)

        back_result = lax.cond(jnp.int32(0) <= pos_last, attend_work, unchanged, back_state)
        grad_q = back_result[0]
        summed_k, summed_v = side_by_side(
            (back_result[1].astype(jnp.bfloat16), back_result[2].astype(jnp.bfloat16)),
            ("ctx", "fsdp"),
            0,
            1,
        )
        d_q_raw = rotate(grad_q.reshape(tok_count, H, HD) * factor, cosine, -sine_table).reshape(
            tok_count, H * HD
        )
        d_k_raw = rotate(summed_k.reshape(tok_count, KVH, HD), cosine, -sine_table).reshape(
            tok_count, KVH * HD
        )
        d_mixed = jnp.concatenate([d_q_raw, d_k_raw, summed_v], axis=1).astype(jnp.bfloat16)
        sums[1] = sums[1] + inner(normed, d_mixed)
        d_normed = outer(d_mixed, mix_qkv)
        _, pull_one = jax.vjp(rms_norm, inputs, gain_one.astype(jnp.float32))
        d_inputs_norm, d_gain_one = pull_one(d_normed)
        sums[0] = sums[0] + d_gain_one
        in_grads.append((d_resid + d_inputs_norm).astype(jnp.bfloat16))
    grad_gain_one, grad_qkv, grad_out, grad_gain_two, grad_gate_up, grad_down = (
        lax.psum_scatter(sums[0], ("dp", "ctx", "fsdp"), scatter_dimension=0, tiled=True),
        lax.psum_scatter(sums[1], ("dp", "ctx", "fsdp"), scatter_dimension=1, tiled=True),
        lax.psum_scatter(sums[2], ("dp", "ctx", "fsdp"), scatter_dimension=0, tiled=True),
        lax.psum_scatter(sums[3], ("dp", "ctx", "fsdp"), scatter_dimension=0, tiled=True),
        lax.psum_scatter(sums[4], ("dp", "ctx", "fsdp"), scatter_dimension=1, tiled=True),
        lax.psum_scatter(sums[5], ("dp", "ctx", "fsdp"), scatter_dimension=0, tiled=True),
    )
    block_out = jnp.stack(outputs)[:, None]
    grad_tokens = jnp.stack(in_grads)[:, None]
    return (
        block_out,
        grad_tokens,
        grad_gain_one,
        grad_qkv,
        grad_out,
        grad_gain_two,
        grad_gate_up,
        grad_down,
    )


TP = ("dp", "ctx")
ALL = ("dp", "ctx", "fsdp")


def dot(left, right):
    return jnp.dot(left, right, preferred_element_type=jnp.float32)


def qkv_owner(sizes):
    moves = []
    for head in range(H + 2 * KVH):
        if head < H:
            group, slot = head // 2, head % 2
        elif head < H + KVH:
            group, slot = head - H, 2
        else:
            group, slot = head - H - KVH, 3
        device = group % sizes["dp"] * sizes["ctx"] + group // sizes["dp"]
        moves.append((head, device * sizes["fsdp"] + slot))
    return moves


def hidden_of(device, sizes):
    ctx = sizes["ctx"]
    return (device % ctx) * sizes["dp"] + device // ctx


def down_owner(sizes):
    n, f = sizes["dp"] * sizes["ctx"], sizes["fsdp"]
    return [
        (hidden_of(device, sizes) * f + slot, device * f + slot)
        for device in range(n)
        for slot in range(f)
    ]


def up_owner(sizes):
    n, f = sizes["dp"] * sizes["ctx"], sizes["fsdp"]
    half = n * f // 2
    moves = []
    for device in range(n):
        first = hidden_of(device, sizes) * (f // 2)
        for slot in range(f):
            source = first + slot if slot < f // 2 else half + first + slot - f // 2
            moves.append((source, device * f + slot))
    return moves


def back(moves):
    return [(to, source) for source, to in moves]


MESH = pl.DeviceIdType.MESH
VM = pltpu.VMEM
ANY = pl.ANY


def place():
    return lax.axis_index("dp"), lax.axis_index("ctx"), lax.axis_index("fsdp")


def at_device(dp, ctx, fs):
    return {"dp": dp, "ctx": ctx, "fsdp": fs}


def remote(src, dst, send, recv, device):
    return pltpu.make_async_remote_copy(
        src_ref=src, dst_ref=dst, send_sem=send, recv_sem=recv, device_id=device, device_id_type=MESH
    )


def arrived(dst, recv, device):
    remote(dst, dst, recv, recv, device).wait_recv()


def left(src, send, device):
    remote(src, src, send, send, device).wait_send()


def greet_all(sizes):
    dp, ctx, fs = sizes
    n = dp * ctx * fs
    d, c, f = place()
    me = (d * ctx + c) * fs + f
    barrier = pltpu.get_barrier_semaphore()

    def tell(step, carry):
        other = lax.rem(me + step, n)
        pl.semaphore_signal(
            barrier,
            inc=1,
            device_id=at_device(other // (ctx * fs), lax.rem(other // fs, ctx), lax.rem(other, fs)),
            device_id_type=MESH,
        )
        return carry

    lax.fori_loop(1, n, tell, 0)
    pl.semaphore_wait(barrier, n - 1)


class LineGather:
    def __init__(self, n, own, whole, send, recv, local):
        self.n, self.own, self.whole, self.send, self.recv, self.local = n, own, whole, send, recv, local
        self.d, self.c, self.f = place()

    def slot(self, at):
        return self.whole.at[self.d, at]

    def up(self, src, at):
        return remote(src, self.slot(at), self.send.at[0, at], self.recv.at[self.d, at], at_device(self.d, self.c + 1, self.f))

    def down(self, src, at):
        return remote(src, self.slot(at), self.send.at[1, at], self.recv.at[self.d, at], at_device(self.d, self.c - 1, self.f))

    def across(self, src, at):
        return remote(src, self.slot(at), self.send.at[2, at], self.recv.at[self.d, at], at_device(1 - self.d, self.c, self.f))

    def start(self):
        c = self.c

        @pl.when(c < self.n - 1)
        def _():
            self.up(self.own, c).start()

        @pl.when(c > 0)
        def _():
            self.down(self.own, c).start()

        self.across(self.own, c).start()
        if self.local is not None:
            pltpu.make_async_copy(self.own, self.slot(c), self.local).start()

    def forward(self, k):
        c = self.c

        @pl.when(c - k >= 0)
        def _():
            arrived(self.slot(c - k), self.recv.at[self.d, c - k], at_device(self.d, c, self.f))

            @pl.when(c < self.n - 1)
            def _():
                self.up(self.slot(c - k), c - k).start()

            self.across(self.slot(c - k), c - k).start()

        @pl.when(c + k < self.n)
        def _():
            arrived(self.slot(c + k), self.recv.at[self.d, c + k], at_device(self.d, c, self.f))

            @pl.when(c > 0)
            def _():
                self.down(self.slot(c + k), c + k).start()

            self.across(self.slot(c + k), c + k).start()

    def other(self, at):
        arrived(self.whole.at[1 - self.d, at], self.recv.at[1 - self.d, at], at_device(self.d, self.c, self.f))

    def finish(self):
        c = self.c
        for at in range(self.n):

            @pl.when(jnp.logical_and(at <= c, c < self.n - 1))
            def _():
                left(self.slot(at), self.send.at[0, at], at_device(self.d, c, self.f))

            @pl.when(jnp.logical_and(at >= c, c > 0))
            def _():
                left(self.slot(at), self.send.at[1, at], at_device(self.d, c, self.f))

            left(self.slot(at), self.send.at[2, at], at_device(self.d, c, self.f))
        if self.local is not None:
            pltpu.make_async_copy(self.own, self.slot(c), self.local).wait()


FACTOR = HD ** (-0.5)
LANES = 128


def ordered(c, step, n):
    at = jnp.int32(0)
    for here in range(n):
        near = sorted(range(n), key=lambda place_: (abs(place_ - here), place_))
        for index, value in enumerate(near):
            at = jnp.where(jnp.logical_and(c == here, step == index), value, at)
    return at


def first_kernel(
    sizes, x_ref, gains_ref, w_ref, cos_ref, sin_up_ref, sin_down_ref,
    normed_out, unit_out, att_out, wide_out, gains_out,
    x_all, w_all, wide, normed, stage, unit, att_stage, att, gain_all, gain_vec,
    line_send, line_recv, line_local, w_send, w_recv, w_pass, g_send, g_recv, u_send, u_recv, a_send, a_recv, out_sem,
):
    dp, ctx, fs = sizes
    n = dp * ctx * fs
    d, c, f = place()
    here = at_device(d, c, f)
    span = stage.shape[2]
    greet_all(sizes)

    q_core = f // 2
    kv_slot = 2 + c // 2
    kv_ctx = 2 * lax.rem(c, 2) + f // 2
    kv_core = lax.rem(f, 2)
    relay = f == 2 * lax.rem(c, 2) + d

    @pl.when(jnp.logical_and(d == 1, jnp.logical_or(kv_core != 1, kv_ctx != c)))
    def _():
        remote(w_ref, w_all.at[kv_slot], w_send.at[0], w_recv.at[kv_slot], at_device(kv_core, kv_ctx, f)).start()

    @pl.when(jnp.logical_and(d == 1, jnp.logical_and(kv_core == 1, kv_ctx == c)))
    def _():
        pltpu.make_async_copy(w_ref, w_all.at[kv_slot], w_recv.at[kv_slot]).start()

    line = LineGather(ctx, x_ref, x_all, line_send, line_recv, line_local)
    line.start()

    @pl.when(d == 0)
    def _():
        slot = lax.rem(f, 2)
        for to in range(fs):

            @pl.when(jnp.logical_or(q_core != 0, to != f))
            def _():
                remote(w_ref, w_all.at[slot], w_send.at[to], w_recv.at[slot], at_device(q_core, c, to)).start()

            @pl.when(jnp.logical_and(q_core == 0, to == f))
            def _():
                pltpu.make_async_copy(w_ref, w_all.at[slot], w_recv.at[slot]).start()

    me = (d * ctx + c) * fs + f

    def gain_to(step, carry):
        other = lax.rem(me + step, n)
        remote(
            gains_ref, gain_all.at[me], g_send.at[other], g_recv.at[me],
            at_device(other // (ctx * fs), lax.rem(other // fs, ctx), lax.rem(other, fs)),
        ).start()
        return carry

    lax.fori_loop(1, n, gain_to, 0)
    gain_all[me] = gains_ref[...]

    @pl.when(relay)
    def _():
        for slot in (2, 3):
            arrived(w_all.at[slot], w_recv.at[slot], here)
            for step in range(1, fs):
                to = lax.rem(f + step, fs)
                remote(w_all.at[slot], w_all.at[slot], w_pass.at[slot - 2, step], w_recv.at[slot], at_device(d, c, to)).start()

    def gain_from(step, carry):
        other = lax.rem(me + step, n)
        arrived(gain_all.at[other], g_recv.at[other], here)
        return carry

    lax.fori_loop(1, n, gain_from, 0)
    each = D // n
    for index in range(n):
        gain_vec[:, index * each : (index + 1) * each] = gain_all[index][:, :each]
    gain = gain_vec[0:1, :]

    wide[...] = jnp.zeros_like(wide)
    for slot in (0, 1, 2, 3):
        if slot < 2:
            arrived(w_all.at[slot], w_recv.at[slot], here)
        else:

            @pl.when(jnp.logical_not(relay))
            def _():
                arrived(w_all.at[slot], w_recv.at[slot], here)

        wide[:, slot * LANES : slot * LANES + HD] = w_all[slot]

    pltpu.make_async_copy(line.own, line.slot(c), line.local).wait()

    def block(step, carry):
        at = ordered(c, step, ctx)

        @pl.when(at != c)
        def _():
            arrived(line.slot(at), line_recv.at[d, at], here)

            @pl.when(jnp.logical_and(at < c, c < ctx - 1))
            def _():
                line.up(line.slot(at), at).start()

            @pl.when(jnp.logical_and(at > c, c > 0))
            def _():
                line.down(line.slot(at), at).start()

            line.across(line.slot(at), at).start()

        line.other(at)
        values = x_all[:, at].reshape(dp * 2 * span, D).astype(jnp.float32)
        scale = lax.rsqrt(jnp.mean(values * values, axis=-1, keepdims=True) + EPS)
        low = (values * scale * gain).astype(jnp.bfloat16)
        normed[:, at] = low.reshape(dp, 2 * span, D)
        heads = jnp.dot(low, wide[...], preferred_element_type=jnp.float32)
        cosine, sine_up, sine_down = cos_ref[at], sin_up_ref[at], sin_down_ref[at]
        for slot in range(4):
            head = heads[:, slot * LANES : (slot + 1) * LANES]
            if slot < 3:
                turned_up = pltpu.roll(head, HD // 2, 1).reshape(2 * dp, span, LANES)
                turned_down = pltpu.roll(head, LANES - HD // 2, 1).reshape(2 * dp, span, LANES)
                head = head.reshape(2 * dp, span, LANES)
                head = head * cosine[None] + turned_up * sine_up[None] + turned_down * sine_down[None]
            else:
                head = head.reshape(2 * dp, span, LANES)
            stage[at, :, :, slot * LANES : (slot + 1) * LANES] = head.astype(jnp.bfloat16)
        for to in range(2 * dp):

            @pl.when(to != f)
            def _():
                remote(stage.at[at, to], unit.at[at, f], u_send.at[at, to], u_recv.at[at, f], at_device(d, c, to)).start()

            @pl.when(to == f)
            def _():
                unit[at, f] = stage[at, to]

        return carry

    lax.fori_loop(0, ctx, block, 0)
    normed_copy = pltpu.make_async_copy(normed, normed_out, out_sem.at[0])
    wide_copy = pltpu.make_async_copy(wide, wide_out, out_sem.at[1])
    gains_copy = pltpu.make_async_copy(gain_vec, gains_out, out_sem.at[2])
    normed_copy.start()
    wide_copy.start()
    gains_copy.start()

    for at in range(ctx):
        for step in range(1, fs):
            other = lax.rem(f + step, fs)
            arrived(unit.at[at, other], u_recv.at[at, other], here)
    unit_copy = pltpu.make_async_copy(unit, unit_out, out_sem.at[3])
    unit_copy.start()

    rows = fs * span
    for at in range(ctx):
        keys = rows * (at + 1)
        k_rows = unit[0 : at + 1, :, :, 2 * LANES : 3 * LANES].reshape(keys, LANES)
        v_rows = unit[0 : at + 1, :, :, 3 * LANES : 4 * LANES].reshape(keys, LANES)
        allowed = lax.broadcasted_iota(jnp.int32, (rows, keys), 1) <= rows * at + lax.broadcasted_iota(
            jnp.int32, (rows, keys), 0
        )
        for head in range(2):
            q_rows = unit[at, :, :, head * LANES : (head + 1) * LANES].reshape(rows, LANES)
            scores = outer(q_rows, k_rows) * FACTOR
            scores = jnp.where(allowed, scores, NEG)
            best = jnp.max(scores, axis=-1, keepdims=True)
            weights = jnp.exp(scores - best)
            probs = weights / jnp.sum(weights, axis=-1, keepdims=True)
            mixed = jnp.dot(probs.astype(jnp.bfloat16), v_rows, preferred_element_type=jnp.float32)
            att_stage[at, :, :, head * LANES : (head + 1) * LANES] = mixed.astype(jnp.bfloat16).reshape(fs, span, LANES)
        for to in range(fs):

            @pl.when(to != f)
            def _():
                remote(
                    att_stage.at[at, to], att.at[f // 2, at, lax.rem(f, 2)], a_send.at[at, to], a_recv.at[f, at], at_device(d, c, to)
                ).start()

            @pl.when(to == f)
            def _():
                att[f // 2, at, lax.rem(f, 2)] = att_stage[at, to]

    for at in range(ctx):
        for step in range(1, fs):
            other = lax.rem(f + step, fs)
            arrived(att.at[other // 2, at, lax.rem(other, 2)], a_recv.at[other, at], here)
    att_copy = pltpu.make_async_copy(att, att_out, out_sem.at[4])
    att_copy.start()

    for at in range(ctx):

        @pl.when(jnp.logical_and(at <= c, c < ctx - 1))
        def _():
            left(line.slot(at), line_send.at[0, at], here)

        @pl.when(jnp.logical_and(at >= c, c > 0))
        def _():
            left(line.slot(at), line_send.at[1, at], here)

        left(line.slot(at), line_send.at[2, at], here)
        for to in range(fs):

            @pl.when(to != f)
            def _():
                left(stage.at[at, to], u_send.at[at, to], here)
                left(att_stage.at[at, to], a_send.at[at, to], here)

    @pl.when(jnp.logical_and(d == 1, jnp.logical_or(kv_core != 1, kv_ctx != c)))
    def _():
        left(w_ref, w_send.at[0], here)

    @pl.when(d == 0)
    def _():
        for to in range(fs):

            @pl.when(jnp.logical_or(q_core != 0, to != f))
            def _():
                left(w_ref, w_send.at[to], here)

    @pl.when(relay)
    def _():
        for slot in (2, 3):
            for step in range(1, fs):
                left(w_all.at[slot], w_pass.at[slot - 2, step], here)

    def gain_left(step, carry):
        other = lax.rem(me + step, n)
        left(gains_ref, g_send.at[other], here)
        return carry

    lax.fori_loop(1, n, gain_left, 0)
    for copy in (normed_copy, wide_copy, gains_copy, unit_copy, att_copy):
        copy.wait()


def first(sizes, x, gains, w_qkv, cosine, sine_up, sine_down):
    dp, ctx, fs = sizes
    n = dp * ctx * fs
    rows = x.shape[0]
    span = rows // 2
    low, wide_t = jnp.bfloat16, jnp.float32
    dma = pltpu.SemaphoreType.DMA
    shapes = (
        jax.ShapeDtypeStruct((dp, ctx, rows, D), low),
        jax.ShapeDtypeStruct((ctx, fs, span, 4 * LANES), low),
        jax.ShapeDtypeStruct((dp, ctx, 2, span, 2 * LANES), low),
        jax.ShapeDtypeStruct((D, 4 * LANES), low),
        jax.ShapeDtypeStruct((8, D), wide_t),
    )
    any_spec, vm_spec = pl.BlockSpec(memory_space=ANY), pl.BlockSpec(memory_space=VM)
    return pl.pallas_call(
        functools.partial(first_kernel, sizes),
        name="first",
        out_shape=shapes,
        in_specs=[vm_spec, vm_spec, any_spec, vm_spec, vm_spec, vm_spec],
        out_specs=[any_spec] * 5,
        scratch_shapes=[
            VM((dp, ctx, rows, D), low),
            VM((4, D, HD), low),
            VM((D, 4 * LANES), low),
            VM((dp, ctx, rows, D), low),
            VM((ctx, 2 * dp, span, 4 * LANES), low),
            VM((ctx, fs, span, 4 * LANES), low),
            VM((ctx, fs, span, 2 * LANES), low),
            VM((dp, ctx, 2, span, 2 * LANES), low),
            VM((n, 8, LANES), wide_t),
            VM((8, D), wide_t),
            dma((3, ctx)), dma((dp, ctx)), dma,
            dma((fs,)), dma((4,)), dma((2, fs)),
            dma((n,)), dma((n,)),
            dma((ctx, 2 * dp)), dma((ctx, fs)),
            dma((ctx, fs)), dma((fs, ctx)),
            dma((5,)),
        ],
        compiler_params=pltpu.CompilerParams(collective_id=1, has_side_effects=True, vmem_limit_bytes=60 * 1024 * 1024),
    )(x, gains, w_qkv, cosine, sine_up, sine_down)


def angle_tables(ctx, fs, span):
    f_index = lax.axis_index("fsdp")
    positions = (jnp.arange(ctx, dtype=jnp.int32)[:, None] * fs + f_index) * span + jnp.arange(span, dtype=jnp.int32)[None, :]
    return lane_tables(positions)


def lane_tables(positions):
    lane = jnp.arange(LANES, dtype=jnp.int32)
    pair = (lane % (HD // 2)).astype(jnp.float32)
    frequency = THETA ** (-(pair * 2.0) / HD)
    angles = positions.astype(jnp.float32)[..., None] * frequency
    inside = lane < HD
    low_half = lane < HD // 2
    cosine = jnp.where(inside, jnp.cos(angles), 0.0)
    sine = jnp.sin(angles)
    sine_up = jnp.where(jnp.logical_and(inside, jnp.logical_not(low_half)), sine, 0.0)
    sine_down = jnp.where(low_half, -sine, 0.0)
    return cosine, sine_up, sine_down


def gather_tp(value):
    return lax.all_gather(value, TP, axis=0, tiled=True)


def sum_tp(value):
    return lax.psum_scatter(value.astype(jnp.bfloat16), TP, scatter_dimension=0, tiled=True).astype(
        jnp.float32
    )


def norm_back(values, scale, gain, incoming):
    weighted = incoming * gain
    mean = jnp.mean(weighted * values, axis=-1, keepdims=True)
    return scale * weighted - values * (scale * scale * scale) * mean


def on_device(tokens, cotangent, attn_gain, w_qkv, w_out, mlp_gain, w_gate_up, w_down):
    sizes = {name: lax.axis_size(name) for name in ALL}
    dp, ctx, fs = sizes["dp"], sizes["ctx"], sizes["fsdp"]
    mb, _, span, _ = tokens.shape
    rows = mb * span
    f_index = lax.axis_index("fsdp")
    length = span * ctx * fs
    factor = HD ** (-0.5)
    hidden = FF // (dp * ctx)

    x_low = tokens.reshape(rows, D)
    gain_rows = jnp.zeros((8, LANES), jnp.float32)
    gain_rows = gain_rows.at[0, : attn_gain.shape[0]].set(attn_gain.astype(jnp.float32))
    gain_rows = gain_rows.at[1, : mlp_gain.shape[0]].set(mlp_gain.astype(jnp.float32))
    cosine, sine_up, sine_down = angle_tables(ctx, fs, span)
    normed, unit, att, qkv, gains = first((dp, ctx, fs), x_low, gain_rows, w_qkv, cosine, sine_up, sine_down)
    gain_one, gain_two = gains[0], gains[1]
    normed = normed.reshape(dp * ctx * rows, D)
    unit = unit.reshape(length, 4, LANES)
    attended = att.reshape(dp * ctx * rows, 2 * LANES)

    out_w = lax.all_gather(lax.ppermute(w_out, ALL, down_owner(sizes)), "fsdp", axis=0, tiled=True)
    out_w = jnp.pad(out_w.reshape(2, HD, D), ((0, 0), (0, LANES - HD), (0, 0))).reshape(2 * LANES, D)
    gate_up = lax.all_gather(lax.ppermute(w_gate_up, ALL, up_owner(sizes)), "fsdp", axis=1, tiled=True)
    down = lax.all_gather(lax.ppermute(w_down, ALL, down_owner(sizes)), "fsdp", axis=0, tiled=True)

    x = x_low.astype(jnp.float32)
    dy = cotangent.reshape(rows, D)
    scale_one = lax.rsqrt(jnp.mean(x * x, axis=-1, keepdims=True) + EPS)
    dy_all = gather_tp(dy)

    def to_units(values):
        count = values.shape[0]
        values = values.transpose(1, 3, 0, 2, 4, 5)
        values = values.reshape(dp * mb, count, ctx, span, -1)
        values = lax.all_to_all(values, "fsdp", split_axis=0, concat_axis=0, tiled=True)
        return values.transpose(1, 2, 0, 3, 4).reshape(count, length, -1)

    def to_rows(values):
        count = values.shape[0]
        values = values.reshape(count, ctx, fs, span, -1).transpose(2, 0, 1, 3, 4)
        values = lax.all_to_all(values, "fsdp", split_axis=0, concat_axis=0, tiled=True)
        values = values.reshape(dp, mb, count, ctx, span, -1).transpose(2, 0, 3, 1, 4, 5)
        return values.reshape(count, dp * ctx * rows, -1)

    q = jnp.stack([unit[:, 0], unit[:, 1]])
    k, v = unit[:, 2], unit[:, 3]
    scores = jnp.einsum("hqd,kd->hqk", q, k, preferred_element_type=jnp.float32) * factor
    allowed = jnp.arange(length)[None, :] <= jnp.arange(length)[:, None]
    scores = jnp.where(allowed, scores, NEG)
    best = jnp.max(scores, axis=-1, keepdims=True)
    weights = jnp.where(allowed, jnp.exp(scores - best), 0.0)
    probs = weights / jnp.sum(weights, axis=-1, keepdims=True)
    probs_low = probs.astype(jnp.bfloat16)
    partial = dot(attended, out_w)
    resid = x + sum_tp(partial)
    scale_two = lax.rsqrt(jnp.mean(resid * resid, axis=-1, keepdims=True) + EPS)
    normed_two = gather_tp((resid * scale_two * gain_two).astype(jnp.bfloat16))
    gate = dot(normed_two, gate_up[:, :hidden])
    up = dot(normed_two, gate_up[:, hidden:])
    sig = 1.0 / (1.0 + jnp.exp(-gate))
    silu = gate * sig
    act = (silu * up).astype(jnp.bfloat16)
    block_out = (resid + sum_tp(dot(act, down))).astype(jnp.bfloat16)

    grad_down = inner(act, dy_all)
    d_act = outer(dy_all, down)
    d_gate = d_act * up * (sig * (1.0 + gate * (1.0 - sig)))
    d_up = d_act * silu
    d_both = jnp.concatenate([d_gate, d_up], axis=1).astype(jnp.bfloat16)
    grad_gate_up = inner(normed_two, d_both)
    d_two = sum_tp(outer(d_both, gate_up))
    grad_two = jnp.sum(d_two * resid * scale_two, axis=0)
    d_resid = dy.astype(jnp.float32) + norm_back(resid, scale_two, gain_two, d_two)
    d_resid_all = gather_tp(d_resid.astype(jnp.bfloat16))
    grad_out = inner(attended, d_resid_all).reshape(2, LANES, D)[:, :HD].reshape(2 * HD, D)
    d_att = outer(d_resid_all, out_w).astype(jnp.bfloat16)
    d_unit = to_units(jnp.moveaxis(d_att.reshape(dp, ctx, mb, span, 2, LANES), 4, 0))
    d_probs = jnp.einsum("hqd,kd->hqk", d_unit, v, preferred_element_type=jnp.float32)
    delta = jnp.sum(probs * d_probs, axis=-1, keepdims=True)
    d_scores = (probs * (d_probs - delta)).astype(jnp.bfloat16)
    d_q = jnp.einsum("hqk,kd->hqd", d_scores, k, preferred_element_type=jnp.float32) * factor
    d_k = jnp.einsum("hqk,hqd->kd", d_scores, q, preferred_element_type=jnp.float32) * factor
    d_v = jnp.einsum("hqk,hqd->kd", probs_low, d_unit, preferred_element_type=jnp.float32)
    cos_u, up_u, down_u = lane_tables(jnp.arange(length, dtype=jnp.int32))

    def unturn(values):
        return values * cos_u - jnp.roll(values, HD // 2, -1) * up_u - jnp.roll(values, -(HD // 2), -1) * down_u

    d_heads = jnp.concatenate([unturn(d_q), unturn(d_k)[None], d_v[None]]).astype(jnp.bfloat16)
    d_mixed = to_rows(d_heads)
    d_mixed = jnp.moveaxis(d_mixed, 0, 1).reshape(dp * ctx * rows, 4 * LANES)
    grad_qkv = jnp.moveaxis(inner(normed, d_mixed).reshape(D, 4, LANES)[:, :, :HD], 1, 0)
    d_normed = sum_tp(outer(d_mixed, qkv))
    grad_one = jnp.sum(d_normed * x * scale_one, axis=0)
    grad_tokens = (d_resid + norm_back(x, scale_one, gain_one, d_normed)).astype(jnp.bfloat16)

    def reduce_rows(value, dim, moves):
        value = lax.psum_scatter(value.astype(jnp.bfloat16), "fsdp", scatter_dimension=dim, tiled=True)
        if moves is not None:
            value = lax.ppermute(value, ALL, back(moves))
        return value.astype(jnp.float32)

    gain_grads = lax.psum_scatter(jnp.stack([grad_one, grad_two]), ALL, scatter_dimension=1, tiled=True)
    return (
        block_out.reshape(tokens.shape),
        grad_tokens.reshape(tokens.shape),
        gain_grads[0],
        reduce_rows(grad_qkv, 0, qkv_owner(sizes)).reshape(D, HD),
        reduce_rows(grad_out, 0, down_owner(sizes)),
        gain_grads[1],
        reduce_rows(grad_gate_up, 1, up_owner(sizes)),
        reduce_rows(grad_down, 0, down_owner(sizes)),
    )


def fits(mesh):
    return mesh.shape["dp"] * mesh.shape["ctx"] == KVH and mesh.shape["fsdp"] == 4


def solution(mesh):
    placed = (
        P(None, "dp", ("ctx", "fsdp"), None),
        P(None, "dp", ("ctx", "fsdp"), None),
        P(("dp", "ctx", "fsdp")),
        P(None, ("dp", "ctx", "fsdp")),
        P(("dp", "ctx", "fsdp"), None),
        P(("dp", "ctx", "fsdp")),
        P(None, ("dp", "ctx", "fsdp")),
        P(("dp", "ctx", "fsdp"), None),
    )
    return jax.shard_map(
        on_device if fits(mesh) else on_device_gathered,
        mesh=mesh,
        in_specs=placed,
        out_specs=(
            P(None, "dp", ("ctx", "fsdp"), None),
            P(None, "dp", ("ctx", "fsdp"), None),
            P(("dp", "ctx", "fsdp")),
            P(None, ("dp", "ctx", "fsdp")),
            P(("dp", "ctx", "fsdp"), None),
            P(("dp", "ctx", "fsdp")),
            P(None, ("dp", "ctx", "fsdp")),
            P(("dp", "ctx", "fsdp"), None),
        ),
        check_vma=False,
    )
```

```python
import functools

import jax
import jax.numpy as jnp
from jax import lax
from jax.experimental import pallas as pl
from jax.experimental.pallas import tpu as pltpu
from jax.sharding import PartitionSpec as P

D = 1536
H = 16
KVH = 8
HD = 96
FF = 4096


EPS = 1e-05
THETA = 100000.0
NEG = -1e30


def in_blocks(value, dim, length):
    lengths = value.shape
    pieces = value.reshape(*lengths[:dim], length, lengths[dim] // length, *lengths[dim + 1 :])
    return jnp.moveaxis(pieces, dim, 0)


def sum_at_owner(value, axis, dim):
    pieces = in_blocks(value, dim, lax.axis_size(axis))
    arrived = lax.all_to_all(pieces, axis, split_axis=0, concat_axis=0, tiled=True)
    return arrived.astype(jnp.float32).sum(axis=0)


def side_by_side(arrays, axis, dim, along):
    both = jnp.concatenate(arrays, axis=along)
    whole, at, finished = (sum_at_owner(both, axis, dim), 0, [])
    for a in arrays:
        finished.append(lax.slice_in_dim(whole, at, at + a.shape[along], axis=along))
        at += a.shape[along]
    return tuple(finished)


def rms_norm(values, gain_vec):
    return values * lax.rsqrt(jnp.mean(values * values, axis=-1, keepdims=True) + EPS) * gain_vec


def tables(start, length, width):
    half_width = width // 2
    frequency = THETA ** (-(jnp.arange(half_width, dtype=jnp.float32) * 2.0) / width)
    angles = (start + jnp.arange(length, dtype=jnp.int32)).astype(jnp.float32)[:, None] * frequency[
        None, :
    ]
    return (jnp.cos(angles), jnp.sin(angles))


def rotate(values, cosine, sine_table):
    half_width = values.shape[-1] // 2
    first_half = values[..., :half_width]
    second_half = values[..., half_width:]
    cos_b = cosine[:, None, :]
    sin_b = sine_table[:, None, :]
    return jnp.concatenate(
        [first_half * cos_b - second_half * sin_b, second_half * cos_b + first_half * sin_b],
        axis=-1,
    )


def swiglu(both):
    return jax.nn.silu(both[:, :FF]) * both[:, FF:]


def inner(left, right):
    return lax.dot_general(
        left, right, (((0,), (0,)), ((), ())), preferred_element_type=jnp.float32
    )


def outer(left, right):
    return lax.dot_general(
        left, right, (((1,), (1,)), ((), ())), preferred_element_type=jnp.float32
    )


def unchanged(state):
    return state


def on_device_gathered(tokens, cotangent, attn_gain, w_qkv, w_out, mlp_gain, w_gate_up, w_down):
    tok_count = tokens.shape[2]
    groups = H // KVH
    factor = HD ** (-0.5)
    seq_length = tok_count * lax.axis_size(("ctx", "fsdp"))
    pos_first = lax.axis_index(("ctx", "fsdp")) * tok_count
    positions = pos_first + jnp.arange(tok_count, dtype=jnp.int32)
    pos_last = pos_first + tok_count - 1
    cosine, sine_table = tables(pos_first, tok_count, HD)
    sums = [
        jnp.zeros((D,), jnp.float32),
        jnp.zeros((D, (H + 2 * KVH) * HD), jnp.float32),
        jnp.zeros((H * HD, D), jnp.float32),
        jnp.zeros((D,), jnp.float32),
        jnp.zeros((D, 2 * FF), jnp.float32),
        jnp.zeros((FF, D), jnp.float32),
    ]
    outputs = []
    in_grads = []
    whole = (
        lax.all_gather(attn_gain, ("dp", "ctx", "fsdp"), axis=0, tiled=True),
        lax.all_gather(w_qkv, ("dp", "ctx", "fsdp"), axis=1, tiled=True),
        lax.all_gather(w_out, ("dp", "ctx", "fsdp"), axis=0, tiled=True),
        lax.all_gather(mlp_gain, ("dp", "ctx", "fsdp"), axis=0, tiled=True),
        lax.all_gather(w_gate_up, ("dp", "ctx", "fsdp"), axis=1, tiled=True),
        lax.all_gather(w_down, ("dp", "ctx", "fsdp"), axis=0, tiled=True),
    )
    for step_index in range(tokens.shape[0]):
        gain_one, mix_qkv, mix_out, gain_two, mix_gate_up, mix_down = whole
        inputs = tokens[step_index, 0].astype(jnp.float32)
        normed = rms_norm(inputs, gain_one.astype(jnp.float32)).astype(jnp.bfloat16)
        mixed = jnp.dot(normed, mix_qkv, preferred_element_type=jnp.float32)
        queries = rotate(mixed[:, : H * HD].reshape(tok_count, H, HD), cosine, sine_table).astype(
            jnp.bfloat16
        )
        key_rows = rotate(
            mixed[:, H * HD : (H + KVH) * HD].reshape(tok_count, KVH, HD), cosine, sine_table
        )
        key_rows = key_rows.astype(jnp.bfloat16).reshape(tok_count, KVH * HD)
        value_rows = mixed[:, (H + KVH) * HD :].astype(jnp.bfloat16)
        grouped = queries.reshape(tok_count, KVH, groups, HD)
        start_state = (
            jnp.full((KVH, groups, tok_count), NEG, jnp.float32),
            jnp.zeros((KVH, groups, tok_count), jnp.float32),
            jnp.zeros((KVH, groups, tok_count, HD), jnp.float32),
        )
        piece = (
            lax.all_gather(key_rows, ("ctx", "fsdp"), axis=0, tiled=True),
            lax.all_gather(value_rows, ("ctx", "fsdp"), axis=0, tiled=True),
        )

        def work(state):
            best, total, summed = state
            key_count = piece[0].shape[0]
            keys = piece[0].reshape(key_count, KVH, HD)
            values = piece[1].reshape(key_count, KVH, HD)
            scores = (
                jnp.einsum("qkgd,tkd->kgqt", grouped, keys, preferred_element_type=jnp.float32)
                * factor
            )
            allowed = jnp.arange(key_count, dtype=jnp.int32)[None, :] <= positions[:, None]
            scores = jnp.where(allowed, scores, NEG)
            new_best = jnp.maximum(best, jnp.max(scores, axis=-1))
            weights = jnp.where(allowed, jnp.exp(scores - new_best[..., None]), 0.0)
            total = jnp.sum(weights, axis=-1)
            summed = jnp.einsum(
                "kgqt,tkd->kgqd",
                weights.astype(jnp.bfloat16),
                values,
                preferred_element_type=jnp.float32,
            )
            return (new_best, total, summed)

        best, total, summed = lax.cond(jnp.int32(0) <= pos_last, work, unchanged, start_state)
        head_out = summed / total[..., None]
        log_total = best + jnp.log(total)
        attended = (
            jnp.transpose(head_out, (2, 0, 1, 3)).reshape(tok_count, H * HD).astype(jnp.bfloat16)
        )
        resid = inputs + jnp.dot(attended, mix_out, preferred_element_type=jnp.float32)
        normed_two = rms_norm(resid, gain_two.astype(jnp.float32)).astype(jnp.bfloat16)
        both = jnp.dot(normed_two, mix_gate_up, preferred_element_type=jnp.float32)
        acted = swiglu(both).astype(jnp.bfloat16)
        result = resid + jnp.dot(acted, mix_down, preferred_element_type=jnp.float32)
        outputs.append(result.astype(jnp.bfloat16))
        gain_one, mix_qkv, mix_out, gain_two, mix_gate_up, mix_down = whole
        up_low = cotangent[step_index, 0]
        upstream = up_low.astype(jnp.float32)
        sums[5] = sums[5] + inner(acted, up_low)
        d_act = outer(up_low, mix_down)
        _, pull_glu = jax.vjp(swiglu, both)
        d_both = pull_glu(d_act)[0].astype(jnp.bfloat16)
        sums[4] = sums[4] + inner(normed_two, d_both)
        d_normed_two = outer(d_both, mix_gate_up)
        _, pull_two = jax.vjp(rms_norm, resid, gain_two.astype(jnp.float32))
        d_resid_norm, d_gain_two = pull_two(d_normed_two)
        sums[3] = sums[3] + d_gain_two
        d_resid = upstream + d_resid_norm
        d_resid_low = d_resid.astype(jnp.bfloat16)
        sums[2] = sums[2] + inner(attended, d_resid_low)
        d_attended = outer(d_resid_low, mix_out).astype(jnp.bfloat16)
        d_grouped = d_attended.reshape(tok_count, KVH, groups, HD)
        delta = jnp.einsum("qkgd,kgqd->kgq", d_grouped.astype(jnp.float32), head_out)
        zero_q = jnp.zeros((tok_count, KVH, groups, HD), jnp.float32)
        back_state = (
            zero_q,
            jnp.zeros((seq_length, KVH * HD), jnp.float32),
            jnp.zeros((seq_length, KVH * HD), jnp.float32),
        )
        attend_piece = (
            lax.all_gather(key_rows, ("ctx", "fsdp"), axis=0, tiled=True),
            lax.all_gather(value_rows, ("ctx", "fsdp"), axis=0, tiled=True),
        )

        def attend_work(state):
            key_count = attend_piece[0].shape[0]
            keys = attend_piece[0].reshape(key_count, KVH, HD)
            values = attend_piece[1].reshape(key_count, KVH, HD)
            scores = (
                jnp.einsum("qkgd,tkd->kgqt", grouped, keys, preferred_element_type=jnp.float32)
                * factor
            )
            allowed = jnp.arange(key_count, dtype=jnp.int32)[None, :] <= positions[:, None]
            scores = jnp.where(allowed, scores, NEG)
            probs = jnp.where(allowed, jnp.exp(scores - log_total[..., None]), 0.0)
            d_probs = jnp.einsum(
                "qkgd,tkd->kgqt", d_grouped, values, preferred_element_type=jnp.float32
            )
            d_scores = (probs * (d_probs - delta[..., None])).astype(jnp.bfloat16)
            grad_q = jnp.einsum(
                "kgqt,tkd->qkgd", d_scores, keys, preferred_element_type=jnp.float32
            )
            piece_k = (
                jnp.einsum("kgqt,qkgd->tkd", d_scores, grouped, preferred_element_type=jnp.float32)
                * factor
            )
            piece_v = jnp.einsum(
                "kgqt,qkgd->tkd",
                probs.astype(jnp.bfloat16),
                d_grouped,
                preferred_element_type=jnp.float32,
            )
            grad_k = piece_k.reshape(key_count, KVH * HD)
            grad_v = piece_v.reshape(key_count, KVH * HD)
            return (grad_q, grad_k, grad_v)

        back_result = lax.cond(jnp.int32(0) <= pos_last, attend_work, unchanged, back_state)
        grad_q = back_result[0]
        summed_k, summed_v = side_by_side(
            (back_result[1].astype(jnp.bfloat16), back_result[2].astype(jnp.bfloat16)),
            ("ctx", "fsdp"),
            0,
            1,
        )
        d_q_raw = rotate(grad_q.reshape(tok_count, H, HD) * factor, cosine, -sine_table).reshape(
            tok_count, H * HD
        )
        d_k_raw = rotate(summed_k.reshape(tok_count, KVH, HD), cosine, -sine_table).reshape(
            tok_count, KVH * HD
        )
        d_mixed = jnp.concatenate([d_q_raw, d_k_raw, summed_v], axis=1).astype(jnp.bfloat16)
        sums[1] = sums[1] + inner(normed, d_mixed)
        d_normed = outer(d_mixed, mix_qkv)
        _, pull_one = jax.vjp(rms_norm, inputs, gain_one.astype(jnp.float32))
        d_inputs_norm, d_gain_one = pull_one(d_normed)
        sums[0] = sums[0] + d_gain_one
        in_grads.append((d_resid + d_inputs_norm).astype(jnp.bfloat16))
    grad_gain_one, grad_qkv, grad_out, grad_gain_two, grad_gate_up, grad_down = (
        lax.psum_scatter(sums[0], ("dp", "ctx", "fsdp"), scatter_dimension=0, tiled=True),
        lax.psum_scatter(sums[1], ("dp", "ctx", "fsdp"), scatter_dimension=1, tiled=True),
        lax.psum_scatter(sums[2], ("dp", "ctx", "fsdp"), scatter_dimension=0, tiled=True),
        lax.psum_scatter(sums[3], ("dp", "ctx", "fsdp"), scatter_dimension=0, tiled=True),
        lax.psum_scatter(sums[4], ("dp", "ctx", "fsdp"), scatter_dimension=1, tiled=True),
        lax.psum_scatter(sums[5], ("dp", "ctx", "fsdp"), scatter_dimension=0, tiled=True),
    )
    block_out = jnp.stack(outputs)[:, None]
    grad_tokens = jnp.stack(in_grads)[:, None]
    return (
        block_out,
        grad_tokens,
        grad_gain_one,
        grad_qkv,
        grad_out,
        grad_gain_two,
        grad_gate_up,
        grad_down,
    )


TP = ("dp", "ctx")
ALL = ("dp", "ctx", "fsdp")


def dot(left, right):
    return jnp.dot(left, right, preferred_element_type=jnp.float32)


def qkv_owner(sizes):
    moves = []
    for head in range(H + 2 * KVH):
        if head < H:
            group, slot = head // 2, head % 2
        elif head < H + KVH:
            group, slot = head - H, 2
        else:
            group, slot = head - H - KVH, 3
        device = group % sizes["dp"] * sizes["ctx"] + group // sizes["dp"]
        moves.append((head, device * sizes["fsdp"] + slot))
    return moves


def hidden_of(device, sizes):
    ctx = sizes["ctx"]
    return (device % ctx) * sizes["dp"] + device // ctx


def down_owner(sizes):
    n, f = sizes["dp"] * sizes["ctx"], sizes["fsdp"]
    return [
        (hidden_of(device, sizes) * f + slot, device * f + slot)
        for device in range(n)
        for slot in range(f)
    ]


def up_owner(sizes):
    n, f = sizes["dp"] * sizes["ctx"], sizes["fsdp"]
    half = n * f // 2
    moves = []
    for device in range(n):
        first = hidden_of(device, sizes) * (f // 2)
        for slot in range(f):
            source = first + slot if slot < f // 2 else half + first + slot - f // 2
            moves.append((source, device * f + slot))
    return moves


def back(moves):
    return [(to, source) for source, to in moves]


MESH = pl.DeviceIdType.MESH
VM = pltpu.VMEM
ANY = pl.ANY


def place():
    return lax.axis_index("dp"), lax.axis_index("ctx"), lax.axis_index("fsdp")


def at_device(dp, ctx, fs):
    return {"dp": dp, "ctx": ctx, "fsdp": fs}


def remote(src, dst, send, recv, device):
    return pltpu.make_async_remote_copy(
        src_ref=src, dst_ref=dst, send_sem=send, recv_sem=recv, device_id=device, device_id_type=MESH
    )


def arrived(dst, recv, device):
    remote(dst, dst, recv, recv, device).wait_recv()


def left(src, send, device):
    remote(src, src, send, send, device).wait_send()


def greet_all(sizes):
    dp, ctx, fs = sizes
    n = dp * ctx * fs
    d, c, f = place()
    me = (d * ctx + c) * fs + f
    barrier = pltpu.get_barrier_semaphore()

    def tell(step, carry):
        other = lax.rem(me + step, n)
        pl.semaphore_signal(
            barrier,
            inc=1,
            device_id=at_device(other // (ctx * fs), lax.rem(other // fs, ctx), lax.rem(other, fs)),
            device_id_type=MESH,
        )
        return carry

    lax.fori_loop(1, n, tell, 0)
    pl.semaphore_wait(barrier, n - 1)


class LineGather:
    def __init__(self, n, own, whole, send, recv, local):
        self.n, self.own, self.whole, self.send, self.recv, self.local = n, own, whole, send, recv, local
        self.d, self.c, self.f = place()

    def slot(self, at):
        return self.whole.at[self.d, at]

    def up(self, src, at):
        return remote(src, self.slot(at), self.send.at[0, at], self.recv.at[self.d, at], at_device(self.d, self.c + 1, self.f))

    def down(self, src, at):
        return remote(src, self.slot(at), self.send.at[1, at], self.recv.at[self.d, at], at_device(self.d, self.c - 1, self.f))

    def across(self, src, at):
        return remote(src, self.slot(at), self.send.at[2, at], self.recv.at[self.d, at], at_device(1 - self.d, self.c, self.f))

    def start(self):
        c = self.c

        @pl.when(c < self.n - 1)
        def _():
            self.up(self.own, c).start()

        @pl.when(c > 0)
        def _():
            self.down(self.own, c).start()

        self.across(self.own, c).start()
        pltpu.make_async_copy(self.own, self.slot(c), self.local).start()

    def forward(self, k):
        c = self.c

        @pl.when(c - k >= 0)
        def _():
            arrived(self.slot(c - k), self.recv.at[self.d, c - k], at_device(self.d, c, self.f))

            @pl.when(c < self.n - 1)
            def _():
                self.up(self.slot(c - k), c - k).start()

            self.across(self.slot(c - k), c - k).start()

        @pl.when(c + k < self.n)
        def _():
            arrived(self.slot(c + k), self.recv.at[self.d, c + k], at_device(self.d, c, self.f))

            @pl.when(c > 0)
            def _():
                self.down(self.slot(c + k), c + k).start()

            self.across(self.slot(c + k), c + k).start()

    def take(self, at):
        c = self.c

        @pl.when(at != c)
        def _():
            arrived(self.slot(at), self.recv.at[self.d, at], at_device(self.d, c, self.f))

            @pl.when(jnp.logical_and(at < c, c < self.n - 1))
            def _():
                self.up(self.slot(at), at).start()

            @pl.when(jnp.logical_and(at > c, c > 0))
            def _():
                self.down(self.slot(at), at).start()

            self.across(self.slot(at), at).start()

        self.other(at)

    def other(self, at):
        arrived(self.whole.at[1 - self.d, at], self.recv.at[1 - self.d, at], at_device(self.d, self.c, self.f))

    def finish_sends(self):
        c = self.c
        for at in range(self.n):

            @pl.when(jnp.logical_and(at <= c, c < self.n - 1))
            def _():
                left(self.slot(at), self.send.at[0, at], at_device(self.d, c, self.f))

            @pl.when(jnp.logical_and(at >= c, c > 0))
            def _():
                left(self.slot(at), self.send.at[1, at], at_device(self.d, c, self.f))

            left(self.slot(at), self.send.at[2, at], at_device(self.d, c, self.f))

    def finish(self):
        self.finish_sends()
        pltpu.make_async_copy(self.own, self.slot(self.c), self.local).wait()


FACTOR = HD ** (-0.5)
LANES = 128


def ordered(c, step, n):
    at = jnp.int32(0)
    for here in range(n):
        near = sorted(range(n), key=lambda place_: (abs(place_ - here), place_))
        for index, value in enumerate(near):
            at = jnp.where(jnp.logical_and(c == here, step == index), value, at)
    return at


def first_kernel(
    sizes, x_ref, gains_ref, w_ref, cos_ref, sin_up_ref, sin_down_ref, dy_ref, proj_ref, down_ref,
    normed_out, unit_out, att_out, wide_out, gains_out, dy_all, proj_all, down_all,
    x_all, w_all, wide, normed, stage, unit, att_stage, att, gain_all, gain_vec,
    line_send, line_recv, line_local, w_send, w_recv, w_pass, g_send, g_recv, u_send, u_recv, a_send, a_recv, out_sem,
    dy_send, dy_recv, dy_local, m_send, m_recv, m_pass,
):
    dp, ctx, fs = sizes
    n = dp * ctx * fs
    d, c, f = place()
    here = at_device(d, c, f)
    span = stage.shape[2]
    greet_all(sizes)

    q_core = f // 2
    kv_slot = 2 + c // 2
    kv_ctx = 2 * lax.rem(c, 2) + f // 2
    kv_core = lax.rem(f, 2)
    relay = f == 2 * lax.rem(c, 2) + d

    @pl.when(jnp.logical_and(d == 1, jnp.logical_or(kv_core != 1, kv_ctx != c)))
    def _():
        remote(w_ref, w_all.at[kv_slot], w_send.at[0], w_recv.at[kv_slot], at_device(kv_core, kv_ctx, f)).start()

    @pl.when(jnp.logical_and(d == 1, jnp.logical_and(kv_core == 1, kv_ctx == c)))
    def _():
        pltpu.make_async_copy(w_ref, w_all.at[kv_slot], w_recv.at[kv_slot]).start()

    line = LineGather(ctx, x_ref, x_all, line_send, line_recv, line_local)
    line.start()

    @pl.when(d == 0)
    def _():
        slot = lax.rem(f, 2)
        for to in range(fs):

            @pl.when(jnp.logical_or(q_core != 0, to != f))
            def _():
                remote(w_ref, w_all.at[slot], w_send.at[to], w_recv.at[slot], at_device(q_core, c, to)).start()

            @pl.when(jnp.logical_and(q_core == 0, to == f))
            def _():
                pltpu.make_async_copy(w_ref, w_all.at[slot], w_recv.at[slot]).start()

    me = (d * ctx + c) * fs + f

    def gain_to(step, carry):
        other = lax.rem(me + step, n)
        remote(
            gains_ref, gain_all.at[me], g_send.at[other], g_recv.at[me],
            at_device(other // (ctx * fs), lax.rem(other // fs, ctx), lax.rem(other, fs)),
        ).start()
        return carry

    lax.fori_loop(1, n, gain_to, 0)
    gain_all[me] = gains_ref[...]

    @pl.when(relay)
    def _():
        for slot in (2, 3):
            arrived(w_all.at[slot], w_recv.at[slot], here)
            for step in range(1, fs):
                to = lax.rem(f + step, fs)
                remote(w_all.at[slot], w_all.at[slot], w_pass.at[slot - 2, step], w_recv.at[slot], at_device(d, c, to)).start()

    def gain_from(step, carry):
        other = lax.rem(me + step, n)
        arrived(gain_all.at[other], g_recv.at[other], here)
        return carry

    lax.fori_loop(1, n, gain_from, 0)
    each = D // n
    for index in range(n):
        gain_vec[:, index * each : (index + 1) * each] = gain_all[index][:, :each]
    gain = gain_vec[0:1, :]

    wide[...] = jnp.zeros_like(wide)
    for slot in (0, 1, 2, 3):
        if slot < 2:
            arrived(w_all.at[slot], w_recv.at[slot], here)
        else:

            @pl.when(jnp.logical_not(relay))
            def _():
                arrived(w_all.at[slot], w_recv.at[slot], here)

        wide[:, slot * LANES : slot * LANES + HD] = w_all[slot]

    pltpu.make_async_copy(line.own, line.slot(c), line.local).wait()

    def block(step, carry):
        at = ordered(c, step, ctx)

        line.take(at)
        values = x_all[:, at].reshape(dp * 2 * span, D).astype(jnp.float32)
        scale = lax.rsqrt(jnp.mean(values * values, axis=-1, keepdims=True) + EPS)
        low = (values * scale * gain).astype(jnp.bfloat16)
        normed[:, at] = low.reshape(dp, 2 * span, D)
        heads = jnp.dot(low, wide[...], preferred_element_type=jnp.float32)
        cosine, sine_up, sine_down = cos_ref[at], sin_up_ref[at], sin_down_ref[at]
        for slot in range(4):
            head = heads[:, slot * LANES : (slot + 1) * LANES]
            if slot < 3:
                turned_up = pltpu.roll(head, HD // 2, 1).reshape(2 * dp, span, LANES)
                turned_down = pltpu.roll(head, LANES - HD // 2, 1).reshape(2 * dp, span, LANES)
                head = head.reshape(2 * dp, span, LANES)
                head = head * cosine[None] + turned_up * sine_up[None] + turned_down * sine_down[None]
            else:
                head = head.reshape(2 * dp, span, LANES)
            stage[at, :, :, slot * LANES : (slot + 1) * LANES] = head.astype(jnp.bfloat16)
        for to in range(2 * dp):

            @pl.when(to != f)
            def _():
                remote(stage.at[at, to], unit.at[at, f], u_send.at[at, to], u_recv.at[at, f], at_device(d, c, to)).start()

            @pl.when(to == f)
            def _():
                unit[at, f] = stage[at, to]

        return carry

    lax.fori_loop(0, ctx, block, 0)
    normed_copy = pltpu.make_async_copy(normed, normed_out, out_sem.at[0])
    wide_copy = pltpu.make_async_copy(wide, wide_out, out_sem.at[1])
    gains_copy = pltpu.make_async_copy(gain_vec, gains_out, out_sem.at[2])
    normed_copy.start()
    wide_copy.start()
    gains_copy.start()

    to_core, to_ctx = lax.rem(c, 2), 2 * d + c // 2
    stays = jnp.logical_and(to_core == d, to_ctx == c)
    moved = ((proj_ref, proj_all), (down_ref, down_all))
    for index, (shard, whole) in enumerate(moved):

        @pl.when(jnp.logical_not(stays))
        def _():
            remote(shard, whole.at[f], m_send.at[index], m_recv.at[index, f], at_device(to_core, to_ctx, f)).start()

        @pl.when(stays)
        def _():
            pltpu.make_async_copy(shard, whole.at[f], m_recv.at[index, f]).start()

    dy_line = LineGather(ctx, dy_ref, dy_all, dy_send, dy_recv, dy_local)
    dy_line.start()

    def pass_on():
        for index, (shard, whole) in enumerate(moved):
            arrived(whole.at[f], m_recv.at[index, f], here)
            for step in range(1, fs):
                to = lax.rem(f + step, fs)
                remote(whole.at[f], whole.at[f], m_pass.at[index, step], m_recv.at[index, f], at_device(d, c, to)).start()

    for at in range(ctx):
        for step in range(1, fs):
            other = lax.rem(f + step, fs)
            arrived(unit.at[at, other], u_recv.at[at, other], here)
    unit_copy = pltpu.make_async_copy(unit, unit_out, out_sem.at[3])
    unit_copy.start()

    rows = fs * span
    for at in range(ctx):
        keys = rows * (at + 1)
        k_rows = unit[0 : at + 1, :, :, 2 * LANES : 3 * LANES].reshape(keys, LANES)
        v_rows = unit[0 : at + 1, :, :, 3 * LANES : 4 * LANES].reshape(keys, LANES)
        allowed = lax.broadcasted_iota(jnp.int32, (rows, keys), 1) <= rows * at + lax.broadcasted_iota(
            jnp.int32, (rows, keys), 0
        )
        for head in range(2):
            q_rows = unit[at, :, :, head * LANES : (head + 1) * LANES].reshape(rows, LANES)
            scores = outer(q_rows, k_rows) * FACTOR
            scores = jnp.where(allowed, scores, NEG)
            best = jnp.max(scores, axis=-1, keepdims=True)
            weights = jnp.exp(scores - best)
            probs = weights / jnp.sum(weights, axis=-1, keepdims=True)
            mixed = jnp.dot(probs.astype(jnp.bfloat16), v_rows, preferred_element_type=jnp.float32)
            att_stage[at, :, :, head * LANES : (head + 1) * LANES] = mixed.astype(jnp.bfloat16).reshape(fs, span, LANES)
        for to in range(fs):

            @pl.when(to != f)
            def _():
                remote(
                    att_stage.at[at, to], att.at[f // 2, at, lax.rem(f, 2)], a_send.at[at, to], a_recv.at[f, at], at_device(d, c, to)
                ).start()

            @pl.when(to == f)
            def _():
                att[f // 2, at, lax.rem(f, 2)] = att_stage[at, to]

        if at == 0:
            pass_on()
        else:
            dy_line.forward(at)

    for at in range(ctx):
        for step in range(1, fs):
            other = lax.rem(f + step, fs)
            arrived(att.at[other // 2, at, lax.rem(other, 2)], a_recv.at[other, at], here)
    att_copy = pltpu.make_async_copy(att, att_out, out_sem.at[4])
    att_copy.start()

    for at in range(ctx):
        dy_line.other(at)
    dy_line.finish()
    for index, (shard, whole) in enumerate(moved):
        for step in range(1, fs):
            other = lax.rem(f + step, fs)
            arrived(whole.at[other], m_recv.at[index, other], here)
            left(whole.at[f], m_pass.at[index, step], here)

        @pl.when(jnp.logical_not(stays))
        def _():
            left(shard, m_send.at[index], here)

    line.finish_sends()
    for at in range(ctx):

        for to in range(fs):

            @pl.when(to != f)
            def _():
                left(stage.at[at, to], u_send.at[at, to], here)
                left(att_stage.at[at, to], a_send.at[at, to], here)

    @pl.when(jnp.logical_and(d == 1, jnp.logical_or(kv_core != 1, kv_ctx != c)))
    def _():
        left(w_ref, w_send.at[0], here)

    @pl.when(d == 0)
    def _():
        for to in range(fs):

            @pl.when(jnp.logical_or(q_core != 0, to != f))
            def _():
                left(w_ref, w_send.at[to], here)

    @pl.when(relay)
    def _():
        for slot in (2, 3):
            for step in range(1, fs):
                left(w_all.at[slot], w_pass.at[slot - 2, step], here)

    def gain_left(step, carry):
        other = lax.rem(me + step, n)
        left(gains_ref, g_send.at[other], here)
        return carry

    lax.fori_loop(1, n, gain_left, 0)
    for copy in (normed_copy, wide_copy, gains_copy, unit_copy, att_copy):
        copy.wait()


def first(sizes, x, gains, w_qkv, cosine, sine_up, sine_down, dy, w_out, w_down):
    dp, ctx, fs = sizes
    n = dp * ctx * fs
    rows = x.shape[0]
    span = rows // 2
    low, wide_t = jnp.bfloat16, jnp.float32
    dma = pltpu.SemaphoreType.DMA
    shapes = (
        jax.ShapeDtypeStruct((dp, ctx, rows, D), low),
        jax.ShapeDtypeStruct((ctx, fs, span, 4 * LANES), low),
        jax.ShapeDtypeStruct((dp, ctx, 2, span, 2 * LANES), low),
        jax.ShapeDtypeStruct((D, 4 * LANES), low),
        jax.ShapeDtypeStruct((8, D), wide_t),
        jax.ShapeDtypeStruct((dp, ctx, rows, D), low),
        jax.ShapeDtypeStruct((fs,) + w_out.shape, low),
        jax.ShapeDtypeStruct((fs,) + w_down.shape, low),
    )
    any_spec, vm_spec = pl.BlockSpec(memory_space=ANY), pl.BlockSpec(memory_space=VM)
    return pl.pallas_call(
        functools.partial(first_kernel, sizes),
        name="first",
        out_shape=shapes,
        in_specs=[vm_spec, vm_spec, any_spec, vm_spec, vm_spec, vm_spec, vm_spec, any_spec, any_spec],
        out_specs=[any_spec] * 8,
        scratch_shapes=[
            VM((dp, ctx, rows, D), low),
            VM((4, D, HD), low),
            VM((D, 4 * LANES), low),
            VM((dp, ctx, rows, D), low),
            VM((ctx, 2 * dp, span, 4 * LANES), low),
            VM((ctx, fs, span, 4 * LANES), low),
            VM((ctx, fs, span, 2 * LANES), low),
            VM((dp, ctx, 2, span, 2 * LANES), low),
            VM((n, 8, LANES), wide_t),
            VM((8, D), wide_t),
            dma((3, ctx)), dma((dp, ctx)), dma,
            dma((fs,)), dma((4,)), dma((2, fs)),
            dma((n,)), dma((n,)),
            dma((ctx, 2 * dp)), dma((ctx, fs)),
            dma((ctx, fs)), dma((fs, ctx)),
            dma((5,)),
            dma((3, ctx)), dma((dp, ctx)), dma,
            dma((2,)), dma((2, fs)), dma((2, fs)),
        ],
        compiler_params=pltpu.CompilerParams(collective_id=1, has_side_effects=True, vmem_limit_bytes=60 * 1024 * 1024),
    )(x, gains, w_qkv, cosine, sine_up, sine_down, dy, w_out, w_down)


def angle_tables(ctx, fs, span):
    f_index = lax.axis_index("fsdp")
    positions = (jnp.arange(ctx, dtype=jnp.int32)[:, None] * fs + f_index) * span + jnp.arange(span, dtype=jnp.int32)[None, :]
    return lane_tables(positions)


def lane_tables(positions):
    lane = jnp.arange(LANES, dtype=jnp.int32)
    pair = (lane % (HD // 2)).astype(jnp.float32)
    frequency = THETA ** (-(pair * 2.0) / HD)
    angles = positions.astype(jnp.float32)[..., None] * frequency
    inside = lane < HD
    low_half = lane < HD // 2
    cosine = jnp.where(inside, jnp.cos(angles), 0.0)
    sine = jnp.sin(angles)
    sine_up = jnp.where(jnp.logical_and(inside, jnp.logical_not(low_half)), sine, 0.0)
    sine_down = jnp.where(low_half, -sine, 0.0)
    return cosine, sine_up, sine_down


class LineSum:
    def __init__(self, n, mine, out_core, in_core, out_line, in_line, total, sems):
        self.n, self.mine, self.out_core, self.in_core = n, mine, out_core, in_core
        self.out_line, self.in_line, self.total = out_line, in_line, total
        self.core_send, self.core_recv, self.line_send, self.line_recv = sems
        self.d, self.c, self.f = place()
        self.here = at_device(self.d, self.c, self.f)

    def give(self, at, both):
        d = self.d
        low = both.astype(jnp.bfloat16)

        @pl.when(d == 0)
        def _():
            self.mine[at] = low[0]
            self.out_core[at] = low[1]

        @pl.when(d != 0)
        def _():
            self.mine[at] = low[1]
            self.out_core[at] = low[0]

        remote(
            self.out_core.at[at], self.in_core.at[at], self.core_send.at[at], self.core_recv.at[at], at_device(1 - d, self.c, self.f)
        ).start()

    def step(self, at):
        n, d, c, f = self.n, self.d, self.c, self.f
        arrived(self.in_core.at[at], self.core_recv.at[at], self.here)
        self.total[...] = self.mine[at].astype(jnp.float32) + self.in_core[at].astype(jnp.float32)

        @pl.when(jnp.logical_and(at <= c, c < n - 1))
        def _():
            arrived(self.in_line.at[0, at], self.line_recv.at[0, at], self.here)
            self.total[...] += self.in_line[0, at].astype(jnp.float32)

        @pl.when(jnp.logical_and(at >= c, c > 0))
        def _():
            arrived(self.in_line.at[1, at], self.line_recv.at[1, at], self.here)
            self.total[...] += self.in_line[1, at].astype(jnp.float32)

        @pl.when(at != c)
        def _():
            self.out_line[at] = self.total[...].astype(jnp.bfloat16)

        @pl.when(at < c)
        def _():
            remote(
                self.out_line.at[at], self.in_line.at[0, at], self.line_send.at[at], self.line_recv.at[0, at], at_device(d, c - 1, f)
            ).start()

        @pl.when(at > c)
        def _():
            remote(
                self.out_line.at[at], self.in_line.at[1, at], self.line_send.at[at], self.line_recv.at[1, at], at_device(d, c + 1, f)
            ).start()

    def finish(self):
        for at in range(self.n):
            left(self.out_core.at[at], self.core_send.at[at], self.here)

            @pl.when(at != self.c)
            def _():
                left(self.out_line.at[at], self.line_send.at[at], self.here)

    @staticmethod
    def scratch(ctx, rows):
        low = jnp.bfloat16
        dma = pltpu.SemaphoreType.DMA
        return [
            VM((ctx, rows, D), low), VM((ctx, rows, D), low), VM((ctx, rows, D), low), VM((ctx, rows, D), low),
            VM((2, ctx, rows, D), low), VM((rows, D), jnp.float32),
            dma((ctx,)), dma((ctx,)), dma((ctx,)), dma((2, ctx)),
        ]


def greet_near(sizes):
    dp, ctx, fs = sizes
    d, c, f = place()
    barrier = pltpu.get_barrier_semaphore()

    def tell(device):
        pl.semaphore_signal(barrier, inc=1, device_id=device, device_id_type=MESH)

    tell(at_device(1 - d, c, f))
    for step in range(1, fs):
        for core in range(dp):
            tell(at_device(core, c, lax.rem(f + step, fs)))

    @pl.when(c > 0)
    def _():
        tell(at_device(d, c - 1, f))

    @pl.when(c < ctx - 1)
    def _():
        tell(at_device(d, c + 1, f))

    known = 1 + dp * (fs - 1)
    ends = jnp.logical_or(c == 0, c == ctx - 1)

    @pl.when(ends)
    def _():
        pl.semaphore_wait(barrier, known + 1)

    @pl.when(jnp.logical_not(ends))
    def _():
        pl.semaphore_wait(barrier, known + 2)


def middle_kernel(
    sizes, hidden, att_ref, x_ref, dy_ref, gains_ref, proj_ref, down_ref, gate_up_ref, dy_all_ref,
    resid_out, d_resid_out, gain_out, partial_out, unit_out, grad_up_out, grad_down_out, grad_proj_out,
    att, dy_all, proj, down, gate_up, resid, own_two, normed_two, act, d_both, part_stage, own_d, d_resid_all, d_stage, unit,
    grad_up, grad_down, grad_proj,
    in_sem, gu_send, gu_recv, two_send, two_recv, two_local, dr_send, dr_recv, dr_local, u_send, u_recv, out_sem, part_sem,
    *sums,
):
    dp, ctx, fs = sizes
    d, c, f = place()
    here = at_device(d, c, f)
    rows = x_ref.shape[0]
    span = rows // 2
    both_rows = dp * rows
    half = hidden // 2
    line_sum = LineSum(ctx, *sums[:6], sums[6:10])
    second_sum = LineSum(ctx, *sums[10:16], sums[16:20])

    att_copy = pltpu.make_async_copy(att_ref, att, in_sem.at[0])
    dy_copy = pltpu.make_async_copy(dy_all_ref, dy_all, in_sem.at[1])
    down_copy = pltpu.make_async_copy(down_ref, down, in_sem.at[2])
    att_copy.start()
    proj[...] = jnp.zeros_like(proj)
    each = proj_ref.shape[1]
    proj_copies = []
    for slot in range(fs):
        start = slot // 2 * LANES + slot % 2 * each
        proj_copies.append(pltpu.make_async_copy(proj_ref.at[slot], proj.at[start : start + each], in_sem.at[3 + slot]))
        proj_copies[-1].start()
    dy_copy.start()
    down_copy.start()
    greet_near(sizes)

    to_core = f // 2
    gu_slot = 2 * d + lax.rem(f, 2)
    for to in range(fs):
        own_place = jnp.logical_and(to_core == d, f == to)

        @pl.when(jnp.logical_not(own_place))
        def _():
            remote(gate_up_ref, gate_up.at[gu_slot], gu_send.at[to], gu_recv.at[gu_slot], at_device(to_core, c, to)).start()

        @pl.when(own_place)
        def _():
            pltpu.make_async_copy(gate_up_ref, gate_up.at[gu_slot], gu_recv.at[gu_slot]).start()

    att_copy.wait()
    for copy in proj_copies:
        copy.wait()

    def project(step, carry):
        at = ordered(c, ctx - 1 - step, ctx)
        terms = jnp.dot(att[:, at].reshape(both_rows, 2 * LANES), proj[...], preferred_element_type=jnp.float32)
        line_sum.give(at, terms.reshape(dp, rows, D))
        return carry

    lax.fori_loop(0, ctx, project, 0)

    def sum_up(step, carry):
        line_sum.step(ordered(c, ctx - 1 - step, ctx))
        return carry

    lax.fori_loop(0, ctx, sum_up, 0)
    gain = gains_ref[1:2, :]
    values = x_ref[...].astype(jnp.float32) + line_sum.total[...]
    resid[...] = values
    scale = lax.rsqrt(jnp.mean(values * values, axis=-1, keepdims=True) + EPS)
    own_two[...] = (values * scale * gain).astype(jnp.bfloat16)
    resid_copy = pltpu.make_async_copy(resid, resid_out, out_sem.at[0])
    resid_copy.start()
    line = LineGather(ctx, own_two, normed_two, two_send, two_recv, two_local)
    line.start()
    line_sum.finish()
    for slot in range(4):
        arrived(gate_up.at[slot], gu_recv.at[slot], here)
    dy_copy.wait()
    down_copy.wait()
    pltpu.make_async_copy(line.own, line.slot(c), line.local).wait()

    def mlp(step, carry):
        at = ordered(c, step, ctx)

        line.take(at)
        inputs = normed_two[:, at].reshape(both_rows, D)
        dy_rows = dy_all[:, at].reshape(both_rows, D)
        for part in range(2):
            cols = slice(part * half, (part + 1) * half)
            gate = jnp.dot(inputs, gate_up[part], preferred_element_type=jnp.float32)
            up = jnp.dot(inputs, gate_up[2 + part], preferred_element_type=jnp.float32)
            d_act = outer(dy_rows, down[cols, :])
            sig = 1.0 / (1.0 + jnp.exp(-gate))
            silu = gate * sig
            act[:, at, :, cols] = (silu * up).astype(jnp.bfloat16).reshape(dp, rows, half)
            d_gate = d_act * up * (sig * (1.0 + gate * (1.0 - sig)))
            d_both[:, at, :, cols] = d_gate.astype(jnp.bfloat16).reshape(dp, rows, half)
            d_both[:, at, :, hidden + part * half : hidden + (part + 1) * half] = (
                (d_act * silu).astype(jnp.bfloat16).reshape(dp, rows, half)
            )
        terms = outer(d_both[:, at, :, 0:half].reshape(both_rows, half), gate_up[0])
        for part in range(1, 4):
            terms += outer(d_both[:, at, :, part * half : (part + 1) * half].reshape(both_rows, half), gate_up[part])
        second_sum.give(at, terms.reshape(dp, rows, D))
        return carry

    lax.fori_loop(0, ctx, mlp, 0)

    wide_rows = D // ctx

    def grads(step):
        first = pl.multiple_of(step * wide_rows, LANES)
        left_rows = normed_two[:, :, :, pl.ds(first, wide_rows)].reshape(dp * ctx * rows, wide_rows)
        for part in range(2):
            cols = slice(part * hidden, (part + 1) * hidden)
            grad_up[pl.ds(first, wide_rows), cols] = inner(left_rows, d_both[:, :, :, cols].reshape(dp * ctx * rows, hidden)).astype(jnp.bfloat16)
        dy_cols = dy_all[:, :, :, pl.ds(first, wide_rows)].reshape(dp * ctx * rows, wide_rows)
        grad_down[:, pl.ds(first, wide_rows)] = inner(act[...].reshape(dp * ctx * rows, hidden), dy_cols).astype(jnp.bfloat16)

    def sum_two(step, carry):
        second_sum.step(ordered(c, ctx - 1 - step, ctx))

        @pl.when(step < ctx - 1)
        def _():
            grads(step)

        return carry

    lax.fori_loop(0, ctx, sum_two, 0)
    values = resid[...]
    scale = lax.rsqrt(jnp.mean(values * values, axis=-1, keepdims=True) + EPS)
    incoming = second_sum.total[...]
    weighted = incoming * gain
    mean = jnp.mean(weighted * values, axis=-1, keepdims=True)
    d_resid = dy_ref[...].astype(jnp.float32) + scale * weighted - values * (scale * scale * scale) * mean
    own_d[...] = d_resid.astype(jnp.bfloat16)
    d_resid_out[...] = d_resid
    gain_out[...] = jnp.broadcast_to(jnp.sum(incoming * values * scale, axis=0, keepdims=True), gain_out.shape)
    d_line = LineGather(ctx, own_d, d_resid_all, dr_send, dr_recv, dr_local)
    d_line.start()
    line.finish_sends()
    second_sum.finish()
    grads(ctx - 1)
    grad_up_copy = pltpu.make_async_copy(grad_up, grad_up_out, out_sem.at[1])
    grad_down_copy = pltpu.make_async_copy(grad_down, grad_down_out, out_sem.at[2])
    grad_up_copy.start()
    grad_down_copy.start()
    pltpu.make_async_copy(d_line.own, d_line.slot(c), d_line.local).wait()
    grad_proj[...] = jnp.zeros_like(grad_proj)

    def back(step, carry):
        at = ordered(c, step, ctx)

        d_line.take(at)
        incoming = d_resid_all[:, at].reshape(both_rows, D)
        d_att = outer(incoming, proj[...]).astype(jnp.bfloat16)
        d_stage[at] = d_att.reshape(2 * dp, span, 2 * LANES)
        for to in range(2 * dp):

            @pl.when(to != f)
            def _():
                remote(d_stage.at[at, to], unit.at[at, f], u_send.at[at, to], u_recv.at[at, f], at_device(d, c, to)).start()

            @pl.when(to == f)
            def _():
                unit[at, f] = d_stage[at, to]

        grad_proj[...] += inner(att[:, at].reshape(both_rows, 2 * LANES), incoming)

        outputs = jnp.dot(act[:, at].reshape(both_rows, hidden), down[...], preferred_element_type=jnp.float32)
        slot = lax.rem(step, 2)

        @pl.when(step >= 2)
        def _():
            pltpu.make_async_copy(part_stage.at[slot], partial_out.at[:, at], part_sem.at[slot]).wait()

        part_stage[slot] = outputs.reshape(dp, rows, D).astype(jnp.bfloat16)
        pltpu.make_async_copy(part_stage.at[slot], partial_out.at[:, at], part_sem.at[slot]).start()
        return carry

    lax.fori_loop(0, ctx, back, 0)
    grad_proj_copy = pltpu.make_async_copy(grad_proj, grad_proj_out, out_sem.at[3])
    grad_proj_copy.start()
    for at in range(ctx):
        for step in range(1, fs):
            other = lax.rem(f + step, fs)
            arrived(unit.at[at, other], u_recv.at[at, other], here)
    unit_copy = pltpu.make_async_copy(unit, unit_out, out_sem.at[4])
    unit_copy.start()
    d_line.finish_sends()
    for at in range(ctx):
        for to in range(fs):

            @pl.when(to != f)
            def _():
                left(d_stage.at[at, to], u_send.at[at, to], here)

    for to in range(fs):

        @pl.when(jnp.logical_not(jnp.logical_and(to_core == d, f == to)))
        def _():
            left(gate_up_ref, gu_send.at[to], here)

    for slot in range(2):
        pltpu.make_async_copy(part_stage.at[slot], partial_out.at[:, 0], part_sem.at[slot]).wait()
    for copy in (resid_copy, grad_up_copy, grad_down_copy, grad_proj_copy, unit_copy):
        copy.wait()


def middle(sizes, att, x, dy, gains, proj, down, w_gate_up, dy_all):
    dp, ctx, fs = sizes
    rows = x.shape[0]
    span = rows // 2
    hidden = FF // (dp * ctx)
    low, wide_t = jnp.bfloat16, jnp.float32
    dma = pltpu.SemaphoreType.DMA
    any_spec, vm_spec = pl.BlockSpec(memory_space=ANY), pl.BlockSpec(memory_space=VM)
    shapes = (
        jax.ShapeDtypeStruct((rows, D), wide_t),
        jax.ShapeDtypeStruct((rows, D), wide_t),
        jax.ShapeDtypeStruct((8, D), wide_t),
        jax.ShapeDtypeStruct((dp, ctx, rows, D), low),
        jax.ShapeDtypeStruct((ctx, fs, span, 2 * LANES), low),
        jax.ShapeDtypeStruct((D, 2 * hidden), low),
        jax.ShapeDtypeStruct((hidden, D), low),
        jax.ShapeDtypeStruct((2 * LANES, D), wide_t),
    )
    return pl.pallas_call(
        functools.partial(middle_kernel, sizes, hidden),
        name="middle",
        out_shape=shapes,
        in_specs=[any_spec, vm_spec, vm_spec, vm_spec, any_spec, any_spec, any_spec, any_spec],
        out_specs=[any_spec, vm_spec, vm_spec] + [any_spec] * 5,
        scratch_shapes=[
            VM((dp, ctx, rows, 2 * LANES), low),
            VM((dp, ctx, rows, D), low),
            VM((2 * LANES, D), low),
            VM((hidden, D), low),
            VM((4, D, hidden // 2), low),
            VM((rows, D), wide_t),
            VM((rows, D), low),
            VM((dp, ctx, rows, D), low),
            VM((dp, ctx, rows, hidden), low),
            VM((dp, ctx, rows, 2 * hidden), low),
            VM((2, dp, rows, D), low),
            VM((rows, D), low),
            VM((dp, ctx, rows, D), low),
            VM((ctx, 2 * dp, span, 2 * LANES), low),
            VM((ctx, fs, span, 2 * LANES), low),
            VM((D, 2 * hidden), low),
            VM((hidden, D), low),
            VM((2 * LANES, D), wide_t),
            dma((3 + fs,)), dma((fs,)), dma((4,)),
            dma((3, ctx)), dma((dp, ctx)), dma,
            dma((3, ctx)), dma((dp, ctx)), dma,
            dma((ctx, 2 * dp)), dma((ctx, fs)),
            dma((5,)), dma((2,)),
        ] + LineSum.scratch(ctx, rows) + LineSum.scratch(ctx, rows),
        compiler_params=pltpu.CompilerParams(collective_id=2, has_side_effects=True, vmem_limit_bytes=63 * 1024 * 1024),
    )(att, x, dy, gains, proj, down.reshape(hidden, D), w_gate_up, dy_all)


def gather_tp(value):
    return lax.all_gather(value, TP, axis=0, tiled=True)


def sum_tp(value):
    return lax.psum_scatter(value.astype(jnp.bfloat16), TP, scatter_dimension=0, tiled=True).astype(
        jnp.float32
    )


def norm_back(values, scale, gain, incoming):
    weighted = incoming * gain
    mean = jnp.mean(weighted * values, axis=-1, keepdims=True)
    return scale * weighted - values * (scale * scale * scale) * mean


def on_device(tokens, cotangent, attn_gain, w_qkv, w_out, mlp_gain, w_gate_up, w_down):
    sizes = {name: lax.axis_size(name) for name in ALL}
    dp, ctx, fs = sizes["dp"], sizes["ctx"], sizes["fsdp"]
    mb, _, span, _ = tokens.shape
    rows = mb * span
    f_index = lax.axis_index("fsdp")
    length = span * ctx * fs
    factor = HD ** (-0.5)
    hidden = FF // (dp * ctx)

    x_low = tokens.reshape(rows, D)
    gain_rows = jnp.zeros((8, LANES), jnp.float32)
    gain_rows = gain_rows.at[0, : attn_gain.shape[0]].set(attn_gain.astype(jnp.float32))
    gain_rows = gain_rows.at[1, : mlp_gain.shape[0]].set(mlp_gain.astype(jnp.float32))
    cosine, sine_up, sine_down = angle_tables(ctx, fs, span)
    dy = cotangent.reshape(rows, D)
    where = (dp, ctx, fs)
    normed, unit, att, qkv, gains, dy_all, proj, down = first(
        where, x_low, gain_rows, w_qkv, cosine, sine_up, sine_down, dy, w_out, w_down
    )
    att = att.reshape(dp, ctx, rows, 2 * LANES)
    resid, d_resid, grad_two, partial, d_unit, grad_gate_up, grad_down, grad_out = middle(
        where, att, x_low, dy, gains, proj, down, w_gate_up, dy_all
    )
    block_out = (resid + sum_tp(partial.reshape(dp * ctx * rows, D))).astype(jnp.bfloat16)
    grad_two = grad_two[0]
    grad_out = grad_out.reshape(2, LANES, D)[:, :HD].reshape(2 * HD, D)
    d_unit = jnp.moveaxis(d_unit.reshape(length, 2, LANES), 1, 0)
    gain_one, gain_two = gains[0], gains[1]
    normed = normed.reshape(dp * ctx * rows, D)
    unit = unit.reshape(length, 4, LANES)

    x = x_low.astype(jnp.float32)
    scale_one = lax.rsqrt(jnp.mean(x * x, axis=-1, keepdims=True) + EPS)

    def to_units(values):
        count = values.shape[0]
        values = values.transpose(1, 3, 0, 2, 4, 5)
        values = values.reshape(dp * mb, count, ctx, span, -1)
        values = lax.all_to_all(values, "fsdp", split_axis=0, concat_axis=0, tiled=True)
        return values.transpose(1, 2, 0, 3, 4).reshape(count, length, -1)

    def to_rows(values):
        count = values.shape[0]
        values = values.reshape(count, ctx, fs, span, -1).transpose(2, 0, 1, 3, 4)
        values = lax.all_to_all(values, "fsdp", split_axis=0, concat_axis=0, tiled=True)
        values = values.reshape(dp, mb, count, ctx, span, -1).transpose(2, 0, 3, 1, 4, 5)
        return values.reshape(count, dp * ctx * rows, -1)

    q = jnp.stack([unit[:, 0], unit[:, 1]])
    k, v = unit[:, 2], unit[:, 3]
    scores = jnp.einsum("hqd,kd->hqk", q, k, preferred_element_type=jnp.float32) * factor
    allowed = jnp.arange(length)[None, :] <= jnp.arange(length)[:, None]
    scores = jnp.where(allowed, scores, NEG)
    best = jnp.max(scores, axis=-1, keepdims=True)
    weights = jnp.where(allowed, jnp.exp(scores - best), 0.0)
    probs = weights / jnp.sum(weights, axis=-1, keepdims=True)
    probs_low = probs.astype(jnp.bfloat16)
    d_probs = jnp.einsum("hqd,kd->hqk", d_unit, v, preferred_element_type=jnp.float32)
    delta = jnp.sum(probs * d_probs, axis=-1, keepdims=True)
    d_scores = (probs * (d_probs - delta)).astype(jnp.bfloat16)
    d_q = jnp.einsum("hqk,kd->hqd", d_scores, k, preferred_element_type=jnp.float32) * factor
    d_k = jnp.einsum("hqk,hqd->kd", d_scores, q, preferred_element_type=jnp.float32) * factor
    d_v = jnp.einsum("hqk,hqd->kd", probs_low, d_unit, preferred_element_type=jnp.float32)
    cos_u, up_u, down_u = lane_tables(jnp.arange(length, dtype=jnp.int32))

    def unturn(values):
        return values * cos_u - jnp.roll(values, HD // 2, -1) * up_u - jnp.roll(values, -(HD // 2), -1) * down_u

    d_heads = jnp.concatenate([unturn(d_q), unturn(d_k)[None], d_v[None]]).astype(jnp.bfloat16)
    d_mixed = to_rows(d_heads)
    d_mixed = jnp.moveaxis(d_mixed, 0, 1).reshape(dp * ctx * rows, 4 * LANES)
    grad_qkv = jnp.moveaxis(inner(normed, d_mixed).reshape(D, 4, LANES)[:, :, :HD], 1, 0)
    d_normed = sum_tp(outer(d_mixed, qkv))
    grad_one = jnp.sum(d_normed * x * scale_one, axis=0)
    grad_tokens = (d_resid + norm_back(x, scale_one, gain_one, d_normed)).astype(jnp.bfloat16)

    def reduce_rows(value, dim, moves):
        value = lax.psum_scatter(value.astype(jnp.bfloat16), "fsdp", scatter_dimension=dim, tiled=True)
        if moves is not None:
            value = lax.ppermute(value, ALL, back(moves))
        return value.astype(jnp.float32)

    gain_grads = lax.psum_scatter(jnp.stack([grad_one, grad_two]), ALL, scatter_dimension=1, tiled=True)
    return (
        block_out.reshape(tokens.shape),
        grad_tokens.reshape(tokens.shape),
        gain_grads[0],
        reduce_rows(grad_qkv, 0, qkv_owner(sizes)).reshape(D, HD),
        reduce_rows(grad_out, 0, down_owner(sizes)),
        gain_grads[1],
        reduce_rows(grad_gate_up, 1, up_owner(sizes)),
        reduce_rows(grad_down, 0, down_owner(sizes)),
    )


def fits(mesh):
    return mesh.shape["dp"] * mesh.shape["ctx"] == KVH and mesh.shape["fsdp"] == 4


def solution(mesh):
    placed = (
        P(None, "dp", ("ctx", "fsdp"), None),
        P(None, "dp", ("ctx", "fsdp"), None),
        P(("dp", "ctx", "fsdp")),
        P(None, ("dp", "ctx", "fsdp")),
        P(("dp", "ctx", "fsdp"), None),
        P(("dp", "ctx", "fsdp")),
        P(None, ("dp", "ctx", "fsdp")),
        P(("dp", "ctx", "fsdp"), None),
    )
    return jax.shard_map(
        on_device if fits(mesh) else on_device_gathered,
        mesh=mesh,
        in_specs=placed,
        out_specs=(
            P(None, "dp", ("ctx", "fsdp"), None),
            P(None, "dp", ("ctx", "fsdp"), None),
            P(("dp", "ctx", "fsdp")),
            P(None, ("dp", "ctx", "fsdp")),
            P(("dp", "ctx", "fsdp"), None),
            P(("dp", "ctx", "fsdp")),
            P(None, ("dp", "ctx", "fsdp")),
            P(("dp", "ctx", "fsdp"), None),
        ),
        check_vma=False,
    )
```

```python
import functools

import jax
import jax.numpy as jnp
from jax import lax
from jax.experimental import pallas as pl
from jax.experimental.pallas import tpu as pltpu
from jax.sharding import PartitionSpec as P

D = 1536
H = 16
KVH = 8
HD = 96
FF = 4096


EPS = 1e-05
THETA = 100000.0
NEG = -1e30


def in_blocks(value, dim, length):
    lengths = value.shape
    pieces = value.reshape(*lengths[:dim], length, lengths[dim] // length, *lengths[dim + 1 :])
    return jnp.moveaxis(pieces, dim, 0)


def sum_at_owner(value, axis, dim):
    pieces = in_blocks(value, dim, lax.axis_size(axis))
    arrived = lax.all_to_all(pieces, axis, split_axis=0, concat_axis=0, tiled=True)
    return arrived.astype(jnp.float32).sum(axis=0)


def side_by_side(arrays, axis, dim, along):
    both = jnp.concatenate(arrays, axis=along)
    whole, at, finished = (sum_at_owner(both, axis, dim), 0, [])
    for a in arrays:
        finished.append(lax.slice_in_dim(whole, at, at + a.shape[along], axis=along))
        at += a.shape[along]
    return tuple(finished)


def rms_norm(values, gain_vec):
    return values * lax.rsqrt(jnp.mean(values * values, axis=-1, keepdims=True) + EPS) * gain_vec


def tables(start, length, width):
    half_width = width // 2
    frequency = THETA ** (-(jnp.arange(half_width, dtype=jnp.float32) * 2.0) / width)
    angles = (start + jnp.arange(length, dtype=jnp.int32)).astype(jnp.float32)[:, None] * frequency[
        None, :
    ]
    return (jnp.cos(angles), jnp.sin(angles))


def rotate(values, cosine, sine_table):
    half_width = values.shape[-1] // 2
    first_half = values[..., :half_width]
    second_half = values[..., half_width:]
    cos_b = cosine[:, None, :]
    sin_b = sine_table[:, None, :]
    return jnp.concatenate(
        [first_half * cos_b - second_half * sin_b, second_half * cos_b + first_half * sin_b],
        axis=-1,
    )


def swiglu(both):
    return jax.nn.silu(both[:, :FF]) * both[:, FF:]


def inner(left, right):
    return lax.dot_general(
        left, right, (((0,), (0,)), ((), ())), preferred_element_type=jnp.float32
    )


def outer(left, right):
    return lax.dot_general(
        left, right, (((1,), (1,)), ((), ())), preferred_element_type=jnp.float32
    )


def unchanged(state):
    return state


def on_device_gathered(tokens, cotangent, attn_gain, w_qkv, w_out, mlp_gain, w_gate_up, w_down):
    tok_count = tokens.shape[2]
    groups = H // KVH
    factor = HD ** (-0.5)
    seq_length = tok_count * lax.axis_size(("ctx", "fsdp"))
    pos_first = lax.axis_index(("ctx", "fsdp")) * tok_count
    positions = pos_first + jnp.arange(tok_count, dtype=jnp.int32)
    pos_last = pos_first + tok_count - 1
    cosine, sine_table = tables(pos_first, tok_count, HD)
    sums = [
        jnp.zeros((D,), jnp.float32),
        jnp.zeros((D, (H + 2 * KVH) * HD), jnp.float32),
        jnp.zeros((H * HD, D), jnp.float32),
        jnp.zeros((D,), jnp.float32),
        jnp.zeros((D, 2 * FF), jnp.float32),
        jnp.zeros((FF, D), jnp.float32),
    ]
    outputs = []
    in_grads = []
    whole = (
        lax.all_gather(attn_gain, ("dp", "ctx", "fsdp"), axis=0, tiled=True),
        lax.all_gather(w_qkv, ("dp", "ctx", "fsdp"), axis=1, tiled=True),
        lax.all_gather(w_out, ("dp", "ctx", "fsdp"), axis=0, tiled=True),
        lax.all_gather(mlp_gain, ("dp", "ctx", "fsdp"), axis=0, tiled=True),
        lax.all_gather(w_gate_up, ("dp", "ctx", "fsdp"), axis=1, tiled=True),
        lax.all_gather(w_down, ("dp", "ctx", "fsdp"), axis=0, tiled=True),
    )
    for step_index in range(tokens.shape[0]):
        gain_one, mix_qkv, mix_out, gain_two, mix_gate_up, mix_down = whole
        inputs = tokens[step_index, 0].astype(jnp.float32)
        normed = rms_norm(inputs, gain_one.astype(jnp.float32)).astype(jnp.bfloat16)
        mixed = jnp.dot(normed, mix_qkv, preferred_element_type=jnp.float32)
        queries = rotate(mixed[:, : H * HD].reshape(tok_count, H, HD), cosine, sine_table).astype(
            jnp.bfloat16
        )
        key_rows = rotate(
            mixed[:, H * HD : (H + KVH) * HD].reshape(tok_count, KVH, HD), cosine, sine_table
        )
        key_rows = key_rows.astype(jnp.bfloat16).reshape(tok_count, KVH * HD)
        value_rows = mixed[:, (H + KVH) * HD :].astype(jnp.bfloat16)
        grouped = queries.reshape(tok_count, KVH, groups, HD)
        start_state = (
            jnp.full((KVH, groups, tok_count), NEG, jnp.float32),
            jnp.zeros((KVH, groups, tok_count), jnp.float32),
            jnp.zeros((KVH, groups, tok_count, HD), jnp.float32),
        )
        piece = (
            lax.all_gather(key_rows, ("ctx", "fsdp"), axis=0, tiled=True),
            lax.all_gather(value_rows, ("ctx", "fsdp"), axis=0, tiled=True),
        )

        def work(state):
            best, total, summed = state
            key_count = piece[0].shape[0]
            keys = piece[0].reshape(key_count, KVH, HD)
            values = piece[1].reshape(key_count, KVH, HD)
            scores = (
                jnp.einsum("qkgd,tkd->kgqt", grouped, keys, preferred_element_type=jnp.float32)
                * factor
            )
            allowed = jnp.arange(key_count, dtype=jnp.int32)[None, :] <= positions[:, None]
            scores = jnp.where(allowed, scores, NEG)
            new_best = jnp.maximum(best, jnp.max(scores, axis=-1))
            weights = jnp.where(allowed, jnp.exp(scores - new_best[..., None]), 0.0)
            total = jnp.sum(weights, axis=-1)
            summed = jnp.einsum(
                "kgqt,tkd->kgqd",
                weights.astype(jnp.bfloat16),
                values,
                preferred_element_type=jnp.float32,
            )
            return (new_best, total, summed)

        best, total, summed = lax.cond(jnp.int32(0) <= pos_last, work, unchanged, start_state)
        head_out = summed / total[..., None]
        log_total = best + jnp.log(total)
        attended = (
            jnp.transpose(head_out, (2, 0, 1, 3)).reshape(tok_count, H * HD).astype(jnp.bfloat16)
        )
        resid = inputs + jnp.dot(attended, mix_out, preferred_element_type=jnp.float32)
        normed_two = rms_norm(resid, gain_two.astype(jnp.float32)).astype(jnp.bfloat16)
        both = jnp.dot(normed_two, mix_gate_up, preferred_element_type=jnp.float32)
        acted = swiglu(both).astype(jnp.bfloat16)
        result = resid + jnp.dot(acted, mix_down, preferred_element_type=jnp.float32)
        outputs.append(result.astype(jnp.bfloat16))
        gain_one, mix_qkv, mix_out, gain_two, mix_gate_up, mix_down = whole
        up_low = cotangent[step_index, 0]
        upstream = up_low.astype(jnp.float32)
        sums[5] = sums[5] + inner(acted, up_low)
        d_act = outer(up_low, mix_down)
        _, pull_glu = jax.vjp(swiglu, both)
        d_both = pull_glu(d_act)[0].astype(jnp.bfloat16)
        sums[4] = sums[4] + inner(normed_two, d_both)
        d_normed_two = outer(d_both, mix_gate_up)
        _, pull_two = jax.vjp(rms_norm, resid, gain_two.astype(jnp.float32))
        d_resid_norm, d_gain_two = pull_two(d_normed_two)
        sums[3] = sums[3] + d_gain_two
        d_resid = upstream + d_resid_norm
        d_resid_low = d_resid.astype(jnp.bfloat16)
        sums[2] = sums[2] + inner(attended, d_resid_low)
        d_attended = outer(d_resid_low, mix_out).astype(jnp.bfloat16)
        d_grouped = d_attended.reshape(tok_count, KVH, groups, HD)
        delta = jnp.einsum("qkgd,kgqd->kgq", d_grouped.astype(jnp.float32), head_out)
        zero_q = jnp.zeros((tok_count, KVH, groups, HD), jnp.float32)
        back_state = (
            zero_q,
            jnp.zeros((seq_length, KVH * HD), jnp.float32),
            jnp.zeros((seq_length, KVH * HD), jnp.float32),
        )
        attend_piece = (
            lax.all_gather(key_rows, ("ctx", "fsdp"), axis=0, tiled=True),
            lax.all_gather(value_rows, ("ctx", "fsdp"), axis=0, tiled=True),
        )

        def attend_work(state):
            key_count = attend_piece[0].shape[0]
            keys = attend_piece[0].reshape(key_count, KVH, HD)
            values = attend_piece[1].reshape(key_count, KVH, HD)
            scores = (
                jnp.einsum("qkgd,tkd->kgqt", grouped, keys, preferred_element_type=jnp.float32)
                * factor
            )
            allowed = jnp.arange(key_count, dtype=jnp.int32)[None, :] <= positions[:, None]
            scores = jnp.where(allowed, scores, NEG)
            probs = jnp.where(allowed, jnp.exp(scores - log_total[..., None]), 0.0)
            d_probs = jnp.einsum(
                "qkgd,tkd->kgqt", d_grouped, values, preferred_element_type=jnp.float32
            )
            d_scores = (probs * (d_probs - delta[..., None])).astype(jnp.bfloat16)
            grad_q = jnp.einsum(
                "kgqt,tkd->qkgd", d_scores, keys, preferred_element_type=jnp.float32
            )
            piece_k = (
                jnp.einsum("kgqt,qkgd->tkd", d_scores, grouped, preferred_element_type=jnp.float32)
                * factor
            )
            piece_v = jnp.einsum(
                "kgqt,qkgd->tkd",
                probs.astype(jnp.bfloat16),
                d_grouped,
                preferred_element_type=jnp.float32,
            )
            grad_k = piece_k.reshape(key_count, KVH * HD)
            grad_v = piece_v.reshape(key_count, KVH * HD)
            return (grad_q, grad_k, grad_v)

        back_result = lax.cond(jnp.int32(0) <= pos_last, attend_work, unchanged, back_state)
        grad_q = back_result[0]
        summed_k, summed_v = side_by_side(
            (back_result[1].astype(jnp.bfloat16), back_result[2].astype(jnp.bfloat16)),
            ("ctx", "fsdp"),
            0,
            1,
        )
        d_q_raw = rotate(grad_q.reshape(tok_count, H, HD) * factor, cosine, -sine_table).reshape(
            tok_count, H * HD
        )
        d_k_raw = rotate(summed_k.reshape(tok_count, KVH, HD), cosine, -sine_table).reshape(
            tok_count, KVH * HD
        )
        d_mixed = jnp.concatenate([d_q_raw, d_k_raw, summed_v], axis=1).astype(jnp.bfloat16)
        sums[1] = sums[1] + inner(normed, d_mixed)
        d_normed = outer(d_mixed, mix_qkv)
        _, pull_one = jax.vjp(rms_norm, inputs, gain_one.astype(jnp.float32))
        d_inputs_norm, d_gain_one = pull_one(d_normed)
        sums[0] = sums[0] + d_gain_one
        in_grads.append((d_resid + d_inputs_norm).astype(jnp.bfloat16))
    grad_gain_one, grad_qkv, grad_out, grad_gain_two, grad_gate_up, grad_down = (
        lax.psum_scatter(sums[0], ("dp", "ctx", "fsdp"), scatter_dimension=0, tiled=True),
        lax.psum_scatter(sums[1], ("dp", "ctx", "fsdp"), scatter_dimension=1, tiled=True),
        lax.psum_scatter(sums[2], ("dp", "ctx", "fsdp"), scatter_dimension=0, tiled=True),
        lax.psum_scatter(sums[3], ("dp", "ctx", "fsdp"), scatter_dimension=0, tiled=True),
        lax.psum_scatter(sums[4], ("dp", "ctx", "fsdp"), scatter_dimension=1, tiled=True),
        lax.psum_scatter(sums[5], ("dp", "ctx", "fsdp"), scatter_dimension=0, tiled=True),
    )
    block_out = jnp.stack(outputs)[:, None]
    grad_tokens = jnp.stack(in_grads)[:, None]
    return (
        block_out,
        grad_tokens,
        grad_gain_one,
        grad_qkv,
        grad_out,
        grad_gain_two,
        grad_gate_up,
        grad_down,
    )


MESH = pl.DeviceIdType.MESH
VM = pltpu.VMEM
ANY = pl.ANY


def place():
    return lax.axis_index("dp"), lax.axis_index("ctx"), lax.axis_index("fsdp")


def at_device(dp, ctx, fs):
    return {"dp": dp, "ctx": ctx, "fsdp": fs}


def remote(src, dst, send, recv, device):
    return pltpu.make_async_remote_copy(
        src_ref=src, dst_ref=dst, send_sem=send, recv_sem=recv, device_id=device, device_id_type=MESH
    )


def arrived(dst, recv, device):
    remote(dst, dst, recv, recv, device).wait_recv()


def left(src, send, device):
    remote(src, src, send, send, device).wait_send()


def greet_all(sizes):
    dp, ctx, fs = sizes
    n = dp * ctx * fs
    d, c, f = place()
    me = (d * ctx + c) * fs + f
    barrier = pltpu.get_barrier_semaphore()

    def tell(step, carry):
        other = lax.rem(me + step, n)
        pl.semaphore_signal(
            barrier,
            inc=1,
            device_id=at_device(other // (ctx * fs), lax.rem(other // fs, ctx), lax.rem(other, fs)),
            device_id_type=MESH,
        )
        return carry

    lax.fori_loop(1, n, tell, 0)
    pl.semaphore_wait(barrier, n - 1)


class LineGather:
    def __init__(self, n, own, whole, send, recv, local):
        self.n, self.own, self.whole, self.send, self.recv, self.local = n, own, whole, send, recv, local
        self.d, self.c, self.f = place()

    def slot(self, at):
        return self.whole.at[self.d, at]

    def up(self, src, at):
        return remote(src, self.slot(at), self.send.at[0, at], self.recv.at[self.d, at], at_device(self.d, self.c + 1, self.f))

    def down(self, src, at):
        return remote(src, self.slot(at), self.send.at[1, at], self.recv.at[self.d, at], at_device(self.d, self.c - 1, self.f))

    def across(self, src, at):
        return remote(src, self.slot(at), self.send.at[2, at], self.recv.at[self.d, at], at_device(1 - self.d, self.c, self.f))

    def start(self):
        c = self.c

        @pl.when(c < self.n - 1)
        def _():
            self.up(self.own, c).start()

        @pl.when(c > 0)
        def _():
            self.down(self.own, c).start()

        self.across(self.own, c).start()
        pltpu.make_async_copy(self.own, self.slot(c), self.local).start()

    def forward(self, k):
        c = self.c

        @pl.when(c - k >= 0)
        def _():
            arrived(self.slot(c - k), self.recv.at[self.d, c - k], at_device(self.d, c, self.f))

            @pl.when(c < self.n - 1)
            def _():
                self.up(self.slot(c - k), c - k).start()

            self.across(self.slot(c - k), c - k).start()

        @pl.when(c + k < self.n)
        def _():
            arrived(self.slot(c + k), self.recv.at[self.d, c + k], at_device(self.d, c, self.f))

            @pl.when(c > 0)
            def _():
                self.down(self.slot(c + k), c + k).start()

            self.across(self.slot(c + k), c + k).start()

    def take(self, at):
        c = self.c

        @pl.when(at != c)
        def _():
            arrived(self.slot(at), self.recv.at[self.d, at], at_device(self.d, c, self.f))

            @pl.when(jnp.logical_and(at < c, c < self.n - 1))
            def _():
                self.up(self.slot(at), at).start()

            @pl.when(jnp.logical_and(at > c, c > 0))
            def _():
                self.down(self.slot(at), at).start()

            self.across(self.slot(at), at).start()

        self.other(at)

    def other(self, at):
        arrived(self.whole.at[1 - self.d, at], self.recv.at[1 - self.d, at], at_device(self.d, self.c, self.f))

    def finish_sends(self):
        c = self.c
        for at in range(self.n):

            @pl.when(jnp.logical_and(at <= c, c < self.n - 1))
            def _():
                left(self.slot(at), self.send.at[0, at], at_device(self.d, c, self.f))

            @pl.when(jnp.logical_and(at >= c, c > 0))
            def _():
                left(self.slot(at), self.send.at[1, at], at_device(self.d, c, self.f))

            left(self.slot(at), self.send.at[2, at], at_device(self.d, c, self.f))

    def finish(self):
        self.finish_sends()
        pltpu.make_async_copy(self.own, self.slot(self.c), self.local).wait()


FACTOR = HD ** (-0.5)
LANES = 128


def ordered(c, step, n):
    at = jnp.int32(0)
    for here in range(n):
        near = sorted(range(n), key=lambda place_: (abs(place_ - here), place_))
        for index, value in enumerate(near):
            at = jnp.where(jnp.logical_and(c == here, step == index), value, at)
    return at


def first_kernel(
    sizes, x_ref, gains_ref, w_ref, cos_ref, sin_up_ref, sin_down_ref, dy_ref, proj_ref, down_ref,
    normed_out, unit_out, att_out, wide_out, gains_out, dy_all, proj_all, down_all,
    x_all, w_all, wide, normed, stage, unit, att_stage, att, gain_all, gain_vec,
    line_send, line_recv, line_local, w_send, w_recv, w_pass, g_send, g_recv, u_send, u_recv, a_send, a_recv, out_sem,
    dy_send, dy_recv, dy_local, m_send, m_recv, m_pass,
):
    dp, ctx, fs = sizes
    n = dp * ctx * fs
    d, c, f = place()
    here = at_device(d, c, f)
    span = stage.shape[2]
    greet_all(sizes)

    q_core = f // 2
    kv_slot = 2 + c // 2
    kv_ctx = 2 * lax.rem(c, 2) + f // 2
    kv_core = lax.rem(f, 2)
    relay = f == 2 * lax.rem(c, 2) + d

    @pl.when(jnp.logical_and(d == 1, jnp.logical_or(kv_core != 1, kv_ctx != c)))
    def _():
        remote(w_ref, w_all.at[kv_slot], w_send.at[0], w_recv.at[kv_slot], at_device(kv_core, kv_ctx, f)).start()

    @pl.when(jnp.logical_and(d == 1, jnp.logical_and(kv_core == 1, kv_ctx == c)))
    def _():
        pltpu.make_async_copy(w_ref, w_all.at[kv_slot], w_recv.at[kv_slot]).start()

    line = LineGather(ctx, x_ref, x_all, line_send, line_recv, line_local)
    line.start()

    @pl.when(d == 0)
    def _():
        slot = lax.rem(f, 2)
        for to in range(fs):

            @pl.when(jnp.logical_or(q_core != 0, to != f))
            def _():
                remote(w_ref, w_all.at[slot], w_send.at[to], w_recv.at[slot], at_device(q_core, c, to)).start()

            @pl.when(jnp.logical_and(q_core == 0, to == f))
            def _():
                pltpu.make_async_copy(w_ref, w_all.at[slot], w_recv.at[slot]).start()

    me = (d * ctx + c) * fs + f

    def gain_to(step, carry):
        other = lax.rem(me + step, n)
        remote(
            gains_ref, gain_all.at[me], g_send.at[other], g_recv.at[me],
            at_device(other // (ctx * fs), lax.rem(other // fs, ctx), lax.rem(other, fs)),
        ).start()
        return carry

    lax.fori_loop(1, n, gain_to, 0)
    gain_all[me] = gains_ref[...]

    @pl.when(relay)
    def _():
        for slot in (2, 3):
            arrived(w_all.at[slot], w_recv.at[slot], here)
            for step in range(1, fs):
                to = lax.rem(f + step, fs)
                remote(w_all.at[slot], w_all.at[slot], w_pass.at[slot - 2, step], w_recv.at[slot], at_device(d, c, to)).start()

    def gain_from(step, carry):
        other = lax.rem(me + step, n)
        arrived(gain_all.at[other], g_recv.at[other], here)
        return carry

    lax.fori_loop(1, n, gain_from, 0)
    each = D // n
    for index in range(n):
        gain_vec[:, index * each : (index + 1) * each] = gain_all[index][:, :each]
    gain = gain_vec[0:1, :]

    wide[...] = jnp.zeros_like(wide)
    for slot in (0, 1, 2, 3):
        if slot < 2:
            arrived(w_all.at[slot], w_recv.at[slot], here)
        else:

            @pl.when(jnp.logical_not(relay))
            def _():
                arrived(w_all.at[slot], w_recv.at[slot], here)

        wide[:, slot * LANES : slot * LANES + HD] = w_all[slot]

    pltpu.make_async_copy(line.own, line.slot(c), line.local).wait()

    def block(step, carry):
        at = ordered(c, step, ctx)

        line.take(at)
        values = x_all[:, at].reshape(dp * 2 * span, D).astype(jnp.float32)
        scale = lax.rsqrt(jnp.mean(values * values, axis=-1, keepdims=True) + EPS)
        low = (values * scale * gain).astype(jnp.bfloat16)
        normed[:, at] = low.reshape(dp, 2 * span, D)
        heads = jnp.dot(low, wide[...], preferred_element_type=jnp.float32)
        cosine, sine_up, sine_down = cos_ref[at, f], sin_up_ref[at, f], sin_down_ref[at, f]
        for slot in range(4):
            head = heads[:, slot * LANES : (slot + 1) * LANES]
            if slot < 3:
                turned_up = pltpu.roll(head, HD // 2, 1).reshape(2 * dp, span, LANES)
                turned_down = pltpu.roll(head, LANES - HD // 2, 1).reshape(2 * dp, span, LANES)
                head = head.reshape(2 * dp, span, LANES)
                head = head * cosine[None] + turned_up * sine_up[None] + turned_down * sine_down[None]
            else:
                head = head.reshape(2 * dp, span, LANES)
            stage[at, :, :, slot * LANES : (slot + 1) * LANES] = head.astype(jnp.bfloat16)
        for to in range(2 * dp):

            @pl.when(to != f)
            def _():
                remote(stage.at[at, to], unit.at[at, f], u_send.at[at, to], u_recv.at[at, f], at_device(d, c, to)).start()

            @pl.when(to == f)
            def _():
                unit[at, f] = stage[at, to]

        return carry

    lax.fori_loop(0, ctx, block, 0)
    normed_copy = pltpu.make_async_copy(normed, normed_out, out_sem.at[0])
    wide_copy = pltpu.make_async_copy(wide, wide_out, out_sem.at[1])
    gains_copy = pltpu.make_async_copy(gain_vec, gains_out, out_sem.at[2])
    normed_copy.start()
    wide_copy.start()
    gains_copy.start()

    to_core, to_ctx = lax.rem(c, 2), 2 * d + c // 2
    stays = jnp.logical_and(to_core == d, to_ctx == c)
    moved = ((proj_ref, proj_all), (down_ref, down_all))
    for index, (shard, whole) in enumerate(moved):

        @pl.when(jnp.logical_not(stays))
        def _():
            remote(shard, whole.at[f], m_send.at[index], m_recv.at[index, f], at_device(to_core, to_ctx, f)).start()

        @pl.when(stays)
        def _():
            pltpu.make_async_copy(shard, whole.at[f], m_recv.at[index, f]).start()

    dy_line = LineGather(ctx, dy_ref, dy_all, dy_send, dy_recv, dy_local)
    dy_line.start()

    def pass_on():
        for index, (shard, whole) in enumerate(moved):
            arrived(whole.at[f], m_recv.at[index, f], here)
            for step in range(1, fs):
                to = lax.rem(f + step, fs)
                remote(whole.at[f], whole.at[f], m_pass.at[index, step], m_recv.at[index, f], at_device(d, c, to)).start()

    for at in range(ctx):
        for step in range(1, fs):
            other = lax.rem(f + step, fs)
            arrived(unit.at[at, other], u_recv.at[at, other], here)
    unit_copy = pltpu.make_async_copy(unit, unit_out, out_sem.at[3])
    unit_copy.start()

    rows = fs * span
    for at in range(ctx):
        keys = rows * (at + 1)
        k_rows = unit[0 : at + 1, :, :, 2 * LANES : 3 * LANES].reshape(keys, LANES)
        v_rows = unit[0 : at + 1, :, :, 3 * LANES : 4 * LANES].reshape(keys, LANES)
        allowed = lax.broadcasted_iota(jnp.int32, (rows, keys), 1) <= rows * at + lax.broadcasted_iota(
            jnp.int32, (rows, keys), 0
        )
        for head in range(2):
            q_rows = unit[at, :, :, head * LANES : (head + 1) * LANES].reshape(rows, LANES)
            scores = outer(q_rows, k_rows) * FACTOR
            scores = jnp.where(allowed, scores, NEG)
            best = jnp.max(scores, axis=-1, keepdims=True)
            weights = jnp.exp(scores - best)
            probs = weights / jnp.sum(weights, axis=-1, keepdims=True)
            mixed = jnp.dot(probs.astype(jnp.bfloat16), v_rows, preferred_element_type=jnp.float32)
            att_stage[at, :, :, head * LANES : (head + 1) * LANES] = mixed.astype(jnp.bfloat16).reshape(fs, span, LANES)
        for to in range(fs):

            @pl.when(to != f)
            def _():
                remote(
                    att_stage.at[at, to], att.at[f // 2, at, lax.rem(f, 2)], a_send.at[at, to], a_recv.at[f, at], at_device(d, c, to)
                ).start()

            @pl.when(to == f)
            def _():
                att[f // 2, at, lax.rem(f, 2)] = att_stage[at, to]

        if at == 0:
            pass_on()
        else:
            dy_line.forward(at)

    for at in range(ctx):
        for step in range(1, fs):
            other = lax.rem(f + step, fs)
            arrived(att.at[other // 2, at, lax.rem(other, 2)], a_recv.at[other, at], here)
    att_copy = pltpu.make_async_copy(att, att_out, out_sem.at[4])
    att_copy.start()

    for at in range(ctx):
        dy_line.other(at)
    dy_line.finish()
    for index, (shard, whole) in enumerate(moved):
        for step in range(1, fs):
            other = lax.rem(f + step, fs)
            arrived(whole.at[other], m_recv.at[index, other], here)
            left(whole.at[f], m_pass.at[index, step], here)

        @pl.when(jnp.logical_not(stays))
        def _():
            left(shard, m_send.at[index], here)

    line.finish_sends()
    for at in range(ctx):

        for to in range(fs):

            @pl.when(to != f)
            def _():
                left(stage.at[at, to], u_send.at[at, to], here)
                left(att_stage.at[at, to], a_send.at[at, to], here)

    @pl.when(jnp.logical_and(d == 1, jnp.logical_or(kv_core != 1, kv_ctx != c)))
    def _():
        left(w_ref, w_send.at[0], here)

    @pl.when(d == 0)
    def _():
        for to in range(fs):

            @pl.when(jnp.logical_or(q_core != 0, to != f))
            def _():
                left(w_ref, w_send.at[to], here)

    @pl.when(relay)
    def _():
        for slot in (2, 3):
            for step in range(1, fs):
                left(w_all.at[slot], w_pass.at[slot - 2, step], here)

    def gain_left(step, carry):
        other = lax.rem(me + step, n)
        left(gains_ref, g_send.at[other], here)
        return carry

    lax.fori_loop(1, n, gain_left, 0)
    for copy in (normed_copy, wide_copy, gains_copy, unit_copy, att_copy):
        copy.wait()


def first(sizes, x, gains, w_qkv, cosine, sine_up, sine_down, dy, w_out, w_down):
    dp, ctx, fs = sizes
    n = dp * ctx * fs
    rows = x.shape[0]
    span = rows // 2
    low, wide_t = jnp.bfloat16, jnp.float32
    dma = pltpu.SemaphoreType.DMA
    shapes = (
        jax.ShapeDtypeStruct((dp, ctx, rows, D), low),
        jax.ShapeDtypeStruct((ctx, fs, span, 4 * LANES), low),
        jax.ShapeDtypeStruct((dp, ctx, 2, span, 2 * LANES), low),
        jax.ShapeDtypeStruct((D, 4 * LANES), low),
        jax.ShapeDtypeStruct((8, D), wide_t),
        jax.ShapeDtypeStruct((dp, ctx, rows, D), low),
        jax.ShapeDtypeStruct((fs,) + w_out.shape, low),
        jax.ShapeDtypeStruct((fs,) + w_down.shape, low),
    )
    any_spec, vm_spec = pl.BlockSpec(memory_space=ANY), pl.BlockSpec(memory_space=VM)
    return pl.pallas_call(
        functools.partial(first_kernel, sizes),
        name="first",
        out_shape=shapes,
        in_specs=[vm_spec, vm_spec, any_spec, vm_spec, vm_spec, vm_spec, vm_spec, any_spec, any_spec],
        out_specs=[any_spec] * 8,
        scratch_shapes=[
            VM((dp, ctx, rows, D), low),
            VM((4, D, HD), low),
            VM((D, 4 * LANES), low),
            VM((dp, ctx, rows, D), low),
            VM((ctx, 2 * dp, span, 4 * LANES), low),
            VM((ctx, fs, span, 4 * LANES), low),
            VM((ctx, fs, span, 2 * LANES), low),
            VM((dp, ctx, 2, span, 2 * LANES), low),
            VM((n, 8, LANES), wide_t),
            VM((8, D), wide_t),
            dma((3, ctx)), dma((dp, ctx)), dma,
            dma((fs,)), dma((4,)), dma((2, fs)),
            dma((n,)), dma((n,)),
            dma((ctx, 2 * dp)), dma((ctx, fs)),
            dma((ctx, fs)), dma((fs, ctx)),
            dma((5,)),
            dma((3, ctx)), dma((dp, ctx)), dma,
            dma((2,)), dma((2, fs)), dma((2, fs)),
        ],
        compiler_params=pltpu.CompilerParams(collective_id=1, has_side_effects=True, vmem_limit_bytes=60 * 1024 * 1024),
    )(x, gains, w_qkv, cosine, sine_up, sine_down, dy, w_out, w_down)


def angle_tables(ctx, fs, span):
    return lane_tables(jnp.arange(ctx * fs * span, dtype=jnp.int32).reshape(ctx, fs, span))


def lane_tables(positions):
    lane = jnp.arange(LANES, dtype=jnp.int32)
    pair = (lane % (HD // 2)).astype(jnp.float32)
    frequency = THETA ** (-(pair * 2.0) / HD)
    angles = positions.astype(jnp.float32)[..., None] * frequency
    inside = lane < HD
    low_half = lane < HD // 2
    cosine = jnp.where(inside, jnp.cos(angles), 0.0)
    sine = jnp.sin(angles)
    sine_up = jnp.where(jnp.logical_and(inside, jnp.logical_not(low_half)), sine, 0.0)
    sine_down = jnp.where(low_half, -sine, 0.0)
    return cosine, sine_up, sine_down


class LineSum:
    def __init__(self, n, mine, out_core, in_core, out_line, in_line, total, sems):
        self.n, self.mine, self.out_core, self.in_core = n, mine, out_core, in_core
        self.out_line, self.in_line, self.total = out_line, in_line, total
        self.core_send, self.core_recv, self.line_send, self.line_recv = sems
        self.d, self.c, self.f = place()
        self.here = at_device(self.d, self.c, self.f)

    def give(self, at, both):
        d = self.d
        low = both.astype(jnp.bfloat16)

        @pl.when(d == 0)
        def _():
            self.mine[at] = low[0]
            self.out_core[at] = low[1]

        @pl.when(d != 0)
        def _():
            self.mine[at] = low[1]
            self.out_core[at] = low[0]

        remote(
            self.out_core.at[at], self.in_core.at[at], self.core_send.at[at], self.core_recv.at[at], at_device(1 - d, self.c, self.f)
        ).start()

    def step(self, at):
        n, d, c, f = self.n, self.d, self.c, self.f
        arrived(self.in_core.at[at], self.core_recv.at[at], self.here)
        self.total[...] = self.mine[at].astype(jnp.float32) + self.in_core[at].astype(jnp.float32)

        @pl.when(jnp.logical_and(at <= c, c < n - 1))
        def _():
            arrived(self.in_line.at[0, at], self.line_recv.at[0, at], self.here)
            self.total[...] += self.in_line[0, at].astype(jnp.float32)

        @pl.when(jnp.logical_and(at >= c, c > 0))
        def _():
            arrived(self.in_line.at[1, at], self.line_recv.at[1, at], self.here)
            self.total[...] += self.in_line[1, at].astype(jnp.float32)

        @pl.when(at != c)
        def _():
            self.out_line[at] = self.total[...].astype(jnp.bfloat16)

        @pl.when(at < c)
        def _():
            remote(
                self.out_line.at[at], self.in_line.at[0, at], self.line_send.at[at], self.line_recv.at[0, at], at_device(d, c - 1, f)
            ).start()

        @pl.when(at > c)
        def _():
            remote(
                self.out_line.at[at], self.in_line.at[1, at], self.line_send.at[at], self.line_recv.at[1, at], at_device(d, c + 1, f)
            ).start()

    def finish(self):
        for at in range(self.n):
            left(self.out_core.at[at], self.core_send.at[at], self.here)

            @pl.when(at != self.c)
            def _():
                left(self.out_line.at[at], self.line_send.at[at], self.here)

    @staticmethod
    def scratch(ctx, rows):
        low = jnp.bfloat16
        dma = pltpu.SemaphoreType.DMA
        return [
            VM((ctx, rows, D), low), VM((ctx, rows, D), low), VM((ctx, rows, D), low), VM((ctx, rows, D), low),
            VM((2, ctx, rows, D), low), VM((rows, D), jnp.float32),
            dma((ctx,)), dma((ctx,)), dma((ctx,)), dma((2, ctx)),
        ]


def greet_near(sizes):
    dp, ctx, fs = sizes
    d, c, f = place()
    barrier = pltpu.get_barrier_semaphore()

    def tell(device):
        pl.semaphore_signal(barrier, inc=1, device_id=device, device_id_type=MESH)

    tell(at_device(1 - d, c, f))
    for step in range(1, fs):
        for core in range(dp):
            tell(at_device(core, c, lax.rem(f + step, fs)))

    @pl.when(c > 0)
    def _():
        tell(at_device(d, c - 1, f))

    @pl.when(c < ctx - 1)
    def _():
        tell(at_device(d, c + 1, f))

    known = 1 + dp * (fs - 1)
    ends = jnp.logical_or(c == 0, c == ctx - 1)

    @pl.when(ends)
    def _():
        pl.semaphore_wait(barrier, known + 1)

    @pl.when(jnp.logical_not(ends))
    def _():
        pl.semaphore_wait(barrier, known + 2)


def middle_kernel(
    sizes, hidden, att_ref, x_ref, dy_ref, gains_ref, proj_ref, down_ref, gate_up_ref, dy_all_ref,
    resid_out, d_resid_out, gain_out, partial_out, unit_out, grad_up_out, grad_down_out, grad_proj_out,
    att, dy_all, proj, down, gate_up, resid, own_two, normed_two, act, d_both, part_stage, own_d, d_resid_all, d_stage, unit,
    grad_up, grad_down, grad_proj, grad_proj_low,
    in_sem, gu_send, gu_recv, two_send, two_recv, two_local, dr_send, dr_recv, dr_local, u_send, u_recv, out_sem, part_sem,
    *sums,
):
    dp, ctx, fs = sizes
    d, c, f = place()
    here = at_device(d, c, f)
    rows = x_ref.shape[0]
    span = rows // 2
    both_rows = dp * rows
    half = hidden // 2
    line_sum = LineSum(ctx, *sums[:6], sums[6:10])
    second_sum = LineSum(ctx, *sums[10:16], sums[16:20])

    att_copy = pltpu.make_async_copy(att_ref, att, in_sem.at[0])
    dy_copy = pltpu.make_async_copy(dy_all_ref, dy_all, in_sem.at[1])
    down_copy = pltpu.make_async_copy(down_ref, down, in_sem.at[2])
    att_copy.start()
    proj[...] = jnp.zeros_like(proj)
    each = proj_ref.shape[1]
    proj_copies = []
    for slot in range(fs):
        start = slot // 2 * LANES + slot % 2 * each
        proj_copies.append(pltpu.make_async_copy(proj_ref.at[slot], proj.at[start : start + each], in_sem.at[3 + slot]))
        proj_copies[-1].start()
    dy_copy.start()
    down_copy.start()
    greet_near(sizes)

    to_core = f // 2
    gu_slot = 2 * d + lax.rem(f, 2)
    for to in range(fs):
        own_place = jnp.logical_and(to_core == d, f == to)

        @pl.when(jnp.logical_not(own_place))
        def _():
            remote(gate_up_ref, gate_up.at[gu_slot], gu_send.at[to], gu_recv.at[gu_slot], at_device(to_core, c, to)).start()

        @pl.when(own_place)
        def _():
            pltpu.make_async_copy(gate_up_ref, gate_up.at[gu_slot], gu_recv.at[gu_slot]).start()

    att_copy.wait()
    for copy in proj_copies:
        copy.wait()

    def project(step, carry):
        at = ordered(c, ctx - 1 - step, ctx)
        terms = jnp.dot(att[:, at].reshape(both_rows, 2 * LANES), proj[...], preferred_element_type=jnp.float32)
        line_sum.give(at, terms.reshape(dp, rows, D))
        return carry

    lax.fori_loop(0, ctx, project, 0)

    def sum_up(step, carry):
        line_sum.step(ordered(c, ctx - 1 - step, ctx))
        return carry

    lax.fori_loop(0, ctx, sum_up, 0)
    gain = gains_ref[1:2, :]
    values = x_ref[...].astype(jnp.float32) + line_sum.total[...]
    resid[...] = values
    scale = lax.rsqrt(jnp.mean(values * values, axis=-1, keepdims=True) + EPS)
    own_two[...] = (values * scale * gain).astype(jnp.bfloat16)
    resid_copy = pltpu.make_async_copy(resid, resid_out, out_sem.at[0])
    resid_copy.start()
    line = LineGather(ctx, own_two, normed_two, two_send, two_recv, two_local)
    line.start()
    line_sum.finish()
    for slot in range(4):
        arrived(gate_up.at[slot], gu_recv.at[slot], here)
    dy_copy.wait()
    down_copy.wait()
    pltpu.make_async_copy(line.own, line.slot(c), line.local).wait()

    def mlp(step, carry):
        at = ordered(c, step, ctx)

        line.take(at)
        inputs = normed_two[:, at].reshape(both_rows, D)
        dy_rows = dy_all[:, at].reshape(both_rows, D)
        for part in range(2):
            cols = slice(part * half, (part + 1) * half)
            gate = jnp.dot(inputs, gate_up[part], preferred_element_type=jnp.float32)
            up = jnp.dot(inputs, gate_up[2 + part], preferred_element_type=jnp.float32)
            d_act = outer(dy_rows, down[cols, :])
            sig = 1.0 / (1.0 + jnp.exp(-gate))
            silu = gate * sig
            act[:, at, :, cols] = (silu * up).astype(jnp.bfloat16).reshape(dp, rows, half)
            d_gate = d_act * up * (sig * (1.0 + gate * (1.0 - sig)))
            d_both[:, at, :, cols] = d_gate.astype(jnp.bfloat16).reshape(dp, rows, half)
            d_both[:, at, :, hidden + part * half : hidden + (part + 1) * half] = (
                (d_act * silu).astype(jnp.bfloat16).reshape(dp, rows, half)
            )
        terms = outer(d_both[:, at, :, 0:half].reshape(both_rows, half), gate_up[0])
        for part in range(1, 4):
            terms += outer(d_both[:, at, :, part * half : (part + 1) * half].reshape(both_rows, half), gate_up[part])
        second_sum.give(at, terms.reshape(dp, rows, D))
        return carry

    lax.fori_loop(0, ctx, mlp, 0)

    wide_rows = D // ctx

    def grads(step):
        first = pl.multiple_of(step * wide_rows, LANES)
        left_rows = normed_two[:, :, :, pl.ds(first, wide_rows)].reshape(dp * ctx * rows, wide_rows)
        for part in range(2):
            cols = slice(part * hidden, (part + 1) * hidden)
            terms = inner(left_rows, d_both[:, :, :, cols].reshape(dp * ctx * rows, hidden)).astype(jnp.bfloat16)
            grad_up[2 * part, pl.ds(first, wide_rows), :] = terms[:, :half]
            grad_up[2 * part + 1, pl.ds(first, wide_rows), :] = terms[:, half:]
        dy_cols = dy_all[:, :, :, pl.ds(first, wide_rows)].reshape(dp * ctx * rows, wide_rows)
        grad_down[:, pl.ds(first, wide_rows)] = inner(act[...].reshape(dp * ctx * rows, hidden), dy_cols).astype(jnp.bfloat16)

    def sum_two(step, carry):
        second_sum.step(ordered(c, ctx - 1 - step, ctx))

        @pl.when(step < ctx - 1)
        def _():
            grads(step)

        return carry

    lax.fori_loop(0, ctx, sum_two, 0)
    values = resid[...]
    scale = lax.rsqrt(jnp.mean(values * values, axis=-1, keepdims=True) + EPS)
    incoming = second_sum.total[...]
    weighted = incoming * gain
    mean = jnp.mean(weighted * values, axis=-1, keepdims=True)
    d_resid = dy_ref[...].astype(jnp.float32) + scale * weighted - values * (scale * scale * scale) * mean
    own_d[...] = d_resid.astype(jnp.bfloat16)
    d_resid_out[...] = d_resid
    gain_out[...] = jnp.broadcast_to(jnp.sum(incoming * values * scale, axis=0, keepdims=True), gain_out.shape)
    d_line = LineGather(ctx, own_d, d_resid_all, dr_send, dr_recv, dr_local)
    d_line.start()
    line.finish_sends()
    second_sum.finish()
    grads(ctx - 1)
    grad_up_copy = pltpu.make_async_copy(grad_up, grad_up_out, out_sem.at[1])
    grad_down_copy = pltpu.make_async_copy(grad_down, grad_down_out, out_sem.at[2])
    grad_up_copy.start()
    grad_down_copy.start()
    pltpu.make_async_copy(d_line.own, d_line.slot(c), d_line.local).wait()
    grad_proj[...] = jnp.zeros_like(grad_proj)

    def back(step, carry):
        at = ordered(c, step, ctx)

        d_line.take(at)
        incoming = d_resid_all[:, at].reshape(both_rows, D)
        d_att = outer(incoming, proj[...]).astype(jnp.bfloat16)
        d_stage[at] = d_att.reshape(2 * dp, span, 2 * LANES)
        for to in range(2 * dp):

            @pl.when(to != f)
            def _():
                remote(d_stage.at[at, to], unit.at[at, f], u_send.at[at, to], u_recv.at[at, f], at_device(d, c, to)).start()

            @pl.when(to == f)
            def _():
                unit[at, f] = d_stage[at, to]

        grad_proj[...] += inner(att[:, at].reshape(both_rows, 2 * LANES), incoming)

        outputs = jnp.dot(act[:, at].reshape(both_rows, hidden), down[...], preferred_element_type=jnp.float32)
        slot = lax.rem(step, 2)

        @pl.when(step >= 2)
        def _():
            pltpu.make_async_copy(part_stage.at[slot], partial_out.at[:, at], part_sem.at[slot]).wait()

        part_stage[slot] = outputs.reshape(dp, rows, D).astype(jnp.bfloat16)
        pltpu.make_async_copy(part_stage.at[slot], partial_out.at[:, at], part_sem.at[slot]).start()
        return carry

    lax.fori_loop(0, ctx, back, 0)
    for slot in range(fs):
        start = slot // 2 * LANES + slot % 2 * each
        grad_proj_low[slot] = grad_proj[start : start + each, :].astype(jnp.bfloat16)
    grad_proj_copy = pltpu.make_async_copy(grad_proj_low, grad_proj_out, out_sem.at[3])
    grad_proj_copy.start()
    for at in range(ctx):
        for step in range(1, fs):
            other = lax.rem(f + step, fs)
            arrived(unit.at[at, other], u_recv.at[at, other], here)
    unit_copy = pltpu.make_async_copy(unit, unit_out, out_sem.at[4])
    unit_copy.start()
    d_line.finish_sends()
    for at in range(ctx):
        for to in range(fs):

            @pl.when(to != f)
            def _():
                left(d_stage.at[at, to], u_send.at[at, to], here)

    for to in range(fs):

        @pl.when(jnp.logical_not(jnp.logical_and(to_core == d, f == to)))
        def _():
            left(gate_up_ref, gu_send.at[to], here)

    for slot in range(2):
        pltpu.make_async_copy(part_stage.at[slot], partial_out.at[:, 0], part_sem.at[slot]).wait()
    for copy in (resid_copy, grad_up_copy, grad_down_copy, grad_proj_copy, unit_copy):
        copy.wait()


def middle(sizes, att, x, dy, gains, proj, down, w_gate_up, dy_all):
    dp, ctx, fs = sizes
    rows = x.shape[0]
    span = rows // 2
    hidden = FF // (dp * ctx)
    low, wide_t = jnp.bfloat16, jnp.float32
    dma = pltpu.SemaphoreType.DMA
    any_spec, vm_spec = pl.BlockSpec(memory_space=ANY), pl.BlockSpec(memory_space=VM)
    shapes = (
        jax.ShapeDtypeStruct((rows, D), wide_t),
        jax.ShapeDtypeStruct((rows, D), wide_t),
        jax.ShapeDtypeStruct((8, D), wide_t),
        jax.ShapeDtypeStruct((dp, ctx, rows, D), low),
        jax.ShapeDtypeStruct((ctx, fs, span, 2 * LANES), low),
        jax.ShapeDtypeStruct((4, D, hidden // 2), low),
        jax.ShapeDtypeStruct((hidden, D), low),
        jax.ShapeDtypeStruct(proj.shape, low),
    )
    return pl.pallas_call(
        functools.partial(middle_kernel, sizes, hidden),
        name="middle",
        out_shape=shapes,
        in_specs=[any_spec, vm_spec, vm_spec, vm_spec, any_spec, any_spec, any_spec, any_spec],
        out_specs=[any_spec, vm_spec, vm_spec] + [any_spec] * 5,
        scratch_shapes=[
            VM((dp, ctx, rows, 2 * LANES), low),
            VM((dp, ctx, rows, D), low),
            VM((2 * LANES, D), low),
            VM((hidden, D), low),
            VM((4, D, hidden // 2), low),
            VM((rows, D), wide_t),
            VM((rows, D), low),
            VM((dp, ctx, rows, D), low),
            VM((dp, ctx, rows, hidden), low),
            VM((dp, ctx, rows, 2 * hidden), low),
            VM((2, dp, rows, D), low),
            VM((rows, D), low),
            VM((dp, ctx, rows, D), low),
            VM((ctx, 2 * dp, span, 2 * LANES), low),
            VM((ctx, fs, span, 2 * LANES), low),
            VM((4, D, hidden // 2), low),
            VM((hidden, D), low),
            VM((2 * LANES, D), wide_t),
            VM(proj.shape, low),
            dma((3 + fs,)), dma((fs,)), dma((4,)),
            dma((3, ctx)), dma((dp, ctx)), dma,
            dma((3, ctx)), dma((dp, ctx)), dma,
            dma((ctx, 2 * dp)), dma((ctx, fs)),
            dma((5,)), dma((2,)),
        ] + LineSum.scratch(ctx, rows) + LineSum.scratch(ctx, rows),
        compiler_params=pltpu.CompilerParams(collective_id=2, has_side_effects=True, vmem_limit_bytes=63 * 1024 * 1024),
    )(att, x, dy, gains, proj, down.reshape(hidden, D), w_gate_up, dy_all)


def last_kernel(
    sizes, x_ref, gains_ref, cos_ref, sin_up_ref, sin_down_ref, resid_ref, d_resid_ref, gain_two_ref,
    unit_ref, d_unit_ref, normed_ref, wide_ref, partial_ref, up_ref, down_ref, proj_ref,
    out_ref, d_x_ref, gains_out, qkv_out, proj_out, up_out, down_out,
    unit, d_unit, d_k, d_v, stage, mixed, normed, wide, grad_wide, grad_heads,
    up_land, down_land, proj_land, q_land, kv_land, down_sum, proj_sum, kv_sum, down_last, proj_last, kv_last, gain_vec, gain_stage, gain_land,
    in_sem, up_send, up_recv, down_send, down_recv, proj_send, proj_recv, head_send, head_recv, move_send, move_recv,
    u_send, u_recv, g_send, g_recv, mine_sem,
    *sums,
):
    dp, ctx, fs = sizes
    n = dp * ctx * fs
    d, c, f = place()
    here = at_device(d, c, f)
    me = (d * ctx + c) * fs + f
    rows = x_ref.shape[0]
    span = rows // 2
    both_rows = dp * rows
    low, wide_t = jnp.bfloat16, jnp.float32
    loads = [
        pltpu.make_async_copy(src, dst, in_sem.at[index])
        for index, (src, dst) in enumerate(((unit_ref, unit), (d_unit_ref, d_unit), (normed_ref, normed), (wide_ref, wide)))
    ]
    for load in loads:
        load.start()
    out_sum = LineSum(ctx, *sums[:6], sums[6:10])
    in_sum = LineSum(ctx, *sums[10:16], sums[16:20])
    for at in range(ctx):
        pltpu.make_async_copy(partial_ref.at[d, at], out_sum.mine.at[at], mine_sem.at[at]).start()
    greet_all(sizes)

    for at in range(ctx):
        remote(
            partial_ref.at[1 - d, at], out_sum.in_core.at[at], out_sum.core_send.at[at], out_sum.core_recv.at[at], at_device(1 - d, c, f)
        ).start()

    def push(src, land, send, recv, core, fs_to):
        to_self = jnp.logical_and(core == d, fs_to == f)

        @pl.when(jnp.logical_not(to_self))
        def _():
            remote(src, land.at[f], send, recv.at[f], at_device(core, c, fs_to)).start()

        @pl.when(to_self)
        def _():
            pltpu.make_async_copy(src, land.at[f], recv.at[f]).start()

    def pushed(src, send, core, fs_to):
        @pl.when(jnp.logical_not(jnp.logical_and(core == d, fs_to == f)))
        def _():
            left(src, send, here)

    def push_down():
        for slot in range(fs):
            push(down_ref.at[slot], down_land, down_send.at[slot], down_recv, d, slot)
            push(proj_ref.at[slot], proj_land, proj_send.at[slot], proj_recv, d, slot)

    def push_up():
        for slot in range(4):
            push(up_ref.at[slot], up_land, up_send.at[slot], up_recv, slot // 2, 2 * d + slot % 2)

    push_up()
    push_down()
    loads[0].wait()
    loads[1].wait()
    d_k[...] = jnp.zeros_like(d_k)
    d_v[...] = jnp.zeros_like(d_v)
    block = fs * span

    def unturn(values, at):
        up = pltpu.roll(values, HD // 2, 1).reshape(fs, span, LANES)
        down = pltpu.roll(values, LANES - HD // 2, 1).reshape(fs, span, LANES)
        return values.reshape(fs, span, LANES) * cos_ref[at] - up * sin_up_ref[at] - down * sin_down_ref[at]

    for at in reversed(range(ctx)):
        keys = block * (at + 1)
        k_rows = unit[0 : at + 1, :, :, 2 * LANES : 3 * LANES].reshape(keys, LANES)
        v_rows = unit[0 : at + 1, :, :, 3 * LANES : 4 * LANES].reshape(keys, LANES)
        allowed = lax.broadcasted_iota(jnp.int32, (block, keys), 1) <= block * at + lax.broadcasted_iota(
            jnp.int32, (block, keys), 0
        )
        for head in range(2):
            lanes = slice(head * LANES, (head + 1) * LANES)
            q_rows = unit[at, :, :, lanes].reshape(block, LANES)
            d_rows = d_unit[at, :, :, lanes].reshape(block, LANES)
            scores = jnp.where(allowed, outer(q_rows, k_rows) * FACTOR, NEG)
            weights = jnp.exp(scores - jnp.max(scores, axis=-1, keepdims=True))
            probs = weights / jnp.sum(weights, axis=-1, keepdims=True)
            d_probs = outer(d_rows, v_rows)
            delta = jnp.sum(probs * d_probs, axis=-1, keepdims=True)
            d_scores = (probs * (d_probs - delta)).astype(low)
            d_q = jnp.dot(d_scores, k_rows, preferred_element_type=wide_t) * FACTOR
            stage[at, :, :, lanes] = unturn(d_q, at).astype(low)
            d_k[0:keys, :] += inner(d_scores, q_rows) * FACTOR
            d_v[0:keys, :] += inner(probs.astype(low), d_rows)
        stage[at, :, :, 2 * LANES : 3 * LANES] = unturn(d_k[block * at : keys, :], at).astype(low)
        stage[at, :, :, 3 * LANES : 4 * LANES] = d_v[block * at : keys, :].astype(low).reshape(fs, span, LANES)
        for to in range(fs):

            @pl.when(to != f)
            def _():
                remote(
                    stage.at[at, to], mixed.at[f // 2, at, lax.rem(f, 2)], u_send.at[at, to], u_recv.at[f, at], at_device(d, c, to)
                ).start()

            @pl.when(to == f)
            def _():
                mixed[f // 2, at, lax.rem(f, 2)] = stage[at, to]

    loads[2].wait()
    loads[3].wait()

    def give(step, carry):
        at = ordered(c, ctx - 1 - step, ctx)
        for move in range(1, fs):
            other = lax.rem(f + move, fs)
            arrived(mixed.at[other // 2, at, lax.rem(other, 2)], u_recv.at[other, at], here)
        terms = outer(mixed[:, at].reshape(both_rows, 4 * LANES), wide[...])
        in_sum.give(at, terms.reshape(dp, rows, D))
        return carry

    lax.fori_loop(0, ctx, give, 0)

    every = dp * ctx * rows
    quarter = D // ctx

    def grads(step, carry):
        first_row = pl.multiple_of(step * quarter, LANES)
        rows_of = normed[:, :, :, pl.ds(first_row, quarter)].reshape(every, quarter)
        grad_wide[pl.ds(first_row, quarter), :] = inner(rows_of, mixed[...].reshape(every, 4 * LANES)).astype(low)
        return carry

    relay_f = 2 * lax.rem(c, 2) + d

    def push_heads():
        for slot in range(4):
            grad_heads[slot] = grad_wide[:, slot * LANES : slot * LANES + HD]
        for slot in range(2):
            push(grad_heads.at[slot], q_land, head_send.at[slot], head_recv.at[0], 0, 2 * d + slot)
        for slot in range(2):
            push(grad_heads.at[2 + slot], kv_land.at[slot], head_send.at[2 + slot], head_recv.at[1 + slot], d, relay_f)

    def out_step(step, carry):
        at = ordered(c, ctx - 1 - step, ctx)
        pltpu.make_async_copy(partial_ref.at[d, at], out_sum.mine.at[at], mine_sem.at[at]).wait()
        out_sum.step(at)
        return carry

    lax.fori_loop(0, ctx, out_step, 0)
    out_ref[...] = (resid_ref[...] + out_sum.total[...]).astype(low)
    in_sum.step(ordered(c, ctx - 1, ctx))
    lax.fori_loop(0, ctx, grads, 0)
    push_heads()

    def in_step(step, carry):
        in_sum.step(ordered(c, ctx - 1 - step, ctx))
        return carry

    lax.fori_loop(1, ctx - 1, in_step, 0)

    def sum_of(land):
        total = land[0].astype(wide_t)
        for source in range(1, fs):
            total += land[source].astype(wide_t)
        return total

    for source in range(fs):
        arrived(down_land.at[source], down_recv.at[source], here)
        arrived(proj_land.at[source], proj_recv.at[source], here)
    down_sum[...] = sum_of(down_land).astype(low)
    proj_sum[...] = sum_of(proj_land).astype(low)
    own_core, own_ctx = c // 2, 2 * lax.rem(c, 2) + d
    stays = jnp.logical_and(own_core == d, own_ctx == c)
    moves = ((down_sum, down_last), (proj_sum, proj_last))
    for index, (src, dst) in enumerate(moves):

        @pl.when(jnp.logical_not(stays))
        def _():
            remote(src, dst, move_send.at[index], move_recv.at[index], at_device(own_core, own_ctx, f)).start()

        @pl.when(stays)
        def _():
            pltpu.make_async_copy(src, dst, move_recv.at[index]).start()

    in_sum.step(c)

    gain = gains_ref[0:1, :]
    values = x_ref[...].astype(wide_t)
    scale = lax.rsqrt(jnp.mean(values * values, axis=-1, keepdims=True) + EPS)
    incoming = in_sum.total[...]
    weighted = incoming * gain
    mean = jnp.mean(weighted * values, axis=-1, keepdims=True)
    d_x_ref[...] = (d_resid_ref[...] + scale * weighted - values * (scale * scale * scale) * mean).astype(low)
    gain_vec[0:1, :] = jnp.sum(incoming * values * scale, axis=0, keepdims=True)
    gain_vec[1:2, :] = gain_two_ref[0:1, :]
    each = D // n
    for index in range(n):
        gain_stage[index, :, 0:each] = gain_vec[:, index * each : (index + 1) * each]
    gain_land[me] = gain_stage[me]

    def gain_to(step, carry):
        other = lax.rem(me + step, n)
        remote(
            gain_stage.at[other], gain_land.at[me], g_send.at[other], g_recv.at[me],
            at_device(other // (ctx * fs), lax.rem(other // fs, ctx), lax.rem(other, fs)),
        ).start()
        return carry

    lax.fori_loop(1, n, gain_to, 0)

    for slot in range(2):
        owner = slot * 2 + c // 2

        @pl.when(f == relay_f)
        def _():
            for source in range(fs):
                arrived(kv_land.at[slot, source], head_recv.at[1 + slot, source], here)
            kv_sum[slot] = sum_of(kv_land.at[slot]).astype(low)
            away = jnp.logical_or(d != 1, owner != c)

            @pl.when(away)
            def _():
                remote(kv_sum.at[slot], kv_last, move_send.at[2 + slot], move_recv.at[2], at_device(1, owner, f)).start()

            @pl.when(jnp.logical_not(away))
            def _():
                pltpu.make_async_copy(kv_sum.at[slot], kv_last, move_recv.at[2]).start()

    for source in range(fs):
        arrived(up_land.at[source], up_recv.at[source], here)
    up_out[...] = sum_of(up_land)
    for index, (src, dst) in enumerate(moves):
        arrived(dst, move_recv.at[index], here)
    down_out[...] = down_last[...].astype(wide_t)
    proj_out[...] = proj_last[...].astype(wide_t)

    @pl.when(d == 0)
    def _():
        for source in range(fs):
            arrived(q_land.at[source], head_recv.at[0, source], here)
        qkv_out[...] = sum_of(q_land)

    @pl.when(d == 1)
    def _():
        arrived(kv_last, move_recv.at[2], here)
        qkv_out[...] = kv_last[...].astype(wide_t)

    def gain_from(step, carry):
        other = lax.rem(me + step, n)
        arrived(gain_land.at[other], g_recv.at[other], here)
        return carry

    lax.fori_loop(1, n, gain_from, 0)
    total = gain_land[0]
    for index in range(1, n):
        total += gain_land[index]
    gains_out[...] = total

    for slot in range(4):
        pushed(up_ref.at[slot], up_send.at[slot], slot // 2, 2 * d + slot % 2)
        pushed(down_ref.at[slot], down_send.at[slot], d, slot)
        pushed(proj_ref.at[slot], proj_send.at[slot], d, slot)
    for slot in range(2):
        pushed(grad_heads.at[slot], head_send.at[slot], 0, 2 * d + slot)
        pushed(grad_heads.at[2 + slot], head_send.at[2 + slot], d, relay_f)
        owner = slot * 2 + c // 2

        @pl.when(jnp.logical_and(f == relay_f, jnp.logical_or(d != 1, owner != c)))
        def _():
            left(kv_sum.at[slot], move_send.at[2 + slot], here)

        @pl.when(jnp.logical_not(stays))
        def _():
            left(moves[slot][0], move_send.at[slot], here)

    for at in range(ctx):
        for to in range(fs):

            @pl.when(to != f)
            def _():
                left(stage.at[at, to], u_send.at[at, to], here)

        left(partial_ref.at[1 - d, at], out_sum.core_send.at[at], here)

        @pl.when(at != c)
        def _():
            left(out_sum.out_line.at[at], out_sum.line_send.at[at], here)

    in_sum.finish()

    def gain_left(step, carry):
        other = lax.rem(me + step, n)
        left(gain_stage.at[other], g_send.at[other], here)
        return carry

    lax.fori_loop(1, n, gain_left, 0)


def last(sizes, x, gains, tables, resid, d_resid, gain_two, unit, d_unit, normed, wide, partial, grad_up, grad_down, grad_proj):
    dp, ctx, fs = sizes
    n = dp * ctx * fs
    rows = x.shape[0]
    span = rows // 2
    low, wide_t = jnp.bfloat16, jnp.float32
    dma = pltpu.SemaphoreType.DMA
    any_spec, vm_spec = pl.BlockSpec(memory_space=ANY), pl.BlockSpec(memory_space=VM)
    down_rows, proj_rows, half = grad_down.shape[0] // fs, grad_proj.shape[1], grad_up.shape[2]
    shapes = (
        jax.ShapeDtypeStruct((rows, D), low),
        jax.ShapeDtypeStruct((rows, D), low),
        jax.ShapeDtypeStruct((8, LANES), wide_t),
        jax.ShapeDtypeStruct((D, HD), wide_t),
        jax.ShapeDtypeStruct((proj_rows, D), wide_t),
        jax.ShapeDtypeStruct((D, half), wide_t),
        jax.ShapeDtypeStruct((down_rows, D), wide_t),
    )
    return pl.pallas_call(
        functools.partial(last_kernel, sizes),
        name="last",
        out_shape=shapes,
        in_specs=[vm_spec] * 8 + [any_spec] * 8,
        out_specs=[vm_spec] * 7,
        scratch_shapes=[
            VM(unit.shape, low),
            VM(d_unit.shape, low),
            VM((ctx * fs * span, LANES), wide_t),
            VM((ctx * fs * span, LANES), wide_t),
            VM((ctx, fs, span, 4 * LANES), low),
            VM((dp, ctx, 2, span, 4 * LANES), low),
            VM(normed.shape, low),
            VM(wide.shape, low),
            VM(wide.shape, low),
            VM((4, D, HD), low),
            VM((fs, D, half), low),
            VM((fs, down_rows, D), low),
            VM((fs, proj_rows, D), low),
            VM((fs, D, HD), low),
            VM((2, fs, D, HD), low),
            VM((down_rows, D), low),
            VM((proj_rows, D), low),
            VM((2, D, HD), low),
            VM((down_rows, D), low),
            VM((proj_rows, D), low),
            VM((D, HD), low),
            VM((8, D), wide_t),
            VM((n, 8, LANES), wide_t),
            VM((n, 8, LANES), wide_t),
            dma((4,)),
            dma((4,)), dma((fs,)), dma((fs,)), dma((fs,)), dma((fs,)), dma((fs,)),
            dma((4,)), dma((3, fs)), dma((4,)), dma((3,)),
            dma((ctx, fs)), dma((fs, ctx)), dma((n,)), dma((n,)), dma((ctx,)),
        ] + LineSum.scratch(ctx, rows) + LineSum.scratch(ctx, rows),
        compiler_params=pltpu.CompilerParams(collective_id=3, has_side_effects=True, vmem_limit_bytes=63 * 1024 * 1024),
    )(
        x, gains, *tables, resid, d_resid, gain_two, unit, d_unit, normed, wide, partial,
        grad_up, grad_down.reshape(fs, down_rows, D), grad_proj,
    )


def on_device(tokens, cotangent, attn_gain, w_qkv, w_out, mlp_gain, w_gate_up, w_down):
    dp, ctx, fs = where = tuple(lax.axis_size(name) for name in ("dp", "ctx", "fsdp"))
    mb, _, span, _ = tokens.shape
    rows = mb * span
    x = tokens.reshape(rows, D)
    dy = cotangent.reshape(rows, D)
    each = attn_gain.shape[0]
    gain_rows = jnp.concatenate([attn_gain[None], mlp_gain[None]]).astype(jnp.float32)
    gain_rows = jnp.pad(gain_rows, ((0, 6), (0, LANES - each)))
    tables = angle_tables(ctx, fs, span)
    normed, unit, att, qkv, gains, dy_all, proj, down = first(where, x, gain_rows, w_qkv, *tables, dy, w_out, w_down)
    att = att.reshape(dp, ctx, rows, 2 * LANES)
    resid, d_resid, grad_two, partial, d_unit, grad_up, grad_down, grad_proj = middle(
        where, att, x, dy, gains, proj, down, w_gate_up, dy_all
    )
    block_out, grad_tokens, gain_grads, grad_qkv, grad_out, grad_gate_up, grad_down = last(
        where, x, gains, tables, resid, d_resid, grad_two, unit, d_unit, normed, qkv, partial, grad_up, grad_down, grad_proj
    )
    return (
        block_out.reshape(tokens.shape),
        grad_tokens.reshape(tokens.shape),
        gain_grads[0, :each],
        grad_qkv,
        grad_out,
        gain_grads[1, :each],
        grad_gate_up,
        grad_down,
    )


def fits(mesh):
    return mesh.shape["dp"] == 2 and mesh.shape["ctx"] == 4 and mesh.shape["fsdp"] == 4


def solution(mesh):
    placed = (
        P(None, "dp", ("ctx", "fsdp"), None),
        P(None, "dp", ("ctx", "fsdp"), None),
        P(("dp", "ctx", "fsdp")),
        P(None, ("dp", "ctx", "fsdp")),
        P(("dp", "ctx", "fsdp"), None),
        P(("dp", "ctx", "fsdp")),
        P(None, ("dp", "ctx", "fsdp")),
        P(("dp", "ctx", "fsdp"), None),
    )
    return jax.shard_map(
        on_device if fits(mesh) else on_device_gathered,
        mesh=mesh,
        in_specs=placed,
        out_specs=(
            P(None, "dp", ("ctx", "fsdp"), None),
            P(None, "dp", ("ctx", "fsdp"), None),
            P(("dp", "ctx", "fsdp")),
            P(None, ("dp", "ctx", "fsdp")),
            P(("dp", "ctx", "fsdp"), None),
            P(("dp", "ctx", "fsdp")),
            P(None, ("dp", "ctx", "fsdp")),
            P(("dp", "ctx", "fsdp"), None),
        ),
        check_vma=False,
    )
```

```python
import functools

import jax
import jax.numpy as jnp
from jax import lax
from jax.experimental import pallas as pl
from jax.experimental.pallas import tpu as pltpu
from jax.sharding import PartitionSpec as P

D = 1536
H = 16
KVH = 8
HD = 96
FF = 4096


EPS = 1e-05
THETA = 100000.0
NEG = -1e30


def in_blocks(value, dim, length):
    lengths = value.shape
    pieces = value.reshape(*lengths[:dim], length, lengths[dim] // length, *lengths[dim + 1 :])
    return jnp.moveaxis(pieces, dim, 0)


def sum_at_owner(value, axis, dim):
    pieces = in_blocks(value, dim, lax.axis_size(axis))
    arrived = lax.all_to_all(pieces, axis, split_axis=0, concat_axis=0, tiled=True)
    return arrived.astype(jnp.float32).sum(axis=0)


def side_by_side(arrays, axis, dim, along):
    both = jnp.concatenate(arrays, axis=along)
    whole, at, finished = (sum_at_owner(both, axis, dim), 0, [])
    for a in arrays:
        finished.append(lax.slice_in_dim(whole, at, at + a.shape[along], axis=along))
        at += a.shape[along]
    return tuple(finished)


def rms_norm(values, gain_vec):
    return values * lax.rsqrt(jnp.mean(values * values, axis=-1, keepdims=True) + EPS) * gain_vec


def tables(start, length, width):
    half_width = width // 2
    frequency = THETA ** (-(jnp.arange(half_width, dtype=jnp.float32) * 2.0) / width)
    angles = (start + jnp.arange(length, dtype=jnp.int32)).astype(jnp.float32)[:, None] * frequency[
        None, :
    ]
    return (jnp.cos(angles), jnp.sin(angles))


def rotate(values, cosine, sine_table):
    half_width = values.shape[-1] // 2
    first_half = values[..., :half_width]
    second_half = values[..., half_width:]
    cos_b = cosine[:, None, :]
    sin_b = sine_table[:, None, :]
    return jnp.concatenate(
        [first_half * cos_b - second_half * sin_b, second_half * cos_b + first_half * sin_b],
        axis=-1,
    )


def swiglu(both):
    return jax.nn.silu(both[:, :FF]) * both[:, FF:]


def inner(left, right):
    return lax.dot_general(
        left, right, (((0,), (0,)), ((), ())), preferred_element_type=jnp.float32
    )


def outer(left, right):
    return lax.dot_general(
        left, right, (((1,), (1,)), ((), ())), preferred_element_type=jnp.float32
    )


def unchanged(state):
    return state


def on_device_gathered(tokens, cotangent, attn_gain, w_qkv, w_out, mlp_gain, w_gate_up, w_down):
    tok_count = tokens.shape[2]
    groups = H // KVH
    factor = HD ** (-0.5)
    seq_length = tok_count * lax.axis_size(("ctx", "fsdp"))
    pos_first = lax.axis_index(("ctx", "fsdp")) * tok_count
    positions = pos_first + jnp.arange(tok_count, dtype=jnp.int32)
    pos_last = pos_first + tok_count - 1
    cosine, sine_table = tables(pos_first, tok_count, HD)
    sums = [
        jnp.zeros((D,), jnp.float32),
        jnp.zeros((D, (H + 2 * KVH) * HD), jnp.float32),
        jnp.zeros((H * HD, D), jnp.float32),
        jnp.zeros((D,), jnp.float32),
        jnp.zeros((D, 2 * FF), jnp.float32),
        jnp.zeros((FF, D), jnp.float32),
    ]
    outputs = []
    in_grads = []
    whole = (
        lax.all_gather(attn_gain, ("dp", "ctx", "fsdp"), axis=0, tiled=True),
        lax.all_gather(w_qkv, ("dp", "ctx", "fsdp"), axis=1, tiled=True),
        lax.all_gather(w_out, ("dp", "ctx", "fsdp"), axis=0, tiled=True),
        lax.all_gather(mlp_gain, ("dp", "ctx", "fsdp"), axis=0, tiled=True),
        lax.all_gather(w_gate_up, ("dp", "ctx", "fsdp"), axis=1, tiled=True),
        lax.all_gather(w_down, ("dp", "ctx", "fsdp"), axis=0, tiled=True),
    )
    for step_index in range(tokens.shape[0]):
        gain_one, mix_qkv, mix_out, gain_two, mix_gate_up, mix_down = whole
        inputs = tokens[step_index, 0].astype(jnp.float32)
        normed = rms_norm(inputs, gain_one.astype(jnp.float32)).astype(jnp.bfloat16)
        mixed = jnp.dot(normed, mix_qkv, preferred_element_type=jnp.float32)
        queries = rotate(mixed[:, : H * HD].reshape(tok_count, H, HD), cosine, sine_table).astype(
            jnp.bfloat16
        )
        key_rows = rotate(
            mixed[:, H * HD : (H + KVH) * HD].reshape(tok_count, KVH, HD), cosine, sine_table
        )
        key_rows = key_rows.astype(jnp.bfloat16).reshape(tok_count, KVH * HD)
        value_rows = mixed[:, (H + KVH) * HD :].astype(jnp.bfloat16)
        grouped = queries.reshape(tok_count, KVH, groups, HD)
        start_state = (
            jnp.full((KVH, groups, tok_count), NEG, jnp.float32),
            jnp.zeros((KVH, groups, tok_count), jnp.float32),
            jnp.zeros((KVH, groups, tok_count, HD), jnp.float32),
        )
        piece = (
            lax.all_gather(key_rows, ("ctx", "fsdp"), axis=0, tiled=True),
            lax.all_gather(value_rows, ("ctx", "fsdp"), axis=0, tiled=True),
        )

        def work(state):
            best, total, summed = state
            key_count = piece[0].shape[0]
            keys = piece[0].reshape(key_count, KVH, HD)
            values = piece[1].reshape(key_count, KVH, HD)
            scores = (
                jnp.einsum("qkgd,tkd->kgqt", grouped, keys, preferred_element_type=jnp.float32)
                * factor
            )
            allowed = jnp.arange(key_count, dtype=jnp.int32)[None, :] <= positions[:, None]
            scores = jnp.where(allowed, scores, NEG)
            new_best = jnp.maximum(best, jnp.max(scores, axis=-1))
            weights = jnp.where(allowed, jnp.exp(scores - new_best[..., None]), 0.0)
            total = jnp.sum(weights, axis=-1)
            summed = jnp.einsum(
                "kgqt,tkd->kgqd",
                weights.astype(jnp.bfloat16),
                values,
                preferred_element_type=jnp.float32,
            )
            return (new_best, total, summed)

        best, total, summed = lax.cond(jnp.int32(0) <= pos_last, work, unchanged, start_state)
        head_out = summed / total[..., None]
        log_total = best + jnp.log(total)
        attended = (
            jnp.transpose(head_out, (2, 0, 1, 3)).reshape(tok_count, H * HD).astype(jnp.bfloat16)
        )
        resid = inputs + jnp.dot(attended, mix_out, preferred_element_type=jnp.float32)
        normed_two = rms_norm(resid, gain_two.astype(jnp.float32)).astype(jnp.bfloat16)
        both = jnp.dot(normed_two, mix_gate_up, preferred_element_type=jnp.float32)
        acted = swiglu(both).astype(jnp.bfloat16)
        result = resid + jnp.dot(acted, mix_down, preferred_element_type=jnp.float32)
        outputs.append(result.astype(jnp.bfloat16))
        gain_one, mix_qkv, mix_out, gain_two, mix_gate_up, mix_down = whole
        up_low = cotangent[step_index, 0]
        upstream = up_low.astype(jnp.float32)
        sums[5] = sums[5] + inner(acted, up_low)
        d_act = outer(up_low, mix_down)
        _, pull_glu = jax.vjp(swiglu, both)
        d_both = pull_glu(d_act)[0].astype(jnp.bfloat16)
        sums[4] = sums[4] + inner(normed_two, d_both)
        d_normed_two = outer(d_both, mix_gate_up)
        _, pull_two = jax.vjp(rms_norm, resid, gain_two.astype(jnp.float32))
        d_resid_norm, d_gain_two = pull_two(d_normed_two)
        sums[3] = sums[3] + d_gain_two
        d_resid = upstream + d_resid_norm
        d_resid_low = d_resid.astype(jnp.bfloat16)
        sums[2] = sums[2] + inner(attended, d_resid_low)
        d_attended = outer(d_resid_low, mix_out).astype(jnp.bfloat16)
        d_grouped = d_attended.reshape(tok_count, KVH, groups, HD)
        delta = jnp.einsum("qkgd,kgqd->kgq", d_grouped.astype(jnp.float32), head_out)
        zero_q = jnp.zeros((tok_count, KVH, groups, HD), jnp.float32)
        back_state = (
            zero_q,
            jnp.zeros((seq_length, KVH * HD), jnp.float32),
            jnp.zeros((seq_length, KVH * HD), jnp.float32),
        )
        attend_piece = (
            lax.all_gather(key_rows, ("ctx", "fsdp"), axis=0, tiled=True),
            lax.all_gather(value_rows, ("ctx", "fsdp"), axis=0, tiled=True),
        )

        def attend_work(state):
            key_count = attend_piece[0].shape[0]
            keys = attend_piece[0].reshape(key_count, KVH, HD)
            values = attend_piece[1].reshape(key_count, KVH, HD)
            scores = (
                jnp.einsum("qkgd,tkd->kgqt", grouped, keys, preferred_element_type=jnp.float32)
                * factor
            )
            allowed = jnp.arange(key_count, dtype=jnp.int32)[None, :] <= positions[:, None]
            scores = jnp.where(allowed, scores, NEG)
            probs = jnp.where(allowed, jnp.exp(scores - log_total[..., None]), 0.0)
            d_probs = jnp.einsum(
                "qkgd,tkd->kgqt", d_grouped, values, preferred_element_type=jnp.float32
            )
            d_scores = (probs * (d_probs - delta[..., None])).astype(jnp.bfloat16)
            grad_q = jnp.einsum(
                "kgqt,tkd->qkgd", d_scores, keys, preferred_element_type=jnp.float32
            )
            piece_k = (
                jnp.einsum("kgqt,qkgd->tkd", d_scores, grouped, preferred_element_type=jnp.float32)
                * factor
            )
            piece_v = jnp.einsum(
                "kgqt,qkgd->tkd",
                probs.astype(jnp.bfloat16),
                d_grouped,
                preferred_element_type=jnp.float32,
            )
            grad_k = piece_k.reshape(key_count, KVH * HD)
            grad_v = piece_v.reshape(key_count, KVH * HD)
            return (grad_q, grad_k, grad_v)

        back_result = lax.cond(jnp.int32(0) <= pos_last, attend_work, unchanged, back_state)
        grad_q = back_result[0]
        summed_k, summed_v = side_by_side(
            (back_result[1].astype(jnp.bfloat16), back_result[2].astype(jnp.bfloat16)),
            ("ctx", "fsdp"),
            0,
            1,
        )
        d_q_raw = rotate(grad_q.reshape(tok_count, H, HD) * factor, cosine, -sine_table).reshape(
            tok_count, H * HD
        )
        d_k_raw = rotate(summed_k.reshape(tok_count, KVH, HD), cosine, -sine_table).reshape(
            tok_count, KVH * HD
        )
        d_mixed = jnp.concatenate([d_q_raw, d_k_raw, summed_v], axis=1).astype(jnp.bfloat16)
        sums[1] = sums[1] + inner(normed, d_mixed)
        d_normed = outer(d_mixed, mix_qkv)
        _, pull_one = jax.vjp(rms_norm, inputs, gain_one.astype(jnp.float32))
        d_inputs_norm, d_gain_one = pull_one(d_normed)
        sums[0] = sums[0] + d_gain_one
        in_grads.append((d_resid + d_inputs_norm).astype(jnp.bfloat16))
    grad_gain_one, grad_qkv, grad_out, grad_gain_two, grad_gate_up, grad_down = (
        lax.psum_scatter(sums[0], ("dp", "ctx", "fsdp"), scatter_dimension=0, tiled=True),
        lax.psum_scatter(sums[1], ("dp", "ctx", "fsdp"), scatter_dimension=1, tiled=True),
        lax.psum_scatter(sums[2], ("dp", "ctx", "fsdp"), scatter_dimension=0, tiled=True),
        lax.psum_scatter(sums[3], ("dp", "ctx", "fsdp"), scatter_dimension=0, tiled=True),
        lax.psum_scatter(sums[4], ("dp", "ctx", "fsdp"), scatter_dimension=1, tiled=True),
        lax.psum_scatter(sums[5], ("dp", "ctx", "fsdp"), scatter_dimension=0, tiled=True),
    )
    block_out = jnp.stack(outputs)[:, None]
    grad_tokens = jnp.stack(in_grads)[:, None]
    return (
        block_out,
        grad_tokens,
        grad_gain_one,
        grad_qkv,
        grad_out,
        grad_gain_two,
        grad_gate_up,
        grad_down,
    )


MESH = pl.DeviceIdType.MESH
VM = pltpu.VMEM
ANY = pl.ANY


def place():
    return lax.axis_index("dp"), lax.axis_index("ctx"), lax.axis_index("fsdp")


def at_device(dp, ctx, fs):
    return {"dp": dp, "ctx": ctx, "fsdp": fs}


def remote(src, dst, send, recv, device):
    return pltpu.make_async_remote_copy(
        src_ref=src, dst_ref=dst, send_sem=send, recv_sem=recv, device_id=device, device_id_type=MESH
    )


def arrived(dst, recv, device):
    remote(dst, dst, recv, recv, device).wait_recv()


def left(src, send, device):
    remote(src, src, send, send, device).wait_send()


def tell_all(sizes):
    dp, ctx, fs = sizes
    n = dp * ctx * fs
    d, c, f = place()
    me = (d * ctx + c) * fs + f
    barrier = pltpu.get_barrier_semaphore()

    def tell(step, carry):
        other = lax.rem(me + step, n)
        pl.semaphore_signal(
            barrier,
            inc=1,
            device_id=at_device(other // (ctx * fs), lax.rem(other // fs, ctx), lax.rem(other, fs)),
            device_id_type=MESH,
        )
        return carry

    lax.fori_loop(1, n, tell, 0)


def hear_all(sizes):
    dp, ctx, fs = sizes
    pl.semaphore_wait(pltpu.get_barrier_semaphore(), dp * ctx * fs - 1)


class LineGather:
    def __init__(self, n, own, whole, send, recv, local):
        self.n, self.own, self.whole, self.send, self.recv, self.local = n, own, whole, send, recv, local
        self.d, self.c, self.f = place()

    def slot(self, at):
        return self.whole.at[self.d, at]

    def up(self, src, at):
        return remote(src, self.slot(at), self.send.at[0, at], self.recv.at[self.d, at], at_device(self.d, self.c + 1, self.f))

    def down(self, src, at):
        return remote(src, self.slot(at), self.send.at[1, at], self.recv.at[self.d, at], at_device(self.d, self.c - 1, self.f))

    def across(self, src, at):
        return remote(src, self.slot(at), self.send.at[2, at], self.recv.at[self.d, at], at_device(1 - self.d, self.c, self.f))

    def start(self):
        c = self.c

        @pl.when(c < self.n - 1)
        def _():
            self.up(self.own, c).start()

        @pl.when(c > 0)
        def _():
            self.down(self.own, c).start()

        self.across(self.own, c).start()
        pltpu.make_async_copy(self.own, self.slot(c), self.local).start()

    def forward(self, k):
        c = self.c

        @pl.when(c - k >= 0)
        def _():
            arrived(self.slot(c - k), self.recv.at[self.d, c - k], at_device(self.d, c, self.f))

            @pl.when(c < self.n - 1)
            def _():
                self.up(self.slot(c - k), c - k).start()

            self.across(self.slot(c - k), c - k).start()

        @pl.when(c + k < self.n)
        def _():
            arrived(self.slot(c + k), self.recv.at[self.d, c + k], at_device(self.d, c, self.f))

            @pl.when(c > 0)
            def _():
                self.down(self.slot(c + k), c + k).start()

            self.across(self.slot(c + k), c + k).start()

    def take(self, at):
        c = self.c

        @pl.when(at != c)
        def _():
            arrived(self.slot(at), self.recv.at[self.d, at], at_device(self.d, c, self.f))

            @pl.when(jnp.logical_and(at < c, c < self.n - 1))
            def _():
                self.up(self.slot(at), at).start()

            @pl.when(jnp.logical_and(at > c, c > 0))
            def _():
                self.down(self.slot(at), at).start()

            self.across(self.slot(at), at).start()

        self.other(at)

    def other(self, at):
        arrived(self.whole.at[1 - self.d, at], self.recv.at[1 - self.d, at], at_device(self.d, self.c, self.f))

    def finish_sends(self):
        c = self.c
        for at in range(self.n):

            @pl.when(jnp.logical_and(at <= c, c < self.n - 1))
            def _():
                left(self.slot(at), self.send.at[0, at], at_device(self.d, c, self.f))

            @pl.when(jnp.logical_and(at >= c, c > 0))
            def _():
                left(self.slot(at), self.send.at[1, at], at_device(self.d, c, self.f))

            left(self.slot(at), self.send.at[2, at], at_device(self.d, c, self.f))

    def finish(self):
        self.finish_sends()
        pltpu.make_async_copy(self.own, self.slot(self.c), self.local).wait()


FACTOR = HD ** (-0.5)
LANES = 128


def ordered(c, step, n):
    at = jnp.int32(0)
    for here in range(n):
        near = sorted(range(n), key=lambda place_: (abs(place_ - here), place_))
        for index, value in enumerate(near):
            at = jnp.where(jnp.logical_and(c == here, step == index), value, at)
    return at


def first_kernel(
    sizes, parts, x_ref, gains_ref, w_ref, block_ref, step_ref, dy_ref, proj_ref, gate_up_ref,
    normed_out, unit_out, att_out, wide_out, gains_out, dy_all, proj_all, gate_up_all,
    x_all, wide, normed, stage, unit, att_stage, att, gain_all, gain_vec,
    line_send, line_recv, line_local, w_send, w_recv, w_pass, g_send, g_recv, u_send, u_recv, a_send, a_recv, out_sem,
    dy_send, dy_recv, dy_local, m_send, m_recv, m_pass, gu_send, gu_recv,
):
    dp, ctx, fs = sizes
    n = dp * ctx * fs
    d, c, f = place()
    here = at_device(d, c, f)
    span = stage.shape[2]
    tell_all(sizes)
    for slot in range(4):
        wide[slot * LANES + HD : (slot + 1) * LANES, :] = jnp.zeros((LANES - HD, D), jnp.bfloat16)
    hear_all(sizes)

    def head_rows(slot):
        return wide.at[pl.ds(pl.multiple_of(slot * LANES, LANES), HD)]

    q_core = f // 2
    kv_slot = 2 + c // 2
    kv_ctx = 2 * lax.rem(c, 2) + f // 2
    kv_core = lax.rem(f, 2)
    kv_f = lax.rem(f + 2 * (c // 2), fs)
    kv_away = jnp.logical_or(jnp.logical_or(kv_core != d, kv_ctx != c), kv_f != f)
    relay_of = {slot: f == lax.rem(2 * lax.rem(c, 2) + d + 2 * (slot - 2), fs) for slot in (2, 3)}

    @pl.when(jnp.logical_and(d == 1, kv_away))
    def _():
        remote(w_ref, head_rows(kv_slot), w_send.at[0], w_recv.at[kv_slot], at_device(kv_core, kv_ctx, kv_f)).start()

    @pl.when(jnp.logical_and(d == 1, jnp.logical_not(kv_away)))
    def _():
        pltpu.make_async_copy(w_ref, head_rows(kv_slot), w_recv.at[kv_slot]).start()

    line = LineGather(ctx, x_ref, x_all, line_send, line_recv, line_local)
    line.start()

    @pl.when(d == 0)
    def _():
        slot = lax.rem(f, 2)
        for to in range(fs):

            @pl.when(jnp.logical_or(q_core != 0, to != f))
            def _():
                remote(w_ref, head_rows(slot), w_send.at[to], w_recv.at[slot], at_device(q_core, c, to)).start()

            @pl.when(jnp.logical_and(q_core == 0, to == f))
            def _():
                pltpu.make_async_copy(w_ref, head_rows(slot), w_recv.at[slot]).start()

    me = (d * ctx + c) * fs + f

    def gain_to(step, carry):
        other = lax.rem(me + step, n)
        remote(
            gains_ref, gain_all.at[me], g_send.at[other], g_recv.at[me],
            at_device(other // (ctx * fs), lax.rem(other // fs, ctx), lax.rem(other, fs)),
        ).start()
        return carry

    lax.fori_loop(1, n, gain_to, 0)
    gain_all[me] = gains_ref[...]

    for slot in (2, 3):

        @pl.when(relay_of[slot])
        def _():
            arrived(head_rows(slot), w_recv.at[slot], here)
            for step in range(1, fs):
                to = lax.rem(f + step, fs)
                remote(head_rows(slot), head_rows(slot), w_pass.at[slot - 2, step], w_recv.at[slot], at_device(d, c, to)).start()

    gu_core = f // 2
    gu_slot = 2 * d + lax.rem(f, 2)
    part_rows = gate_up_ref.shape[0] // parts

    def push_part(part):
        first_row = part * part_rows
        src = gate_up_ref.at[first_row : first_row + part_rows]
        dst = gate_up_all.at[gu_slot, first_row : first_row + part_rows]
        for to in range(fs):
            own_place = jnp.logical_and(gu_core == d, f == to)

            @pl.when(jnp.logical_not(own_place))
            def _():
                remote(src, dst, gu_send.at[part, to], gu_recv.at[part, gu_slot], at_device(gu_core, c, to)).start()

            @pl.when(own_place)
            def _():
                pltpu.make_async_copy(src, dst, gu_recv.at[part, gu_slot]).start()

    push_part(0)

    def gain_from(step, carry):
        other = lax.rem(me + step, n)
        arrived(gain_all.at[other], g_recv.at[other], here)
        return carry

    lax.fori_loop(1, n, gain_from, 0)
    each = D // n
    for index in range(n):
        gain_vec[:, index * each : (index + 1) * each] = gain_all[index][:, :each]
    gain = gain_vec[0:1, :]

    for slot in range(4):
        if slot < 2:
            arrived(head_rows(slot), w_recv.at[slot], here)
        else:

            @pl.when(jnp.logical_not(relay_of[slot]))
            def _():
                arrived(head_rows(slot), w_recv.at[slot], here)

    pltpu.make_async_copy(line.own, line.slot(c), line.local).wait()

    def block(step, carry):
        at = ordered(c, step, ctx)

        line.take(at)
        values = x_all[:, at].reshape(dp * 2 * span, D).astype(jnp.float32)
        scale = lax.rsqrt(jnp.mean(values * values, axis=-1, keepdims=True) + EPS)
        low = (values * scale * gain).astype(jnp.bfloat16)
        normed[:, at] = low.reshape(dp, 2 * span, D)
        heads = outer(low, wide[...])
        cosine, sine_up, sine_down = turns(block_ref, step_ref, at * fs + f)
        for slot in range(4):
            head = heads[:, slot * LANES : (slot + 1) * LANES]
            if slot < 3:
                turned_up = pltpu.roll(head, HD // 2, 1).reshape(2 * dp, span, LANES)
                turned_down = pltpu.roll(head, LANES - HD // 2, 1).reshape(2 * dp, span, LANES)
                head = head.reshape(2 * dp, span, LANES)
                head = head * cosine[None] + turned_up * sine_up[None] + turned_down * sine_down[None]
            else:
                head = head.reshape(2 * dp, span, LANES)
            stage[at, :, :, slot * LANES : (slot + 1) * LANES] = head.astype(jnp.bfloat16)
        for to in range(2 * dp):

            @pl.when(to != f)
            def _():
                remote(stage.at[at, to], unit.at[at, f], u_send.at[at, to], u_recv.at[at, f], at_device(d, c, to)).start()

            @pl.when(to == f)
            def _():
                unit[at, f] = stage[at, to]

        return carry

    lax.fori_loop(0, ctx, block, 0)
    normed_copy = pltpu.make_async_copy(normed, normed_out, out_sem.at[0])
    wide_copy = pltpu.make_async_copy(wide, wide_out, out_sem.at[1])
    gains_copy = pltpu.make_async_copy(gain_vec, gains_out, out_sem.at[2])
    normed_copy.start()
    wide_copy.start()
    gains_copy.start()

    to_core, to_ctx = lax.rem(c, 2), 2 * d + c // 2
    stays = jnp.logical_and(to_core == d, to_ctx == c)
    moved = ((proj_ref, proj_all),)
    for index, (shard, whole) in enumerate(moved):

        @pl.when(jnp.logical_not(stays))
        def _():
            remote(shard, whole.at[f], m_send.at[index], m_recv.at[index, f], at_device(to_core, to_ctx, f)).start()

        @pl.when(stays)
        def _():
            pltpu.make_async_copy(shard, whole.at[f], m_recv.at[index, f]).start()

    dy_line = LineGather(ctx, dy_ref, dy_all, dy_send, dy_recv, dy_local)
    dy_line.start()

    def pass_on():
        for index, (shard, whole) in enumerate(moved):
            arrived(whole.at[f], m_recv.at[index, f], here)
            for step in range(1, fs):
                to = lax.rem(f + step, fs)
                remote(whole.at[f], whole.at[f], m_pass.at[index, step], m_recv.at[index, f], at_device(d, c, to)).start()

    for at in range(ctx):
        for step in range(1, fs):
            other = lax.rem(f + step, fs)
            arrived(unit.at[at, other], u_recv.at[at, other], here)
    unit_copy = pltpu.make_async_copy(unit, unit_out, out_sem.at[3])
    unit_copy.start()

    rows = fs * span
    for at in range(ctx):
        keys = rows * (at + 1)
        k_rows = unit[0 : at + 1, :, :, 2 * LANES : 3 * LANES].reshape(keys, LANES)
        v_rows = unit[0 : at + 1, :, :, 3 * LANES : 4 * LANES].reshape(keys, LANES)
        allowed = lax.broadcasted_iota(jnp.int32, (rows, keys), 1) <= rows * at + lax.broadcasted_iota(
            jnp.int32, (rows, keys), 0
        )
        for head in range(2):
            q_rows = unit[at, :, :, head * LANES : (head + 1) * LANES].reshape(rows, LANES)
            scores = outer(q_rows, k_rows) * FACTOR
            scores = jnp.where(allowed, scores, NEG)
            best = jnp.max(scores, axis=-1, keepdims=True)
            weights = jnp.exp(scores - best)
            probs = weights / jnp.sum(weights, axis=-1, keepdims=True)
            mixed = jnp.dot(probs.astype(jnp.bfloat16), v_rows, preferred_element_type=jnp.float32)
            att_stage[at, :, :, head * LANES : (head + 1) * LANES] = mixed.astype(jnp.bfloat16).reshape(fs, span, LANES)
        for to in range(fs):

            @pl.when(to != f)
            def _():
                remote(
                    att_stage.at[at, to], att.at[f // 2, at, lax.rem(f, 2)], a_send.at[at, to], a_recv.at[f, at], at_device(d, c, to)
                ).start()

            @pl.when(to == f)
            def _():
                att[f // 2, at, lax.rem(f, 2)] = att_stage[at, to]

        if at == 0:
            pass_on()
        elif at == 1:
            dy_line.forward(1)
        elif at == ctx - 1:
            for part in range(1, gu_send.shape[0]):
                push_part(part)

    for at in range(ctx):
        for step in range(1, fs):
            other = lax.rem(f + step, fs)
            arrived(att.at[other // 2, at, lax.rem(other, 2)], a_recv.at[other, at], here)
    att_copy = pltpu.make_async_copy(att, att_out, out_sem.at[4])
    att_copy.start()

    for k in range(2, ctx):
        dy_line.forward(k)
    for at in range(ctx):
        dy_line.other(at)
    dy_line.finish()
    for index, (shard, whole) in enumerate(moved):
        for step in range(1, fs):
            other = lax.rem(f + step, fs)
            arrived(whole.at[other], m_recv.at[index, other], here)
            left(whole.at[f], m_pass.at[index, step], here)

        @pl.when(jnp.logical_not(stays))
        def _():
            left(shard, m_send.at[index], here)

    for part in range(gu_send.shape[0]):
        src = gate_up_ref.at[part * part_rows : (part + 1) * part_rows]
        for slot in range(4):
            arrived(gate_up_all.at[slot, part * part_rows : (part + 1) * part_rows], gu_recv.at[part, slot], here)
        for to in range(fs):

            @pl.when(jnp.logical_not(jnp.logical_and(gu_core == d, f == to)))
            def _():
                left(src, gu_send.at[part, to], here)

    line.finish_sends()
    for at in range(ctx):

        for to in range(fs):

            @pl.when(to != f)
            def _():
                left(stage.at[at, to], u_send.at[at, to], here)
                left(att_stage.at[at, to], a_send.at[at, to], here)

    @pl.when(jnp.logical_and(d == 1, kv_away))
    def _():
        left(w_ref, w_send.at[0], here)

    @pl.when(d == 0)
    def _():
        for to in range(fs):

            @pl.when(jnp.logical_or(q_core != 0, to != f))
            def _():
                left(w_ref, w_send.at[to], here)

    for slot in (2, 3):

        @pl.when(relay_of[slot])
        def _():
            for step in range(1, fs):
                left(head_rows(slot), w_pass.at[slot - 2, step], here)

    def gain_left(step, carry):
        other = lax.rem(me + step, n)
        left(gains_ref, g_send.at[other], here)
        return carry

    lax.fori_loop(1, n, gain_left, 0)
    for copy in (normed_copy, wide_copy, gains_copy, unit_copy, att_copy):
        copy.wait()


def first(sizes, parts, sent, x, gains, w_qkv, blocks, steps, dy, w_out, w_gate_up):
    dp, ctx, fs = sizes
    n = dp * ctx * fs
    rows = x.shape[0]
    span = rows // 2
    low, wide_t = jnp.bfloat16, jnp.float32
    dma = pltpu.SemaphoreType.DMA
    shapes = (
        jax.ShapeDtypeStruct((dp, ctx, rows, D), low),
        jax.ShapeDtypeStruct((ctx, fs, span, 4 * LANES), low),
        jax.ShapeDtypeStruct((dp, ctx, 2, span, 2 * LANES), low),
        jax.ShapeDtypeStruct((4 * LANES, D), low),
        jax.ShapeDtypeStruct((8, D), wide_t),
        jax.ShapeDtypeStruct((dp, ctx, rows, D), low),
        jax.ShapeDtypeStruct((fs,) + w_out.shape, low),
        jax.ShapeDtypeStruct((4, D // parts * sent, w_gate_up.shape[1]), low),
    )
    any_spec, vm_spec = pl.BlockSpec(memory_space=ANY), pl.BlockSpec(memory_space=VM)
    return pl.pallas_call(
        functools.partial(first_kernel, sizes, parts),
        name="first",
        out_shape=shapes,
        in_specs=[vm_spec] * 8,
        out_specs=[any_spec] * 8,
        scratch_shapes=[
            VM((dp, ctx, rows, D), low),
            VM((4 * LANES, D), low),
            VM((dp, ctx, rows, D), low),
            VM((ctx, 2 * dp, span, 4 * LANES), low),
            VM((ctx, fs, span, 4 * LANES), low),
            VM((ctx, fs, span, 2 * LANES), low),
            VM((dp, ctx, 2, span, 2 * LANES), low),
            VM((n, 8, LANES), wide_t),
            VM((8, D), wide_t),
            dma((3, ctx)), dma((dp, ctx)), dma,
            dma((fs,)), dma((4,)), dma((2, fs)),
            dma((n,)), dma((n,)),
            dma((ctx, 2 * dp)), dma((ctx, fs)),
            dma((ctx, fs)), dma((fs, ctx)),
            dma((5,)),
            dma((3, ctx)), dma((dp, ctx)), dma,
            dma((1,)), dma((1, fs)), dma((1, fs)),
            dma((sent, fs)), dma((sent, 4)),
        ],
        compiler_params=pltpu.CompilerParams(collective_id=1, has_side_effects=True, vmem_limit_bytes=60 * 1024 * 1024),
    )(x, gains, w_qkv, blocks, steps, dy, w_out, w_gate_up)


def angle_tables(count, span):
    lane = jnp.arange(LANES, dtype=jnp.int32)
    frequency = THETA ** (-((lane % (HD // 2)).astype(jnp.float32) * 2.0) / HD)

    def both(positions):
        angles = positions.astype(jnp.float32)[:, None] * frequency
        return jnp.stack([jnp.cos(angles), jnp.sin(angles)])

    return both(jnp.arange(count, dtype=jnp.int32) * span), both(jnp.arange(span, dtype=jnp.int32))


def turns(block_ref, step_ref, block):
    cos_b, sin_b = block_ref[0, pl.ds(block, 1)], block_ref[1, pl.ds(block, 1)]
    cos_s, sin_s = step_ref[0], step_ref[1]
    cosine = cos_b * cos_s - sin_b * sin_s
    sine = sin_b * cos_s + cos_b * sin_s
    lane = lax.broadcasted_iota(jnp.int32, sine.shape, 1)
    first_half = lane < HD // 2
    sine_up = jnp.where(jnp.logical_and(lane >= HD // 2, lane < HD), sine, 0.0)
    return cosine, sine_up, jnp.where(first_half, -sine, 0.0)


class LineSum:
    def __init__(self, n, mine, out_core, in_core, out_line, in_line, total, sems):
        self.n, self.mine, self.out_core, self.in_core = n, mine, out_core, in_core
        self.out_line, self.in_line, self.total = out_line, in_line, total
        self.core_send, self.core_recv, self.line_send, self.line_recv = sems
        self.d, self.c, self.f = place()
        self.here = at_device(self.d, self.c, self.f)

    def give(self, at, both):
        d = self.d
        low = both.astype(jnp.bfloat16)

        @pl.when(d == 0)
        def _():
            self.mine[at] = low[0]
            self.out_core[at] = low[1]

        @pl.when(d != 0)
        def _():
            self.mine[at] = low[1]
            self.out_core[at] = low[0]

        remote(
            self.out_core.at[at], self.in_core.at[at], self.core_send.at[at], self.core_recv.at[at], at_device(1 - d, self.c, self.f)
        ).start()

    def step(self, at):
        n, d, c, f = self.n, self.d, self.c, self.f
        arrived(self.in_core.at[at], self.core_recv.at[at], self.here)
        self.total[...] = self.mine[at].astype(jnp.float32) + self.in_core[at].astype(jnp.float32)

        @pl.when(jnp.logical_and(at <= c, c < n - 1))
        def _():
            arrived(self.in_line.at[0, at], self.line_recv.at[0, at], self.here)
            self.total[...] += self.in_line[0, at].astype(jnp.float32)

        @pl.when(jnp.logical_and(at >= c, c > 0))
        def _():
            arrived(self.in_line.at[1, at], self.line_recv.at[1, at], self.here)
            self.total[...] += self.in_line[1, at].astype(jnp.float32)

        @pl.when(at != c)
        def _():
            self.out_line[at] = self.total[...].astype(jnp.bfloat16)

        @pl.when(at < c)
        def _():
            remote(
                self.out_line.at[at], self.in_line.at[0, at], self.line_send.at[at], self.line_recv.at[0, at], at_device(d, c - 1, f)
            ).start()

        @pl.when(at > c)
        def _():
            remote(
                self.out_line.at[at], self.in_line.at[1, at], self.line_send.at[at], self.line_recv.at[1, at], at_device(d, c + 1, f)
            ).start()

    def finish(self):
        for at in range(self.n):
            left(self.out_core.at[at], self.core_send.at[at], self.here)

            @pl.when(at != self.c)
            def _():
                left(self.out_line.at[at], self.line_send.at[at], self.here)

    @staticmethod
    def scratch(ctx, rows):
        low = jnp.bfloat16
        dma = pltpu.SemaphoreType.DMA
        return [
            VM((ctx, rows, D), low), VM((ctx, rows, D), low), VM((ctx, rows, D), low), VM((ctx, rows, D), low),
            VM((2, ctx, rows, D), low), VM((rows, D), jnp.float32),
            dma((ctx,)), dma((ctx,)), dma((ctx,)), dma((2, ctx)),
        ]


def down_route(d, c):
    return (lax.rem(c, 2), 2 * d + c // 2), (c // 2, 2 * lax.rem(c, 2) + d)


def near_devices(sizes):
    dp, ctx, fs = sizes
    d, c, f = place()
    yes = c >= 0
    found = [(at_device(1 - d, c, f), yes)]
    for step in range(1, fs):
        for core in range(dp):
            found.append((at_device(core, c, lax.rem(f + step, fs)), yes))
    found.append((at_device(d, c - 1, f), c > 0))
    found.append((at_device(d, c + 1, f), c < ctx - 1))
    for core, place_ in down_route(d, c):
        found.append((at_device(core, place_, f), jnp.logical_or(core != d, place_ != c)))
    return found


def tell_near(sizes):
    barrier = pltpu.get_barrier_semaphore()
    for device, counts in near_devices(sizes):

        @pl.when(counts)
        def _():
            pl.semaphore_signal(barrier, inc=1, device_id=device, device_id_type=MESH)


def hear_near(sizes):
    peers = sum(jnp.where(counts, 1, 0) for _, counts in near_devices(sizes))
    pl.semaphore_wait(pltpu.get_barrier_semaphore(), peers)


def middle_kernel(
    sizes, hidden, parts, sent, att_ref, x_ref, dy_ref, gains_ref, proj_ref, down_ref, gate_up_ref, gate_up_part_ref, dy_all_ref,
    resid_out, d_resid_out, gain_out, partial_out, unit_out, grad_proj_out, up_land, down_land,
    att, dy_all, proj, down, gate_up, resid, own_two, normed_two, act, d_both, part_stage, own_d, d_resid_all, d_stage, unit,
    grad_up, grad_down, grad_proj, grad_proj_low,
    in_sem, gu_send, gu_recv, m_send, m_recv, m_pass, two_send, two_recv, two_local, dr_send, dr_recv, dr_local, u_send, u_recv,
    out_sem, part_sem, gup_send, gup_recv, gdn_send, gdn_recv,
    *sums,
):
    dp, ctx, fs = sizes
    d, c, f = place()
    here = at_device(d, c, f)
    rows = x_ref.shape[0]
    span = rows // 2
    both_rows = dp * rows
    half = hidden // 2
    line_sum = LineSum(ctx, *sums[:6], sums[6:10])
    second_sum = LineSum(ctx, *sums[10:16], sums[16:20])
    part_rows = D // parts
    tell_near(sizes)

    att_copy = pltpu.make_async_copy(att_ref, att, in_sem.at[0])
    dy_copy = pltpu.make_async_copy(dy_all_ref, dy_all, in_sem.at[1])
    part_copy = pltpu.make_async_copy(gate_up_part_ref, gate_up.at[:, 0 : part_rows * sent], in_sem.at[2])
    att_copy.start()
    proj[...] = jnp.zeros_like(proj)
    each = proj_ref.shape[1]
    proj_copies = []
    for slot in range(fs):
        start = slot // 2 * LANES + slot % 2 * each
        proj_copies.append(pltpu.make_async_copy(proj_ref.at[slot], proj.at[start : start + each], in_sem.at[3 + slot]))
        proj_copies[-1].start()
    dy_copy.start()
    part_copy.start()
    hear_near(sizes)

    (to_core, to_ctx), _ = down_route(d, c)
    stays = jnp.logical_and(to_core == d, to_ctx == c)

    @pl.when(jnp.logical_not(stays))
    def _():
        remote(down_ref, down.at[f], m_send, m_recv.at[f], at_device(to_core, to_ctx, f)).start()

    @pl.when(stays)
    def _():
        pltpu.make_async_copy(down_ref, down.at[f], m_recv.at[f]).start()

    gu_core = f // 2
    gu_slot = 2 * d + lax.rem(f, 2)
    rest = slice(part_rows * sent, D)
    for to in range(fs):
        own_place = jnp.logical_and(gu_core == d, f == to)

        @pl.when(jnp.logical_not(own_place))
        def _():
            remote(gate_up_ref.at[rest], gate_up.at[gu_slot, rest], gu_send.at[to], gu_recv.at[gu_slot], at_device(gu_core, c, to)).start()

        @pl.when(own_place)
        def _():
            pltpu.make_async_copy(gate_up_ref.at[rest], gate_up.at[gu_slot, rest], gu_recv.at[gu_slot]).start()

    att_copy.wait()
    for copy in proj_copies:
        copy.wait()

    def project(step, carry):
        at = ordered(c, ctx - 1 - step, ctx)
        terms = jnp.dot(att[:, at].reshape(both_rows, 2 * LANES), proj[...], preferred_element_type=jnp.float32)
        line_sum.give(at, terms.reshape(dp, rows, D))
        return carry

    lax.fori_loop(0, ctx, project, 0)

    line_sum.step(ordered(c, ctx - 1, ctx))
    line_sum.step(ordered(c, ctx - 2, ctx))
    arrived(down.at[f], m_recv.at[f], here)
    for step in range(1, fs):
        to = lax.rem(f + step, fs)
        remote(down.at[f], down.at[f], m_pass.at[step], m_recv.at[f], at_device(d, c, to)).start()

    def sum_up(step, carry):
        line_sum.step(ordered(c, ctx - 1 - step, ctx))
        return carry

    lax.fori_loop(2, ctx, sum_up, 0)
    gain = gains_ref[1:2, :]
    values = x_ref[...].astype(jnp.float32) + line_sum.total[...]
    resid[...] = values
    scale = lax.rsqrt(jnp.mean(values * values, axis=-1, keepdims=True) + EPS)
    own_two[...] = (values * scale * gain).astype(jnp.bfloat16)
    resid_copy = pltpu.make_async_copy(resid, resid_out, out_sem.at[0])
    resid_copy.start()
    line = LineGather(ctx, own_two, normed_two, two_send, two_recv, two_local)
    line.start()
    line_sum.finish()
    for slot in range(4):
        arrived(gate_up.at[slot, rest], gu_recv.at[slot], here)
    dy_copy.wait()
    part_copy.wait()
    for step in range(1, fs):
        other = lax.rem(f + step, fs)
        arrived(down.at[other], m_recv.at[other], here)
    pltpu.make_async_copy(line.own, line.slot(c), line.local).wait()

    def mlp(step, carry):
        at = ordered(c, step, ctx)

        line.take(at)
        inputs = normed_two[:, at].reshape(both_rows, D)
        dy_rows = dy_all[:, at].reshape(both_rows, D)
        for part in range(2):
            cols = slice(part * half, (part + 1) * half)
            gate = jnp.dot(inputs, gate_up[part], preferred_element_type=jnp.float32)
            up = jnp.dot(inputs, gate_up[2 + part], preferred_element_type=jnp.float32)
            d_act = outer(dy_rows, down[2 * part : 2 * part + 2].reshape(half, D))
            sig = 1.0 / (1.0 + jnp.exp(-gate))
            silu = gate * sig
            act[:, at, :, cols] = (silu * up).astype(jnp.bfloat16).reshape(dp, rows, half)
            d_gate = d_act * up * (sig * (1.0 + gate * (1.0 - sig)))
            d_both[:, at, :, cols] = d_gate.astype(jnp.bfloat16).reshape(dp, rows, half)
            d_both[:, at, :, hidden + part * half : hidden + (part + 1) * half] = (
                (d_act * silu).astype(jnp.bfloat16).reshape(dp, rows, half)
            )
        terms = outer(d_both[:, at, :, 0:half].reshape(both_rows, half), gate_up[0])
        for part in range(1, 4):
            terms += outer(d_both[:, at, :, part * half : (part + 1) * half].reshape(both_rows, half), gate_up[part])
        second_sum.give(at, terms.reshape(dp, rows, D))
        return carry

    lax.fori_loop(0, ctx, mlp, 0)

    wide_rows = D // ctx

    def push(src, dst, send, recv, core, to):
        to_self = jnp.logical_and(core == d, to == f)

        @pl.when(jnp.logical_not(to_self))
        def _():
            remote(src, dst, send, recv, at_device(core, c, to)).start()

        @pl.when(to_self)
        def _():
            pltpu.make_async_copy(src, dst, recv).start()

    def grads(step):
        first = pl.multiple_of(step * wide_rows, LANES)
        left_rows = normed_two[:, :, :, pl.ds(first, wide_rows)].reshape(dp * ctx * rows, wide_rows)
        for part in range(2):
            cols = slice(part * hidden, (part + 1) * hidden)
            terms = inner(left_rows, d_both[:, :, :, cols].reshape(dp * ctx * rows, hidden)).astype(jnp.bfloat16)
            grad_up[2 * part, pl.ds(first, wide_rows), :] = terms[:, :half]
            grad_up[2 * part + 1, pl.ds(first, wide_rows), :] = terms[:, half:]
        dy_cols = dy_all[:, :, :, pl.ds(first, wide_rows)].reshape(dp * ctx * rows, wide_rows)
        terms = inner(act[...].reshape(dp * ctx * rows, hidden), dy_cols).astype(jnp.bfloat16)
        grad_down[:, :, pl.ds(first, wide_rows)] = terms.reshape(fs, hidden // fs, wide_rows)
        for slot in range(4):
            push(
                grad_up.at[slot, pl.ds(first, wide_rows)], up_land.at[f, pl.ds(first, wide_rows)],
                gup_send.at[slot, step], gup_recv.at[f, step], slot // 2, 2 * d + slot % 2,
            )
            push(
                grad_down.at[slot, :, pl.ds(first, wide_rows)], down_land.at[f, :, pl.ds(first, wide_rows)],
                gdn_send.at[slot, step], gdn_recv.at[f, step], d, slot,
            )

    def sum_two(step, carry):
        second_sum.step(ordered(c, ctx - 1 - step, ctx))

        @pl.when(step < ctx - 1)
        def _():
            grads(step)

        return carry

    lax.fori_loop(0, ctx, sum_two, 0)
    values = resid[...]
    scale = lax.rsqrt(jnp.mean(values * values, axis=-1, keepdims=True) + EPS)
    incoming = second_sum.total[...]
    weighted = incoming * gain
    mean = jnp.mean(weighted * values, axis=-1, keepdims=True)
    d_resid = dy_ref[...].astype(jnp.float32) + scale * weighted - values * (scale * scale * scale) * mean
    own_d[...] = d_resid.astype(jnp.bfloat16)
    d_resid_out[...] = d_resid
    gain_out[...] = jnp.broadcast_to(jnp.sum(incoming * values * scale, axis=0, keepdims=True), gain_out.shape)
    d_line = LineGather(ctx, own_d, d_resid_all, dr_send, dr_recv, dr_local)
    d_line.start()
    line.finish_sends()
    second_sum.finish()
    grads(ctx - 1)
    pltpu.make_async_copy(d_line.own, d_line.slot(c), d_line.local).wait()
    grad_proj[...] = jnp.zeros_like(grad_proj)

    def back(step, carry):
        at = ordered(c, step, ctx)

        d_line.take(at)
        incoming = d_resid_all[:, at].reshape(both_rows, D)
        d_att = outer(incoming, proj[...]).astype(jnp.bfloat16)
        d_stage[at] = d_att.reshape(2 * dp, span, 2 * LANES)
        for to in range(2 * dp):

            @pl.when(to != f)
            def _():
                remote(d_stage.at[at, to], unit.at[at, f], u_send.at[at, to], u_recv.at[at, f], at_device(d, c, to)).start()

            @pl.when(to == f)
            def _():
                unit[at, f] = d_stage[at, to]

        grad_proj[...] += inner(att[:, at].reshape(both_rows, 2 * LANES), incoming)

        outputs = jnp.dot(act[:, at].reshape(both_rows, hidden), down[...].reshape(hidden, D), preferred_element_type=jnp.float32)
        slot = lax.rem(step, 2)

        @pl.when(step >= 2)
        def _():
            pltpu.make_async_copy(part_stage.at[slot], partial_out.at[:, at], part_sem.at[slot]).wait()

        part_stage[slot] = outputs.reshape(dp, rows, D).astype(jnp.bfloat16)
        pltpu.make_async_copy(part_stage.at[slot], partial_out.at[:, at], part_sem.at[slot]).start()
        return carry

    lax.fori_loop(0, ctx, back, 0)
    for slot in range(fs):
        start = slot // 2 * LANES + slot % 2 * each
        grad_proj_low[slot] = grad_proj[start : start + each, :].astype(jnp.bfloat16)
    grad_proj_copy = pltpu.make_async_copy(grad_proj_low, grad_proj_out, out_sem.at[1])
    grad_proj_copy.start()
    for at in range(ctx):
        for step in range(1, fs):
            other = lax.rem(f + step, fs)
            arrived(unit.at[at, other], u_recv.at[at, other], here)
    unit_copy = pltpu.make_async_copy(unit, unit_out, out_sem.at[2])
    unit_copy.start()
    d_line.finish_sends()
    for at in range(ctx):
        for to in range(fs):

            @pl.when(to != f)
            def _():
                left(d_stage.at[at, to], u_send.at[at, to], here)

    for to in range(fs):

        @pl.when(jnp.logical_not(jnp.logical_and(gu_core == d, f == to)))
        def _():
            left(gate_up_ref.at[rest], gu_send.at[to], here)

    @pl.when(jnp.logical_not(stays))
    def _():
        left(down_ref, m_send, here)

    for step in range(1, fs):
        left(down.at[f], m_pass.at[step], here)

    def settle(step, carry):
        first = pl.multiple_of(step * wide_rows, LANES)
        for slot in range(4):
            up_src, down_src = grad_up.at[slot, pl.ds(first, wide_rows)], grad_down.at[slot, :, pl.ds(first, wide_rows)]
            arrived(up_land.at[slot, pl.ds(first, wide_rows)], gup_recv.at[slot, step], here)
            arrived(down_land.at[slot, :, pl.ds(first, wide_rows)], gdn_recv.at[slot, step], here)

            @pl.when(jnp.logical_or(slot // 2 != d, 2 * d + slot % 2 != f))
            def _():
                left(up_src, gup_send.at[slot, step], here)

            @pl.when(slot != f)
            def _():
                left(down_src, gdn_send.at[slot, step], here)

        return carry

    lax.fori_loop(0, ctx, settle, 0)
    for slot in range(2):
        pltpu.make_async_copy(part_stage.at[slot], partial_out.at[:, 0], part_sem.at[slot]).wait()
    for copy in (resid_copy, grad_proj_copy, unit_copy):
        copy.wait()


def middle(sizes, parts, sent, att, x, dy, gains, proj, w_down, w_gate_up, gate_up_part, dy_all):
    dp, ctx, fs = sizes
    rows = x.shape[0]
    span = rows // 2
    hidden = FF // (dp * ctx)
    low, wide_t = jnp.bfloat16, jnp.float32
    dma = pltpu.SemaphoreType.DMA
    any_spec, vm_spec = pl.BlockSpec(memory_space=ANY), pl.BlockSpec(memory_space=VM)
    shapes = (
        jax.ShapeDtypeStruct((rows, D), wide_t),
        jax.ShapeDtypeStruct((rows, D), wide_t),
        jax.ShapeDtypeStruct((8, D), wide_t),
        jax.ShapeDtypeStruct((dp, ctx, rows, D), low),
        jax.ShapeDtypeStruct((ctx, fs, span, 2 * LANES), low),
        jax.ShapeDtypeStruct(proj.shape, low),
        jax.ShapeDtypeStruct((fs, D, hidden // 2), low),
        jax.ShapeDtypeStruct((fs, hidden // fs, D), low),
    )
    return pl.pallas_call(
        functools.partial(middle_kernel, sizes, hidden, parts, sent),
        name="middle",
        out_shape=shapes,
        in_specs=[any_spec, vm_spec, vm_spec, vm_spec, any_spec, vm_spec, vm_spec, any_spec, any_spec],
        out_specs=[any_spec, vm_spec, vm_spec] + [any_spec] * 5,
        scratch_shapes=[
            VM((dp, ctx, rows, 2 * LANES), low),
            VM((dp, ctx, rows, D), low),
            VM((2 * LANES, D), low),
            VM((fs, hidden // fs, D), low),
            VM((4, D, hidden // 2), low),
            VM((rows, D), wide_t),
            VM((rows, D), low),
            VM((dp, ctx, rows, D), low),
            VM((dp, ctx, rows, hidden), low),
            VM((dp, ctx, rows, 2 * hidden), low),
            VM((2, dp, rows, D), low),
            VM((rows, D), low),
            VM((dp, ctx, rows, D), low),
            VM((ctx, 2 * dp, span, 2 * LANES), low),
            VM((ctx, fs, span, 2 * LANES), low),
            VM((4, D, hidden // 2), low),
            VM((fs, hidden // fs, D), low),
            VM((2 * LANES, D), wide_t),
            VM(proj.shape, low),
            dma((3 + fs,)), dma((fs,)), dma((4,)), dma, dma((fs,)), dma((fs,)),
            dma((3, ctx)), dma((dp, ctx)), dma,
            dma((3, ctx)), dma((dp, ctx)), dma,
            dma((ctx, 2 * dp)), dma((ctx, fs)),
            dma((3,)), dma((2,)),
            dma((4, ctx)), dma((fs, ctx)), dma((fs, ctx)), dma((fs, ctx)),
        ] + LineSum.scratch(ctx, rows) + LineSum.scratch(ctx, rows),
        compiler_params=pltpu.CompilerParams(collective_id=2, has_side_effects=True, vmem_limit_bytes=63 * 1024 * 1024),
    )(att, x, dy, gains, proj, w_down, w_gate_up, gate_up_part, dy_all)


def last_kernel(
    sizes, x_ref, gains_ref, block_ref, step_ref, resid_ref, d_resid_ref, gain_two_ref, proj_ref,
    unit_ref, d_unit_ref, normed_ref, wide_ref, partial_ref, up_land_ref, down_land_ref,
    out_ref, d_x_ref, gains_out, qkv_out, proj_out, up_out, down_out,
    unit, d_unit, d_k, d_v, stage, mixed, normed, wide, grad_heads,
    up_land, down_land, proj_land, q_land, kv_land, down_sum, proj_sum, kv_sum, down_last, proj_last, kv_last, gain_vec, gain_stage, gain_land,
    in_sem, proj_send, proj_recv, head_send, head_recv, move_send, move_recv,
    u_send, u_recv, g_send, g_recv, mine_sem,
    *sums,
):
    dp, ctx, fs = sizes
    n = dp * ctx * fs
    d, c, f = place()
    here = at_device(d, c, f)
    me = (d * ctx + c) * fs + f
    rows = x_ref.shape[0]
    span = rows // 2
    both_rows = dp * rows
    low, wide_t = jnp.bfloat16, jnp.float32
    loads = [
        pltpu.make_async_copy(src, dst, in_sem.at[index])
        for index, (src, dst) in enumerate((
            (unit_ref, unit), (d_unit_ref, d_unit), (normed_ref, normed), (wide_ref, wide), (down_land_ref, down_land), (up_land_ref, up_land),
        ))
    ]
    tell_all(sizes)
    for load in loads:
        load.start()
    out_sum = LineSum(ctx, *sums[:6], sums[6:10])
    in_sum = LineSum(ctx, *sums[10:16], sums[16:20])
    for at in range(ctx):
        pltpu.make_async_copy(partial_ref.at[d, at], out_sum.mine.at[at], mine_sem.at[at]).start()
    d_k[...] = jnp.zeros_like(d_k)
    d_v[...] = jnp.zeros_like(d_v)
    hear_all(sizes)

    for at in range(ctx):
        remote(
            partial_ref.at[1 - d, at], out_sum.in_core.at[at], out_sum.core_send.at[at], out_sum.core_recv.at[at], at_device(1 - d, c, f)
        ).start()

    def push(src, land, send, recv, core, fs_to):
        to_self = jnp.logical_and(core == d, fs_to == f)

        @pl.when(jnp.logical_not(to_self))
        def _():
            remote(src, land.at[f], send, recv.at[f], at_device(core, c, fs_to)).start()

        @pl.when(to_self)
        def _():
            pltpu.make_async_copy(src, land.at[f], recv.at[f]).start()

    def pushed(src, send, core, fs_to):
        @pl.when(jnp.logical_not(jnp.logical_and(core == d, fs_to == f)))
        def _():
            left(src, send, here)

    def sum_of(land):
        total = land[0].astype(wide_t)
        for source in range(1, fs):
            total += land[source].astype(wide_t)
        return total

    _, (own_core, own_ctx) = down_route(d, c)
    stays = jnp.logical_and(own_core == d, own_ctx == c)

    def move(index, src, dst):
        @pl.when(jnp.logical_not(stays))
        def _():
            remote(src, dst, move_send.at[index], move_recv.at[index], at_device(own_core, own_ctx, f)).start()

        @pl.when(stays)
        def _():
            pltpu.make_async_copy(src, dst, move_recv.at[index]).start()

    loads[4].wait()
    down_sum[...] = sum_of(down_land).astype(low)
    move(0, down_sum, down_last)
    loads[0].wait()
    loads[1].wait()
    block = fs * span

    def unturn(values, at):
        up = pltpu.roll(values, HD // 2, 1)
        down = pltpu.roll(values, LANES - HD // 2, 1)
        pieces = []
        for index in range(fs):
            own = slice(index * span, (index + 1) * span)
            cosine, sine_up, sine_down = turns(block_ref, step_ref, at * fs + index)
            pieces.append(values[own] * cosine - up[own] * sine_up - down[own] * sine_down)
        return jnp.concatenate(pieces, axis=0).reshape(fs, span, LANES)

    for at in reversed(range(ctx)):
        keys = block * (at + 1)
        k_rows = unit[0 : at + 1, :, :, 2 * LANES : 3 * LANES].reshape(keys, LANES)
        v_rows = unit[0 : at + 1, :, :, 3 * LANES : 4 * LANES].reshape(keys, LANES)
        allowed = lax.broadcasted_iota(jnp.int32, (block, keys), 1) <= block * at + lax.broadcasted_iota(
            jnp.int32, (block, keys), 0
        )
        for head in range(2):
            lanes = slice(head * LANES, (head + 1) * LANES)
            q_rows = unit[at, :, :, lanes].reshape(block, LANES)
            d_rows = d_unit[at, :, :, lanes].reshape(block, LANES)
            scores = jnp.where(allowed, outer(q_rows, k_rows) * FACTOR, NEG)
            weights = jnp.exp(scores - jnp.max(scores, axis=-1, keepdims=True))
            probs = weights / jnp.sum(weights, axis=-1, keepdims=True)
            d_probs = outer(d_rows, v_rows)
            delta = jnp.sum(probs * d_probs, axis=-1, keepdims=True)
            d_scores = (probs * (d_probs - delta)).astype(low)
            d_q = jnp.dot(d_scores, k_rows, preferred_element_type=wide_t) * FACTOR
            stage[at, :, :, lanes] = unturn(d_q, at).astype(low)
            d_k[0:keys, :] += inner(d_scores, q_rows) * FACTOR
            d_v[0:keys, :] += inner(probs.astype(low), d_rows)
        stage[at, :, :, 2 * LANES : 3 * LANES] = unturn(d_k[block * at : keys, :], at).astype(low)
        stage[at, :, :, 3 * LANES : 4 * LANES] = d_v[block * at : keys, :].astype(low).reshape(fs, span, LANES)
        for to in range(fs):

            @pl.when(to != f)
            def _():
                remote(
                    stage.at[at, to], mixed.at[f // 2, at, lax.rem(f, 2)], u_send.at[at, to], u_recv.at[f, at], at_device(d, c, to)
                ).start()

            @pl.when(to == f)
            def _():
                mixed[f // 2, at, lax.rem(f, 2)] = stage[at, to]

    for slot in range(fs):
        push(proj_ref.at[slot], proj_land, proj_send.at[slot], proj_recv, d, slot)
    loads[2].wait()
    loads[3].wait()

    def give(step, carry):
        at = ordered(c, ctx - 1 - step, ctx)
        for step_ in range(1, fs):
            other = lax.rem(f + step_, fs)
            arrived(mixed.at[other // 2, at, lax.rem(other, 2)], u_recv.at[other, at], here)
        terms = jnp.dot(mixed[:, at].reshape(both_rows, 4 * LANES), wide[...], preferred_element_type=wide_t)
        in_sum.give(at, terms.reshape(dp, rows, D))
        return carry

    lax.fori_loop(0, ctx, give, 0)
    in_sum.step(ordered(c, ctx - 1, ctx))

    every = dp * ctx * rows
    k_relay = 2 * lax.rem(c, 2) + d
    relays = (k_relay, lax.rem(k_relay + 2, fs))
    for slot in (2, 3, 0, 1):
        heads = inner(mixed[:, :, :, :, slot * LANES : (slot + 1) * LANES].reshape(every, LANES), normed[...].reshape(every, D))
        grad_heads[slot] = heads[:HD].astype(low)
        if slot < 2:
            push(grad_heads.at[slot], q_land, head_send.at[slot], head_recv.at[0], 0, 2 * d + slot)
        else:
            push(grad_heads.at[slot], kv_land.at[slot - 2], head_send.at[slot], head_recv.at[slot - 1], d, relays[slot - 2])

    def steps(step, carry):
        at = ordered(c, ctx - 1 - step, ctx)
        pltpu.make_async_copy(partial_ref.at[d, at], out_sum.mine.at[at], mine_sem.at[at]).wait()
        out_sum.step(at)

        @pl.when(step < ctx - 2)
        def _():
            in_sum.step(ordered(c, ctx - 2 - step, ctx))

        return carry

    lax.fori_loop(0, ctx, steps, 0)
    out_ref[...] = (resid_ref[...] + out_sum.total[...]).astype(low)
    for source in range(fs):
        arrived(proj_land.at[source], proj_recv.at[source], here)
    proj_sum[...] = sum_of(proj_land).astype(low)
    move(1, proj_sum, proj_last)

    def kv_route(slot):
        owner, owner_f = slot * 2 + c // 2, k_relay
        return owner, owner_f, jnp.logical_or(jnp.logical_or(d != 1, owner != c), owner_f != f)

    for slot in range(2):
        owner, owner_f, away = kv_route(slot)

        @pl.when(f == relays[slot])
        def _():
            for source in range(fs):
                arrived(kv_land.at[slot, source], head_recv.at[1 + slot, source], here)
            kv_sum[slot] = sum_of(kv_land.at[slot]).astype(low)

            @pl.when(away)
            def _():
                remote(kv_sum.at[slot], kv_last, move_send.at[2 + slot], move_recv.at[2], at_device(1, owner, owner_f)).start()

            @pl.when(jnp.logical_not(away))
            def _():
                pltpu.make_async_copy(kv_sum.at[slot], kv_last, move_recv.at[2]).start()

    loads[5].wait()
    up_out[...] = sum_of(up_land)
    in_sum.step(c)

    gain = gains_ref[0:1, :]
    values = x_ref[...].astype(wide_t)
    scale = lax.rsqrt(jnp.mean(values * values, axis=-1, keepdims=True) + EPS)
    incoming = in_sum.total[...]
    weighted = incoming * gain
    mean = jnp.mean(weighted * values, axis=-1, keepdims=True)
    d_x_ref[...] = (d_resid_ref[...] + scale * weighted - values * (scale * scale * scale) * mean).astype(low)
    gain_vec[0:1, :] = jnp.sum(incoming * values * scale, axis=0, keepdims=True)
    gain_vec[1:2, :] = gain_two_ref[0:1, :]
    each = D // n
    for index in range(n):
        gain_stage[index, :, 0:each] = gain_vec[:, index * each : (index + 1) * each]
    gain_land[me] = gain_stage[me]

    def gain_to(step, carry):
        other = lax.rem(me + step, n)
        remote(
            gain_stage.at[other], gain_land.at[me], g_send.at[other], g_recv.at[me],
            at_device(other // (ctx * fs), lax.rem(other // fs, ctx), lax.rem(other, fs)),
        ).start()
        return carry

    lax.fori_loop(1, n, gain_to, 0)

    for index, dst in enumerate((down_last, proj_last)):
        arrived(dst, move_recv.at[index], here)
    down_out[...] = down_last[...].astype(wide_t)
    proj_out[...] = proj_last[...].astype(wide_t)

    @pl.when(d == 0)
    def _():
        for source in range(fs):
            arrived(q_land.at[source], head_recv.at[0, source], here)
        qkv_out[...] = sum_of(q_land)

    @pl.when(d == 1)
    def _():
        arrived(kv_last, move_recv.at[2], here)
        qkv_out[...] = kv_last[...].astype(wide_t)

    def gain_from(step, carry):
        other = lax.rem(me + step, n)
        arrived(gain_land.at[other], g_recv.at[other], here)
        return carry

    lax.fori_loop(1, n, gain_from, 0)
    total = gain_land[0]
    for index in range(1, n):
        total += gain_land[index]
    gains_out[...] = total

    for slot in range(fs):
        pushed(proj_ref.at[slot], proj_send.at[slot], d, slot)
    for slot in range(2):
        pushed(grad_heads.at[slot], head_send.at[slot], 0, 2 * d + slot)
        pushed(grad_heads.at[2 + slot], head_send.at[2 + slot], d, relays[slot])
        away = kv_route(slot)[2]

        @pl.when(jnp.logical_and(f == relays[slot], away))
        def _():
            left(kv_sum.at[slot], move_send.at[2 + slot], here)

        @pl.when(jnp.logical_not(stays))
        def _():
            left((down_sum, proj_sum)[slot], move_send.at[slot], here)

    for at in range(ctx):
        for to in range(fs):

            @pl.when(to != f)
            def _():
                left(stage.at[at, to], u_send.at[at, to], here)

        left(partial_ref.at[1 - d, at], out_sum.core_send.at[at], here)

        @pl.when(at != c)
        def _():
            left(out_sum.out_line.at[at], out_sum.line_send.at[at], here)

    in_sum.finish()

    def gain_left(step, carry):
        other = lax.rem(me + step, n)
        left(gain_stage.at[other], g_send.at[other], here)
        return carry

    lax.fori_loop(1, n, gain_left, 0)


def last(sizes, x, gains, tables, resid, d_resid, gain_two, grad_proj, unit, d_unit, normed, wide, partial, up_land, down_land):
    dp, ctx, fs = sizes
    n = dp * ctx * fs
    rows = x.shape[0]
    span = rows // 2
    low, wide_t = jnp.bfloat16, jnp.float32
    dma = pltpu.SemaphoreType.DMA
    any_spec, vm_spec = pl.BlockSpec(memory_space=ANY), pl.BlockSpec(memory_space=VM)
    down_rows, proj_rows, half = down_land.shape[1], grad_proj.shape[1], up_land.shape[2]
    shapes = (
        jax.ShapeDtypeStruct((rows, D), low),
        jax.ShapeDtypeStruct((rows, D), low),
        jax.ShapeDtypeStruct((8, LANES), wide_t),
        jax.ShapeDtypeStruct((HD, D), wide_t),
        jax.ShapeDtypeStruct((proj_rows, D), wide_t),
        jax.ShapeDtypeStruct((D, half), wide_t),
        jax.ShapeDtypeStruct((down_rows, D), wide_t),
    )
    return pl.pallas_call(
        functools.partial(last_kernel, sizes),
        name="last",
        out_shape=shapes,
        in_specs=[vm_spec] * 8 + [any_spec] * 7,
        out_specs=[vm_spec] * 7,
        scratch_shapes=[
            VM(unit.shape, low),
            VM(d_unit.shape, low),
            VM((ctx * fs * span, LANES), wide_t),
            VM((ctx * fs * span, LANES), wide_t),
            VM((ctx, fs, span, 4 * LANES), low),
            VM((dp, ctx, 2, span, 4 * LANES), low),
            VM(normed.shape, low),
            VM(wide.shape, low),
            VM((4, HD, D), low),
            VM((fs, D, half), low),
            VM((fs, down_rows, D), low),
            VM((fs, proj_rows, D), low),
            VM((fs, HD, D), low),
            VM((2, fs, HD, D), low),
            VM((down_rows, D), low),
            VM((proj_rows, D), low),
            VM((2, HD, D), low),
            VM((down_rows, D), low),
            VM((proj_rows, D), low),
            VM((HD, D), low),
            VM((8, D), wide_t),
            VM((n, 8, LANES), wide_t),
            VM((n, 8, LANES), wide_t),
            dma((6,)), dma((fs,)), dma((fs,)),
            dma((4,)), dma((3, fs)), dma((4,)), dma((3,)),
            dma((ctx, fs)), dma((fs, ctx)), dma((n,)), dma((n,)), dma((ctx,)),
        ] + LineSum.scratch(ctx, rows) + LineSum.scratch(ctx, rows),
        compiler_params=pltpu.CompilerParams(collective_id=3, has_side_effects=True, vmem_limit_bytes=63 * 1024 * 1024),
    )(x, gains, *tables, resid, d_resid, gain_two, grad_proj, unit, d_unit, normed, wide, partial, up_land, down_land)


def on_device(tokens, cotangent, attn_gain, w_qkv, w_out, mlp_gain, w_gate_up, w_down):
    dp, ctx, fs = where = tuple(lax.axis_size(name) for name in ("dp", "ctx", "fsdp"))
    mb, _, span, _ = tokens.shape
    rows = mb * span
    x = tokens.reshape(rows, D)
    dy = cotangent.reshape(rows, D)
    each = attn_gain.shape[0]
    gain_rows = jnp.concatenate([attn_gain[None], mlp_gain[None]]).astype(jnp.float32)
    gain_rows = jnp.pad(gain_rows, ((0, 6), (0, LANES - each)))
    tables = angle_tables(ctx * fs, span)
    parts, sent = 4, 3
    normed, unit, att, qkv, gains, dy_all, proj, gate_up = first(
        where, parts, sent, x, gain_rows, w_qkv.T, *tables, dy, w_out, w_gate_up
    )
    att = att.reshape(dp, ctx, rows, 2 * LANES)
    resid, d_resid, grad_two, partial, d_unit, grad_proj, up_land, down_land = middle(
        where, parts, sent, att, x, dy, gains, proj, w_down, w_gate_up, gate_up, dy_all
    )
    block_out, grad_tokens, gain_grads, grad_qkv, grad_out, grad_gate_up, grad_down = last(
        where, x, gains, tables, resid, d_resid, grad_two, grad_proj, unit, d_unit, normed, qkv, partial, up_land, down_land
    )
    return (
        block_out.reshape(tokens.shape),
        grad_tokens.reshape(tokens.shape),
        gain_grads[0, :each],
        grad_qkv.T,
        grad_out,
        gain_grads[1, :each],
        grad_gate_up,
        grad_down,
    )


def fits(mesh):
    return mesh.shape["dp"] == 2 and mesh.shape["ctx"] == 4 and mesh.shape["fsdp"] == 4


def solution(mesh):
    placed = (
        P(None, "dp", ("ctx", "fsdp"), None),
        P(None, "dp", ("ctx", "fsdp"), None),
        P(("dp", "ctx", "fsdp")),
        P(None, ("dp", "ctx", "fsdp")),
        P(("dp", "ctx", "fsdp"), None),
        P(("dp", "ctx", "fsdp")),
        P(None, ("dp", "ctx", "fsdp")),
        P(("dp", "ctx", "fsdp"), None),
    )
    return jax.shard_map(
        on_device if fits(mesh) else on_device_gathered,
        mesh=mesh,
        in_specs=placed,
        out_specs=(
            P(None, "dp", ("ctx", "fsdp"), None),
            P(None, "dp", ("ctx", "fsdp"), None),
            P(("dp", "ctx", "fsdp")),
            P(None, ("dp", "ctx", "fsdp")),
            P(("dp", "ctx", "fsdp"), None),
            P(("dp", "ctx", "fsdp")),
            P(None, ("dp", "ctx", "fsdp")),
            P(("dp", "ctx", "fsdp"), None),
        ),
        check_vma=False,
    )
```

```python
import functools

import jax
import jax.numpy as jnp
from jax import lax
from jax.experimental import pallas as pl
from jax.experimental.pallas import tpu as pltpu
from jax.sharding import PartitionSpec as P

D = 1536
H = 16
KVH = 8
HD = 96
FF = 4096


EPS = 1e-05
THETA = 100000.0
NEG = -1e30


def in_blocks(value, dim, length):
    lengths = value.shape
    pieces = value.reshape(*lengths[:dim], length, lengths[dim] // length, *lengths[dim + 1 :])
    return jnp.moveaxis(pieces, dim, 0)


def sum_at_owner(value, axis, dim):
    pieces = in_blocks(value, dim, lax.axis_size(axis))
    arrived = lax.all_to_all(pieces, axis, split_axis=0, concat_axis=0, tiled=True)
    return arrived.astype(jnp.float32).sum(axis=0)


def side_by_side(arrays, axis, dim, along):
    both = jnp.concatenate(arrays, axis=along)
    whole, at, finished = (sum_at_owner(both, axis, dim), 0, [])
    for a in arrays:
        finished.append(lax.slice_in_dim(whole, at, at + a.shape[along], axis=along))
        at += a.shape[along]
    return tuple(finished)


def rms_norm(values, gain_vec):
    return values * lax.rsqrt(jnp.mean(values * values, axis=-1, keepdims=True) + EPS) * gain_vec


def tables(start, length, width):
    half_width = width // 2
    frequency = THETA ** (-(jnp.arange(half_width, dtype=jnp.float32) * 2.0) / width)
    angles = (start + jnp.arange(length, dtype=jnp.int32)).astype(jnp.float32)[:, None] * frequency[
        None, :
    ]
    return (jnp.cos(angles), jnp.sin(angles))


def rotate(values, cosine, sine_table):
    half_width = values.shape[-1] // 2
    first_half = values[..., :half_width]
    second_half = values[..., half_width:]
    cos_b = cosine[:, None, :]
    sin_b = sine_table[:, None, :]
    return jnp.concatenate(
        [first_half * cos_b - second_half * sin_b, second_half * cos_b + first_half * sin_b],
        axis=-1,
    )


def swiglu(both):
    return jax.nn.silu(both[:, :FF]) * both[:, FF:]


def inner(left, right):
    return lax.dot_general(
        left, right, (((0,), (0,)), ((), ())), preferred_element_type=jnp.float32
    )


def outer(left, right):
    return lax.dot_general(
        left, right, (((1,), (1,)), ((), ())), preferred_element_type=jnp.float32
    )


def unchanged(state):
    return state


def on_device_gathered(tokens, cotangent, attn_gain, w_qkv, w_out, mlp_gain, w_gate_up, w_down):
    tok_count = tokens.shape[2]
    groups = H // KVH
    factor = HD ** (-0.5)
    seq_length = tok_count * lax.axis_size(("ctx", "fsdp"))
    pos_first = lax.axis_index(("ctx", "fsdp")) * tok_count
    positions = pos_first + jnp.arange(tok_count, dtype=jnp.int32)
    pos_last = pos_first + tok_count - 1
    cosine, sine_table = tables(pos_first, tok_count, HD)
    sums = [
        jnp.zeros((D,), jnp.float32),
        jnp.zeros((D, (H + 2 * KVH) * HD), jnp.float32),
        jnp.zeros((H * HD, D), jnp.float32),
        jnp.zeros((D,), jnp.float32),
        jnp.zeros((D, 2 * FF), jnp.float32),
        jnp.zeros((FF, D), jnp.float32),
    ]
    outputs = []
    in_grads = []
    whole = (
        lax.all_gather(attn_gain, ("dp", "ctx", "fsdp"), axis=0, tiled=True),
        lax.all_gather(w_qkv, ("dp", "ctx", "fsdp"), axis=1, tiled=True),
        lax.all_gather(w_out, ("dp", "ctx", "fsdp"), axis=0, tiled=True),
        lax.all_gather(mlp_gain, ("dp", "ctx", "fsdp"), axis=0, tiled=True),
        lax.all_gather(w_gate_up, ("dp", "ctx", "fsdp"), axis=1, tiled=True),
        lax.all_gather(w_down, ("dp", "ctx", "fsdp"), axis=0, tiled=True),
    )
    for step_index in range(tokens.shape[0]):
        gain_one, mix_qkv, mix_out, gain_two, mix_gate_up, mix_down = whole
        inputs = tokens[step_index, 0].astype(jnp.float32)
        normed = rms_norm(inputs, gain_one.astype(jnp.float32)).astype(jnp.bfloat16)
        mixed = jnp.dot(normed, mix_qkv, preferred_element_type=jnp.float32)
        queries = rotate(mixed[:, : H * HD].reshape(tok_count, H, HD), cosine, sine_table).astype(
            jnp.bfloat16
        )
        key_rows = rotate(
            mixed[:, H * HD : (H + KVH) * HD].reshape(tok_count, KVH, HD), cosine, sine_table
        )
        key_rows = key_rows.astype(jnp.bfloat16).reshape(tok_count, KVH * HD)
        value_rows = mixed[:, (H + KVH) * HD :].astype(jnp.bfloat16)
        grouped = queries.reshape(tok_count, KVH, groups, HD)
        start_state = (
            jnp.full((KVH, groups, tok_count), NEG, jnp.float32),
            jnp.zeros((KVH, groups, tok_count), jnp.float32),
            jnp.zeros((KVH, groups, tok_count, HD), jnp.float32),
        )
        piece = (
            lax.all_gather(key_rows, ("ctx", "fsdp"), axis=0, tiled=True),
            lax.all_gather(value_rows, ("ctx", "fsdp"), axis=0, tiled=True),
        )

        def work(state):
            best, total, summed = state
            key_count = piece[0].shape[0]
            keys = piece[0].reshape(key_count, KVH, HD)
            values = piece[1].reshape(key_count, KVH, HD)
            scores = (
                jnp.einsum("qkgd,tkd->kgqt", grouped, keys, preferred_element_type=jnp.float32)
                * factor
            )
            allowed = jnp.arange(key_count, dtype=jnp.int32)[None, :] <= positions[:, None]
            scores = jnp.where(allowed, scores, NEG)
            new_best = jnp.maximum(best, jnp.max(scores, axis=-1))
            weights = jnp.where(allowed, jnp.exp(scores - new_best[..., None]), 0.0)
            total = jnp.sum(weights, axis=-1)
            summed = jnp.einsum(
                "kgqt,tkd->kgqd",
                weights.astype(jnp.bfloat16),
                values,
                preferred_element_type=jnp.float32,
            )
            return (new_best, total, summed)

        best, total, summed = lax.cond(jnp.int32(0) <= pos_last, work, unchanged, start_state)
        head_out = summed / total[..., None]
        log_total = best + jnp.log(total)
        attended = (
            jnp.transpose(head_out, (2, 0, 1, 3)).reshape(tok_count, H * HD).astype(jnp.bfloat16)
        )
        resid = inputs + jnp.dot(attended, mix_out, preferred_element_type=jnp.float32)
        normed_two = rms_norm(resid, gain_two.astype(jnp.float32)).astype(jnp.bfloat16)
        both = jnp.dot(normed_two, mix_gate_up, preferred_element_type=jnp.float32)
        acted = swiglu(both).astype(jnp.bfloat16)
        result = resid + jnp.dot(acted, mix_down, preferred_element_type=jnp.float32)
        outputs.append(result.astype(jnp.bfloat16))
        gain_one, mix_qkv, mix_out, gain_two, mix_gate_up, mix_down = whole
        up_low = cotangent[step_index, 0]
        upstream = up_low.astype(jnp.float32)
        sums[5] = sums[5] + inner(acted, up_low)
        d_act = outer(up_low, mix_down)
        _, pull_glu = jax.vjp(swiglu, both)
        d_both = pull_glu(d_act)[0].astype(jnp.bfloat16)
        sums[4] = sums[4] + inner(normed_two, d_both)
        d_normed_two = outer(d_both, mix_gate_up)
        _, pull_two = jax.vjp(rms_norm, resid, gain_two.astype(jnp.float32))
        d_resid_norm, d_gain_two = pull_two(d_normed_two)
        sums[3] = sums[3] + d_gain_two
        d_resid = upstream + d_resid_norm
        d_resid_low = d_resid.astype(jnp.bfloat16)
        sums[2] = sums[2] + inner(attended, d_resid_low)
        d_attended = outer(d_resid_low, mix_out).astype(jnp.bfloat16)
        d_grouped = d_attended.reshape(tok_count, KVH, groups, HD)
        delta = jnp.einsum("qkgd,kgqd->kgq", d_grouped.astype(jnp.float32), head_out)
        zero_q = jnp.zeros((tok_count, KVH, groups, HD), jnp.float32)
        back_state = (
            zero_q,
            jnp.zeros((seq_length, KVH * HD), jnp.float32),
            jnp.zeros((seq_length, KVH * HD), jnp.float32),
        )
        attend_piece = (
            lax.all_gather(key_rows, ("ctx", "fsdp"), axis=0, tiled=True),
            lax.all_gather(value_rows, ("ctx", "fsdp"), axis=0, tiled=True),
        )

        def attend_work(state):
            key_count = attend_piece[0].shape[0]
            keys = attend_piece[0].reshape(key_count, KVH, HD)
            values = attend_piece[1].reshape(key_count, KVH, HD)
            scores = (
                jnp.einsum("qkgd,tkd->kgqt", grouped, keys, preferred_element_type=jnp.float32)
                * factor
            )
            allowed = jnp.arange(key_count, dtype=jnp.int32)[None, :] <= positions[:, None]
            scores = jnp.where(allowed, scores, NEG)
            probs = jnp.where(allowed, jnp.exp(scores - log_total[..., None]), 0.0)
            d_probs = jnp.einsum(
                "qkgd,tkd->kgqt", d_grouped, values, preferred_element_type=jnp.float32
            )
            d_scores = (probs * (d_probs - delta[..., None])).astype(jnp.bfloat16)
            grad_q = jnp.einsum(
                "kgqt,tkd->qkgd", d_scores, keys, preferred_element_type=jnp.float32
            )
            piece_k = (
                jnp.einsum("kgqt,qkgd->tkd", d_scores, grouped, preferred_element_type=jnp.float32)
                * factor
            )
            piece_v = jnp.einsum(
                "kgqt,qkgd->tkd",
                probs.astype(jnp.bfloat16),
                d_grouped,
                preferred_element_type=jnp.float32,
            )
            grad_k = piece_k.reshape(key_count, KVH * HD)
            grad_v = piece_v.reshape(key_count, KVH * HD)
            return (grad_q, grad_k, grad_v)

        back_result = lax.cond(jnp.int32(0) <= pos_last, attend_work, unchanged, back_state)
        grad_q = back_result[0]
        summed_k, summed_v = side_by_side(
            (back_result[1].astype(jnp.bfloat16), back_result[2].astype(jnp.bfloat16)),
            ("ctx", "fsdp"),
            0,
            1,
        )
        d_q_raw = rotate(grad_q.reshape(tok_count, H, HD) * factor, cosine, -sine_table).reshape(
            tok_count, H * HD
        )
        d_k_raw = rotate(summed_k.reshape(tok_count, KVH, HD), cosine, -sine_table).reshape(
            tok_count, KVH * HD
        )
        d_mixed = jnp.concatenate([d_q_raw, d_k_raw, summed_v], axis=1).astype(jnp.bfloat16)
        sums[1] = sums[1] + inner(normed, d_mixed)
        d_normed = outer(d_mixed, mix_qkv)
        _, pull_one = jax.vjp(rms_norm, inputs, gain_one.astype(jnp.float32))
        d_inputs_norm, d_gain_one = pull_one(d_normed)
        sums[0] = sums[0] + d_gain_one
        in_grads.append((d_resid + d_inputs_norm).astype(jnp.bfloat16))
    grad_gain_one, grad_qkv, grad_out, grad_gain_two, grad_gate_up, grad_down = (
        lax.psum_scatter(sums[0], ("dp", "ctx", "fsdp"), scatter_dimension=0, tiled=True),
        lax.psum_scatter(sums[1], ("dp", "ctx", "fsdp"), scatter_dimension=1, tiled=True),
        lax.psum_scatter(sums[2], ("dp", "ctx", "fsdp"), scatter_dimension=0, tiled=True),
        lax.psum_scatter(sums[3], ("dp", "ctx", "fsdp"), scatter_dimension=0, tiled=True),
        lax.psum_scatter(sums[4], ("dp", "ctx", "fsdp"), scatter_dimension=1, tiled=True),
        lax.psum_scatter(sums[5], ("dp", "ctx", "fsdp"), scatter_dimension=0, tiled=True),
    )
    block_out = jnp.stack(outputs)[:, None]
    grad_tokens = jnp.stack(in_grads)[:, None]
    return (
        block_out,
        grad_tokens,
        grad_gain_one,
        grad_qkv,
        grad_out,
        grad_gain_two,
        grad_gate_up,
        grad_down,
    )


MESH = pl.DeviceIdType.MESH
VM = pltpu.VMEM
ANY = pl.ANY


def place():
    return lax.axis_index("dp"), lax.axis_index("ctx"), lax.axis_index("fsdp")


def at_device(dp, ctx, fs):
    return {"dp": dp, "ctx": ctx, "fsdp": fs}


def remote(src, dst, send, recv, device):
    return pltpu.make_async_remote_copy(
        src_ref=src, dst_ref=dst, send_sem=send, recv_sem=recv, device_id=device, device_id_type=MESH
    )


def arrived(dst, recv, device):
    remote(dst, dst, recv, recv, device).wait_recv()


def left(src, send, device):
    remote(src, src, send, send, device).wait_send()


def tell_all(sizes):
    dp, ctx, fs = sizes
    n = dp * ctx * fs
    d, c, f = place()
    me = (d * ctx + c) * fs + f
    barrier = pltpu.get_barrier_semaphore()

    def tell(step, carry):
        other = lax.rem(me + step, n)
        pl.semaphore_signal(
            barrier,
            inc=1,
            device_id=at_device(other // (ctx * fs), lax.rem(other // fs, ctx), lax.rem(other, fs)),
            device_id_type=MESH,
        )
        return carry

    lax.fori_loop(1, n, tell, 0)


def hear_all(sizes):
    dp, ctx, fs = sizes
    pl.semaphore_wait(pltpu.get_barrier_semaphore(), dp * ctx * fs - 1)


HALVES = 2


def half(ref, index):
    rows = ref.shape[-2] // HALVES
    return ref.at[index * rows : (index + 1) * rows]


class LineGather:
    def __init__(self, n, own, whole, send, recv, local):
        self.n, self.own, self.whole, self.send, self.recv, self.local = n, own, whole, send, recv, local
        self.d, self.c, self.f = place()
        self.here = at_device(self.d, self.c, self.f)

    def slot(self, at):
        return self.whole.at[self.d, at]

    def along(self, way, block, at, part):
        to = (at_device(self.d, self.c + 1, self.f), at_device(self.d, self.c - 1, self.f), at_device(1 - self.d, self.c, self.f))[way]
        return remote(half(block, part), half(self.slot(at), part), self.send.at[way, at, part], self.recv.at[self.d, at, part], to)

    def start(self):
        c = self.c
        for part in range(HALVES):

            @pl.when(c < self.n - 1)
            def _():
                self.along(0, self.own, c, part).start()

            @pl.when(c > 0)
            def _():
                self.along(1, self.own, c, part).start()

        for part in range(HALVES):
            self.along(2, self.own, c, part).start()
        pltpu.make_async_copy(self.own, self.slot(c), self.local).start()

    def forward(self, k):
        c = self.c
        for part in range(HALVES):

            @pl.when(c - k >= 0)
            def _():
                arrived(half(self.slot(c - k), part), self.recv.at[self.d, c - k, part], self.here)

                @pl.when(c < self.n - 1)
                def _():
                    self.along(0, self.slot(c - k), c - k, part).start()

                self.along(2, self.slot(c - k), c - k, part).start()

            @pl.when(c + k < self.n)
            def _():
                arrived(half(self.slot(c + k), part), self.recv.at[self.d, c + k, part], self.here)

                @pl.when(c > 0)
                def _():
                    self.along(1, self.slot(c + k), c + k, part).start()

                self.along(2, self.slot(c + k), c + k, part).start()

    def reach(self, step):
        now = jnp.abs(ordered(self.c, step, self.n) - self.c)
        before = jnp.abs(ordered(self.c, step - 1, self.n) - self.c)

        @pl.when(jnp.logical_and(step > 0, now != before))
        def _():
            self.forward(now)

    def other(self, at):
        for part in range(HALVES):
            arrived(half(self.whole.at[1 - self.d, at], part), self.recv.at[1 - self.d, at, part], self.here)

    def finish_sends(self):
        c = self.c
        for at in range(self.n):
            for part in range(HALVES):
                block = half(self.slot(at), part)

                @pl.when(jnp.logical_and(at <= c, c < self.n - 1))
                def _():
                    left(block, self.send.at[0, at, part], self.here)

                @pl.when(jnp.logical_and(at >= c, c > 0))
                def _():
                    left(block, self.send.at[1, at, part], self.here)

                left(block, self.send.at[2, at, part], self.here)

    def finish(self):
        self.finish_sends()
        pltpu.make_async_copy(self.own, self.slot(self.c), self.local).wait()


FACTOR = HD ** (-0.5)
LANES = 128


def ordered(c, step, n):
    at = jnp.int32(0)
    for here in range(n):
        near = sorted(range(n), key=lambda place_: (abs(place_ - here), place_))
        for index, value in enumerate(near):
            at = jnp.where(jnp.logical_and(c == here, step == index), value, at)
    return at


def towards(c, step, n):
    at = c
    for here in range(n):
        due = []
        for to in range(n):
            if to != here:
                hops = here if to > here else n - 1 - here
                due.append((hops + (n - 1 - to if to > here else to), -hops, to))
        for index, (_, _, to) in enumerate(sorted(due)):
            at = jnp.where(jnp.logical_and(c == here, step == index), to, at)
    return at


def first_kernel(
    sizes, parts, x_ref, gains_ref, w_ref, block_ref, step_ref, dy_ref, proj_ref, down_ref, gate_up_ref,
    normed_out, unit_out, att_out, wide_out, gains_out, dy_all, proj_all, down_out, gate_up_all,
    x_all, wide, normed, stage, unit, att_stage, att, gain_all, gain_vec,
    line_send, line_recv, line_local, w_send, w_recv, w_pass, g_send, g_recv, u_send, u_recv, a_send, a_recv, out_sem,
    dy_send, dy_recv, dy_local, m_send, m_recv, m_pass, down_send, down_recv, gu_send, gu_recv,
):
    dp, ctx, fs = sizes
    n = dp * ctx * fs
    d, c, f = place()
    here = at_device(d, c, f)
    span = stage.shape[2]
    tell_all(sizes)
    for slot in range(4):
        wide[slot * LANES + HD : (slot + 1) * LANES, :] = jnp.zeros((LANES - HD, D), jnp.bfloat16)
    hear_all(sizes)

    def head_rows(slot):
        return wide.at[pl.ds(pl.multiple_of(slot * LANES, LANES), HD)]

    q_core = f // 2
    kv_slot = 2 + c // 2
    kv_ctx = 2 * lax.rem(c, 2) + f // 2
    kv_core = lax.rem(f, 2)
    kv_f = lax.rem(f + 2 * (c // 2), fs)
    kv_away = jnp.logical_or(jnp.logical_or(kv_core != d, kv_ctx != c), kv_f != f)
    relay_of = {slot: f == lax.rem(2 * lax.rem(c, 2) + d + 2 * (slot - 2), fs) for slot in (2, 3)}

    me = (d * ctx + c) * fs + f

    def gain_to(step, carry):
        other = lax.rem(me + step, n)
        remote(
            gains_ref, gain_all.at[me], g_send.at[other], g_recv.at[me],
            at_device(other // (ctx * fs), lax.rem(other // fs, ctx), lax.rem(other, fs)),
        ).start()
        return carry

    lax.fori_loop(1, n, gain_to, 0)
    gain_all[me] = gains_ref[...]

    @pl.when(jnp.logical_and(d == 1, kv_away))
    def _():
        remote(w_ref, head_rows(kv_slot), w_send.at[0], w_recv.at[kv_slot], at_device(kv_core, kv_ctx, kv_f)).start()

    @pl.when(jnp.logical_and(d == 1, jnp.logical_not(kv_away)))
    def _():
        pltpu.make_async_copy(w_ref, head_rows(kv_slot), w_recv.at[kv_slot]).start()

    line = LineGather(ctx, x_ref, x_all, line_send, line_recv, line_local)
    line.start()

    @pl.when(d == 0)
    def _():
        slot = lax.rem(f, 2)
        for to in range(fs):

            @pl.when(jnp.logical_or(q_core != 0, to != f))
            def _():
                remote(w_ref, head_rows(slot), w_send.at[to], w_recv.at[slot], at_device(q_core, c, to)).start()

            @pl.when(jnp.logical_and(q_core == 0, to == f))
            def _():
                pltpu.make_async_copy(w_ref, head_rows(slot), w_recv.at[slot]).start()

    for slot in (2, 3):

        @pl.when(relay_of[slot])
        def _():
            arrived(head_rows(slot), w_recv.at[slot], here)
            for step in range(1, fs):
                to = lax.rem(f + step, fs)
                remote(head_rows(slot), head_rows(slot), w_pass.at[slot - 2, step], w_recv.at[slot], at_device(d, c, to)).start()

    gu_core = f // 2
    gu_slot = 2 * d + lax.rem(f, 2)
    part_rows = gate_up_ref.shape[0] // parts

    def push_part(part):
        first_row = part * part_rows
        src = gate_up_ref.at[first_row : first_row + part_rows]
        dst = gate_up_all.at[gu_slot, first_row : first_row + part_rows]
        for to in range(fs):
            own_place = jnp.logical_and(gu_core == d, f == to)

            @pl.when(jnp.logical_not(own_place))
            def _():
                remote(src, dst, gu_send.at[part, to], gu_recv.at[part, gu_slot], at_device(gu_core, c, to)).start()

            @pl.when(own_place)
            def _():
                pltpu.make_async_copy(src, dst, gu_recv.at[part, gu_slot]).start()

    def gain_from(step, carry):
        other = lax.rem(me + step, n)
        arrived(gain_all.at[other], g_recv.at[other], here)
        return carry

    lax.fori_loop(1, n, gain_from, 0)
    each = D // n
    for index in range(n):
        gain_vec[:, index * each : (index + 1) * each] = gain_all[index][:, :each]
    gain = gain_vec[0:1, :]

    for k in range(1, ctx - 1):
        line.forward(k)
    dy_line = LineGather(ctx, dy_ref, dy_all, dy_send, dy_recv, dy_local)
    dy_line.start()
    for slot in range(4):
        if slot < 2:
            arrived(head_rows(slot), w_recv.at[slot], here)
        else:

            @pl.when(jnp.logical_not(relay_of[slot]))
            def _():
                arrived(head_rows(slot), w_recv.at[slot], here)

    push_part(0)
    pltpu.make_async_copy(line.own, line.slot(c), line.local).wait()

    def block(step, carry):
        at = ordered(c, step, ctx)

        line.other(at)
        values = x_all[:, at].reshape(dp * 2 * span, D).astype(jnp.float32)
        scale = lax.rsqrt(jnp.mean(values * values, axis=-1, keepdims=True) + EPS)
        low = (values * scale * gain).astype(jnp.bfloat16)
        normed[:, at] = low.reshape(dp, 2 * span, D)
        heads = outer(low, wide[...])
        cosine, sine_up, sine_down = turns(block_ref, step_ref, at * fs + f)
        for slot in range(4):
            head = heads[:, slot * LANES : (slot + 1) * LANES]
            if slot < 3:
                turned_up = pltpu.roll(head, HD // 2, 1).reshape(2 * dp, span, LANES)
                turned_down = pltpu.roll(head, LANES - HD // 2, 1).reshape(2 * dp, span, LANES)
                head = head.reshape(2 * dp, span, LANES)
                head = head * cosine[None] + turned_up * sine_up[None] + turned_down * sine_down[None]
            else:
                head = head.reshape(2 * dp, span, LANES)
            stage[at, :, :, slot * LANES : (slot + 1) * LANES] = head.astype(jnp.bfloat16)
        for to in range(2 * dp):

            @pl.when(to != f)
            def _():
                remote(stage.at[at, to], unit.at[at, f], u_send.at[at, to], u_recv.at[at, f], at_device(d, c, to)).start()

            @pl.when(to == f)
            def _():
                unit[at, f] = stage[at, to]

        return carry

    def near(step, carry):
        @pl.when(step == ctx - 1)
        def _():
            line.forward(ctx - 1)

        return block(step, carry)

    lax.fori_loop(0, ctx, near, 0)
    normed_copy = pltpu.make_async_copy(normed, normed_out, out_sem.at[0])
    wide_copy = pltpu.make_async_copy(wide, wide_out, out_sem.at[1])
    gains_copy = pltpu.make_async_copy(gain_vec, gains_out, out_sem.at[2])
    normed_copy.start()
    wide_copy.start()
    gains_copy.start()

    to_core, to_ctx = lax.rem(c, 2), 2 * d + c // 2
    stays = jnp.logical_and(to_core == d, to_ctx == c)
    moved = ((proj_ref, proj_all),)
    for index, (shard, whole) in enumerate(moved):

        @pl.when(jnp.logical_not(stays))
        def _():
            remote(shard, whole.at[f], m_send.at[index], m_recv.at[index, f], at_device(to_core, to_ctx, f)).start()

        @pl.when(stays)
        def _():
            pltpu.make_async_copy(shard, whole.at[f], m_recv.at[index, f]).start()


    push_part(1)
    dy_line.forward(1)

    def pass_on():
        for index, (shard, whole) in enumerate(moved):
            arrived(whole.at[f], m_recv.at[index, f], here)
            for step in range(1, fs):
                to = lax.rem(f + step, fs)
                remote(whole.at[f], whole.at[f], m_pass.at[index, step], m_recv.at[index, f], at_device(d, c, to)).start()

    for at in range(ctx):
        for step in range(1, fs):
            other = lax.rem(f + step, fs)
            arrived(unit.at[at, other], u_recv.at[at, other], here)
    unit_copy = pltpu.make_async_copy(unit, unit_out, out_sem.at[3])
    unit_copy.start()

    rows = fs * span
    for at in range(ctx):
        keys = rows * (at + 1)
        k_rows = unit[0 : at + 1, :, :, 2 * LANES : 3 * LANES].reshape(keys, LANES)
        v_rows = unit[0 : at + 1, :, :, 3 * LANES : 4 * LANES].reshape(keys, LANES)
        allowed = lax.broadcasted_iota(jnp.int32, (rows, keys), 1) <= rows * at + lax.broadcasted_iota(
            jnp.int32, (rows, keys), 0
        )
        for head in range(2):
            q_rows = unit[at, :, :, head * LANES : (head + 1) * LANES].reshape(rows, LANES)
            scores = outer(q_rows, k_rows) * FACTOR
            scores = jnp.where(allowed, scores, NEG)
            best = jnp.max(scores, axis=-1, keepdims=True)
            weights = jnp.exp(scores - best)
            probs = weights / jnp.sum(weights, axis=-1, keepdims=True)
            mixed = jnp.dot(probs.astype(jnp.bfloat16), v_rows, preferred_element_type=jnp.float32)
            att_stage[at, :, :, head * LANES : (head + 1) * LANES] = mixed.astype(jnp.bfloat16).reshape(fs, span, LANES)
        for to in range(fs):

            @pl.when(to != f)
            def _():
                remote(
                    att_stage.at[at, to], att.at[f // 2, at, lax.rem(f, 2)], a_send.at[at, to], a_recv.at[f, at], at_device(d, c, to)
                ).start()

            @pl.when(to == f)
            def _():
                att[f // 2, at, lax.rem(f, 2)] = att_stage[at, to]

        if at == 0:
            pass_on()
        elif at == ctx - 1:
            for part in range(2, gu_send.shape[0]):
                push_part(part)
            dy_line.forward(2)

            @pl.when(jnp.logical_not(stays))
            def _():
                remote(down_ref, down_out, down_send, down_recv, at_device(to_core, to_ctx, f)).start()

            @pl.when(stays)
            def _():
                pltpu.make_async_copy(down_ref, down_out, down_recv).start()


    for at in range(ctx):
        for step in range(1, fs):
            other = lax.rem(f + step, fs)
            arrived(att.at[other // 2, at, lax.rem(other, 2)], a_recv.at[other, at], here)
    att_copy = pltpu.make_async_copy(att, att_out, out_sem.at[4])
    att_copy.start()

    for k in range(3, ctx):
        dy_line.forward(k)
    for at in range(ctx):
        dy_line.other(at)
    dy_line.finish()
    for index, (shard, whole) in enumerate(moved):
        for step in range(1, fs):
            other = lax.rem(f + step, fs)
            arrived(whole.at[other], m_recv.at[index, other], here)
            left(whole.at[f], m_pass.at[index, step], here)

        @pl.when(jnp.logical_not(stays))
        def _():
            left(shard, m_send.at[index], here)

    arrived(down_out, down_recv, here)

    @pl.when(jnp.logical_not(stays))
    def _():
        left(down_ref, down_send, here)

    for part in range(gu_send.shape[0]):
        src = gate_up_ref.at[part * part_rows : (part + 1) * part_rows]
        for slot in range(4):
            arrived(gate_up_all.at[slot, part * part_rows : (part + 1) * part_rows], gu_recv.at[part, slot], here)
        for to in range(fs):

            @pl.when(jnp.logical_not(jnp.logical_and(gu_core == d, f == to)))
            def _():
                left(src, gu_send.at[part, to], here)

    line.finish_sends()
    for at in range(ctx):

        for to in range(fs):

            @pl.when(to != f)
            def _():
                left(stage.at[at, to], u_send.at[at, to], here)
                left(att_stage.at[at, to], a_send.at[at, to], here)

    @pl.when(jnp.logical_and(d == 1, kv_away))
    def _():
        left(w_ref, w_send.at[0], here)

    @pl.when(d == 0)
    def _():
        for to in range(fs):

            @pl.when(jnp.logical_or(q_core != 0, to != f))
            def _():
                left(w_ref, w_send.at[to], here)

    for slot in (2, 3):

        @pl.when(relay_of[slot])
        def _():
            for step in range(1, fs):
                left(head_rows(slot), w_pass.at[slot - 2, step], here)

    def gain_left(step, carry):
        other = lax.rem(me + step, n)
        left(gains_ref, g_send.at[other], here)
        return carry

    lax.fori_loop(1, n, gain_left, 0)
    for copy in (normed_copy, wide_copy, gains_copy, unit_copy, att_copy):
        copy.wait()


def first(sizes, parts, sent, x, gains, w_qkv, blocks, steps, dy, w_out, w_down, w_gate_up):
    dp, ctx, fs = sizes
    n = dp * ctx * fs
    rows = x.shape[0]
    span = rows // 2
    low, wide_t = jnp.bfloat16, jnp.float32
    dma = pltpu.SemaphoreType.DMA
    shapes = (
        jax.ShapeDtypeStruct((dp, ctx, rows, D), low),
        jax.ShapeDtypeStruct((ctx, fs, span, 4 * LANES), low),
        jax.ShapeDtypeStruct((dp, ctx, 2, span, 2 * LANES), low),
        jax.ShapeDtypeStruct((4 * LANES, D), low),
        jax.ShapeDtypeStruct((8, D), wide_t),
        jax.ShapeDtypeStruct((dp, ctx, rows, D), low),
        jax.ShapeDtypeStruct((fs,) + w_out.shape, low),
        jax.ShapeDtypeStruct(w_down.shape, low),
        jax.ShapeDtypeStruct((4, D // parts * sent, w_gate_up.shape[1]), low),
    )
    any_spec, vm_spec = pl.BlockSpec(memory_space=ANY), pl.BlockSpec(memory_space=VM)
    return pl.pallas_call(
        functools.partial(first_kernel, sizes, parts),
        name="first",
        out_shape=shapes,
        in_specs=[vm_spec] * 9,
        out_specs=[any_spec] * 9,
        scratch_shapes=[
            VM((dp, ctx, rows, D), low),
            VM((4 * LANES, D), low),
            VM((dp, ctx, rows, D), low),
            VM((ctx, 2 * dp, span, 4 * LANES), low),
            VM((ctx, fs, span, 4 * LANES), low),
            VM((ctx, fs, span, 2 * LANES), low),
            VM((dp, ctx, 2, span, 2 * LANES), low),
            VM((n, 8, LANES), wide_t),
            VM((8, D), wide_t),
            dma((3, ctx, HALVES)), dma((dp, ctx, HALVES)), dma,
            dma((fs,)), dma((4,)), dma((2, fs)),
            dma((n,)), dma((n,)),
            dma((ctx, 2 * dp)), dma((ctx, fs)),
            dma((ctx, fs)), dma((fs, ctx)),
            dma((5,)),
            dma((3, ctx, HALVES)), dma((dp, ctx, HALVES)), dma,
            dma((1,)), dma((1, fs)), dma((1, fs)), dma, dma,
            dma((sent, fs)), dma((sent, 4)),
        ],
        compiler_params=pltpu.CompilerParams(collective_id=1, has_side_effects=True, vmem_limit_bytes=60 * 1024 * 1024),
    )(x, gains, w_qkv, blocks, steps, dy, w_out, w_down, w_gate_up)


def angle_tables(count, span):
    lane = jnp.arange(LANES, dtype=jnp.int32)
    frequency = THETA ** (-((lane % (HD // 2)).astype(jnp.float32) * 2.0) / HD)

    def both(positions):
        angles = positions.astype(jnp.float32)[:, None] * frequency
        return jnp.stack([jnp.cos(angles), jnp.sin(angles)])

    return both(jnp.arange(count, dtype=jnp.int32) * span), both(jnp.arange(span, dtype=jnp.int32))


def turns(block_ref, step_ref, block):
    cos_b, sin_b = block_ref[0, pl.ds(block, 1)], block_ref[1, pl.ds(block, 1)]
    cos_s, sin_s = step_ref[0], step_ref[1]
    cosine = cos_b * cos_s - sin_b * sin_s
    sine = sin_b * cos_s + cos_b * sin_s
    lane = lax.broadcasted_iota(jnp.int32, sine.shape, 1)
    first_half = lane < HD // 2
    sine_up = jnp.where(jnp.logical_and(lane >= HD // 2, lane < HD), sine, 0.0)
    return cosine, sine_up, jnp.where(first_half, -sine, 0.0)


class LineSum:
    def __init__(self, n, mine, out_core, in_core, out_line, in_line, total, sems):
        self.n, self.mine, self.out_core, self.in_core = n, mine, out_core, in_core
        self.out_line, self.in_line, self.total = out_line, in_line, total
        self.core_send, self.core_recv, self.line_send, self.line_recv = sems
        self.d, self.c, self.f = place()
        self.here = at_device(self.d, self.c, self.f)

    def give(self, at, both):
        self.keep(at, both)
        self.hand(at)

    def keep(self, at, both):
        d = self.d
        low = both.astype(jnp.bfloat16)

        @pl.when(d == 0)
        def _():
            self.mine[at] = low[0]
            self.out_core[at] = low[1]

        @pl.when(d != 0)
        def _():
            self.mine[at] = low[1]
            self.out_core[at] = low[0]

    def hand(self, at):
        remote(
            self.out_core.at[at], self.in_core.at[at], self.core_send.at[at], self.core_recv.at[at], at_device(1 - self.d, self.c, self.f)
        ).start()

    def step(self, at):
        n, d, c, f = self.n, self.d, self.c, self.f
        arrived(self.in_core.at[at], self.core_recv.at[at], self.here)
        rows = self.total.shape[0] // HALVES
        for part in range(HALVES):
            own = slice(part * rows, (part + 1) * rows)
            self.total[own] = self.mine[at, own].astype(jnp.float32) + self.in_core[at, own].astype(jnp.float32)
            for way, comes in enumerate((jnp.logical_and(at <= c, c < n - 1), jnp.logical_and(at >= c, c > 0))):

                @pl.when(comes)
                def _():
                    arrived(self.in_line.at[way, at, own], self.line_recv.at[way, at, part], self.here)
                    self.total[own] += self.in_line[way, at, own].astype(jnp.float32)

            @pl.when(at != c)
            def _():
                self.out_line[at, own] = self.total[own].astype(jnp.bfloat16)

            for way, (goes, to) in enumerate(((at < c, c - 1), (at > c, c + 1))):

                @pl.when(goes)
                def _():
                    remote(
                        self.out_line.at[at, own], self.in_line.at[way, at, own],
                        self.line_send.at[at, part], self.line_recv.at[way, at, part], at_device(d, to, f),
                    ).start()

    def finish(self):
        rows = self.total.shape[0] // HALVES
        for at in range(self.n):
            left(self.out_core.at[at], self.core_send.at[at], self.here)

            @pl.when(at != self.c)
            def _():
                for part in range(HALVES):
                    left(self.out_line.at[at, part * rows : (part + 1) * rows], self.line_send.at[at, part], self.here)

    @staticmethod
    def scratch(ctx, rows):
        low = jnp.bfloat16
        dma = pltpu.SemaphoreType.DMA
        return [
            VM((ctx, rows, D), low), VM((ctx, rows, D), low), VM((ctx, rows, D), low), VM((ctx, rows, D), low),
            VM((2, ctx, rows, D), low), VM((rows, D), jnp.float32),
            dma((ctx,)), dma((ctx,)), dma((ctx, HALVES)), dma((2, ctx, HALVES)),
        ]


def down_route(d, c):
    return (lax.rem(c, 2), 2 * d + c // 2), (c // 2, 2 * lax.rem(c, 2) + d)


def near_devices(sizes):
    dp, ctx, fs = sizes
    d, c, f = place()
    yes = c >= 0
    found = [(at_device(1 - d, c, f), yes)]
    for step in range(1, fs):
        for core in range(dp):
            found.append((at_device(core, c, lax.rem(f + step, fs)), yes))
    found.append((at_device(d, c - 1, f), c > 0))
    found.append((at_device(d, c + 1, f), c < ctx - 1))
    return found


def tell_near(sizes):
    barrier = pltpu.get_barrier_semaphore()
    for device, counts in near_devices(sizes):

        @pl.when(counts)
        def _():
            pl.semaphore_signal(barrier, inc=1, device_id=device, device_id_type=MESH)


def hear_near(sizes):
    peers = sum(jnp.where(counts, 1, 0) for _, counts in near_devices(sizes))
    pl.semaphore_wait(pltpu.get_barrier_semaphore(), peers)


def middle_kernel(
    sizes, hidden, parts, sent, att_ref, x_ref, dy_ref, gains_ref, proj_ref, down_ref, gate_up_ref, gate_up_part_ref, dy_all_ref,
    out_ref, d_resid_out, gain_out, unit_out, grad_proj_out, up_land, down_land,
    att, dy_all, proj, down, gate_up, resid, own_two, normed_two, act, d_both, own_d, d_resid_all, d_stage, unit,
    grad_up, grad_down, grad_proj, grad_proj_low,
    in_sem, gu_send, gu_recv, m_recv, m_pass, two_send, two_recv, two_local, dr_send, dr_recv, dr_local, u_send, u_recv,
    out_sem, gup_send, gup_recv, gdn_send, gdn_recv,
    *sums,
):
    dp, ctx, fs = sizes
    d, c, f = place()
    here = at_device(d, c, f)
    rows = x_ref.shape[0]
    span = rows // 2
    both_rows = dp * rows
    half = hidden // 2
    line_sum = LineSum(ctx, *sums[:6], sums[6:10])
    second_sum = LineSum(ctx, *sums[10:16], sums[16:20])
    out_sum = LineSum(ctx, *sums[20:26], sums[26:30])
    part_rows = D // parts
    tell_near(sizes)

    att_copy = pltpu.make_async_copy(att_ref, att, in_sem.at[0])
    dy_copy = pltpu.make_async_copy(dy_all_ref, dy_all, in_sem.at[1])
    part_copy = pltpu.make_async_copy(gate_up_part_ref, gate_up.at[:, 0 : part_rows * sent], in_sem.at[2])
    att_copy.start()
    proj[...] = jnp.zeros_like(proj)
    each = proj_ref.shape[1]
    proj_copies = []
    for slot in range(fs):
        start = slot // 2 * LANES + slot % 2 * each
        proj_copies.append(pltpu.make_async_copy(proj_ref.at[slot], proj.at[start : start + each], in_sem.at[3 + slot]))
        proj_copies[-1].start()
    dy_copy.start()
    part_copy.start()
    att_copy.wait()
    for copy in proj_copies:
        copy.wait()

    def project(step, carry):
        at = towards(c, step, ctx)
        terms = jnp.dot(att[:, at].reshape(both_rows, 2 * LANES), proj[...], preferred_element_type=jnp.float32)
        line_sum.keep(at, terms.reshape(dp, rows, D))
        return carry

    lax.fori_loop(0, ctx, project, 0)
    hear_near(sizes)

    pltpu.make_async_copy(down_ref, down.at[f], m_recv.at[f]).start()
    for step in range(1, fs):
        to = lax.rem(f + step, fs)
        remote(down_ref, down.at[f], m_pass.at[step], m_recv.at[f], at_device(d, c, to)).start()
    ends = jnp.logical_or(c == 0, c == ctx - 1)

    for step in range(ctx):
        line_sum.hand(towards(c, step, ctx))

    gu_core = f // 2
    gu_slot = 2 * d + lax.rem(f, 2)
    rest = slice(part_rows * sent, D)
    for to in range(fs):
        own_place = jnp.logical_and(gu_core == d, f == to)

        @pl.when(jnp.logical_not(own_place))
        def _():
            remote(gate_up_ref.at[rest], gate_up.at[gu_slot, rest], gu_send.at[to], gu_recv.at[gu_slot], at_device(gu_core, c, to)).start()

        @pl.when(own_place)
        def _():
            pltpu.make_async_copy(gate_up_ref.at[rest], gate_up.at[gu_slot, rest], gu_recv.at[gu_slot]).start()

    line_sum.step(towards(c, 0, ctx))
    line_sum.step(towards(c, 1, ctx))
    line_sum.step(towards(c, 2, ctx))
    line_sum.step(c)
    gain = gains_ref[1:2, :]
    values = x_ref[...].astype(jnp.float32) + line_sum.total[...]
    resid[...] = values
    scale = lax.rsqrt(jnp.mean(values * values, axis=-1, keepdims=True) + EPS)
    own_two[...] = (values * scale * gain).astype(jnp.bfloat16)
    line = LineGather(ctx, own_two, normed_two, two_send, two_recv, two_local)
    line.start()
    line.forward(1)
    for slot in range(4):
        arrived(gate_up.at[slot, rest], gu_recv.at[slot], here)
    dy_copy.wait()
    part_copy.wait()
    for slot in range(fs):
        arrived(down.at[slot], m_recv.at[slot], here)
    pltpu.make_async_copy(line.own, line.slot(c), line.local).wait()

    def mlp(step, carry):
        at = ordered(c, step, ctx)


        @pl.when(lax.rem(step, 2) == 1)
        def _():
            line.forward(2 + step // 2)

        line.other(at)
        inputs = normed_two[:, at].reshape(both_rows, D)
        dy_rows = dy_all[:, at].reshape(both_rows, D)
        for part in range(2):
            cols = slice(part * half, (part + 1) * half)
            gate = jnp.dot(inputs, gate_up[part], preferred_element_type=jnp.float32)
            up = jnp.dot(inputs, gate_up[2 + part], preferred_element_type=jnp.float32)
            d_act = outer(dy_rows, down[2 * part : 2 * part + 2].reshape(half, D))
            sig = 1.0 / (1.0 + jnp.exp(-gate))
            silu = gate * sig
            act[:, at, :, cols] = (silu * up).astype(jnp.bfloat16).reshape(dp, rows, half)
            d_gate = d_act * up * (sig * (1.0 + gate * (1.0 - sig)))
            d_both[:, at, :, cols] = d_gate.astype(jnp.bfloat16).reshape(dp, rows, half)
            d_both[:, at, :, hidden + part * half : hidden + (part + 1) * half] = (
                (d_act * silu).astype(jnp.bfloat16).reshape(dp, rows, half)
            )
        terms = outer(d_both[:, at, :, 0:half].reshape(both_rows, half), gate_up[0])
        for part in range(1, 4):
            terms += outer(d_both[:, at, :, part * half : (part + 1) * half].reshape(both_rows, half), gate_up[part])
        second_sum.give(at, terms.reshape(dp, rows, D))
        return carry

    lax.fori_loop(0, ctx, mlp, 0)

    wide_rows = D // ctx

    def push(src, dst, send, recv, core, to):
        to_self = jnp.logical_and(core == d, to == f)

        @pl.when(jnp.logical_not(to_self))
        def _():
            remote(src, dst, send, recv, at_device(core, c, to)).start()

        @pl.when(to_self)
        def _():
            pltpu.make_async_copy(src, dst, recv).start()

    def grads(step):
        first = step * wide_rows
        left_rows = normed_two[:, :, :, pl.ds(first, wide_rows)].reshape(dp * ctx * rows, wide_rows)
        for part in range(2):
            cols = slice(part * hidden, (part + 1) * hidden)
            terms = inner(left_rows, d_both[:, :, :, cols].reshape(dp * ctx * rows, hidden)).astype(jnp.bfloat16)
            grad_up[2 * part, pl.ds(first, wide_rows), :] = terms[:, :half]
            grad_up[2 * part + 1, pl.ds(first, wide_rows), :] = terms[:, half:]
        dy_cols = dy_all[:, :, :, pl.ds(first, wide_rows)].reshape(dp * ctx * rows, wide_rows)
        terms = inner(act[...].reshape(dp * ctx * rows, hidden), dy_cols).astype(jnp.bfloat16)
        grad_down[:, :, pl.ds(first, wide_rows)] = terms.reshape(fs, hidden // fs, wide_rows)
        for slot in range(4):
            push(
                grad_up.at[slot, pl.ds(first, wide_rows)], up_land.at[f, pl.ds(first, wide_rows)],
                gup_send.at[slot, step], gup_recv.at[f, step], slot // 2, 2 * d + slot % 2,
            )
            push(
                grad_down.at[slot, :, pl.ds(first, wide_rows)], down_land.at[f, :, pl.ds(first, wide_rows)],
                gdn_send.at[slot, step], gdn_recv.at[f, step], d, slot,
            )

    def out_terms(step):
        at = towards(c, step, ctx)
        terms = jnp.dot(act[:, at].reshape(both_rows, hidden), down[...].reshape(hidden, D), preferred_element_type=jnp.float32)
        out_sum.give(at, terms.reshape(dp, rows, D))

    second_sum.step(towards(c, 0, ctx))
    grads(0)
    out_terms(0)
    second_sum.step(towards(c, 1, ctx))
    second_sum.step(towards(c, 2, ctx))
    for step in range(1, ctx - 1):
        grads(step)
        out_terms(step)
    second_sum.step(c)
    values = resid[...]
    scale = lax.rsqrt(jnp.mean(values * values, axis=-1, keepdims=True) + EPS)
    incoming = second_sum.total[...]
    weighted = incoming * gain
    mean = jnp.mean(weighted * values, axis=-1, keepdims=True)
    d_resid = dy_ref[...].astype(jnp.float32) + scale * weighted - values * (scale * scale * scale) * mean
    own_d[...] = d_resid.astype(jnp.bfloat16)
    d_resid_out[...] = d_resid
    gain_out[...] = jnp.broadcast_to(jnp.sum(incoming * values * scale, axis=0, keepdims=True), gain_out.shape)
    d_line = LineGather(ctx, own_d, d_resid_all, dr_send, dr_recv, dr_local)
    d_line.start()
    def out_step(step, carry):
        out_sum.step(towards(c, step, ctx))
        return carry

    @pl.when(ends)
    def _():
        lax.fori_loop(0, ctx - 1, out_step, 0)

    out_terms(ctx - 1)
    grads(ctx - 1)
    pltpu.make_async_copy(d_line.own, d_line.slot(c), d_line.local).wait()
    grad_proj[...] = jnp.zeros_like(grad_proj)

    def back(step, carry):
        at = ordered(c, step, ctx)

        d_line.reach(step)
        d_line.other(at)
        incoming = d_resid_all[:, at].reshape(both_rows, D)
        d_att = outer(incoming, proj[...]).astype(jnp.bfloat16)
        d_stage[at] = d_att.reshape(2 * dp, span, 2 * LANES)
        for to in range(2 * dp):

            @pl.when(to != f)
            def _():
                remote(d_stage.at[at, to], unit.at[at, f], u_send.at[at, to], u_recv.at[at, f], at_device(d, c, to)).start()

            @pl.when(to == f)
            def _():
                unit[at, f] = d_stage[at, to]

        grad_proj[...] += inner(att[:, at].reshape(both_rows, 2 * LANES), incoming)

        @pl.when(jnp.logical_and(jnp.logical_not(ends), step == ctx - 2))
        def _():
            out_sum.step(towards(c, 0, ctx))

        return carry

    lax.fori_loop(0, ctx, back, 0)

    @pl.when(jnp.logical_not(ends))
    def _():
        lax.fori_loop(1, ctx - 1, out_step, 0)

    line_sum.finish()
    line.finish_sends()
    second_sum.finish()
    for slot in range(fs):
        start = slot // 2 * LANES + slot % 2 * each
        grad_proj_low[slot] = grad_proj[start : start + each, :].astype(jnp.bfloat16)
    grad_proj_copy = pltpu.make_async_copy(grad_proj_low, grad_proj_out, out_sem.at[1])
    grad_proj_copy.start()
    for at in range(ctx):
        for step in range(1, fs):
            other = lax.rem(f + step, fs)
            arrived(unit.at[at, other], u_recv.at[at, other], here)
    unit_copy = pltpu.make_async_copy(unit, unit_out, out_sem.at[2])
    unit_copy.start()
    out_step(ctx - 1, 0)
    out_ref[...] = (resid[...] + out_sum.total[...]).astype(jnp.bfloat16)
    d_line.finish_sends()
    out_sum.finish()
    for at in range(ctx):
        for to in range(fs):

            @pl.when(to != f)
            def _():
                left(d_stage.at[at, to], u_send.at[at, to], here)

    for to in range(fs):

        @pl.when(jnp.logical_not(jnp.logical_and(gu_core == d, f == to)))
        def _():
            left(gate_up_ref.at[rest], gu_send.at[to], here)

    for step in range(1, fs):
        left(down_ref, m_pass.at[step], here)

    def settle_up(step, carry):
        first = pl.multiple_of(step * wide_rows, LANES)
        for slot in range(4):
            arrived(up_land.at[slot, pl.ds(first, wide_rows)], gup_recv.at[slot, step], here)

            @pl.when(jnp.logical_or(slot // 2 != d, 2 * d + slot % 2 != f))
            def _():
                left(grad_up.at[slot, pl.ds(first, wide_rows)], gup_send.at[slot, step], here)

        return carry

    def settle_down(step, carry):
        first = pl.multiple_of(step * wide_rows, LANES)
        for slot in range(4):
            arrived(down_land.at[slot, :, pl.ds(first, wide_rows)], gdn_recv.at[slot, step], here)

            @pl.when(slot != f)
            def _():
                left(grad_down.at[slot, :, pl.ds(first, wide_rows)], gdn_send.at[slot, step], here)

        return carry

    lax.fori_loop(0, ctx, settle_up, 0)
    lax.fori_loop(0, ctx, settle_down, 0)
    for copy in (grad_proj_copy, unit_copy):
        copy.wait()


def middle(sizes, parts, sent, att, x, dy, gains, proj, w_down, w_gate_up, gate_up_part, dy_all):
    dp, ctx, fs = sizes
    rows = x.shape[0]
    span = rows // 2
    hidden = FF // (dp * ctx)
    low, wide_t = jnp.bfloat16, jnp.float32
    dma = pltpu.SemaphoreType.DMA
    any_spec, vm_spec = pl.BlockSpec(memory_space=ANY), pl.BlockSpec(memory_space=VM)
    shapes = (
        jax.ShapeDtypeStruct((rows, D), low),
        jax.ShapeDtypeStruct((rows, D), wide_t),
        jax.ShapeDtypeStruct((8, D), wide_t),
        jax.ShapeDtypeStruct((ctx, fs, span, 2 * LANES), low),
        jax.ShapeDtypeStruct(proj.shape, low),
        jax.ShapeDtypeStruct((fs, D, hidden // 2), low),
        jax.ShapeDtypeStruct((fs, hidden // fs, D), low),
    )
    return pl.pallas_call(
        functools.partial(middle_kernel, sizes, hidden, parts, sent),
        name="middle",
        out_shape=shapes,
        in_specs=[any_spec, vm_spec, vm_spec, vm_spec, any_spec, vm_spec, vm_spec, any_spec, any_spec],
        out_specs=[vm_spec] * 3 + [any_spec] * 4,
        scratch_shapes=[
            VM((dp, ctx, rows, 2 * LANES), low),
            VM((dp, ctx, rows, D), low),
            VM((2 * LANES, D), low),
            VM((fs, hidden // fs, D), low),
            VM((4, D, hidden // 2), low),
            VM((rows, D), wide_t),
            VM((rows, D), low),
            VM((dp, ctx, rows, D), low),
            VM((dp, ctx, rows, hidden), low),
            VM((dp, ctx, rows, 2 * hidden), low),
            VM((rows, D), low),
            VM((dp, ctx, rows, D), low),
            VM((ctx, 2 * dp, span, 2 * LANES), low),
            VM((ctx, fs, span, 2 * LANES), low),
            VM((4, D, hidden // 2), low),
            VM((fs, hidden // fs, D), low),
            VM((2 * LANES, D), wide_t),
            VM(proj.shape, low),
            dma((3 + fs,)), dma((fs,)), dma((4,)), dma((fs,)), dma((fs,)),
            dma((3, ctx, HALVES)), dma((dp, ctx, HALVES)), dma,
            dma((3, ctx, HALVES)), dma((dp, ctx, HALVES)), dma,
            dma((ctx, 2 * dp)), dma((ctx, fs)),
            dma((3,)),
            dma((4, ctx)), dma((fs, ctx)), dma((fs, ctx)), dma((fs, ctx)),
        ] + LineSum.scratch(ctx, rows) * 3,
        compiler_params=pltpu.CompilerParams(collective_id=2, has_side_effects=True, vmem_limit_bytes=63 * 1024 * 1024),
    )(att, x, dy, gains, proj, w_down, w_gate_up, gate_up_part, dy_all)


def last_kernel(
    sizes, x_ref, gains_ref, block_ref, step_ref, d_resid_ref, gain_two_ref, proj_ref,
    unit_ref, d_unit_ref, normed_ref, wide_ref, up_land_ref, down_land_ref,
    d_x_ref, gains_out, qkv_out, proj_out, up_out, down_out,
    unit, d_unit, d_k, d_v, stage, mixed, normed, wide, grad_heads,
    up_land, down_land, proj_land, q_land, kv_land, down_sum, proj_sum, kv_sum, down_last, proj_last, kv_last, gain_vec, gain_stage, gain_land,
    in_sem, proj_send, proj_recv, head_send, head_recv, move_send, move_recv,
    u_send, u_recv, g_send, g_recv,
    *sums,
):
    dp, ctx, fs = sizes
    n = dp * ctx * fs
    d, c, f = place()
    here = at_device(d, c, f)
    me = (d * ctx + c) * fs + f
    rows = x_ref.shape[0]
    span = rows // 2
    both_rows = dp * rows
    low, wide_t = jnp.bfloat16, jnp.float32
    loads = [
        pltpu.make_async_copy(src, dst, in_sem.at[index])
        for index, (src, dst) in enumerate((
            (unit_ref, unit), (d_unit_ref, d_unit), (normed_ref, normed), (wide_ref, wide), (down_land_ref, down_land), (up_land_ref, up_land),
        ))
    ]
    tell_all(sizes)
    for load in loads:
        load.start()
    in_sum = LineSum(ctx, *sums[:6], sums[6:10])
    d_k[...] = jnp.zeros_like(d_k)
    d_v[...] = jnp.zeros_like(d_v)

    def push(src, land, send, recv, core, fs_to):
        to_self = jnp.logical_and(core == d, fs_to == f)

        @pl.when(jnp.logical_not(to_self))
        def _():
            remote(src, land.at[f], send, recv.at[f], at_device(core, c, fs_to)).start()

        @pl.when(to_self)
        def _():
            pltpu.make_async_copy(src, land.at[f], recv.at[f]).start()

    def pushed(src, send, core, fs_to):
        @pl.when(jnp.logical_not(jnp.logical_and(core == d, fs_to == f)))
        def _():
            left(src, send, here)

    def sum_of(land):
        total = land[0].astype(wide_t)
        for source in range(1, fs):
            total += land[source].astype(wide_t)
        return total

    _, (own_core, own_ctx) = down_route(d, c)
    stays = jnp.logical_and(own_core == d, own_ctx == c)

    def move(index, src, dst):
        @pl.when(jnp.logical_not(stays))
        def _():
            remote(src, dst, move_send.at[index], move_recv.at[index], at_device(own_core, own_ctx, f)).start()

        @pl.when(stays)
        def _():
            pltpu.make_async_copy(src, dst, move_recv.at[index]).start()

    loads[0].wait()
    loads[1].wait()
    block = fs * span

    def unturn(values, at):
        up = pltpu.roll(values, HD // 2, 1)
        down = pltpu.roll(values, LANES - HD // 2, 1)
        pieces = []
        for index in range(fs):
            own = slice(index * span, (index + 1) * span)
            cosine, sine_up, sine_down = turns(block_ref, step_ref, at * fs + index)
            pieces.append(values[own] * cosine - up[own] * sine_up - down[own] * sine_down)
        return jnp.concatenate(pieces, axis=0).reshape(fs, span, LANES)

    for at in reversed(range(ctx)):
        keys = block * (at + 1)
        k_rows = unit[0 : at + 1, :, :, 2 * LANES : 3 * LANES].reshape(keys, LANES)
        v_rows = unit[0 : at + 1, :, :, 3 * LANES : 4 * LANES].reshape(keys, LANES)
        allowed = lax.broadcasted_iota(jnp.int32, (block, keys), 1) <= block * at + lax.broadcasted_iota(
            jnp.int32, (block, keys), 0
        )
        for head in range(2):
            lanes = slice(head * LANES, (head + 1) * LANES)
            q_rows = unit[at, :, :, lanes].reshape(block, LANES)
            d_rows = d_unit[at, :, :, lanes].reshape(block, LANES)
            scores = jnp.where(allowed, outer(q_rows, k_rows) * FACTOR, NEG)
            weights = jnp.exp(scores - jnp.max(scores, axis=-1, keepdims=True))
            probs = weights / jnp.sum(weights, axis=-1, keepdims=True)
            d_probs = outer(d_rows, v_rows)
            delta = jnp.sum(probs * d_probs, axis=-1, keepdims=True)
            d_scores = (probs * (d_probs - delta)).astype(low)
            d_q = jnp.dot(d_scores, k_rows, preferred_element_type=wide_t) * FACTOR
            stage[at, :, :, lanes] = unturn(d_q, at).astype(low)
            d_k[0:keys, :] += inner(d_scores, q_rows) * FACTOR
            d_v[0:keys, :] += inner(probs.astype(low), d_rows)
        stage[at, :, :, 2 * LANES : 3 * LANES] = unturn(d_k[block * at : keys, :], at).astype(low)
        stage[at, :, :, 3 * LANES : 4 * LANES] = d_v[block * at : keys, :].astype(low).reshape(fs, span, LANES)
        if at == ctx - 1:
            hear_all(sizes)
            for slot in range(fs):
                push(proj_ref.at[slot], proj_land, proj_send.at[slot], proj_recv, d, slot)
        for to in range(fs):

            @pl.when(to != f)
            def _():
                remote(
                    stage.at[at, to], mixed.at[f // 2, at, lax.rem(f, 2)], u_send.at[at, to], u_recv.at[f, at], at_device(d, c, to)
                ).start()

            @pl.when(to == f)
            def _():
                mixed[f // 2, at, lax.rem(f, 2)] = stage[at, to]

        if at == ctx - 1:
            loads[4].wait()
            down_sum[...] = sum_of(down_land).astype(low)
            move(0, down_sum, down_last)
    for source in range(fs):
        arrived(proj_land.at[source], proj_recv.at[source], here)
    proj_sum[...] = sum_of(proj_land).astype(low)
    move(1, proj_sum, proj_last)

    loads[2].wait()
    loads[3].wait()

    ends = jnp.logical_or(c == 0, c == ctx - 1)

    def give(step, carry):
        at = towards(c, step, ctx)
        for move_ in range(1, fs):
            other = lax.rem(f + move_, fs)
            arrived(mixed.at[other // 2, at, lax.rem(other, 2)], u_recv.at[other, at], here)
        terms = jnp.dot(mixed[:, at].reshape(both_rows, 4 * LANES), wide[...], preferred_element_type=wide_t)
        in_sum.give(at, terms.reshape(dp, rows, D))

        @pl.when(jnp.logical_and(ends, step > 0))
        def _():
            in_sum.step(towards(c, step - 1, ctx))

        return carry

    lax.fori_loop(0, ctx, give, 0)

    every = dp * ctx * rows
    k_relay = 2 * lax.rem(c, 2) + d
    relays = (k_relay, lax.rem(k_relay + 2, fs))
    gain_terms = jnp.zeros((1, D), wide_t)
    for slot in (2, 3, 0, 1):
        heads = inner(mixed[:, :, :, :, slot * LANES : (slot + 1) * LANES].reshape(every, LANES), normed[...].reshape(every, D))
        grad_heads[slot] = heads[:HD].astype(low)
        weights = wide[slot * LANES : slot * LANES + HD, :].astype(wide_t)
        gain_terms += jnp.sum(heads[:HD] * weights, axis=0, keepdims=True)
        if slot < 2:
            push(grad_heads.at[slot], q_land, head_send.at[slot], head_recv.at[0], 0, 2 * d + slot)
        else:
            push(grad_heads.at[slot], kv_land.at[slot - 2], head_send.at[slot], head_recv.at[slot - 1], d, relays[slot - 2])

    gain = gains_ref[0:1, :]
    gain_vec[0:1, :] = gain_terms / gain
    gain_vec[1:2, :] = gain_two_ref[0:1, :]
    each = D // n
    for index in range(n):
        gain_stage[index, :, 0:each] = gain_vec[:, index * each : (index + 1) * each]
    gain_land[me] = gain_stage[me]

    def gain_to(step, carry):
        other = lax.rem(me + step, n)
        remote(
            gain_stage.at[other], gain_land.at[me], g_send.at[other], g_recv.at[me],
            at_device(other // (ctx * fs), lax.rem(other // fs, ctx), lax.rem(other, fs)),
        ).start()
        return carry

    lax.fori_loop(1, n, gain_to, 0)

    def middle_step(step, carry):
        in_sum.step(towards(c, step, ctx))
        return carry

    @pl.when(jnp.logical_not(ends))
    def _():
        lax.fori_loop(0, ctx - 1, middle_step, 0)

    def kv_route(slot):
        owner, owner_f = slot * 2 + c // 2, k_relay
        return owner, owner_f, jnp.logical_or(jnp.logical_or(d != 1, owner != c), owner_f != f)

    for slot in range(2):
        owner, owner_f, away = kv_route(slot)

        @pl.when(f == relays[slot])
        def _():
            for source in range(fs):
                arrived(kv_land.at[slot, source], head_recv.at[1 + slot, source], here)
            kv_sum[slot] = sum_of(kv_land.at[slot]).astype(low)

            @pl.when(away)
            def _():
                remote(kv_sum.at[slot], kv_last, move_send.at[2 + slot], move_recv.at[2], at_device(1, owner, owner_f)).start()

            @pl.when(jnp.logical_not(away))
            def _():
                pltpu.make_async_copy(kv_sum.at[slot], kv_last, move_recv.at[2]).start()

    loads[5].wait()
    up_out[...] = sum_of(up_land)
    in_sum.step(c)

    values = x_ref[...].astype(wide_t)
    scale = lax.rsqrt(jnp.mean(values * values, axis=-1, keepdims=True) + EPS)
    incoming = in_sum.total[...]
    weighted = incoming * gain
    mean = jnp.mean(weighted * values, axis=-1, keepdims=True)
    d_x_ref[...] = (d_resid_ref[...] + scale * weighted - values * (scale * scale * scale) * mean).astype(low)

    @pl.when(d == 0)
    def _():
        for source in range(fs):
            arrived(q_land.at[source], head_recv.at[0, source], here)
        qkv_out[...] = sum_of(q_land)

    for index, dst in enumerate((down_last, proj_last)):
        arrived(dst, move_recv.at[index], here)
    down_out[...] = down_last[...].astype(wide_t)
    proj_out[...] = proj_last[...].astype(wide_t)

    @pl.when(d == 1)
    def _():
        arrived(kv_last, move_recv.at[2], here)
        qkv_out[...] = kv_last[...].astype(wide_t)

    def gain_from(step, carry):
        other = lax.rem(me + step, n)
        arrived(gain_land.at[other], g_recv.at[other], here)
        return carry

    lax.fori_loop(1, n, gain_from, 0)
    total = gain_land[0]
    for index in range(1, n):
        total += gain_land[index]
    gains_out[...] = total

    for slot in range(fs):
        pushed(proj_ref.at[slot], proj_send.at[slot], d, slot)
    for slot in range(2):
        pushed(grad_heads.at[slot], head_send.at[slot], 0, 2 * d + slot)
        pushed(grad_heads.at[2 + slot], head_send.at[2 + slot], d, relays[slot])
        away = kv_route(slot)[2]

        @pl.when(jnp.logical_and(f == relays[slot], away))
        def _():
            left(kv_sum.at[slot], move_send.at[2 + slot], here)

        @pl.when(jnp.logical_not(stays))
        def _():
            left((down_sum, proj_sum)[slot], move_send.at[slot], here)

    for at in range(ctx):
        for to in range(fs):

            @pl.when(to != f)
            def _():
                left(stage.at[at, to], u_send.at[at, to], here)

    in_sum.finish()

    def gain_left(step, carry):
        other = lax.rem(me + step, n)
        left(gain_stage.at[other], g_send.at[other], here)
        return carry

    lax.fori_loop(1, n, gain_left, 0)


def last(sizes, x, gains, tables, d_resid, gain_two, grad_proj, unit, d_unit, normed, wide, up_land, down_land):
    dp, ctx, fs = sizes
    n = dp * ctx * fs
    rows = x.shape[0]
    span = rows // 2
    low, wide_t = jnp.bfloat16, jnp.float32
    dma = pltpu.SemaphoreType.DMA
    any_spec, vm_spec = pl.BlockSpec(memory_space=ANY), pl.BlockSpec(memory_space=VM)
    down_rows, proj_rows, half = down_land.shape[1], grad_proj.shape[1], up_land.shape[2]
    shapes = (
        jax.ShapeDtypeStruct((rows, D), low),
        jax.ShapeDtypeStruct((8, LANES), wide_t),
        jax.ShapeDtypeStruct((HD, D), wide_t),
        jax.ShapeDtypeStruct((proj_rows, D), wide_t),
        jax.ShapeDtypeStruct((D, half), wide_t),
        jax.ShapeDtypeStruct((down_rows, D), wide_t),
    )
    return pl.pallas_call(
        functools.partial(last_kernel, sizes),
        name="last",
        out_shape=shapes,
        in_specs=[vm_spec] * 7 + [any_spec] * 6,
        out_specs=[vm_spec] * 6,
        scratch_shapes=[
            VM(unit.shape, low),
            VM(d_unit.shape, low),
            VM((ctx * fs * span, LANES), wide_t),
            VM((ctx * fs * span, LANES), wide_t),
            VM((ctx, fs, span, 4 * LANES), low),
            VM((dp, ctx, 2, span, 4 * LANES), low),
            VM(normed.shape, low),
            VM(wide.shape, low),
            VM((4, HD, D), low),
            VM(up_land.shape, low),
            VM((fs, down_rows, D), low),
            VM((fs, proj_rows, D), low),
            VM((fs, HD, D), low),
            VM((2, fs, HD, D), low),
            VM((down_rows, D), low),
            VM((proj_rows, D), low),
            VM((2, HD, D), low),
            VM((down_rows, D), low),
            VM((proj_rows, D), low),
            VM((HD, D), low),
            VM((8, D), wide_t),
            VM((n, 8, LANES), wide_t),
            VM((n, 8, LANES), wide_t),
            dma((6,)), dma((fs,)), dma((fs,)),
            dma((4,)), dma((3, fs)), dma((4,)), dma((3,)),
            dma((ctx, fs)), dma((fs, ctx)), dma((n,)), dma((n,)),
        ] + LineSum.scratch(ctx, rows),
        compiler_params=pltpu.CompilerParams(collective_id=3, has_side_effects=True, vmem_limit_bytes=63 * 1024 * 1024),
    )(x, gains, *tables, d_resid, gain_two, grad_proj, unit, d_unit, normed, wide, up_land, down_land)


def emit_kernel(count, gains_ref, *refs):
    sources, outs, one_ref, two_ref = refs[:count], refs[count : 2 * count], refs[2 * count], refs[2 * count + 1]
    held, in_sem, out_sem = refs[2 * count + 2 : 3 * count + 2], refs[-2], refs[-1]
    loads = [pltpu.make_async_copy(sources[i], held[i], in_sem.at[i]) for i in range(count)]
    stores = [pltpu.make_async_copy(held[i], outs[i], out_sem.at[i]) for i in range(count)]
    for load in loads:
        load.start()
    each = one_ref.shape[0]
    one_ref[...] = gains_ref[0, :each]
    two_ref[...] = gains_ref[1, :each]
    for load, store in zip(loads, stores):
        load.wait()
        store.start()
    for store in stores:
        store.wait()


def emit(each, gains, *arrays):
    count = len(arrays)
    any_spec, vm_spec = pl.BlockSpec(memory_space=ANY), pl.BlockSpec(memory_space=VM)
    gain = jax.ShapeDtypeStruct((each,), jnp.float32)
    return pl.pallas_call(
        functools.partial(emit_kernel, count),
        name="emit",
        out_shape=[jax.ShapeDtypeStruct(a.shape, a.dtype) for a in arrays] + [gain, gain],
        in_specs=[vm_spec] + [any_spec] * count,
        out_specs=[any_spec] * count + [vm_spec] * 2,
        scratch_shapes=[VM(a.shape, a.dtype) for a in arrays] + [pltpu.SemaphoreType.DMA((count,))] * 2,
        compiler_params=pltpu.CompilerParams(vmem_limit_bytes=63 * 1024 * 1024),
    )(gains, *arrays)


def on_device(tokens, cotangent, attn_gain, w_qkv, w_out, mlp_gain, w_gate_up, w_down):
    dp, ctx, fs = where = tuple(lax.axis_size(name) for name in ("dp", "ctx", "fsdp"))
    mb, _, span, _ = tokens.shape
    rows = mb * span
    x = tokens.reshape(rows, D)
    dy = cotangent.reshape(rows, D)
    each = attn_gain.shape[0]
    gain_rows = jnp.concatenate([attn_gain[None], mlp_gain[None]]).astype(jnp.float32)
    gain_rows = jnp.pad(gain_rows, ((0, 6), (0, LANES - each)))
    tables = angle_tables(ctx * fs, span)
    parts, sent = 4, 3
    normed, unit, att, qkv, gains, dy_all, proj, down, gate_up = first(
        where, parts, sent, x, gain_rows, w_qkv.T, *tables, dy, w_out, w_down, w_gate_up
    )
    att = att.reshape(dp, ctx, rows, 2 * LANES)
    block_out, d_resid, grad_two, d_unit, grad_proj, up_land, down_land = middle(
        where, parts, sent, att, x, dy, gains, proj, down, w_gate_up, gate_up, dy_all
    )
    grad_tokens, gain_grads, grad_qkv, grad_out, grad_gate_up, grad_down = last(
        where, x, gains, tables, d_resid, grad_two, grad_proj, unit, d_unit, normed, qkv, up_land, down_land
    )
    block_out, grad_tokens, grad_qkv, grad_out, grad_gate_up, grad_down, grad_one, grad_two = emit(
        each, gain_grads, block_out, grad_tokens, grad_qkv, grad_out, grad_gate_up, grad_down
    )
    return (
        block_out.reshape(tokens.shape),
        grad_tokens.reshape(tokens.shape),
        grad_one,
        grad_qkv.T,
        grad_out,
        grad_two,
        grad_gate_up,
        grad_down,
    )


def fits(mesh):
    return mesh.shape["dp"] == 2 and mesh.shape["ctx"] == 4 and mesh.shape["fsdp"] == 4


def solution(mesh):
    placed = (
        P(None, "dp", ("ctx", "fsdp"), None),
        P(None, "dp", ("ctx", "fsdp"), None),
        P(("dp", "ctx", "fsdp")),
        P(None, ("dp", "ctx", "fsdp")),
        P(("dp", "ctx", "fsdp"), None),
        P(("dp", "ctx", "fsdp")),
        P(None, ("dp", "ctx", "fsdp")),
        P(("dp", "ctx", "fsdp"), None),
    )
    return jax.shard_map(
        on_device if fits(mesh) else on_device_gathered,
        mesh=mesh,
        in_specs=placed,
        out_specs=(
            P(None, "dp", ("ctx", "fsdp"), None),
            P(None, "dp", ("ctx", "fsdp"), None),
            P(("dp", "ctx", "fsdp")),
            P(None, ("dp", "ctx", "fsdp")),
            P(("dp", "ctx", "fsdp"), None),
            P(("dp", "ctx", "fsdp")),
            P(None, ("dp", "ctx", "fsdp")),
            P(("dp", "ctx", "fsdp"), None),
        ),
        check_vma=False,
    )
```

```python
import functools

import jax
import jax.numpy as jnp
from jax import lax
from jax.experimental import pallas as pl
from jax.experimental.pallas import tpu as pltpu
from jax.sharding import PartitionSpec as P

D = 1536
H = 16
KVH = 8
HD = 96
FF = 4096


EPS = 1e-05
THETA = 100000.0
NEG = -1e30


def in_blocks(value, dim, length):
    lengths = value.shape
    pieces = value.reshape(*lengths[:dim], length, lengths[dim] // length, *lengths[dim + 1 :])
    return jnp.moveaxis(pieces, dim, 0)


def sum_at_owner(value, axis, dim):
    pieces = in_blocks(value, dim, lax.axis_size(axis))
    arrived = lax.all_to_all(pieces, axis, split_axis=0, concat_axis=0, tiled=True)
    return arrived.astype(jnp.float32).sum(axis=0)


def side_by_side(arrays, axis, dim, along):
    both = jnp.concatenate(arrays, axis=along)
    whole, at, finished = (sum_at_owner(both, axis, dim), 0, [])
    for a in arrays:
        finished.append(lax.slice_in_dim(whole, at, at + a.shape[along], axis=along))
        at += a.shape[along]
    return tuple(finished)


def rms_norm(values, gain_vec):
    return values * lax.rsqrt(jnp.mean(values * values, axis=-1, keepdims=True) + EPS) * gain_vec


def tables(start, length, width):
    half_width = width // 2
    frequency = THETA ** (-(jnp.arange(half_width, dtype=jnp.float32) * 2.0) / width)
    angles = (start + jnp.arange(length, dtype=jnp.int32)).astype(jnp.float32)[:, None] * frequency[
        None, :
    ]
    return (jnp.cos(angles), jnp.sin(angles))


def rotate(values, cosine, sine_table):
    half_width = values.shape[-1] // 2
    first_half = values[..., :half_width]
    second_half = values[..., half_width:]
    cos_b = cosine[:, None, :]
    sin_b = sine_table[:, None, :]
    return jnp.concatenate(
        [first_half * cos_b - second_half * sin_b, second_half * cos_b + first_half * sin_b],
        axis=-1,
    )


def swiglu(both):
    return jax.nn.silu(both[:, :FF]) * both[:, FF:]


def inner(left, right):
    return lax.dot_general(
        left, right, (((0,), (0,)), ((), ())), preferred_element_type=jnp.float32
    )


def outer(left, right):
    return lax.dot_general(
        left, right, (((1,), (1,)), ((), ())), preferred_element_type=jnp.float32
    )


def unchanged(state):
    return state


def on_device_gathered(tokens, cotangent, attn_gain, w_qkv, w_out, mlp_gain, w_gate_up, w_down):
    tok_count = tokens.shape[2]
    groups = H // KVH
    factor = HD ** (-0.5)
    seq_length = tok_count * lax.axis_size(("ctx", "fsdp"))
    pos_first = lax.axis_index(("ctx", "fsdp")) * tok_count
    positions = pos_first + jnp.arange(tok_count, dtype=jnp.int32)
    pos_last = pos_first + tok_count - 1
    cosine, sine_table = tables(pos_first, tok_count, HD)
    sums = [
        jnp.zeros((D,), jnp.float32),
        jnp.zeros((D, (H + 2 * KVH) * HD), jnp.float32),
        jnp.zeros((H * HD, D), jnp.float32),
        jnp.zeros((D,), jnp.float32),
        jnp.zeros((D, 2 * FF), jnp.float32),
        jnp.zeros((FF, D), jnp.float32),
    ]
    outputs = []
    in_grads = []
    whole = (
        lax.all_gather(attn_gain, ("dp", "ctx", "fsdp"), axis=0, tiled=True),
        lax.all_gather(w_qkv, ("dp", "ctx", "fsdp"), axis=1, tiled=True),
        lax.all_gather(w_out, ("dp", "ctx", "fsdp"), axis=0, tiled=True),
        lax.all_gather(mlp_gain, ("dp", "ctx", "fsdp"), axis=0, tiled=True),
        lax.all_gather(w_gate_up, ("dp", "ctx", "fsdp"), axis=1, tiled=True),
        lax.all_gather(w_down, ("dp", "ctx", "fsdp"), axis=0, tiled=True),
    )
    for step_index in range(tokens.shape[0]):
        gain_one, mix_qkv, mix_out, gain_two, mix_gate_up, mix_down = whole
        inputs = tokens[step_index, 0].astype(jnp.float32)
        normed = rms_norm(inputs, gain_one.astype(jnp.float32)).astype(jnp.bfloat16)
        mixed = jnp.dot(normed, mix_qkv, preferred_element_type=jnp.float32)
        queries = rotate(mixed[:, : H * HD].reshape(tok_count, H, HD), cosine, sine_table).astype(
            jnp.bfloat16
        )
        key_rows = rotate(
            mixed[:, H * HD : (H + KVH) * HD].reshape(tok_count, KVH, HD), cosine, sine_table
        )
        key_rows = key_rows.astype(jnp.bfloat16).reshape(tok_count, KVH * HD)
        value_rows = mixed[:, (H + KVH) * HD :].astype(jnp.bfloat16)
        grouped = queries.reshape(tok_count, KVH, groups, HD)
        start_state = (
            jnp.full((KVH, groups, tok_count), NEG, jnp.float32),
            jnp.zeros((KVH, groups, tok_count), jnp.float32),
            jnp.zeros((KVH, groups, tok_count, HD), jnp.float32),
        )
        piece = (
            lax.all_gather(key_rows, ("ctx", "fsdp"), axis=0, tiled=True),
            lax.all_gather(value_rows, ("ctx", "fsdp"), axis=0, tiled=True),
        )

        def work(state):
            best, total, summed = state
            key_count = piece[0].shape[0]
            keys = piece[0].reshape(key_count, KVH, HD)
            values = piece[1].reshape(key_count, KVH, HD)
            scores = (
                jnp.einsum("qkgd,tkd->kgqt", grouped, keys, preferred_element_type=jnp.float32)
                * factor
            )
            allowed = jnp.arange(key_count, dtype=jnp.int32)[None, :] <= positions[:, None]
            scores = jnp.where(allowed, scores, NEG)
            new_best = jnp.maximum(best, jnp.max(scores, axis=-1))
            weights = jnp.where(allowed, jnp.exp(scores - new_best[..., None]), 0.0)
            total = jnp.sum(weights, axis=-1)
            summed = jnp.einsum(
                "kgqt,tkd->kgqd",
                weights.astype(jnp.bfloat16),
                values,
                preferred_element_type=jnp.float32,
            )
            return (new_best, total, summed)

        best, total, summed = lax.cond(jnp.int32(0) <= pos_last, work, unchanged, start_state)
        head_out = summed / total[..., None]
        log_total = best + jnp.log(total)
        attended = (
            jnp.transpose(head_out, (2, 0, 1, 3)).reshape(tok_count, H * HD).astype(jnp.bfloat16)
        )
        resid = inputs + jnp.dot(attended, mix_out, preferred_element_type=jnp.float32)
        normed_two = rms_norm(resid, gain_two.astype(jnp.float32)).astype(jnp.bfloat16)
        both = jnp.dot(normed_two, mix_gate_up, preferred_element_type=jnp.float32)
        acted = swiglu(both).astype(jnp.bfloat16)
        result = resid + jnp.dot(acted, mix_down, preferred_element_type=jnp.float32)
        outputs.append(result.astype(jnp.bfloat16))
        gain_one, mix_qkv, mix_out, gain_two, mix_gate_up, mix_down = whole
        up_low = cotangent[step_index, 0]
        upstream = up_low.astype(jnp.float32)
        sums[5] = sums[5] + inner(acted, up_low)
        d_act = outer(up_low, mix_down)
        _, pull_glu = jax.vjp(swiglu, both)
        d_both = pull_glu(d_act)[0].astype(jnp.bfloat16)
        sums[4] = sums[4] + inner(normed_two, d_both)
        d_normed_two = outer(d_both, mix_gate_up)
        _, pull_two = jax.vjp(rms_norm, resid, gain_two.astype(jnp.float32))
        d_resid_norm, d_gain_two = pull_two(d_normed_two)
        sums[3] = sums[3] + d_gain_two
        d_resid = upstream + d_resid_norm
        d_resid_low = d_resid.astype(jnp.bfloat16)
        sums[2] = sums[2] + inner(attended, d_resid_low)
        d_attended = outer(d_resid_low, mix_out).astype(jnp.bfloat16)
        d_grouped = d_attended.reshape(tok_count, KVH, groups, HD)
        delta = jnp.einsum("qkgd,kgqd->kgq", d_grouped.astype(jnp.float32), head_out)
        zero_q = jnp.zeros((tok_count, KVH, groups, HD), jnp.float32)
        back_state = (
            zero_q,
            jnp.zeros((seq_length, KVH * HD), jnp.float32),
            jnp.zeros((seq_length, KVH * HD), jnp.float32),
        )
        attend_piece = (
            lax.all_gather(key_rows, ("ctx", "fsdp"), axis=0, tiled=True),
            lax.all_gather(value_rows, ("ctx", "fsdp"), axis=0, tiled=True),
        )

        def attend_work(state):
            key_count = attend_piece[0].shape[0]
            keys = attend_piece[0].reshape(key_count, KVH, HD)
            values = attend_piece[1].reshape(key_count, KVH, HD)
            scores = (
                jnp.einsum("qkgd,tkd->kgqt", grouped, keys, preferred_element_type=jnp.float32)
                * factor
            )
            allowed = jnp.arange(key_count, dtype=jnp.int32)[None, :] <= positions[:, None]
            scores = jnp.where(allowed, scores, NEG)
            probs = jnp.where(allowed, jnp.exp(scores - log_total[..., None]), 0.0)
            d_probs = jnp.einsum(
                "qkgd,tkd->kgqt", d_grouped, values, preferred_element_type=jnp.float32
            )
            d_scores = (probs * (d_probs - delta[..., None])).astype(jnp.bfloat16)
            grad_q = jnp.einsum(
                "kgqt,tkd->qkgd", d_scores, keys, preferred_element_type=jnp.float32
            )
            piece_k = (
                jnp.einsum("kgqt,qkgd->tkd", d_scores, grouped, preferred_element_type=jnp.float32)
                * factor
            )
            piece_v = jnp.einsum(
                "kgqt,qkgd->tkd",
                probs.astype(jnp.bfloat16),
                d_grouped,
                preferred_element_type=jnp.float32,
            )
            grad_k = piece_k.reshape(key_count, KVH * HD)
            grad_v = piece_v.reshape(key_count, KVH * HD)
            return (grad_q, grad_k, grad_v)

        back_result = lax.cond(jnp.int32(0) <= pos_last, attend_work, unchanged, back_state)
        grad_q = back_result[0]
        summed_k, summed_v = side_by_side(
            (back_result[1].astype(jnp.bfloat16), back_result[2].astype(jnp.bfloat16)),
            ("ctx", "fsdp"),
            0,
            1,
        )
        d_q_raw = rotate(grad_q.reshape(tok_count, H, HD) * factor, cosine, -sine_table).reshape(
            tok_count, H * HD
        )
        d_k_raw = rotate(summed_k.reshape(tok_count, KVH, HD), cosine, -sine_table).reshape(
            tok_count, KVH * HD
        )
        d_mixed = jnp.concatenate([d_q_raw, d_k_raw, summed_v], axis=1).astype(jnp.bfloat16)
        sums[1] = sums[1] + inner(normed, d_mixed)
        d_normed = outer(d_mixed, mix_qkv)
        _, pull_one = jax.vjp(rms_norm, inputs, gain_one.astype(jnp.float32))
        d_inputs_norm, d_gain_one = pull_one(d_normed)
        sums[0] = sums[0] + d_gain_one
        in_grads.append((d_resid + d_inputs_norm).astype(jnp.bfloat16))
    grad_gain_one, grad_qkv, grad_out, grad_gain_two, grad_gate_up, grad_down = (
        lax.psum_scatter(sums[0], ("dp", "ctx", "fsdp"), scatter_dimension=0, tiled=True),
        lax.psum_scatter(sums[1], ("dp", "ctx", "fsdp"), scatter_dimension=1, tiled=True),
        lax.psum_scatter(sums[2], ("dp", "ctx", "fsdp"), scatter_dimension=0, tiled=True),
        lax.psum_scatter(sums[3], ("dp", "ctx", "fsdp"), scatter_dimension=0, tiled=True),
        lax.psum_scatter(sums[4], ("dp", "ctx", "fsdp"), scatter_dimension=1, tiled=True),
        lax.psum_scatter(sums[5], ("dp", "ctx", "fsdp"), scatter_dimension=0, tiled=True),
    )
    block_out = jnp.stack(outputs)[:, None]
    grad_tokens = jnp.stack(in_grads)[:, None]
    return (
        block_out,
        grad_tokens,
        grad_gain_one,
        grad_qkv,
        grad_out,
        grad_gain_two,
        grad_gate_up,
        grad_down,
    )


MESH = pl.DeviceIdType.MESH
VM = pltpu.VMEM
ANY = pl.ANY


def place():
    return lax.axis_index("dp"), lax.axis_index("ctx"), lax.axis_index("fsdp")


def at_device(dp, ctx, fs):
    return {"dp": dp, "ctx": ctx, "fsdp": fs}


def remote(src, dst, send, recv, device):
    return pltpu.make_async_remote_copy(
        src_ref=src, dst_ref=dst, send_sem=send, recv_sem=recv, device_id=device, device_id_type=MESH
    )


def arrived(dst, recv, device):
    remote(dst, dst, recv, recv, device).wait_recv()


def left(src, send, device):
    remote(src, src, send, send, device).wait_send()


def tell_all(sizes):
    dp, ctx, fs = sizes
    n = dp * ctx * fs
    d, c, f = place()
    me = (d * ctx + c) * fs + f
    barrier = pltpu.get_barrier_semaphore()

    def tell(step, carry):
        other = lax.rem(me + step, n)
        pl.semaphore_signal(
            barrier,
            inc=1,
            device_id=at_device(other // (ctx * fs), lax.rem(other // fs, ctx), lax.rem(other, fs)),
            device_id_type=MESH,
        )
        return carry

    lax.fori_loop(1, n, tell, 0)


def hear_all(sizes):
    dp, ctx, fs = sizes
    pl.semaphore_wait(pltpu.get_barrier_semaphore(), dp * ctx * fs - 1)


HALVES = 2


def part_of(ref, index):
    rows = ref.shape[-2] // HALVES
    return ref.at[index * rows : (index + 1) * rows]


def near_or_inner(c, at, n):
    ends = jnp.logical_or(c == 0, c == n - 1)
    return jnp.logical_or(jnp.logical_not(ends), jnp.abs(at - c) <= 1)


class LineGather:
    def __init__(self, n, own, whole, send, recv, local, short=False):
        self.n, self.own, self.whole, self.send, self.recv, self.local = n, own, whole, send, recv, local
        self.short = short
        self.d, self.c, self.f = place()
        self.here = at_device(self.d, self.c, self.f)

    def slot(self, at):
        return self.whole.at[self.d, at]

    def held(self, at):
        valid = jnp.logical_and(at >= 0, at < self.n)
        return jnp.logical_and(valid, near_or_inner(self.c, at, self.n)) if self.short else valid

    def passes(self, way, at):
        ahead = self.n - 2 - self.c if way == 0 else self.c - 1
        inside = at <= self.c if way == 0 else at >= self.c
        goes = jnp.logical_and(inside, ahead >= 0)
        return jnp.logical_and(goes, jnp.logical_or(at == self.c, ahead > 0)) if self.short else goes

    def along(self, way, block, at, part):
        to = (at_device(self.d, self.c + 1, self.f), at_device(self.d, self.c - 1, self.f), at_device(1 - self.d, self.c, self.f))[way]
        return remote(part_of(block, part), part_of(self.slot(at), part), self.send.at[way, at, part], self.recv.at[self.d, at, part], to)

    def start(self):
        c = self.c
        for part in range(HALVES):

            @pl.when(c < self.n - 1)
            def _():
                self.along(0, self.own, c, part).start()

            @pl.when(c > 0)
            def _():
                self.along(1, self.own, c, part).start()

        for part in range(HALVES):
            self.along(2, self.own, c, part).start()
        pltpu.make_async_copy(self.own, self.slot(c), self.local).start()

    def forward(self, k):
        for part in range(HALVES):
            for way, at in enumerate((self.c - k, self.c + k)):

                @pl.when(self.held(at))
                def _():
                    arrived(part_of(self.slot(at), part), self.recv.at[self.d, at, part], self.here)

                    @pl.when(self.passes(way, at))
                    def _():
                        self.along(way, self.slot(at), at, part).start()

                    self.along(2, self.slot(at), at, part).start()

    def reach(self, step):
        now = jnp.abs(ordered(self.c, step, self.n) - self.c)
        before = jnp.abs(ordered(self.c, step - 1, self.n) - self.c)

        @pl.when(jnp.logical_and(step > 0, now != before))
        def _():
            self.forward(now)

    def other(self, at):
        @pl.when(self.held(at))
        def _():
            for part in range(HALVES):
                arrived(part_of(self.whole.at[1 - self.d, at], part), self.recv.at[1 - self.d, at, part], self.here)

    def finish_sends(self):
        for at in range(self.n):
            for part in range(HALVES):
                block = part_of(self.slot(at), part)
                for way in range(3):

                    @pl.when(self.passes(way, at) if way < 2 else self.held(at))
                    def _():
                        left(block, self.send.at[way, at, part], self.here)

    def finish(self):
        self.finish_sends()
        pltpu.make_async_copy(self.own, self.slot(self.c), self.local).wait()


FACTOR = HD ** (-0.5)
LANES = 128


def ordered(c, step, n):
    at = jnp.int32(0)
    for here in range(n):
        near = sorted(range(n), key=lambda place_: (abs(place_ - here), place_))
        for index, value in enumerate(near):
            at = jnp.where(jnp.logical_and(c == here, step == index), value, at)
    return at


def towards(c, step, n):
    at = c
    for here in range(n):
        due = []
        for to in range(n):
            if to != here:
                hops = here if to > here else n - 1 - here
                due.append((hops + (n - 1 - to if to > here else to), -hops, to))
        for index, (_, _, to) in enumerate(sorted(due)):
            at = jnp.where(jnp.logical_and(c == here, step == index), to, at)
    return at


def first_kernel(
    sizes, parts, x_ref, gains_ref, w_ref, block_ref, step_ref, dy_ref, proj_ref, down_ref, gate_up_ref,
    normed_out, unit_out, att_out, wide_out, gains_out, dy_all, proj_all, down_out, gate_up_all,
    x_all, wide, normed, stage, unit, att_stage, att, gain_all, gain_vec,
    line_send, line_recv, line_local, w_send, w_recv, w_pass, g_send, g_recv, u_send, u_recv, a_send, a_recv, out_sem,
    dy_send, dy_recv, dy_local, m_send, m_recv, m_pass, down_send, down_recv, gu_send, gu_recv,
):
    dp, ctx, fs = sizes
    n = dp * ctx * fs
    d, c, f = place()
    here = at_device(d, c, f)
    span = stage.shape[2]
    tell_all(sizes)
    for slot in range(4):
        wide[slot * LANES + HD : (slot + 1) * LANES, :] = jnp.zeros((LANES - HD, D), jnp.bfloat16)
    hear_all(sizes)

    def head_rows(slot):
        return wide.at[pl.ds(pl.multiple_of(slot * LANES, LANES), HD)]

    q_core = f // 2
    kv_slot = 2 + c // 2
    kv_ctx = 2 * lax.rem(c, 2) + f // 2
    kv_core = lax.rem(f, 2)
    kv_f = lax.rem(f + 2 * (c // 2), fs)
    kv_away = jnp.logical_or(jnp.logical_or(kv_core != d, kv_ctx != c), kv_f != f)
    relay_of = {slot: f == lax.rem(2 * lax.rem(c, 2) + d + 2 * (slot - 2), fs) for slot in (2, 3)}

    me = (d * ctx + c) * fs + f

    def gain_to(step, carry):
        other = lax.rem(me + step, n)
        remote(
            gains_ref, gain_all.at[me], g_send.at[other], g_recv.at[me],
            at_device(other // (ctx * fs), lax.rem(other // fs, ctx), lax.rem(other, fs)),
        ).start()
        return carry

    lax.fori_loop(1, n, gain_to, 0)
    gain_all[me] = gains_ref[...]

    @pl.when(jnp.logical_and(d == 1, kv_away))
    def _():
        remote(w_ref, head_rows(kv_slot), w_send.at[0], w_recv.at[kv_slot], at_device(kv_core, kv_ctx, kv_f)).start()

    @pl.when(jnp.logical_and(d == 1, jnp.logical_not(kv_away)))
    def _():
        pltpu.make_async_copy(w_ref, head_rows(kv_slot), w_recv.at[kv_slot]).start()

    line = LineGather(ctx, x_ref, x_all, line_send, line_recv, line_local)
    line.start()

    @pl.when(d == 0)
    def _():
        slot = lax.rem(f, 2)
        for to in range(fs):

            @pl.when(jnp.logical_or(q_core != 0, to != f))
            def _():
                remote(w_ref, head_rows(slot), w_send.at[to], w_recv.at[slot], at_device(q_core, c, to)).start()

            @pl.when(jnp.logical_and(q_core == 0, to == f))
            def _():
                pltpu.make_async_copy(w_ref, head_rows(slot), w_recv.at[slot]).start()

    for slot in (2, 3):

        @pl.when(relay_of[slot])
        def _():
            arrived(head_rows(slot), w_recv.at[slot], here)
            for step in range(1, fs):
                to = lax.rem(f + step, fs)
                remote(head_rows(slot), head_rows(slot), w_pass.at[slot - 2, step], w_recv.at[slot], at_device(d, c, to)).start()

    gu_core = f // 2
    gu_slot = 2 * d + lax.rem(f, 2)
    part_rows = gate_up_ref.shape[0] // parts

    def push_part(part):
        first_row = part * part_rows
        src = gate_up_ref.at[first_row : first_row + part_rows]
        dst = gate_up_all.at[gu_slot, first_row : first_row + part_rows]
        for to in range(fs):
            own_place = jnp.logical_and(gu_core == d, f == to)

            @pl.when(jnp.logical_not(own_place))
            def _():
                remote(src, dst, gu_send.at[part, to], gu_recv.at[part, gu_slot], at_device(gu_core, c, to)).start()

            @pl.when(own_place)
            def _():
                pltpu.make_async_copy(src, dst, gu_recv.at[part, gu_slot]).start()

    def gain_from(step, carry):
        other = lax.rem(me + step, n)
        arrived(gain_all.at[other], g_recv.at[other], here)
        return carry

    lax.fori_loop(1, n, gain_from, 0)
    each = D // n
    for index in range(n):
        gain_vec[:, index * each : (index + 1) * each] = gain_all[index][:, :each]
    gain = gain_vec[0:1, :]

    for k in range(1, ctx - 1):
        line.forward(k)
    to_core, to_ctx = lax.rem(c, 2), 2 * d + c // 2
    stays = jnp.logical_and(to_core == d, to_ctx == c)
    moved = ((proj_ref, proj_all),)
    for index, (shard, whole) in enumerate(moved):

        @pl.when(jnp.logical_not(stays))
        def _():
            remote(shard, whole.at[f], m_send.at[index], m_recv.at[index, f], at_device(to_core, to_ctx, f)).start()

        @pl.when(stays)
        def _():
            pltpu.make_async_copy(shard, whole.at[f], m_recv.at[index, f]).start()


    dy_line = LineGather(ctx, dy_ref, dy_all, dy_send, dy_recv, dy_local, short=True)
    dy_line.start()
    for slot in range(4):
        if slot < 2:
            arrived(head_rows(slot), w_recv.at[slot], here)
        else:

            @pl.when(jnp.logical_not(relay_of[slot]))
            def _():
                arrived(head_rows(slot), w_recv.at[slot], here)

    for part in range(gu_send.shape[0]):
        push_part(part)
    pltpu.make_async_copy(line.own, line.slot(c), line.local).wait()

    def block(step, carry):
        at = ordered(c, step, ctx)

        line.other(at)
        values = x_all[:, at].reshape(dp * 2 * span, D).astype(jnp.float32)
        scale = lax.rsqrt(jnp.mean(values * values, axis=-1, keepdims=True) + EPS)
        low = (values * scale * gain).astype(jnp.bfloat16)
        normed[:, at] = low.reshape(dp, 2 * span, D)
        heads = outer(low, wide[...])
        cosine, sine_up, sine_down = turns(block_ref, step_ref, at * fs + f)
        for slot in range(4):
            head = heads[:, slot * LANES : (slot + 1) * LANES]
            if slot < 3:
                turned_up = pltpu.roll(head, HD // 2, 1).reshape(2 * dp, span, LANES)
                turned_down = pltpu.roll(head, LANES - HD // 2, 1).reshape(2 * dp, span, LANES)
                head = head.reshape(2 * dp, span, LANES)
                head = head * cosine[None] + turned_up * sine_up[None] + turned_down * sine_down[None]
            else:
                head = head.reshape(2 * dp, span, LANES)
            stage[at, :, :, slot * LANES : (slot + 1) * LANES] = head.astype(jnp.bfloat16)
        for to in range(2 * dp):

            @pl.when(to != f)
            def _():
                remote(stage.at[at, to], unit.at[at, f], u_send.at[at, to], u_recv.at[at, f], at_device(d, c, to)).start()

            @pl.when(to == f)
            def _():
                unit[at, f] = stage[at, to]

        return carry

    def near(step, carry):
        @pl.when(step == ctx - 1)
        def _():
            line.forward(ctx - 1)

        return block(step, carry)

    lax.fori_loop(0, ctx, near, 0)
    normed_copy = pltpu.make_async_copy(normed, normed_out, out_sem.at[0])
    wide_copy = pltpu.make_async_copy(wide, wide_out, out_sem.at[1])
    gains_copy = pltpu.make_async_copy(gain_vec, gains_out, out_sem.at[2])
    normed_copy.start()
    wide_copy.start()
    gains_copy.start()

    @pl.when(jnp.logical_not(stays))
    def _():
        remote(down_ref, down_out, down_send, down_recv, at_device(to_core, to_ctx, f)).start()

    @pl.when(stays)
    def _():
        pltpu.make_async_copy(down_ref, down_out, down_recv).start()

    for index, (shard, whole) in enumerate(moved):
        arrived(whole.at[f], m_recv.at[index, f], here)
        for step in range(1, fs):
            to = lax.rem(f + step, fs)
            remote(whole.at[f], whole.at[f], m_pass.at[index, step], m_recv.at[index, f], at_device(d, c, to)).start()

    dy_line.forward(1)

    for at in range(ctx):
        for step in range(1, fs):
            other = lax.rem(f + step, fs)
            arrived(unit.at[at, other], u_recv.at[at, other], here)
    unit_copy = pltpu.make_async_copy(unit, unit_out, out_sem.at[3])
    unit_copy.start()

    rows = fs * span
    for at in range(ctx):
        keys = rows * (at + 1)
        k_rows = unit[0 : at + 1, :, :, 2 * LANES : 3 * LANES].reshape(keys, LANES)
        v_rows = unit[0 : at + 1, :, :, 3 * LANES : 4 * LANES].reshape(keys, LANES)
        allowed = lax.broadcasted_iota(jnp.int32, (rows, keys), 1) <= rows * at + lax.broadcasted_iota(
            jnp.int32, (rows, keys), 0
        )
        for head in range(2):
            q_rows = unit[at, :, :, head * LANES : (head + 1) * LANES].reshape(rows, LANES)
            scores = outer(q_rows, k_rows) * FACTOR
            scores = jnp.where(allowed, scores, NEG)
            best = jnp.max(scores, axis=-1, keepdims=True)
            weights = jnp.exp(scores - best)
            probs = weights / jnp.sum(weights, axis=-1, keepdims=True)
            mixed = jnp.dot(probs.astype(jnp.bfloat16), v_rows, preferred_element_type=jnp.float32)
            att_stage[at, :, :, head * LANES : (head + 1) * LANES] = mixed.astype(jnp.bfloat16).reshape(fs, span, LANES)
        for to in range(fs):

            @pl.when(to != f)
            def _():
                remote(
                    att_stage.at[at, to], att.at[f // 2, at, lax.rem(f, 2)], a_send.at[at, to], a_recv.at[f, at], at_device(d, c, to)
                ).start()

            @pl.when(to == f)
            def _():
                att[f // 2, at, lax.rem(f, 2)] = att_stage[at, to]

        if at == ctx - 1:
            dy_line.forward(2)

    for at in range(ctx):
        for step in range(1, fs):
            other = lax.rem(f + step, fs)
            arrived(att.at[other // 2, at, lax.rem(other, 2)], a_recv.at[other, at], here)
    att_copy = pltpu.make_async_copy(att, att_out, out_sem.at[4])
    att_copy.start()

    for at in range(ctx):
        dy_line.other(at)
    dy_line.finish()
    for index, (shard, whole) in enumerate(moved):
        for step in range(1, fs):
            other = lax.rem(f + step, fs)
            arrived(whole.at[other], m_recv.at[index, other], here)
            left(whole.at[f], m_pass.at[index, step], here)

        @pl.when(jnp.logical_not(stays))
        def _():
            left(shard, m_send.at[index], here)

    arrived(down_out, down_recv, here)

    @pl.when(jnp.logical_not(stays))
    def _():
        left(down_ref, down_send, here)

    for part in range(gu_send.shape[0]):
        src = gate_up_ref.at[part * part_rows : (part + 1) * part_rows]
        for slot in range(4):
            arrived(gate_up_all.at[slot, part * part_rows : (part + 1) * part_rows], gu_recv.at[part, slot], here)
        for to in range(fs):

            @pl.when(jnp.logical_not(jnp.logical_and(gu_core == d, f == to)))
            def _():
                left(src, gu_send.at[part, to], here)

    line.finish_sends()
    for at in range(ctx):

        for to in range(fs):

            @pl.when(to != f)
            def _():
                left(stage.at[at, to], u_send.at[at, to], here)
                left(att_stage.at[at, to], a_send.at[at, to], here)

    @pl.when(jnp.logical_and(d == 1, kv_away))
    def _():
        left(w_ref, w_send.at[0], here)

    @pl.when(d == 0)
    def _():
        for to in range(fs):

            @pl.when(jnp.logical_or(q_core != 0, to != f))
            def _():
                left(w_ref, w_send.at[to], here)

    for slot in (2, 3):

        @pl.when(relay_of[slot])
        def _():
            for step in range(1, fs):
                left(head_rows(slot), w_pass.at[slot - 2, step], here)

    def gain_left(step, carry):
        other = lax.rem(me + step, n)
        left(gains_ref, g_send.at[other], here)
        return carry

    lax.fori_loop(1, n, gain_left, 0)
    for copy in (normed_copy, wide_copy, gains_copy, unit_copy, att_copy):
        copy.wait()


def first(sizes, parts, sent, x, gains, w_qkv, blocks, steps, dy, w_out, w_down, w_gate_up):
    dp, ctx, fs = sizes
    n = dp * ctx * fs
    rows = x.shape[0]
    span = rows // 2
    low, wide_t = jnp.bfloat16, jnp.float32
    dma = pltpu.SemaphoreType.DMA
    shapes = (
        jax.ShapeDtypeStruct((dp, ctx, rows, D), low),
        jax.ShapeDtypeStruct((ctx, fs, span, 4 * LANES), low),
        jax.ShapeDtypeStruct((dp, ctx, 2, span, 2 * LANES), low),
        jax.ShapeDtypeStruct((4 * LANES, D), low),
        jax.ShapeDtypeStruct((8, D), wide_t),
        jax.ShapeDtypeStruct((dp, ctx, rows, D), low),
        jax.ShapeDtypeStruct((fs,) + w_out.shape, low),
        jax.ShapeDtypeStruct(w_down.shape, low),
        jax.ShapeDtypeStruct((4, D // parts * sent, w_gate_up.shape[1]), low),
    )
    any_spec, vm_spec = pl.BlockSpec(memory_space=ANY), pl.BlockSpec(memory_space=VM)
    return pl.pallas_call(
        functools.partial(first_kernel, sizes, parts),
        name="first",
        out_shape=shapes,
        in_specs=[vm_spec] * 9,
        out_specs=[any_spec] * 9,
        scratch_shapes=[
            VM((dp, ctx, rows, D), low),
            VM((4 * LANES, D), low),
            VM((dp, ctx, rows, D), low),
            VM((ctx, 2 * dp, span, 4 * LANES), low),
            VM((ctx, fs, span, 4 * LANES), low),
            VM((ctx, fs, span, 2 * LANES), low),
            VM((dp, ctx, 2, span, 2 * LANES), low),
            VM((n, 8, LANES), wide_t),
            VM((8, D), wide_t),
            dma((3, ctx, HALVES)), dma((dp, ctx, HALVES)), dma,
            dma((fs,)), dma((4,)), dma((2, fs)),
            dma((n,)), dma((n,)),
            dma((ctx, 2 * dp)), dma((ctx, fs)),
            dma((ctx, fs)), dma((fs, ctx)),
            dma((5,)),
            dma((3, ctx, HALVES)), dma((dp, ctx, HALVES)), dma,
            dma((1,)), dma((1, fs)), dma((1, fs)), dma, dma,
            dma((sent, fs)), dma((sent, 4)),
        ],
        compiler_params=pltpu.CompilerParams(collective_id=1, has_side_effects=True, vmem_limit_bytes=60 * 1024 * 1024),
    )(x, gains, w_qkv, blocks, steps, dy, w_out, w_down, w_gate_up)


def angle_tables(count, span):
    lane = jnp.arange(LANES, dtype=jnp.int32)
    frequency = THETA ** (-((lane % (HD // 2)).astype(jnp.float32) * 2.0) / HD)

    def both(positions):
        angles = positions.astype(jnp.float32)[:, None] * frequency
        return jnp.stack([jnp.cos(angles), jnp.sin(angles)])

    return both(jnp.arange(count, dtype=jnp.int32) * span), both(jnp.arange(span, dtype=jnp.int32))


def turns(block_ref, step_ref, block):
    cos_b, sin_b = block_ref[0, pl.ds(block, 1)], block_ref[1, pl.ds(block, 1)]
    cos_s, sin_s = step_ref[0], step_ref[1]
    cosine = cos_b * cos_s - sin_b * sin_s
    sine = sin_b * cos_s + cos_b * sin_s
    lane = lax.broadcasted_iota(jnp.int32, sine.shape, 1)
    first_half = lane < HD // 2
    sine_up = jnp.where(jnp.logical_and(lane >= HD // 2, lane < HD), sine, 0.0)
    return cosine, sine_up, jnp.where(first_half, -sine, 0.0)


class LineSum:
    def __init__(self, n, mine, out_core, in_core, out_line, in_line, total, sems):
        self.n, self.mine, self.out_core, self.in_core = n, mine, out_core, in_core
        self.out_line, self.in_line, self.total = out_line, in_line, total
        self.core_send, self.core_recv, self.line_send, self.line_recv = sems
        self.d, self.c, self.f = place()
        self.here = at_device(self.d, self.c, self.f)

    def give(self, at, both):
        self.keep(at, both)
        self.hand(at)

    def keep(self, at, both):
        d = self.d
        low = both.astype(jnp.bfloat16)

        @pl.when(d == 0)
        def _():
            self.mine[at] = low[0]
            self.out_core[at] = low[1]

        @pl.when(d != 0)
        def _():
            self.mine[at] = low[1]
            self.out_core[at] = low[0]

    def hand(self, at):
        remote(
            self.out_core.at[at], self.in_core.at[at], self.core_send.at[at], self.core_recv.at[at], at_device(1 - self.d, self.c, self.f)
        ).start()

    def step(self, at):
        n, d, c, f = self.n, self.d, self.c, self.f
        arrived(self.in_core.at[at], self.core_recv.at[at], self.here)
        rows = self.total.shape[0] // HALVES
        for part in range(HALVES):
            own = slice(part * rows, (part + 1) * rows)
            self.total[own] = self.mine[at, own].astype(jnp.float32) + self.in_core[at, own].astype(jnp.float32)
            for way, comes in enumerate((jnp.logical_and(at <= c, c < n - 1), jnp.logical_and(at >= c, c > 0))):

                @pl.when(comes)
                def _():
                    arrived(self.in_line.at[way, at, own], self.line_recv.at[way, at, part], self.here)
                    self.total[own] += self.in_line[way, at, own].astype(jnp.float32)

            @pl.when(at != c)
            def _():
                self.out_line[at, own] = self.total[own].astype(jnp.bfloat16)

            for way, (goes, to) in enumerate(((at < c, c - 1), (at > c, c + 1))):

                @pl.when(goes)
                def _():
                    remote(
                        self.out_line.at[at, own], self.in_line.at[way, at, own],
                        self.line_send.at[at, part], self.line_recv.at[way, at, part], at_device(d, to, f),
                    ).start()

    def finish(self):
        rows = self.total.shape[0] // HALVES
        for at in range(self.n):
            left(self.out_core.at[at], self.core_send.at[at], self.here)

            @pl.when(at != self.c)
            def _():
                for part in range(HALVES):
                    left(self.out_line.at[at, part * rows : (part + 1) * rows], self.line_send.at[at, part], self.here)

    @staticmethod
    def scratch(ctx, rows):
        low = jnp.bfloat16
        dma = pltpu.SemaphoreType.DMA
        return [
            VM((ctx, rows, D), low), VM((ctx, rows, D), low), VM((ctx, rows, D), low), VM((ctx, rows, D), low),
            VM((2, ctx, rows, D), low), VM((rows, D), jnp.float32),
            dma((ctx,)), dma((ctx,)), dma((ctx, HALVES)), dma((2, ctx, HALVES)),
        ]


def down_route(d, c):
    return (lax.rem(c, 2), 2 * d + c // 2), (c // 2, 2 * lax.rem(c, 2) + d)


def near_devices(sizes):
    dp, ctx, fs = sizes
    d, c, f = place()
    yes = c >= 0
    found = [(at_device(1 - d, c, f), yes)]
    for step in range(1, fs):
        for core in range(dp):
            found.append((at_device(core, c, lax.rem(f + step, fs)), yes))
    found.append((at_device(d, c - 1, f), c > 0))
    found.append((at_device(d, c + 1, f), c < ctx - 1))
    return found


def tell_near(sizes):
    barrier = pltpu.get_barrier_semaphore()
    for device, counts in near_devices(sizes):

        @pl.when(counts)
        def _():
            pl.semaphore_signal(barrier, inc=1, device_id=device, device_id_type=MESH)


def hear_near(sizes):
    peers = sum(jnp.where(counts, 1, 0) for _, counts in near_devices(sizes))
    pl.semaphore_wait(pltpu.get_barrier_semaphore(), peers)


def middle_kernel(
    sizes, hidden, parts, sent, att_ref, x_ref, dy_ref, gains_ref, proj_ref, down_ref, gate_up_ref, gate_up_part_ref, dy_all_ref,
    out_ref, d_resid_out, gain_out, unit_out, grad_proj_out, up_land, down_land,
    att, dy_all, proj, down, gate_up, resid, own_two, normed_two, act, d_both, own_d, d_resid_all, d_stage, unit,
    grad_up, grad_down, grad_proj, grad_proj_low,
    in_sem, dy_sem, gu_send, gu_recv, m_recv, m_pass, two_send, two_recv, two_local, dr_send, dr_recv, dr_local, u_send, u_recv,
    late_send, late_recv, late_pass, out_sem, gup_send, gup_recv, gdn_send, gdn_recv,
    *sums,
):
    dp, ctx, fs = sizes
    d, c, f = place()
    here = at_device(d, c, f)
    rows = x_ref.shape[0]
    span = rows // 2
    both_rows = dp * rows
    half = hidden // 2
    line_sum = LineSum(ctx, *sums[:6], sums[6:10])
    second_sum = LineSum(ctx, *sums[10:16], sums[16:20])
    out_sum = LineSum(ctx, *sums[20:26], sums[26:30])
    part_rows = D // parts
    tell_near(sizes)

    att_copy = pltpu.make_async_copy(att_ref, att, in_sem.at[0])
    part_copy = pltpu.make_async_copy(gate_up_part_ref, gate_up.at[:, 0 : part_rows * sent], in_sem.at[2])
    att_copy.start()
    proj[...] = jnp.zeros_like(proj)
    each = proj_ref.shape[1]
    proj_copies = []
    for slot in range(fs):
        start = slot // 2 * LANES + slot % 2 * each
        proj_copies.append(pltpu.make_async_copy(proj_ref.at[slot], proj.at[start : start + each], in_sem.at[3 + slot]))
        proj_copies[-1].start()

    def dy_load(at):
        return pltpu.make_async_copy(dy_all_ref.at[:, at], dy_all.at[:, at], dy_sem.at[at])

    for at in range(ctx):

        @pl.when(near_or_inner(c, at, ctx))
        def _():
            dy_load(at).start()

    part_copy.start()
    att_copy.wait()
    for copy in proj_copies:
        copy.wait()

    def project(step, carry):
        at = towards(c, step, ctx)
        terms = jnp.dot(att[:, at].reshape(both_rows, 2 * LANES), proj[...], preferred_element_type=jnp.float32)
        line_sum.keep(at, terms.reshape(dp, rows, D))
        return carry

    lax.fori_loop(0, ctx, project, 0)
    hear_near(sizes)

    ends = jnp.logical_or(c == 0, c == ctx - 1)
    last_hops = ((c == 1, -1), (c == ctx - 2, 1))

    def late(way, at, part):
        src, dst = part_of(dy_all_ref.at[d, at], part), part_of(dy_all.at[d, at], part)
        return remote(src, dst, late_send.at[at, part], late_recv.at[d, at, part], at_device(d, c + way, f))

    for sends, way in last_hops:
        for step in range(1, ctx - 1):

            @pl.when(sends)
            def _():
                for part in range(HALVES):
                    late(way, c - way * step, part).start()

    def late_across(at, part):
        block = part_of(dy_all.at[d, at], part)
        return remote(block, block, late_pass.at[at, part], late_recv.at[d, at, part], at_device(1 - d, c, f))

    def far(step):
        return jnp.where(c == 0, 1 + step, ctx - 2 - step)

    pltpu.make_async_copy(down_ref, down.at[f], m_recv.at[f]).start()
    for step in range(1, fs):
        to = lax.rem(f + step, fs)
        remote(down_ref, down.at[f], m_pass.at[step], m_recv.at[f], at_device(d, c, to)).start()
    for step in range(ctx):
        line_sum.hand(towards(c, step, ctx))

    gu_core = f // 2
    gu_slot = 2 * d + lax.rem(f, 2)
    rest = slice(part_rows * sent, D)
    for to in range(fs):
        own_place = jnp.logical_and(gu_core == d, f == to)

        @pl.when(jnp.logical_not(own_place))
        def _():
            remote(gate_up_ref.at[rest], gate_up.at[gu_slot, rest], gu_send.at[to], gu_recv.at[gu_slot], at_device(gu_core, c, to)).start()

        @pl.when(own_place)
        def _():
            pltpu.make_async_copy(gate_up_ref.at[rest], gate_up.at[gu_slot, rest], gu_recv.at[gu_slot]).start()

    line_sum.step(towards(c, 0, ctx))
    line_sum.step(towards(c, 1, ctx))
    line_sum.step(towards(c, 2, ctx))

    @pl.when(ends)
    def _():
        for step in range(1, ctx - 1):
            for part in range(HALVES):
                arrived(part_of(dy_all.at[d, far(step)], part), late_recv.at[d, far(step), part], here)
                late_across(far(step), part).start()

    line_sum.step(c)
    gain = gains_ref[1:2, :]
    values = x_ref[...].astype(jnp.float32) + line_sum.total[...]
    resid[...] = values
    scale = lax.rsqrt(jnp.mean(values * values, axis=-1, keepdims=True) + EPS)
    own_two[...] = (values * scale * gain).astype(jnp.bfloat16)
    line = LineGather(ctx, own_two, normed_two, two_send, two_recv, two_local)
    line.start()
    line.forward(1)
    for slot in range(4):
        arrived(gate_up.at[slot, rest], gu_recv.at[slot], here)
    for at in range(ctx):

        @pl.when(near_or_inner(c, at, ctx))
        def _():
            dy_load(at).wait()

    @pl.when(ends)
    def _():
        for step in range(1, ctx - 1):
            for part in range(HALVES):
                arrived(part_of(dy_all.at[1 - d, far(step)], part), late_recv.at[1 - d, far(step), part], here)
    part_copy.wait()
    for slot in range(fs):
        arrived(down.at[slot], m_recv.at[slot], here)
    pltpu.make_async_copy(line.own, line.slot(c), line.local).wait()

    def mlp(step, carry):
        at = ordered(c, step, ctx)


        @pl.when(lax.rem(step, 2) == 1)
        def _():
            line.forward(2 + step // 2)

        line.other(at)
        inputs = normed_two[:, at].reshape(both_rows, D)
        dy_rows = dy_all[:, at].reshape(both_rows, D)
        for part in range(2):
            cols = slice(part * half, (part + 1) * half)
            gate = jnp.dot(inputs, gate_up[part], preferred_element_type=jnp.float32)
            up = jnp.dot(inputs, gate_up[2 + part], preferred_element_type=jnp.float32)
            d_act = outer(dy_rows, down[2 * part : 2 * part + 2].reshape(half, D))
            sig = 1.0 / (1.0 + jnp.exp(-gate))
            silu = gate * sig
            act[:, at, :, cols] = (silu * up).astype(jnp.bfloat16).reshape(dp, rows, half)
            d_gate = d_act * up * (sig * (1.0 + gate * (1.0 - sig)))
            d_both[:, at, :, cols] = d_gate.astype(jnp.bfloat16).reshape(dp, rows, half)
            d_both[:, at, :, hidden + part * half : hidden + (part + 1) * half] = (
                (d_act * silu).astype(jnp.bfloat16).reshape(dp, rows, half)
            )
        terms = outer(d_both[:, at, :, 0:half].reshape(both_rows, half), gate_up[0])
        for part in range(1, 4):
            terms += outer(d_both[:, at, :, part * half : (part + 1) * half].reshape(both_rows, half), gate_up[part])
        second_sum.give(at, terms.reshape(dp, rows, D))
        return carry

    lax.fori_loop(0, ctx, mlp, 0)

    wide_rows = D // ctx

    def push(src, dst, send, recv, core, to):
        to_self = jnp.logical_and(core == d, to == f)

        @pl.when(jnp.logical_not(to_self))
        def _():
            remote(src, dst, send, recv, at_device(core, c, to)).start()

        @pl.when(to_self)
        def _():
            pltpu.make_async_copy(src, dst, recv).start()

    def grads(step):
        first = pl.multiple_of(step * wide_rows, LANES)
        left_rows = normed_two[:, :, :, pl.ds(first, wide_rows)].reshape(dp * ctx * rows, wide_rows)
        for part in range(2):
            cols = slice(part * hidden, (part + 1) * hidden)
            terms = inner(left_rows, d_both[:, :, :, cols].reshape(dp * ctx * rows, hidden)).astype(jnp.bfloat16)
            grad_up[2 * part, pl.ds(first, wide_rows), :] = terms[:, :half]
            grad_up[2 * part + 1, pl.ds(first, wide_rows), :] = terms[:, half:]
        dy_cols = dy_all[:, :, :, pl.ds(first, wide_rows)].reshape(dp * ctx * rows, wide_rows)
        terms = inner(act[...].reshape(dp * ctx * rows, hidden), dy_cols).astype(jnp.bfloat16)
        grad_down[:, :, pl.ds(first, wide_rows)] = terms.reshape(fs, hidden // fs, wide_rows)
        for slot in range(4):
            push(
                grad_up.at[slot, pl.ds(first, wide_rows)], up_land.at[f, pl.ds(first, wide_rows)],
                gup_send.at[slot, step], gup_recv.at[f, step], slot // 2, 2 * d + slot % 2,
            )
            push(
                grad_down.at[slot, :, pl.ds(first, wide_rows)], down_land.at[f, :, pl.ds(first, wide_rows)],
                gdn_send.at[slot, step], gdn_recv.at[f, step], d, slot,
            )

    def out_terms(step):
        at = towards(c, step, ctx)
        terms = jnp.dot(act[:, at].reshape(both_rows, hidden), down[...].reshape(hidden, D), preferred_element_type=jnp.float32)
        out_sum.give(at, terms.reshape(dp, rows, D))

    def second_steps():
        def body(step, carry):
            second_sum.step(towards(c, step, ctx))
            return carry

        lax.fori_loop(0, ctx - 1, body, 0)

    def local_terms(step, carry):
        grads(step)
        out_terms(step)
        return carry

    pl.when(ends)(second_steps)
    lax.fori_loop(0, ctx - 1, local_terms, 0)
    pl.when(jnp.logical_not(ends))(second_steps)
    local_terms(ctx - 1, 0)
    second_sum.step(c)
    values = resid[...]
    scale = lax.rsqrt(jnp.mean(values * values, axis=-1, keepdims=True) + EPS)
    incoming = second_sum.total[...]
    weighted = incoming * gain
    mean = jnp.mean(weighted * values, axis=-1, keepdims=True)
    d_resid = dy_ref[...].astype(jnp.float32) + scale * weighted - values * (scale * scale * scale) * mean
    own_d[...] = d_resid.astype(jnp.bfloat16)
    d_resid_out[...] = d_resid
    gain_out[...] = jnp.broadcast_to(jnp.sum(incoming * values * scale, axis=0, keepdims=True), gain_out.shape)
    d_line = LineGather(ctx, own_d, d_resid_all, dr_send, dr_recv, dr_local)
    d_line.start()
    def out_step(step, carry):
        out_sum.step(towards(c, step, ctx))
        return carry

    @pl.when(ends)
    def _():
        lax.fori_loop(0, ctx - 1, out_step, 0)

    pltpu.make_async_copy(d_line.own, d_line.slot(c), d_line.local).wait()
    grad_proj[...] = jnp.zeros_like(grad_proj)

    def back(step, carry):
        at = ordered(c, step, ctx)

        d_line.reach(step)
        d_line.other(at)
        incoming = d_resid_all[:, at].reshape(both_rows, D)
        d_att = outer(incoming, proj[...]).astype(jnp.bfloat16)
        d_stage[at] = d_att.reshape(2 * dp, span, 2 * LANES)
        for to in range(2 * dp):

            @pl.when(to != f)
            def _():
                remote(d_stage.at[at, to], unit.at[at, f], u_send.at[at, to], u_recv.at[at, f], at_device(d, c, to)).start()

            @pl.when(to == f)
            def _():
                unit[at, f] = d_stage[at, to]

        grad_proj[...] += inner(att[:, at].reshape(both_rows, 2 * LANES), incoming)

        @pl.when(jnp.logical_and(jnp.logical_not(ends), step == ctx - 2))
        def _():
            out_sum.step(towards(c, 0, ctx))

        return carry

    lax.fori_loop(0, ctx, back, 0)

    @pl.when(jnp.logical_not(ends))
    def _():
        lax.fori_loop(1, ctx - 1, out_step, 0)

    line_sum.finish()
    line.finish_sends()
    second_sum.finish()
    for slot in range(fs):
        start = slot // 2 * LANES + slot % 2 * each
        grad_proj_low[slot] = grad_proj[start : start + each, :].astype(jnp.bfloat16)
    grad_proj_copy = pltpu.make_async_copy(grad_proj_low, grad_proj_out, out_sem.at[1])
    grad_proj_copy.start()
    for at in range(ctx):
        for step in range(1, fs):
            other = lax.rem(f + step, fs)
            arrived(unit.at[at, other], u_recv.at[at, other], here)
    unit_copy = pltpu.make_async_copy(unit, unit_out, out_sem.at[2])
    unit_copy.start()
    out_step(ctx - 1, 0)
    out_ref[...] = (resid[...] + out_sum.total[...]).astype(jnp.bfloat16)
    d_line.finish_sends()
    out_sum.finish()
    for at in range(ctx):
        for to in range(fs):

            @pl.when(to != f)
            def _():
                left(d_stage.at[at, to], u_send.at[at, to], here)

    for to in range(fs):

        @pl.when(jnp.logical_not(jnp.logical_and(gu_core == d, f == to)))
        def _():
            left(gate_up_ref.at[rest], gu_send.at[to], here)

    for step in range(1, fs):
        left(down_ref, m_pass.at[step], here)
    for sends, way in last_hops:
        for step in range(1, ctx - 1):

            @pl.when(sends)
            def _():
                for part in range(HALVES):
                    left(part_of(dy_all_ref.at[d, c - way * step], part), late_send.at[c - way * step, part], here)

    @pl.when(ends)
    def _():
        for step in range(1, ctx - 1):
            for part in range(HALVES):
                left(part_of(dy_all.at[d, far(step)], part), late_pass.at[far(step), part], here)

    def settle_up(step, carry):
        first = pl.multiple_of(step * wide_rows, LANES)
        for slot in range(4):
            arrived(up_land.at[slot, pl.ds(first, wide_rows)], gup_recv.at[slot, step], here)

            @pl.when(jnp.logical_or(slot // 2 != d, 2 * d + slot % 2 != f))
            def _():
                left(grad_up.at[slot, pl.ds(first, wide_rows)], gup_send.at[slot, step], here)

        return carry

    def settle_down(step, carry):
        first = pl.multiple_of(step * wide_rows, LANES)
        for slot in range(4):
            arrived(down_land.at[slot, :, pl.ds(first, wide_rows)], gdn_recv.at[slot, step], here)

            @pl.when(slot != f)
            def _():
                left(grad_down.at[slot, :, pl.ds(first, wide_rows)], gdn_send.at[slot, step], here)

        return carry

    lax.fori_loop(0, ctx, settle_up, 0)
    lax.fori_loop(0, ctx, settle_down, 0)
    for copy in (grad_proj_copy, unit_copy):
        copy.wait()


def middle(sizes, parts, sent, att, x, dy, gains, proj, w_down, w_gate_up, gate_up_part, dy_all):
    dp, ctx, fs = sizes
    rows = x.shape[0]
    span = rows // 2
    hidden = FF // (dp * ctx)
    low, wide_t = jnp.bfloat16, jnp.float32
    dma = pltpu.SemaphoreType.DMA
    any_spec, vm_spec = pl.BlockSpec(memory_space=ANY), pl.BlockSpec(memory_space=VM)
    shapes = (
        jax.ShapeDtypeStruct((rows, D), low),
        jax.ShapeDtypeStruct((rows, D), wide_t),
        jax.ShapeDtypeStruct((8, D), wide_t),
        jax.ShapeDtypeStruct((ctx, fs, span, 2 * LANES), low),
        jax.ShapeDtypeStruct(proj.shape, low),
        jax.ShapeDtypeStruct((fs, D, hidden // 2), low),
        jax.ShapeDtypeStruct((fs, hidden // fs, D), low),
    )
    return pl.pallas_call(
        functools.partial(middle_kernel, sizes, hidden, parts, sent),
        name="middle",
        out_shape=shapes,
        in_specs=[any_spec, vm_spec, vm_spec, vm_spec, any_spec, vm_spec, vm_spec, any_spec, any_spec],
        out_specs=[vm_spec] * 3 + [any_spec] * 4,
        scratch_shapes=[
            VM((dp, ctx, rows, 2 * LANES), low),
            VM((dp, ctx, rows, D), low),
            VM((2 * LANES, D), low),
            VM((fs, hidden // fs, D), low),
            VM((4, D, hidden // 2), low),
            VM((rows, D), wide_t),
            VM((rows, D), low),
            VM((dp, ctx, rows, D), low),
            VM((dp, ctx, rows, hidden), low),
            VM((dp, ctx, rows, 2 * hidden), low),
            VM((rows, D), low),
            VM((dp, ctx, rows, D), low),
            VM((ctx, 2 * dp, span, 2 * LANES), low),
            VM((ctx, fs, span, 2 * LANES), low),
            VM((4, D, hidden // 2), low),
            VM((fs, hidden // fs, D), low),
            VM((2 * LANES, D), wide_t),
            VM(proj.shape, low),
            dma((3 + fs,)), dma((ctx,)), dma((fs,)), dma((4,)), dma((fs,)), dma((fs,)),
            dma((3, ctx, HALVES)), dma((dp, ctx, HALVES)), dma,
            dma((3, ctx, HALVES)), dma((dp, ctx, HALVES)), dma,
            dma((ctx, 2 * dp)), dma((ctx, fs)),
            dma((ctx, HALVES)), dma((dp, ctx, HALVES)), dma((ctx, HALVES)), dma((3,)),
            dma((4, ctx)), dma((fs, ctx)), dma((fs, ctx)), dma((fs, ctx)),
        ] + LineSum.scratch(ctx, rows) * 3,
        compiler_params=pltpu.CompilerParams(collective_id=2, has_side_effects=True, vmem_limit_bytes=63 * 1024 * 1024),
    )(att, x, dy, gains, proj, w_down, w_gate_up, gate_up_part, dy_all)


def last_kernel(
    sizes, x_ref, gains_ref, block_ref, step_ref, d_resid_ref, gain_two_ref, proj_ref,
    unit_ref, d_unit_ref, normed_ref, wide_ref, up_land_ref, down_land_ref,
    d_x_ref, gains_out, qkv_out, proj_out, up_out, down_out,
    unit, d_unit, d_k, d_v, stage, mixed, normed, wide, grad_heads,
    up_land, down_land, proj_land, q_land, kv_land, down_sum, proj_sum, kv_sum, down_last, proj_last, kv_last, gain_vec, gain_stage, gain_land,
    in_sem, proj_send, proj_recv, head_send, head_recv, move_send, move_recv,
    u_send, u_recv, g_send, g_recv,
    *sums,
):
    dp, ctx, fs = sizes
    n = dp * ctx * fs
    d, c, f = place()
    here = at_device(d, c, f)
    me = (d * ctx + c) * fs + f
    rows = x_ref.shape[0]
    span = rows // 2
    both_rows = dp * rows
    low, wide_t = jnp.bfloat16, jnp.float32
    loads = [
        pltpu.make_async_copy(src, dst, in_sem.at[index])
        for index, (src, dst) in enumerate((
            (unit_ref, unit), (d_unit_ref, d_unit), (normed_ref, normed), (wide_ref, wide), (down_land_ref, down_land), (up_land_ref, up_land),
        ))
    ]
    tell_all(sizes)
    for load in loads:
        load.start()
    in_sum = LineSum(ctx, *sums[:6], sums[6:10])
    d_k[...] = jnp.zeros_like(d_k)
    d_v[...] = jnp.zeros_like(d_v)

    def push(src, land, send, recv, core, fs_to):
        to_self = jnp.logical_and(core == d, fs_to == f)

        @pl.when(jnp.logical_not(to_self))
        def _():
            remote(src, land.at[f], send, recv.at[f], at_device(core, c, fs_to)).start()

        @pl.when(to_self)
        def _():
            pltpu.make_async_copy(src, land.at[f], recv.at[f]).start()

    def pushed(src, send, core, fs_to):
        @pl.when(jnp.logical_not(jnp.logical_and(core == d, fs_to == f)))
        def _():
            left(src, send, here)

    def sum_of(land):
        total = land[0].astype(wide_t)
        for source in range(1, fs):
            total += land[source].astype(wide_t)
        return total

    _, (own_core, own_ctx) = down_route(d, c)
    stays = jnp.logical_and(own_core == d, own_ctx == c)

    def move(index, src, dst):
        @pl.when(jnp.logical_not(stays))
        def _():
            remote(src, dst, move_send.at[index], move_recv.at[index], at_device(own_core, own_ctx, f)).start()

        @pl.when(stays)
        def _():
            pltpu.make_async_copy(src, dst, move_recv.at[index]).start()

    loads[0].wait()
    loads[1].wait()
    block = fs * span

    def unturn(values, at):
        up = pltpu.roll(values, HD // 2, 1)
        down = pltpu.roll(values, LANES - HD // 2, 1)
        pieces = []
        for index in range(fs):
            own = slice(index * span, (index + 1) * span)
            cosine, sine_up, sine_down = turns(block_ref, step_ref, at * fs + index)
            pieces.append(values[own] * cosine - up[own] * sine_up - down[own] * sine_down)
        return jnp.concatenate(pieces, axis=0).reshape(fs, span, LANES)

    for at in reversed(range(ctx)):
        keys = block * (at + 1)
        k_rows = unit[0 : at + 1, :, :, 2 * LANES : 3 * LANES].reshape(keys, LANES)
        v_rows = unit[0 : at + 1, :, :, 3 * LANES : 4 * LANES].reshape(keys, LANES)
        allowed = lax.broadcasted_iota(jnp.int32, (block, keys), 1) <= block * at + lax.broadcasted_iota(
            jnp.int32, (block, keys), 0
        )
        for head in range(2):
            lanes = slice(head * LANES, (head + 1) * LANES)
            q_rows = unit[at, :, :, lanes].reshape(block, LANES)
            d_rows = d_unit[at, :, :, lanes].reshape(block, LANES)
            scores = jnp.where(allowed, outer(q_rows, k_rows) * FACTOR, NEG)
            weights = jnp.exp(scores - jnp.max(scores, axis=-1, keepdims=True))
            probs = weights / jnp.sum(weights, axis=-1, keepdims=True)
            d_probs = outer(d_rows, v_rows)
            delta = jnp.sum(probs * d_probs, axis=-1, keepdims=True)
            d_scores = (probs * (d_probs - delta)).astype(low)
            d_q = jnp.dot(d_scores, k_rows, preferred_element_type=wide_t) * FACTOR
            stage[at, :, :, lanes] = unturn(d_q, at).astype(low)
            d_k[0:keys, :] += inner(d_scores, q_rows) * FACTOR
            d_v[0:keys, :] += inner(probs.astype(low), d_rows)
        stage[at, :, :, 2 * LANES : 3 * LANES] = unturn(d_k[block * at : keys, :], at).astype(low)
        stage[at, :, :, 3 * LANES : 4 * LANES] = d_v[block * at : keys, :].astype(low).reshape(fs, span, LANES)
        if at == ctx - 1:
            hear_all(sizes)
        for to in range(fs):

            @pl.when(to != f)
            def _():
                remote(
                    stage.at[at, to], mixed.at[f // 2, at, lax.rem(f, 2)], u_send.at[at, to], u_recv.at[f, at], at_device(d, c, to)
                ).start()

            @pl.when(to == f)
            def _():
                mixed[f // 2, at, lax.rem(f, 2)] = stage[at, to]

        if at == ctx - 1:
            loads[4].wait()
            down_sum[...] = sum_of(down_land).astype(low)
            move(0, down_sum, down_last)
    for slot in range(fs):
        push(proj_ref.at[slot], proj_land, proj_send.at[slot], proj_recv, d, slot)
    loads[2].wait()
    loads[3].wait()

    ends = jnp.logical_or(c == 0, c == ctx - 1)

    def give(step, carry):
        at = towards(c, step, ctx)
        for move_ in range(1, fs):
            other = lax.rem(f + move_, fs)
            arrived(mixed.at[other // 2, at, lax.rem(other, 2)], u_recv.at[other, at], here)
        terms = jnp.dot(mixed[:, at].reshape(both_rows, 4 * LANES), wide[...], preferred_element_type=wide_t)
        in_sum.give(at, terms.reshape(dp, rows, D))

        @pl.when(jnp.logical_and(ends, jnp.logical_and(step > 0, step < ctx - 1)))
        def _():
            in_sum.step(towards(c, step - 1, ctx))

        return carry

    lax.fori_loop(0, ctx, give, 0)

    every = dp * ctx * rows
    k_relay = 2 * lax.rem(c, 2) + d
    relays = (k_relay, lax.rem(k_relay + 2, fs))
    gain_terms = jnp.zeros((1, D), wide_t)
    for slot in (2, 3, 0, 1):
        heads = inner(mixed[:, :, :, :, slot * LANES : (slot + 1) * LANES].reshape(every, LANES), normed[...].reshape(every, D))
        grad_heads[slot] = heads[:HD].astype(low)
        weights = wide[slot * LANES : slot * LANES + HD, :].astype(wide_t)
        gain_terms += jnp.sum(heads[:HD] * weights, axis=0, keepdims=True)
        if slot < 2:
            push(grad_heads.at[slot], q_land, head_send.at[slot], head_recv.at[0], 0, 2 * d + slot)
        else:
            push(grad_heads.at[slot], kv_land.at[slot - 2], head_send.at[slot], head_recv.at[slot - 1], d, relays[slot - 2])

    gain = gains_ref[0:1, :]
    gain_vec[0:1, :] = gain_terms / gain
    gain_vec[1:2, :] = gain_two_ref[0:1, :]
    each = D // n
    for index in range(n):
        gain_stage[index, :, 0:each] = gain_vec[:, index * each : (index + 1) * each]
    gain_land[me] = gain_stage[me]

    def gain_to(step, carry):
        other = lax.rem(me + step, n)
        remote(
            gain_stage.at[other], gain_land.at[me], g_send.at[other], g_recv.at[me],
            at_device(other // (ctx * fs), lax.rem(other // fs, ctx), lax.rem(other, fs)),
        ).start()
        return carry

    lax.fori_loop(1, n, gain_to, 0)

    for source in range(fs):
        arrived(proj_land.at[source], proj_recv.at[source], here)
    proj_sum[...] = sum_of(proj_land).astype(low)
    move(1, proj_sum, proj_last)

    def middle_step(step, carry):
        in_sum.step(towards(c, step, ctx))
        return carry

    lax.fori_loop(jnp.where(ends, ctx - 2, 0), ctx - 1, middle_step, 0)

    def kv_route(slot):
        owner, owner_f = slot * 2 + c // 2, k_relay
        return owner, owner_f, jnp.logical_or(jnp.logical_or(d != 1, owner != c), owner_f != f)

    for slot in range(2):
        owner, owner_f, away = kv_route(slot)

        @pl.when(f == relays[slot])
        def _():
            for source in range(fs):
                arrived(kv_land.at[slot, source], head_recv.at[1 + slot, source], here)
            kv_sum[slot] = sum_of(kv_land.at[slot]).astype(low)

            @pl.when(away)
            def _():
                remote(kv_sum.at[slot], kv_last, move_send.at[2 + slot], move_recv.at[2], at_device(1, owner, owner_f)).start()

            @pl.when(jnp.logical_not(away))
            def _():
                pltpu.make_async_copy(kv_sum.at[slot], kv_last, move_recv.at[2]).start()

    loads[5].wait()
    up_out[...] = sum_of(up_land)
    in_sum.step(c)

    values = x_ref[...].astype(wide_t)
    scale = lax.rsqrt(jnp.mean(values * values, axis=-1, keepdims=True) + EPS)
    incoming = in_sum.total[...]
    weighted = incoming * gain
    mean = jnp.mean(weighted * values, axis=-1, keepdims=True)
    d_x_ref[...] = (d_resid_ref[...] + scale * weighted - values * (scale * scale * scale) * mean).astype(low)

    @pl.when(d == 0)
    def _():
        for source in range(fs):
            arrived(q_land.at[source], head_recv.at[0, source], here)
        qkv_out[...] = sum_of(q_land)

    for index, dst in enumerate((down_last, proj_last)):
        arrived(dst, move_recv.at[index], here)
    down_out[...] = down_last[...].astype(wide_t)
    proj_out[...] = proj_last[...].astype(wide_t)

    @pl.when(d == 1)
    def _():
        arrived(kv_last, move_recv.at[2], here)
        qkv_out[...] = kv_last[...].astype(wide_t)

    def gain_from(step, carry):
        other = lax.rem(me + step, n)
        arrived(gain_land.at[other], g_recv.at[other], here)
        return carry

    lax.fori_loop(1, n, gain_from, 0)
    total = gain_land[0]
    for index in range(1, n):
        total += gain_land[index]
    gains_out[...] = total

    for slot in range(fs):
        pushed(proj_ref.at[slot], proj_send.at[slot], d, slot)
    for slot in range(2):
        pushed(grad_heads.at[slot], head_send.at[slot], 0, 2 * d + slot)
        pushed(grad_heads.at[2 + slot], head_send.at[2 + slot], d, relays[slot])
        away = kv_route(slot)[2]

        @pl.when(jnp.logical_and(f == relays[slot], away))
        def _():
            left(kv_sum.at[slot], move_send.at[2 + slot], here)

        @pl.when(jnp.logical_not(stays))
        def _():
            left((down_sum, proj_sum)[slot], move_send.at[slot], here)

    for at in range(ctx):
        for to in range(fs):

            @pl.when(to != f)
            def _():
                left(stage.at[at, to], u_send.at[at, to], here)

    in_sum.finish()

    def gain_left(step, carry):
        other = lax.rem(me + step, n)
        left(gain_stage.at[other], g_send.at[other], here)
        return carry

    lax.fori_loop(1, n, gain_left, 0)


def last(sizes, x, gains, tables, d_resid, gain_two, grad_proj, unit, d_unit, normed, wide, up_land, down_land):
    dp, ctx, fs = sizes
    n = dp * ctx * fs
    rows = x.shape[0]
    span = rows // 2
    low, wide_t = jnp.bfloat16, jnp.float32
    dma = pltpu.SemaphoreType.DMA
    any_spec, vm_spec = pl.BlockSpec(memory_space=ANY), pl.BlockSpec(memory_space=VM)
    down_rows, proj_rows, half = down_land.shape[1], grad_proj.shape[1], up_land.shape[2]
    shapes = (
        jax.ShapeDtypeStruct((rows, D), low),
        jax.ShapeDtypeStruct((8, LANES), wide_t),
        jax.ShapeDtypeStruct((HD, D), wide_t),
        jax.ShapeDtypeStruct((proj_rows, D), wide_t),
        jax.ShapeDtypeStruct((D, half), wide_t),
        jax.ShapeDtypeStruct((down_rows, D), wide_t),
    )
    return pl.pallas_call(
        functools.partial(last_kernel, sizes),
        name="last",
        out_shape=shapes,
        in_specs=[vm_spec] * 7 + [any_spec] * 6,
        out_specs=[vm_spec] * 6,
        scratch_shapes=[
            VM(unit.shape, low),
            VM(d_unit.shape, low),
            VM((ctx * fs * span, LANES), wide_t),
            VM((ctx * fs * span, LANES), wide_t),
            VM((ctx, fs, span, 4 * LANES), low),
            VM((dp, ctx, 2, span, 4 * LANES), low),
            VM(normed.shape, low),
            VM(wide.shape, low),
            VM((4, HD, D), low),
            VM(up_land.shape, low),
            VM((fs, down_rows, D), low),
            VM((fs, proj_rows, D), low),
            VM((fs, HD, D), low),
            VM((2, fs, HD, D), low),
            VM((down_rows, D), low),
            VM((proj_rows, D), low),
            VM((2, HD, D), low),
            VM((down_rows, D), low),
            VM((proj_rows, D), low),
            VM((HD, D), low),
            VM((8, D), wide_t),
            VM((n, 8, LANES), wide_t),
            VM((n, 8, LANES), wide_t),
            dma((6,)), dma((fs,)), dma((fs,)),
            dma((4,)), dma((3, fs)), dma((4,)), dma((3,)),
            dma((ctx, fs)), dma((fs, ctx)), dma((n,)), dma((n,)),
        ] + LineSum.scratch(ctx, rows),
        compiler_params=pltpu.CompilerParams(collective_id=3, has_side_effects=True, vmem_limit_bytes=63 * 1024 * 1024),
    )(x, gains, *tables, d_resid, gain_two, grad_proj, unit, d_unit, normed, wide, up_land, down_land)


def emit_kernel(count, gains_ref, *refs):
    sources, outs, one_ref, two_ref = refs[:count], refs[count : 2 * count], refs[2 * count], refs[2 * count + 1]
    held, in_sem, out_sem = refs[2 * count + 2 : 3 * count + 2], refs[-2], refs[-1]
    loads = [pltpu.make_async_copy(sources[i], held[i], in_sem.at[i]) for i in range(count)]
    stores = [pltpu.make_async_copy(held[i], outs[i], out_sem.at[i]) for i in range(count)]
    for load in loads:
        load.start()
    each = one_ref.shape[0]
    one_ref[...] = gains_ref[0, :each]
    two_ref[...] = gains_ref[1, :each]
    for load, store in zip(loads, stores):
        load.wait()
        store.start()
    for store in stores:
        store.wait()


def emit(each, gains, *arrays):
    count = len(arrays)
    any_spec, vm_spec = pl.BlockSpec(memory_space=ANY), pl.BlockSpec(memory_space=VM)
    gain = jax.ShapeDtypeStruct((each,), jnp.float32)
    return pl.pallas_call(
        functools.partial(emit_kernel, count),
        name="emit",
        out_shape=[jax.ShapeDtypeStruct(a.shape, a.dtype) for a in arrays] + [gain, gain],
        in_specs=[vm_spec] + [any_spec] * count,
        out_specs=[any_spec] * count + [vm_spec] * 2,
        scratch_shapes=[VM(a.shape, a.dtype) for a in arrays] + [pltpu.SemaphoreType.DMA((count,))] * 2,
        compiler_params=pltpu.CompilerParams(vmem_limit_bytes=63 * 1024 * 1024),
    )(gains, *arrays)


def on_device(tokens, cotangent, attn_gain, w_qkv, w_out, mlp_gain, w_gate_up, w_down):
    dp, ctx, fs = where = tuple(lax.axis_size(name) for name in ("dp", "ctx", "fsdp"))
    mb, _, span, _ = tokens.shape
    rows = mb * span
    x = tokens.reshape(rows, D)
    dy = cotangent.reshape(rows, D)
    each = attn_gain.shape[0]
    gain_rows = jnp.concatenate([attn_gain[None], mlp_gain[None]]).astype(jnp.float32)
    gain_rows = jnp.pad(gain_rows, ((0, 6), (0, LANES - each)))
    tables = angle_tables(ctx * fs, span)
    parts, sent = 4, 1
    normed, unit, att, qkv, gains, dy_all, proj, down, gate_up = first(
        where, parts, sent, x, gain_rows, w_qkv.T, *tables, dy, w_out, w_down, w_gate_up
    )
    att = att.reshape(dp, ctx, rows, 2 * LANES)
    block_out, d_resid, grad_two, d_unit, grad_proj, up_land, down_land = middle(
        where, parts, sent, att, x, dy, gains, proj, down, w_gate_up, gate_up, dy_all
    )
    grad_tokens, gain_grads, grad_qkv, grad_out, grad_gate_up, grad_down = last(
        where, x, gains, tables, d_resid, grad_two, grad_proj, unit, d_unit, normed, qkv, up_land, down_land
    )
    block_out, grad_tokens, grad_qkv, grad_out, grad_gate_up, grad_down, grad_one, grad_two = emit(
        each, gain_grads, block_out, grad_tokens, grad_qkv, grad_out, grad_gate_up, grad_down
    )
    return (
        block_out.reshape(tokens.shape),
        grad_tokens.reshape(tokens.shape),
        grad_one,
        grad_qkv.T,
        grad_out,
        grad_two,
        grad_gate_up,
        grad_down,
    )


def fits(mesh):
    return mesh.shape["dp"] == 2 and mesh.shape["ctx"] == 4 and mesh.shape["fsdp"] == 4


def solution(mesh):
    placed = (
        P(None, "dp", ("ctx", "fsdp"), None),
        P(None, "dp", ("ctx", "fsdp"), None),
        P(("dp", "ctx", "fsdp")),
        P(None, ("dp", "ctx", "fsdp")),
        P(("dp", "ctx", "fsdp"), None),
        P(("dp", "ctx", "fsdp")),
        P(None, ("dp", "ctx", "fsdp")),
        P(("dp", "ctx", "fsdp"), None),
    )
    return jax.shard_map(
        on_device if fits(mesh) else on_device_gathered,
        mesh=mesh,
        in_specs=placed,
        out_specs=(
            P(None, "dp", ("ctx", "fsdp"), None),
            P(None, "dp", ("ctx", "fsdp"), None),
            P(("dp", "ctx", "fsdp")),
            P(None, ("dp", "ctx", "fsdp")),
            P(("dp", "ctx", "fsdp"), None),
            P(("dp", "ctx", "fsdp")),
            P(None, ("dp", "ctx", "fsdp")),
            P(("dp", "ctx", "fsdp"), None),
        ),
        check_vma=False,
    )
```

```python
import functools
import math

import jax
import jax.numpy as jnp
from jax import lax
from jax.experimental import pallas as pl
from jax.experimental.pallas import tpu as pltpu
from jax.sharding import PartitionSpec as P

D = 1536
H = 16
KVH = 8
HD = 96
FF = 4096


EPS = 1e-05
THETA = 100000.0
NEG = -1e30


def in_blocks(value, dim, length):
    lengths = value.shape
    pieces = value.reshape(*lengths[:dim], length, lengths[dim] // length, *lengths[dim + 1 :])
    return jnp.moveaxis(pieces, dim, 0)


def sum_at_owner(value, axis, dim):
    pieces = in_blocks(value, dim, lax.axis_size(axis))
    arrived = lax.all_to_all(pieces, axis, split_axis=0, concat_axis=0, tiled=True)
    return arrived.astype(jnp.float32).sum(axis=0)


def side_by_side(arrays, axis, dim, along):
    both = jnp.concatenate(arrays, axis=along)
    whole, at, finished = (sum_at_owner(both, axis, dim), 0, [])
    for a in arrays:
        finished.append(lax.slice_in_dim(whole, at, at + a.shape[along], axis=along))
        at += a.shape[along]
    return tuple(finished)


def rms_norm(values, gain_vec):
    return values * lax.rsqrt(jnp.mean(values * values, axis=-1, keepdims=True) + EPS) * gain_vec


def tables(start, length, width):
    half_width = width // 2
    frequency = THETA ** (-(jnp.arange(half_width, dtype=jnp.float32) * 2.0) / width)
    angles = (start + jnp.arange(length, dtype=jnp.int32)).astype(jnp.float32)[:, None] * frequency[
        None, :
    ]
    return (jnp.cos(angles), jnp.sin(angles))


def rotate(values, cosine, sine_table):
    half_width = values.shape[-1] // 2
    first_half = values[..., :half_width]
    second_half = values[..., half_width:]
    cos_b = cosine[:, None, :]
    sin_b = sine_table[:, None, :]
    return jnp.concatenate(
        [first_half * cos_b - second_half * sin_b, second_half * cos_b + first_half * sin_b],
        axis=-1,
    )


def swiglu(both):
    return jax.nn.silu(both[:, :FF]) * both[:, FF:]


def inner(left, right):
    return lax.dot_general(
        left, right, (((0,), (0,)), ((), ())), preferred_element_type=jnp.float32
    )


def outer(left, right):
    return lax.dot_general(
        left, right, (((1,), (1,)), ((), ())), preferred_element_type=jnp.float32
    )


def unchanged(state):
    return state


def on_device_gathered(tokens, cotangent, attn_gain, w_qkv, w_out, mlp_gain, w_gate_up, w_down):
    tok_count = tokens.shape[2]
    groups = H // KVH
    factor = HD ** (-0.5)
    seq_length = tok_count * lax.axis_size(("ctx", "fsdp"))
    pos_first = lax.axis_index(("ctx", "fsdp")) * tok_count
    positions = pos_first + jnp.arange(tok_count, dtype=jnp.int32)
    pos_last = pos_first + tok_count - 1
    cosine, sine_table = tables(pos_first, tok_count, HD)
    sums = [
        jnp.zeros((D,), jnp.float32),
        jnp.zeros((D, (H + 2 * KVH) * HD), jnp.float32),
        jnp.zeros((H * HD, D), jnp.float32),
        jnp.zeros((D,), jnp.float32),
        jnp.zeros((D, 2 * FF), jnp.float32),
        jnp.zeros((FF, D), jnp.float32),
    ]
    outputs = []
    in_grads = []
    whole = (
        lax.all_gather(attn_gain, ("dp", "ctx", "fsdp"), axis=0, tiled=True),
        lax.all_gather(w_qkv, ("dp", "ctx", "fsdp"), axis=1, tiled=True),
        lax.all_gather(w_out, ("dp", "ctx", "fsdp"), axis=0, tiled=True),
        lax.all_gather(mlp_gain, ("dp", "ctx", "fsdp"), axis=0, tiled=True),
        lax.all_gather(w_gate_up, ("dp", "ctx", "fsdp"), axis=1, tiled=True),
        lax.all_gather(w_down, ("dp", "ctx", "fsdp"), axis=0, tiled=True),
    )
    for step_index in range(tokens.shape[0]):
        gain_one, mix_qkv, mix_out, gain_two, mix_gate_up, mix_down = whole
        inputs = tokens[step_index, 0].astype(jnp.float32)
        normed = rms_norm(inputs, gain_one.astype(jnp.float32)).astype(jnp.bfloat16)
        mixed = jnp.dot(normed, mix_qkv, preferred_element_type=jnp.float32)
        queries = rotate(mixed[:, : H * HD].reshape(tok_count, H, HD), cosine, sine_table).astype(
            jnp.bfloat16
        )
        key_rows = rotate(
            mixed[:, H * HD : (H + KVH) * HD].reshape(tok_count, KVH, HD), cosine, sine_table
        )
        key_rows = key_rows.astype(jnp.bfloat16).reshape(tok_count, KVH * HD)
        value_rows = mixed[:, (H + KVH) * HD :].astype(jnp.bfloat16)
        grouped = queries.reshape(tok_count, KVH, groups, HD)
        start_state = (
            jnp.full((KVH, groups, tok_count), NEG, jnp.float32),
            jnp.zeros((KVH, groups, tok_count), jnp.float32),
            jnp.zeros((KVH, groups, tok_count, HD), jnp.float32),
        )
        piece = (
            lax.all_gather(key_rows, ("ctx", "fsdp"), axis=0, tiled=True),
            lax.all_gather(value_rows, ("ctx", "fsdp"), axis=0, tiled=True),
        )

        def work(state):
            best, total, summed = state
            key_count = piece[0].shape[0]
            keys = piece[0].reshape(key_count, KVH, HD)
            values = piece[1].reshape(key_count, KVH, HD)
            scores = (
                jnp.einsum("qkgd,tkd->kgqt", grouped, keys, preferred_element_type=jnp.float32)
                * factor
            )
            allowed = jnp.arange(key_count, dtype=jnp.int32)[None, :] <= positions[:, None]
            scores = jnp.where(allowed, scores, NEG)
            new_best = jnp.maximum(best, jnp.max(scores, axis=-1))
            weights = jnp.where(allowed, jnp.exp(scores - new_best[..., None]), 0.0)
            total = jnp.sum(weights, axis=-1)
            summed = jnp.einsum(
                "kgqt,tkd->kgqd",
                weights.astype(jnp.bfloat16),
                values,
                preferred_element_type=jnp.float32,
            )
            return (new_best, total, summed)

        best, total, summed = lax.cond(jnp.int32(0) <= pos_last, work, unchanged, start_state)
        head_out = summed / total[..., None]
        log_total = best + jnp.log(total)
        attended = (
            jnp.transpose(head_out, (2, 0, 1, 3)).reshape(tok_count, H * HD).astype(jnp.bfloat16)
        )
        resid = inputs + jnp.dot(attended, mix_out, preferred_element_type=jnp.float32)
        normed_two = rms_norm(resid, gain_two.astype(jnp.float32)).astype(jnp.bfloat16)
        both = jnp.dot(normed_two, mix_gate_up, preferred_element_type=jnp.float32)
        acted = swiglu(both).astype(jnp.bfloat16)
        result = resid + jnp.dot(acted, mix_down, preferred_element_type=jnp.float32)
        outputs.append(result.astype(jnp.bfloat16))
        gain_one, mix_qkv, mix_out, gain_two, mix_gate_up, mix_down = whole
        up_low = cotangent[step_index, 0]
        upstream = up_low.astype(jnp.float32)
        sums[5] = sums[5] + inner(acted, up_low)
        d_act = outer(up_low, mix_down)
        _, pull_glu = jax.vjp(swiglu, both)
        d_both = pull_glu(d_act)[0].astype(jnp.bfloat16)
        sums[4] = sums[4] + inner(normed_two, d_both)
        d_normed_two = outer(d_both, mix_gate_up)
        _, pull_two = jax.vjp(rms_norm, resid, gain_two.astype(jnp.float32))
        d_resid_norm, d_gain_two = pull_two(d_normed_two)
        sums[3] = sums[3] + d_gain_two
        d_resid = upstream + d_resid_norm
        d_resid_low = d_resid.astype(jnp.bfloat16)
        sums[2] = sums[2] + inner(attended, d_resid_low)
        d_attended = outer(d_resid_low, mix_out).astype(jnp.bfloat16)
        d_grouped = d_attended.reshape(tok_count, KVH, groups, HD)
        delta = jnp.einsum("qkgd,kgqd->kgq", d_grouped.astype(jnp.float32), head_out)
        zero_q = jnp.zeros((tok_count, KVH, groups, HD), jnp.float32)
        back_state = (
            zero_q,
            jnp.zeros((seq_length, KVH * HD), jnp.float32),
            jnp.zeros((seq_length, KVH * HD), jnp.float32),
        )
        attend_piece = (
            lax.all_gather(key_rows, ("ctx", "fsdp"), axis=0, tiled=True),
            lax.all_gather(value_rows, ("ctx", "fsdp"), axis=0, tiled=True),
        )

        def attend_work(state):
            key_count = attend_piece[0].shape[0]
            keys = attend_piece[0].reshape(key_count, KVH, HD)
            values = attend_piece[1].reshape(key_count, KVH, HD)
            scores = (
                jnp.einsum("qkgd,tkd->kgqt", grouped, keys, preferred_element_type=jnp.float32)
                * factor
            )
            allowed = jnp.arange(key_count, dtype=jnp.int32)[None, :] <= positions[:, None]
            scores = jnp.where(allowed, scores, NEG)
            probs = jnp.where(allowed, jnp.exp(scores - log_total[..., None]), 0.0)
            d_probs = jnp.einsum(
                "qkgd,tkd->kgqt", d_grouped, values, preferred_element_type=jnp.float32
            )
            d_scores = (probs * (d_probs - delta[..., None])).astype(jnp.bfloat16)
            grad_q = jnp.einsum(
                "kgqt,tkd->qkgd", d_scores, keys, preferred_element_type=jnp.float32
            )
            piece_k = (
                jnp.einsum("kgqt,qkgd->tkd", d_scores, grouped, preferred_element_type=jnp.float32)
                * factor
            )
            piece_v = jnp.einsum(
                "kgqt,qkgd->tkd",
                probs.astype(jnp.bfloat16),
                d_grouped,
                preferred_element_type=jnp.float32,
            )
            grad_k = piece_k.reshape(key_count, KVH * HD)
            grad_v = piece_v.reshape(key_count, KVH * HD)
            return (grad_q, grad_k, grad_v)

        back_result = lax.cond(jnp.int32(0) <= pos_last, attend_work, unchanged, back_state)
        grad_q = back_result[0]
        summed_k, summed_v = side_by_side(
            (back_result[1].astype(jnp.bfloat16), back_result[2].astype(jnp.bfloat16)),
            ("ctx", "fsdp"),
            0,
            1,
        )
        d_q_raw = rotate(grad_q.reshape(tok_count, H, HD) * factor, cosine, -sine_table).reshape(
            tok_count, H * HD
        )
        d_k_raw = rotate(summed_k.reshape(tok_count, KVH, HD), cosine, -sine_table).reshape(
            tok_count, KVH * HD
        )
        d_mixed = jnp.concatenate([d_q_raw, d_k_raw, summed_v], axis=1).astype(jnp.bfloat16)
        sums[1] = sums[1] + inner(normed, d_mixed)
        d_normed = outer(d_mixed, mix_qkv)
        _, pull_one = jax.vjp(rms_norm, inputs, gain_one.astype(jnp.float32))
        d_inputs_norm, d_gain_one = pull_one(d_normed)
        sums[0] = sums[0] + d_gain_one
        in_grads.append((d_resid + d_inputs_norm).astype(jnp.bfloat16))
    grad_gain_one, grad_qkv, grad_out, grad_gain_two, grad_gate_up, grad_down = (
        lax.psum_scatter(sums[0], ("dp", "ctx", "fsdp"), scatter_dimension=0, tiled=True),
        lax.psum_scatter(sums[1], ("dp", "ctx", "fsdp"), scatter_dimension=1, tiled=True),
        lax.psum_scatter(sums[2], ("dp", "ctx", "fsdp"), scatter_dimension=0, tiled=True),
        lax.psum_scatter(sums[3], ("dp", "ctx", "fsdp"), scatter_dimension=0, tiled=True),
        lax.psum_scatter(sums[4], ("dp", "ctx", "fsdp"), scatter_dimension=1, tiled=True),
        lax.psum_scatter(sums[5], ("dp", "ctx", "fsdp"), scatter_dimension=0, tiled=True),
    )
    block_out = jnp.stack(outputs)[:, None]
    grad_tokens = jnp.stack(in_grads)[:, None]
    return (
        block_out,
        grad_tokens,
        grad_gain_one,
        grad_qkv,
        grad_out,
        grad_gain_two,
        grad_gate_up,
        grad_down,
    )


MESH = pl.DeviceIdType.MESH
VM = pltpu.VMEM
ANY = pl.ANY


def place():
    return lax.axis_index("dp"), lax.axis_index("ctx"), lax.axis_index("fsdp")


def at_device(dp, ctx, fs):
    return {"dp": dp, "ctx": ctx, "fsdp": fs}


def remote(src, dst, send, recv, device):
    return pltpu.make_async_remote_copy(
        src_ref=src, dst_ref=dst, send_sem=send, recv_sem=recv, device_id=device, device_id_type=MESH
    )


def arrived(dst, recv, device):
    remote(dst, dst, recv, recv, device).wait_recv()


def left(src, send, device):
    remote(src, src, send, send, device).wait_send()


def tell_all(sizes):
    dp, ctx, fs = sizes
    n = dp * ctx * fs
    d, c, f = place()
    me = (d * ctx + c) * fs + f
    barrier = pltpu.get_barrier_semaphore()

    def tell(step, carry):
        other = lax.rem(me + step, n)
        pl.semaphore_signal(
            barrier,
            inc=1,
            device_id=at_device(other // (ctx * fs), lax.rem(other // fs, ctx), lax.rem(other, fs)),
            device_id_type=MESH,
        )
        return carry

    lax.fori_loop(1, n, tell, 0)


def hear_all(sizes):
    dp, ctx, fs = sizes
    pl.semaphore_wait(pltpu.get_barrier_semaphore(), dp * ctx * fs - 1)


HALVES = 2


def part_of(ref, index):
    rows = ref.shape[-2] // HALVES
    return ref.at[index * rows : (index + 1) * rows]


def near_or_inner(c, at, n):
    ends = jnp.logical_or(c == 0, c == n - 1)
    return jnp.logical_or(jnp.logical_not(ends), jnp.abs(at - c) <= 1)


class LineGather:
    def __init__(self, n, own, whole, send, recv, local, short=False):
        self.n, self.own, self.whole, self.send, self.recv, self.local = n, own, whole, send, recv, local
        self.short = short
        self.d, self.c, self.f = place()
        self.here = at_device(self.d, self.c, self.f)

    def slot(self, at):
        return self.whole.at[self.d, at]

    def held(self, at):
        valid = jnp.logical_and(at >= 0, at < self.n)
        return jnp.logical_and(valid, near_or_inner(self.c, at, self.n)) if self.short else valid

    def passes(self, way, at):
        ahead = self.n - 2 - self.c if way == 0 else self.c - 1
        inside = at <= self.c if way == 0 else at >= self.c
        goes = jnp.logical_and(inside, ahead >= 0)
        return jnp.logical_and(goes, jnp.logical_or(at == self.c, ahead > 0)) if self.short else goes

    def along(self, way, block, at, part):
        to = (at_device(self.d, self.c + 1, self.f), at_device(self.d, self.c - 1, self.f), at_device(1 - self.d, self.c, self.f))[way]
        return remote(part_of(block, part), part_of(self.slot(at), part), self.send.at[way, at, part], self.recv.at[self.d, at, part], to)

    def start(self):
        c = self.c
        for part in range(HALVES):

            @pl.when(c < self.n - 1)
            def _():
                self.along(0, self.own, c, part).start()

            @pl.when(c > 0)
            def _():
                self.along(1, self.own, c, part).start()

        for part in range(HALVES):
            self.along(2, self.own, c, part).start()
        pltpu.make_async_copy(self.own, self.slot(c), self.local).start()

    def forward(self, k):
        for part in range(HALVES):
            for way, at in enumerate((self.c - k, self.c + k)):

                @pl.when(self.held(at))
                def _():
                    arrived(part_of(self.slot(at), part), self.recv.at[self.d, at, part], self.here)

                    @pl.when(self.passes(way, at))
                    def _():
                        self.along(way, self.slot(at), at, part).start()

                    self.along(2, self.slot(at), at, part).start()

    def reach(self, step):
        now = jnp.abs(ordered(self.c, step, self.n) - self.c)
        before = jnp.abs(ordered(self.c, step - 1, self.n) - self.c)

        @pl.when(jnp.logical_and(step > 0, now != before))
        def _():
            self.forward(now)

    def other(self, at):
        @pl.when(self.held(at))
        def _():
            for part in range(HALVES):
                arrived(part_of(self.whole.at[1 - self.d, at], part), self.recv.at[1 - self.d, at, part], self.here)

    def finish_sends(self):
        for at in range(self.n):
            for part in range(HALVES):
                block = part_of(self.slot(at), part)
                for way in range(3):

                    @pl.when(self.passes(way, at) if way < 2 else self.held(at))
                    def _():
                        left(block, self.send.at[way, at, part], self.here)

    def finish(self):
        self.finish_sends()
        pltpu.make_async_copy(self.own, self.slot(self.c), self.local).wait()


FACTOR = HD ** (-0.5)
LANES = 128


def ordered(c, step, n):
    at = jnp.int32(0)
    for here in range(n):
        near = sorted(range(n), key=lambda place_: (abs(place_ - here), place_))
        for index, value in enumerate(near):
            at = jnp.where(jnp.logical_and(c == here, step == index), value, at)
    return at


def towards(c, step, n):
    at = c
    for here in range(n):
        due = []
        for to in range(n):
            if to != here:
                hops = here if to > here else n - 1 - here
                due.append((hops + (n - 1 - to if to > here else to), -hops, to))
        for index, (_, _, to) in enumerate(sorted(due)):
            at = jnp.where(jnp.logical_and(c == here, step == index), to, at)
    return at


class LineSum:
    def __init__(self, n, mine, out_core, in_core, out_line, in_line, total, sems):
        self.n, self.mine, self.out_core, self.in_core = n, mine, out_core, in_core
        self.out_line, self.in_line, self.total = out_line, in_line, total
        self.core_send, self.core_recv, self.line_send, self.line_recv = sems
        self.d, self.c, self.f = place()
        self.here = at_device(self.d, self.c, self.f)

    def give(self, at, both):
        self.keep(at, both)
        self.hand(at)

    def keep(self, at, both):
        d = self.d
        low = both.astype(jnp.bfloat16)

        @pl.when(d == 0)
        def _():
            self.mine[at] = low[0]
            self.out_core[at] = low[1]

        @pl.when(d != 0)
        def _():
            self.mine[at] = low[1]
            self.out_core[at] = low[0]

    def hand(self, at):
        remote(
            self.out_core.at[at], self.in_core.at[at], self.core_send.at[at], self.core_recv.at[at], at_device(1 - self.d, self.c, self.f)
        ).start()

    def step(self, at):
        n, d, c, f = self.n, self.d, self.c, self.f
        arrived(self.in_core.at[at], self.core_recv.at[at], self.here)
        rows = self.total.shape[0] // HALVES
        for part in range(HALVES):
            own = slice(part * rows, (part + 1) * rows)
            self.total[own] = self.mine[at, own].astype(jnp.float32) + self.in_core[at, own].astype(jnp.float32)
            for way, comes in enumerate((jnp.logical_and(at <= c, c < n - 1), jnp.logical_and(at >= c, c > 0))):

                @pl.when(comes)
                def _():
                    arrived(self.in_line.at[way, at, own], self.line_recv.at[way, at, part], self.here)
                    self.total[own] += self.in_line[way, at, own].astype(jnp.float32)

            @pl.when(at != c)
            def _():
                self.out_line[at, own] = self.total[own].astype(jnp.bfloat16)

            for way, (goes, to) in enumerate(((at < c, c - 1), (at > c, c + 1))):

                @pl.when(goes)
                def _():
                    remote(
                        self.out_line.at[at, own], self.in_line.at[way, at, own],
                        self.line_send.at[at, part], self.line_recv.at[way, at, part], at_device(d, to, f),
                    ).start()

    def finish(self):
        rows = self.total.shape[0] // HALVES
        for at in range(self.n):
            left(self.out_core.at[at], self.core_send.at[at], self.here)

            @pl.when(at != self.c)
            def _():
                for part in range(HALVES):
                    left(self.out_line.at[at, part * rows : (part + 1) * rows], self.line_send.at[at, part], self.here)

    @staticmethod
    def scratch(ctx, rows):
        low = jnp.bfloat16
        dma = pltpu.SemaphoreType.DMA
        return [
            VM((ctx, rows, D), low), VM((ctx, rows, D), low), VM((ctx, rows, D), low), VM((ctx, rows, D), low),
            VM((2, ctx, rows, D), low), VM((rows, D), jnp.float32),
            dma((ctx,)), dma((ctx,)), dma((ctx, HALVES)), dma((2, ctx, HALVES)),
        ]


def down_route(d, c):
    return (lax.rem(c, 2), 2 * d + c // 2), (c // 2, 2 * lax.rem(c, 2) + d)


def front_kernel(
    sizes, hidden, parts, x_ref, one_ref, two_ref, w_ref, dy_ref, proj_ref, down_ref, gate_up_ref,
    out_ref, d_resid_out, gain_out, block_ref, step_ref, normed_out, qkv_out, wide_out, gains_out, unit_out, grad_proj_out, up_land, down_land,
    x_all, wide, normed, stage, qkv_unit, att_stage, att, gain_all, gain_vec,
    dy_all, proj, down_mid, down, gate_up, resid, own_two, normed_two, act, d_both, own_d, d_stage, unit,
    grad_up, grad_down, grad_proj, grad_proj_low, gains_ref,
    line_send, line_recv, line_local, w_send, w_recv, w_pass, g_send, g_recv, q_send, q_recv, a_send, a_recv, out_sem,
    dy_send, dy_recv, dy_local, m_send, m_recv, m_pass, down_send, down_recv, d_recv, d_pass, gu_send, gu_recv,
    two_send, two_recv, two_local, dr_send, dr_recv, dr_local, u_send, u_recv, gup_send, gup_recv, gdn_send, gdn_recv,
    *sums,
):
    d_resid_all = x_all
    dp, ctx, fs = sizes
    n = dp * ctx * fs
    d, c, f = place()
    here = at_device(d, c, f)
    span = stage.shape[2]
    tell_all(sizes)
    fill_tables(block_ref, step_ref)
    gains_ref[0:1, 0 : D // n] = one_ref[...].astype(jnp.float32).reshape(1, D // n)
    gains_ref[1:2, 0 : D // n] = two_ref[...].astype(jnp.float32).reshape(1, D // n)
    for slot in range(4):
        wide[slot * LANES + HD : (slot + 1) * LANES, :] = jnp.zeros((LANES - HD, D), jnp.bfloat16)
    each_proj = proj_ref.shape[0]
    for start in range(2 * each_proj, 2 * LANES, LANES):
        proj[start : start + LANES - 2 * each_proj, :] = jnp.zeros((LANES - 2 * each_proj, D), jnp.bfloat16)
    hear_all(sizes)

    def proj_rows(slot):
        start = slot // 2 * LANES + lax.rem(slot, 2) * each_proj
        return proj.at[pl.ds(pl.multiple_of(start, 16), each_proj)]

    def head_rows(slot):
        return wide.at[pl.ds(pl.multiple_of(slot * LANES, LANES), HD)]

    q_core = f // 2
    kv_slot = 2 + c // 2
    kv_ctx = 2 * lax.rem(c, 2) + f // 2
    kv_core = lax.rem(f, 2)
    kv_f = lax.rem(f + 2 * (c // 2), fs)
    kv_away = jnp.logical_or(jnp.logical_or(kv_core != d, kv_ctx != c), kv_f != f)
    relay_of = {slot: f == lax.rem(2 * lax.rem(c, 2) + d + 2 * (slot - 2), fs) for slot in (2, 3)}

    me = (d * ctx + c) * fs + f

    def gain_to(step, carry):
        other = lax.rem(me + step, n)
        remote(
            gains_ref, gain_all.at[me], g_send.at[other], g_recv.at[me],
            at_device(other // (ctx * fs), lax.rem(other // fs, ctx), lax.rem(other, fs)),
        ).start()
        return carry

    lax.fori_loop(1, n, gain_to, 0)
    gain_all[me] = gains_ref[...]

    @pl.when(jnp.logical_and(d == 1, kv_away))
    def _():
        remote(w_ref, head_rows(kv_slot), w_send.at[0], w_recv.at[kv_slot], at_device(kv_core, kv_ctx, kv_f)).start()

    @pl.when(jnp.logical_and(d == 1, jnp.logical_not(kv_away)))
    def _():
        pltpu.make_async_copy(w_ref, head_rows(kv_slot), w_recv.at[kv_slot]).start()

    x_line = LineGather(ctx, x_ref, x_all, line_send, line_recv, line_local)
    x_line.start()

    @pl.when(d == 0)
    def _():
        slot = lax.rem(f, 2)
        for to in range(fs):

            @pl.when(jnp.logical_or(q_core != 0, to != f))
            def _():
                remote(w_ref, head_rows(slot), w_send.at[to], w_recv.at[slot], at_device(q_core, c, to)).start()

            @pl.when(jnp.logical_and(q_core == 0, to == f))
            def _():
                pltpu.make_async_copy(w_ref, head_rows(slot), w_recv.at[slot]).start()

    for slot in (2, 3):

        @pl.when(relay_of[slot])
        def _():
            arrived(head_rows(slot), w_recv.at[slot], here)
            for step in range(1, fs):
                to = lax.rem(f + step, fs)
                remote(head_rows(slot), head_rows(slot), w_pass.at[slot - 2, step], w_recv.at[slot], at_device(d, c, to)).start()

    gu_core = f // 2
    gu_slot = 2 * d + lax.rem(f, 2)
    part_rows = gate_up_ref.shape[0] // parts

    def push_part(part):
        first_row = part * part_rows
        src = gate_up_ref.at[first_row : first_row + part_rows]
        dst = gate_up.at[gu_slot, first_row : first_row + part_rows]
        for to in range(fs):
            own_place = jnp.logical_and(gu_core == d, f == to)

            @pl.when(jnp.logical_not(own_place))
            def _():
                remote(src, dst, gu_send.at[part, to], gu_recv.at[part, gu_slot], at_device(gu_core, c, to)).start()

            @pl.when(own_place)
            def _():
                pltpu.make_async_copy(src, dst, gu_recv.at[part, gu_slot]).start()

    def gain_from(step, carry):
        other = lax.rem(me + step, n)
        arrived(gain_all.at[other], g_recv.at[other], here)
        return carry

    lax.fori_loop(1, n, gain_from, 0)
    each = D // n
    for index in range(n):
        gain_vec[:, index * each : (index + 1) * each] = gain_all[index][:, :each]
    gain = gain_vec[0:1, :]

    for k in range(1, ctx - 1):
        x_line.forward(k)
    to_core, to_ctx = lax.rem(c, 2), 2 * d + c // 2
    stays = jnp.logical_and(to_core == d, to_ctx == c)

    @pl.when(jnp.logical_not(stays))
    def _():
        remote(proj_ref, proj_rows(f), m_send, m_recv.at[f], at_device(to_core, to_ctx, f)).start()

    @pl.when(stays)
    def _():
        pltpu.make_async_copy(proj_ref, proj_rows(f), m_recv.at[f]).start()

    dy_line = LineGather(ctx, dy_ref, dy_all, dy_send, dy_recv, dy_local)
    dy_line.start()
    for slot in range(4):
        if slot < 2:
            arrived(head_rows(slot), w_recv.at[slot], here)
        else:

            @pl.when(jnp.logical_not(relay_of[slot]))
            def _():
                arrived(head_rows(slot), w_recv.at[slot], here)

    push_part(0)
    pltpu.make_async_copy(x_line.own, x_line.slot(c), x_line.local).wait()

    def block(step, carry):
        at = ordered(c, step, ctx)

        x_line.other(at)
        values = x_all[:, at].reshape(dp * 2 * span, D).astype(jnp.float32)
        scale = lax.rsqrt(jnp.mean(values * values, axis=-1, keepdims=True) + EPS)
        low = (values * scale * gain).astype(jnp.bfloat16)
        normed[:, at] = low.reshape(dp, 2 * span, D)
        heads = outer(low, wide[...])
        cosine, sine_up, sine_down = turns(block_ref, step_ref, at * fs + f)
        for slot in range(4):
            head = heads[:, slot * LANES : (slot + 1) * LANES]
            if slot < 3:
                turned_up = pltpu.roll(head, HD // 2, 1).reshape(2 * dp, span, LANES)
                turned_down = pltpu.roll(head, LANES - HD // 2, 1).reshape(2 * dp, span, LANES)
                head = head.reshape(2 * dp, span, LANES)
                head = head * cosine[None] + turned_up * sine_up[None] + turned_down * sine_down[None]
            else:
                head = head.reshape(2 * dp, span, LANES)
            stage[at, :, :, slot * LANES : (slot + 1) * LANES] = head.astype(jnp.bfloat16)
        for to in range(2 * dp):

            @pl.when(to != f)
            def _():
                remote(stage.at[at, to], qkv_unit.at[at, f], q_send.at[at, to], q_recv.at[at, f], at_device(d, c, to)).start()

            @pl.when(to == f)
            def _():
                qkv_unit[at, f] = stage[at, to]

        return carry

    def near(step, carry):
        @pl.when(step == ctx - 1)
        def _():
            x_line.forward(ctx - 1)

        return block(step, carry)

    lax.fori_loop(0, ctx, near, 0)
    normed_copy = pltpu.make_async_copy(normed, normed_out, out_sem.at[3])
    wide_copy = pltpu.make_async_copy(wide, wide_out, out_sem.at[4])
    gains_copy = pltpu.make_async_copy(gain_vec, gains_out, out_sem.at[5])
    normed_copy.start()
    wide_copy.start()
    gains_copy.start()

    @pl.when(jnp.logical_not(stays))
    def _():
        remote(down_ref, down_mid, down_send, down_recv, at_device(to_core, to_ctx, f)).start()

    @pl.when(stays)
    def _():
        pltpu.make_async_copy(down_ref, down_mid, down_recv).start()

    arrived(proj_rows(f), m_recv.at[f], here)
    for step in range(1, fs):
        to = lax.rem(f + step, fs)
        remote(proj_rows(f), proj_rows(f), m_pass.at[step], m_recv.at[f], at_device(d, c, to)).start()

    dy_line.forward(1)

    for at in range(ctx):
        for step in range(1, fs):
            other = lax.rem(f + step, fs)
            arrived(qkv_unit.at[at, other], q_recv.at[at, other], here)
    qkv_copy = pltpu.make_async_copy(qkv_unit, qkv_out, out_sem.at[0])
    qkv_copy.start()

    block_rows = fs * span
    for at in (0, ctx - 1, *range(1, ctx - 1)):
        keys = block_rows * (at + 1)
        k_rows = qkv_unit[0 : at + 1, :, :, 2 * LANES : 3 * LANES].reshape(keys, LANES)
        v_rows = qkv_unit[0 : at + 1, :, :, 3 * LANES : 4 * LANES].reshape(keys, LANES)
        allowed = lax.broadcasted_iota(jnp.int32, (block_rows, keys), 1) <= block_rows * at + lax.broadcasted_iota(
            jnp.int32, (block_rows, keys), 0
        )
        for head in range(2):
            q_rows = qkv_unit[at, :, :, head * LANES : (head + 1) * LANES].reshape(block_rows, LANES)
            scores = outer(q_rows, k_rows) * FACTOR
            scores = jnp.where(allowed, scores, NEG)
            best = jnp.max(scores, axis=-1, keepdims=True)
            weights = jnp.exp(scores - best)
            probs = weights / jnp.sum(weights, axis=-1, keepdims=True)
            mixed = jnp.dot(probs.astype(jnp.bfloat16), v_rows, preferred_element_type=jnp.float32)
            att_stage[at, :, :, head * LANES : (head + 1) * LANES] = mixed.astype(jnp.bfloat16).reshape(fs, span, LANES)
        for to in range(fs):

            @pl.when(to != f)
            def _():
                remote(
                    att_stage.at[at, to], att.at[f // 2, at, lax.rem(f, 2)], a_send.at[at, to], a_recv.at[f, at], at_device(d, c, to)
                ).start()

            @pl.when(to == f)
            def _():
                att[f // 2, at, lax.rem(f, 2)] = att_stage[at, to]


    ends = jnp.logical_or(c == 0, c == ctx - 1)

    @pl.when(jnp.logical_not(ends))
    def _():
        dy_line.forward(2)

    for step in range(1, fs):
        other = lax.rem(f + step, fs)
        arrived(proj_rows(other), m_recv.at[other], here)
    rows = x_ref.shape[0]
    both_rows = dp * rows
    half = hidden // 2
    line_sum = LineSum(ctx, *sums[:6], sums[6:10])
    second_sum = LineSum(ctx, *sums[10:16], sums[16:20])
    out_sum = line_sum

    def project(step, carry):
        at = towards(c, step, ctx)
        for move in range(1, fs):
            other = lax.rem(f + move, fs)
            arrived(att.at[other // 2, at, lax.rem(other, 2)], a_recv.at[other, at], here)
        terms = jnp.dot(att[:, at].reshape(both_rows, 2 * LANES), proj[...], preferred_element_type=jnp.float32)
        line_sum.give(at, terms.reshape(dp, rows, D))

        @pl.when(jnp.logical_and(ends, step > 0))
        def _():
            line_sum.step(towards(c, step - 1, ctx))

        return carry

    lax.fori_loop(0, ctx, project, 0)

    arrived(down_mid, down_recv, here)
    pltpu.make_async_copy(down_mid, down.at[f], d_recv.at[f]).start()
    for step in range(1, fs):
        to = lax.rem(f + step, fs)
        remote(down_mid, down.at[f], d_pass.at[step], d_recv.at[f], at_device(d, c, to)).start()
    for part in range(1, parts):
        push_part(part)

    def sum_step(step, carry):
        line_sum.step(towards(c, step, ctx))
        return carry

    lax.fori_loop(jnp.where(ends, ctx - 1, 0), ctx - 1, sum_step, 0)

    @pl.when(ends)
    def _():
        for k in range(2, ctx):
            dy_line.forward(k)

    line_sum.step(c)
    gain = gain_vec[1:2, :]
    values = x_ref[...].astype(jnp.float32) + line_sum.total[...]
    resid[...] = values
    scale = lax.rsqrt(jnp.mean(values * values, axis=-1, keepdims=True) + EPS)
    own_two[...] = (values * scale * gain).astype(jnp.bfloat16)
    line = LineGather(ctx, own_two, normed_two, two_send, two_recv, two_local)
    line.start()
    line.forward(1)
    line_sum.finish()
    x_line.finish_sends()
    for part in range(parts):
        for slot in range(4):
            arrived(gate_up.at[slot, part * part_rows : (part + 1) * part_rows], gu_recv.at[part, slot], here)
    for slot in range(fs):
        arrived(down.at[slot], d_recv.at[slot], here)
    pltpu.make_async_copy(dy_line.own, dy_line.slot(c), dy_line.local).wait()
    for part in range(parts):
        src = gate_up_ref.at[part * part_rows : (part + 1) * part_rows]
        for to in range(fs):

            @pl.when(jnp.logical_not(jnp.logical_and(gu_core == d, f == to)))
            def _():
                left(src, gu_send.at[part, to], here)

    for at in range(ctx):

        for to in range(fs):

            @pl.when(to != f)
            def _():
                left(stage.at[at, to], q_send.at[at, to], here)
                left(att_stage.at[at, to], a_send.at[at, to], here)

    @pl.when(jnp.logical_and(d == 1, kv_away))
    def _():
        left(w_ref, w_send.at[0], here)

    @pl.when(d == 0)
    def _():
        for to in range(fs):

            @pl.when(jnp.logical_or(q_core != 0, to != f))
            def _():
                left(w_ref, w_send.at[to], here)

    for slot in (2, 3):

        @pl.when(relay_of[slot])
        def _():
            for step in range(1, fs):
                left(head_rows(slot), w_pass.at[slot - 2, step], here)

    def gain_left(step, carry):
        other = lax.rem(me + step, n)
        left(gains_ref, g_send.at[other], here)
        return carry

    lax.fori_loop(1, n, gain_left, 0)
    for copy in (normed_copy, wide_copy, gains_copy, qkv_copy):
        copy.wait()
    for step in range(1, fs):
        left(down_mid, d_pass.at[step], here)
        left(proj_rows(f), m_pass.at[step], here)

    @pl.when(jnp.logical_not(stays))
    def _():
        left(proj_ref, m_send, here)
        left(down_ref, down_send, here)

    dy_line.finish_sends()
    pltpu.make_async_copy(line.own, line.slot(c), line.local).wait()

    def mlp(step, carry):
        at = ordered(c, step, ctx)


        @pl.when(lax.rem(step, 2) == 1)
        def _():
            line.forward(2 + step // 2)

        line.other(at)
        dy_line.other(at)
        inputs = normed_two[:, at].reshape(both_rows, D)
        dy_rows = dy_all[:, at].reshape(both_rows, D)
        for part in range(2):
            cols = slice(part * half, (part + 1) * half)
            gate = jnp.dot(inputs, gate_up[part], preferred_element_type=jnp.float32)
            up = jnp.dot(inputs, gate_up[2 + part], preferred_element_type=jnp.float32)
            d_act = outer(dy_rows, down[2 * part : 2 * part + 2].reshape(half, D))
            sig = 1.0 / (1.0 + jnp.exp(-gate))
            silu = gate * sig
            act[:, at, :, cols] = (silu * up).astype(jnp.bfloat16).reshape(dp, rows, half)
            d_gate = d_act * up * (sig * (1.0 + gate * (1.0 - sig)))
            d_both[:, at, :, cols] = d_gate.astype(jnp.bfloat16).reshape(dp, rows, half)
            d_both[:, at, :, hidden + part * half : hidden + (part + 1) * half] = (
                (d_act * silu).astype(jnp.bfloat16).reshape(dp, rows, half)
            )
        terms = outer(d_both[:, at, :, 0:half].reshape(both_rows, half), gate_up[0])
        for part in range(1, 4):
            terms += outer(d_both[:, at, :, part * half : (part + 1) * half].reshape(both_rows, half), gate_up[part])
        second_sum.give(at, terms.reshape(dp, rows, D))
        return carry

    lax.fori_loop(0, ctx, mlp, 0)

    wide_rows = D // ctx

    def push(src, dst, send, recv, core, to):
        to_self = jnp.logical_and(core == d, to == f)

        @pl.when(jnp.logical_not(to_self))
        def _():
            remote(src, dst, send, recv, at_device(core, c, to)).start()

        @pl.when(to_self)
        def _():
            pltpu.make_async_copy(src, dst, recv).start()

    def grads(step):
        first = pl.multiple_of(step * wide_rows, LANES)
        left_rows = normed_two[:, :, :, pl.ds(first, wide_rows)].reshape(dp * ctx * rows, wide_rows)
        for part in range(2):
            cols = slice(part * hidden, (part + 1) * hidden)
            terms = inner(left_rows, d_both[:, :, :, cols].reshape(dp * ctx * rows, hidden)).astype(jnp.bfloat16)
            grad_up[2 * part, pl.ds(first, wide_rows), :] = terms[:, :half]
            grad_up[2 * part + 1, pl.ds(first, wide_rows), :] = terms[:, half:]
        dy_cols = dy_all[:, :, :, pl.ds(first, wide_rows)].reshape(dp * ctx * rows, wide_rows)
        terms = inner(act[...].reshape(dp * ctx * rows, hidden), dy_cols).astype(jnp.bfloat16)
        grad_down[:, :, pl.ds(first, wide_rows)] = terms.reshape(fs, hidden // fs, wide_rows)
        for slot in range(4):
            push(
                grad_up.at[slot, pl.ds(first, wide_rows)], up_land.at[f, pl.ds(first, wide_rows)],
                gup_send.at[slot, step], gup_recv.at[f, step], slot // 2, 2 * d + slot % 2,
            )
            push(
                grad_down.at[slot, :, pl.ds(first, wide_rows)], down_land.at[f, :, pl.ds(first, wide_rows)],
                gdn_send.at[slot, step], gdn_recv.at[f, step], d, slot,
            )

    def out_terms(step):
        at = towards(c, step, ctx)
        terms = jnp.dot(act[:, at].reshape(both_rows, hidden), down[...].reshape(hidden, D), preferred_element_type=jnp.float32)
        out_sum.give(at, terms.reshape(dp, rows, D))

    def second_steps():
        def body(step, carry):
            second_sum.step(towards(c, step, ctx))
            return carry

        lax.fori_loop(0, ctx - 1, body, 0)

    def local_terms(step, carry):
        grads(step)
        out_terms(step)
        return carry

    pl.when(ends)(second_steps)
    lax.fori_loop(0, ctx - 1, local_terms, 0)
    pl.when(jnp.logical_not(ends))(second_steps)
    local_terms(ctx - 1, 0)
    second_sum.step(c)
    values = resid[...]
    scale = lax.rsqrt(jnp.mean(values * values, axis=-1, keepdims=True) + EPS)
    incoming = second_sum.total[...]
    weighted = incoming * gain
    mean = jnp.mean(weighted * values, axis=-1, keepdims=True)
    d_resid = dy_ref[...].astype(jnp.float32) + scale * weighted - values * (scale * scale * scale) * mean
    own_d[...] = d_resid.astype(jnp.bfloat16)
    d_resid_out[...] = d_resid
    gain_out[...] = jnp.broadcast_to(jnp.sum(incoming * values * scale, axis=0, keepdims=True), gain_out.shape)
    d_line = LineGather(ctx, own_d, d_resid_all, dr_send, dr_recv, dr_local)
    d_line.start()
    def out_step(step, carry):
        out_sum.step(towards(c, step, ctx))
        return carry

    @pl.when(ends)
    def _():
        lax.fori_loop(0, ctx - 1, out_step, 0)

    line.finish_sends()
    second_sum.finish()
    pltpu.make_async_copy(d_line.own, d_line.slot(c), d_line.local).wait()
    grad_proj[...] = jnp.zeros_like(grad_proj)

    def back(step, carry):
        at = ordered(c, step, ctx)

        d_line.reach(step)
        d_line.other(at)
        incoming = d_resid_all[:, at].reshape(both_rows, D)
        d_att = outer(incoming, proj[...]).astype(jnp.bfloat16)
        d_stage[at] = d_att.reshape(2 * dp, span, 2 * LANES)
        for to in range(2 * dp):

            @pl.when(to != f)
            def _():
                remote(d_stage.at[at, to], unit.at[at, f], u_send.at[at, to], u_recv.at[at, f], at_device(d, c, to)).start()

            @pl.when(to == f)
            def _():
                unit[at, f] = d_stage[at, to]

        grad_proj[...] += inner(att[:, at].reshape(both_rows, 2 * LANES), incoming)

        @pl.when(jnp.logical_and(jnp.logical_not(ends), step == ctx - 2))
        def _():
            out_sum.step(towards(c, 0, ctx))

        return carry

    lax.fori_loop(0, ctx, back, 0)

    @pl.when(jnp.logical_not(ends))
    def _():
        lax.fori_loop(1, ctx - 1, out_step, 0)

    for slot in range(fs):
        start = slot // 2 * LANES + slot % 2 * each_proj
        grad_proj_low[slot] = grad_proj[start : start + each_proj, :].astype(jnp.bfloat16)
    grad_proj_copy = pltpu.make_async_copy(grad_proj_low, grad_proj_out, out_sem.at[1])
    grad_proj_copy.start()
    for at in range(ctx):
        for step in range(1, fs):
            other = lax.rem(f + step, fs)
            arrived(unit.at[at, other], u_recv.at[at, other], here)
    unit_copy = pltpu.make_async_copy(unit, unit_out, out_sem.at[2])
    unit_copy.start()
    d_line.finish_sends()
    for at in range(ctx):
        for to in range(fs):

            @pl.when(to != f)
            def _():
                left(d_stage.at[at, to], u_send.at[at, to], here)

    def settle_up(step, carry):
        first = pl.multiple_of(step * wide_rows, LANES)
        for slot in range(4):
            arrived(up_land.at[slot, pl.ds(first, wide_rows)], gup_recv.at[slot, step], here)

            @pl.when(jnp.logical_or(slot // 2 != d, 2 * d + slot % 2 != f))
            def _():
                left(grad_up.at[slot, pl.ds(first, wide_rows)], gup_send.at[slot, step], here)

        return carry

    def settle_down(step, carry):
        first = pl.multiple_of(step * wide_rows, LANES)
        for slot in range(4):
            arrived(down_land.at[slot, :, pl.ds(first, wide_rows)], gdn_recv.at[slot, step], here)

            @pl.when(slot != f)
            def _():
                left(grad_down.at[slot, :, pl.ds(first, wide_rows)], gdn_send.at[slot, step], here)

        return carry

    lax.fori_loop(0, ctx, settle_up, 0)
    lax.fori_loop(0, ctx, settle_down, 0)
    out_step(ctx - 1, 0)
    out_ref[...] = (resid[...] + out_sum.total[...]).astype(jnp.bfloat16)
    out_sum.finish()
    for copy in (grad_proj_copy, unit_copy):
        copy.wait()

def front(sizes, parts, x, attn_gain, mlp_gain, w_qkv, dy, w_out, w_down, w_gate_up):
    dp, ctx, fs = sizes
    n = dp * ctx * fs
    rows = x.shape[0]
    span = rows // 2
    hidden = FF // (dp * ctx)
    low, wide_t = jnp.bfloat16, jnp.float32
    dma = pltpu.SemaphoreType.DMA
    any_spec, vm_spec = pl.BlockSpec(memory_space=ANY), pl.BlockSpec(memory_space=VM)
    line_sems = [dma((3, ctx, HALVES)), dma((dp, ctx, HALVES)), dma]
    shapes = (
        jax.ShapeDtypeStruct((rows, D), low),
        jax.ShapeDtypeStruct((rows, D), wide_t),
        jax.ShapeDtypeStruct((8, D), wide_t),
        jax.ShapeDtypeStruct((2, ctx * fs, LANES), wide_t),
        jax.ShapeDtypeStruct((2, span, LANES), wide_t),
        jax.ShapeDtypeStruct((dp, ctx, rows, D), low),
        jax.ShapeDtypeStruct((ctx, fs, span, 4 * LANES), low),
        jax.ShapeDtypeStruct((4 * LANES, D), low),
        jax.ShapeDtypeStruct((8, D), wide_t),
        jax.ShapeDtypeStruct((ctx, fs, span, 2 * LANES), low),
        jax.ShapeDtypeStruct((fs,) + w_out.shape, low),
        jax.ShapeDtypeStruct((fs, D, hidden // 2), low),
        jax.ShapeDtypeStruct((fs, hidden // fs, D), low),
    )
    return pl.pallas_call(
        functools.partial(front_kernel, sizes, hidden, parts),
        name="front",
        out_shape=shapes,
        in_specs=[vm_spec] * 3 + [any_spec] + [vm_spec] * 4,
        out_specs=[vm_spec] * 5 + [any_spec] * 8,
        scratch_shapes=[
            VM((dp, ctx, rows, D), low),
            VM((4 * LANES, D), low),
            VM((dp, ctx, rows, D), low),
            VM((ctx, 2 * dp, span, 4 * LANES), low),
            VM((ctx, fs, span, 4 * LANES), low),
            VM((ctx, fs, span, 2 * LANES), low),
            VM((dp, ctx, 2, span, 2 * LANES), low),
            VM((n, 8, LANES), wide_t),
            VM((8, D), wide_t),
            VM((dp, ctx, rows, D), low),
            VM((2 * LANES, D), low),
            VM(w_down.shape, low),
            VM((fs, hidden // fs, D), low),
            VM((4, D, hidden // 2), low),
            VM((rows, D), wide_t),
            VM((rows, D), low),
            VM((dp, ctx, rows, D), low),
            VM((dp, ctx, rows, hidden), low),
            VM((dp, ctx, rows, 2 * hidden), low),
            VM((rows, D), low),
            VM((ctx, 2 * dp, span, 2 * LANES), low),
            VM((ctx, fs, span, 2 * LANES), low),
            VM((4, D, hidden // 2), low),
            VM((fs, hidden // fs, D), low),
            VM((2 * LANES, D), wide_t),
            VM((fs,) + w_out.shape, low),
            VM((8, LANES), wide_t),
            *line_sems,
            dma((fs,)), dma((4,)), dma((2, fs)), dma((n,)), dma((n,)),
            dma((ctx, 2 * dp)), dma((ctx, fs)), dma((ctx, fs)), dma((fs, ctx)), dma((6,)),
            *line_sems,
            dma, dma((fs,)), dma((fs,)), dma, dma, dma((fs,)), dma((fs,)), dma((parts, fs)), dma((parts, 4)),
            *line_sems,
            *line_sems,
            dma((ctx, 2 * dp)), dma((ctx, fs)),
            dma((4, ctx)), dma((fs, ctx)), dma((fs, ctx)), dma((fs, ctx)),
        ] + LineSum.scratch(ctx, rows) * 2,
        compiler_params=pltpu.CompilerParams(collective_id=1, has_side_effects=True, vmem_limit_bytes=67043328),
    )(x, attn_gain, mlp_gain, w_qkv, dy, w_out, w_down, w_gate_up)


def fill_tables(block_ref, step_ref):
    span = step_ref.shape[1]
    for ref, scale in ((block_ref, span), (step_ref, 1)):
        shape = ref.shape[1:]
        lane = lax.broadcasted_iota(jnp.int32, shape, 1)
        pair = jnp.where(lane >= HD // 2, lane - HD // 2, lane).astype(jnp.float32)
        frequency = jnp.exp(pair * (-2.0 * math.log(THETA) / HD))
        angles = (lax.broadcasted_iota(jnp.int32, shape, 0) * scale).astype(jnp.float32) * frequency
        ref[0] = jnp.cos(angles)
        ref[1] = jnp.sin(angles)


def turns(block_ref, step_ref, block):
    cos_b, sin_b = block_ref[0, pl.ds(block, 1)], block_ref[1, pl.ds(block, 1)]
    cos_s, sin_s = step_ref[0], step_ref[1]
    cosine = cos_b * cos_s - sin_b * sin_s
    sine = sin_b * cos_s + cos_b * sin_s
    lane = lax.broadcasted_iota(jnp.int32, sine.shape, 1)
    first_half = lane < HD // 2
    sine_up = jnp.where(jnp.logical_and(lane >= HD // 2, lane < HD), sine, 0.0)
    return cosine, sine_up, jnp.where(first_half, -sine, 0.0)


def last_kernel(
    sizes, x_ref, gains_ref, block_ref, step_ref, d_resid_ref, gain_two_ref, proj_ref,
    unit_ref, d_unit_ref, normed_ref, wide_ref, up_land_ref, down_land_ref,
    d_x_ref, gains_out, qkv_out, proj_out, up_out, down_out,
    unit, d_unit, d_k, d_v, stage, mixed, normed, wide, grad_heads,
    up_land, down_land, proj_land, q_land, kv_land, down_sum, proj_sum, kv_sum, down_last, proj_last, kv_last, gain_vec, gain_stage, gain_land, up_sum,
    in_sem, proj_send, proj_recv, head_send, head_recv, move_send, move_recv,
    u_send, u_recv, g_send, g_recv, up_sem,
    *sums,
):
    dp, ctx, fs = sizes
    n = dp * ctx * fs
    d, c, f = place()
    here = at_device(d, c, f)
    me = (d * ctx + c) * fs + f
    rows = x_ref.shape[0]
    span = rows // 2
    both_rows = dp * rows
    low, wide_t = jnp.bfloat16, jnp.float32
    loads = [
        pltpu.make_async_copy(src, dst, in_sem.at[index])
        for index, (src, dst) in enumerate((
            (unit_ref, unit), (d_unit_ref, d_unit), (normed_ref, normed), (wide_ref, wide), (down_land_ref, down_land), (up_land_ref, up_land),
        ))
    ]
    tell_all(sizes)
    for load in loads:
        load.start()
    in_sum = LineSum(ctx, *sums[:6], sums[6:10])
    d_k[...] = jnp.zeros_like(d_k)
    d_v[...] = jnp.zeros_like(d_v)

    def push(src, land, send, recv, core, fs_to):
        to_self = jnp.logical_and(core == d, fs_to == f)

        @pl.when(jnp.logical_not(to_self))
        def _():
            remote(src, land.at[f], send, recv.at[f], at_device(core, c, fs_to)).start()

        @pl.when(to_self)
        def _():
            pltpu.make_async_copy(src, land.at[f], recv.at[f]).start()

    def pushed(src, send, core, fs_to):
        @pl.when(jnp.logical_not(jnp.logical_and(core == d, fs_to == f)))
        def _():
            left(src, send, here)

    def sum_of(land):
        total = land[0].astype(wide_t)
        for source in range(1, fs):
            total += land[source].astype(wide_t)
        return total

    _, (own_core, own_ctx) = down_route(d, c)
    stays = jnp.logical_and(own_core == d, own_ctx == c)

    def move(index, src, dst):
        @pl.when(jnp.logical_not(stays))
        def _():
            remote(src, dst, move_send.at[index], move_recv.at[index], at_device(own_core, own_ctx, f)).start()

        @pl.when(stays)
        def _():
            pltpu.make_async_copy(src, dst, move_recv.at[index]).start()

    loads[0].wait()
    loads[1].wait()
    block = fs * span

    def unturn(values, at):
        up = pltpu.roll(values, HD // 2, 1)
        down = pltpu.roll(values, LANES - HD // 2, 1)
        pieces = []
        for index in range(fs):
            own = slice(index * span, (index + 1) * span)
            cosine, sine_up, sine_down = turns(block_ref, step_ref, at * fs + index)
            pieces.append(values[own] * cosine - up[own] * sine_up - down[own] * sine_down)
        return jnp.concatenate(pieces, axis=0).reshape(fs, span, LANES)

    for at in reversed(range(ctx)):
        keys = block * (at + 1)
        k_rows = unit[0 : at + 1, :, :, 2 * LANES : 3 * LANES].reshape(keys, LANES)
        v_rows = unit[0 : at + 1, :, :, 3 * LANES : 4 * LANES].reshape(keys, LANES)
        allowed = lax.broadcasted_iota(jnp.int32, (block, keys), 1) <= block * at + lax.broadcasted_iota(
            jnp.int32, (block, keys), 0
        )
        for head in range(2):
            lanes = slice(head * LANES, (head + 1) * LANES)
            q_rows = unit[at, :, :, lanes].reshape(block, LANES)
            d_rows = d_unit[at, :, :, lanes].reshape(block, LANES)
            scores = jnp.where(allowed, outer(q_rows, k_rows) * FACTOR, NEG)
            weights = jnp.exp(scores - jnp.max(scores, axis=-1, keepdims=True))
            probs = weights / jnp.sum(weights, axis=-1, keepdims=True)
            d_probs = outer(d_rows, v_rows)
            delta = jnp.sum(probs * d_probs, axis=-1, keepdims=True)
            d_scores = (probs * (d_probs - delta)).astype(low)
            d_q = jnp.dot(d_scores, k_rows, preferred_element_type=wide_t) * FACTOR
            stage[at, :, :, lanes] = unturn(d_q, at).astype(low)
            d_k[0:keys, :] += inner(d_scores, q_rows) * FACTOR
            d_v[0:keys, :] += inner(probs.astype(low), d_rows)
        stage[at, :, :, 2 * LANES : 3 * LANES] = unturn(d_k[block * at : keys, :], at).astype(low)
        stage[at, :, :, 3 * LANES : 4 * LANES] = d_v[block * at : keys, :].astype(low).reshape(fs, span, LANES)
        if at == ctx - 1:
            hear_all(sizes)
        for to in range(fs):

            @pl.when(to != f)
            def _():
                remote(
                    stage.at[at, to], mixed.at[f // 2, at, lax.rem(f, 2)], u_send.at[at, to], u_recv.at[f, at], at_device(d, c, to)
                ).start()

            @pl.when(to == f)
            def _():
                mixed[f // 2, at, lax.rem(f, 2)] = stage[at, to]

        if at == ctx - 1:
            loads[4].wait()
            down_sum[...] = sum_of(down_land).astype(low)
            move(0, down_sum, down_last)
    for slot in range(fs):
        push(proj_ref.at[slot], proj_land, proj_send.at[slot], proj_recv, d, slot)
    loads[2].wait()
    loads[3].wait()

    ends = jnp.logical_or(c == 0, c == ctx - 1)

    def give(step, carry):
        at = towards(c, step, ctx)
        for move_ in range(1, fs):
            other = lax.rem(f + move_, fs)
            arrived(mixed.at[other // 2, at, lax.rem(other, 2)], u_recv.at[other, at], here)
        terms = jnp.dot(mixed[:, at].reshape(both_rows, 4 * LANES), wide[...], preferred_element_type=wide_t)
        in_sum.give(at, terms.reshape(dp, rows, D))

        @pl.when(jnp.logical_and(ends, jnp.logical_and(step > 0, step < ctx - 1)))
        def _():
            in_sum.step(towards(c, step - 1, ctx))

        return carry

    lax.fori_loop(0, ctx, give, 0)

    every = dp * ctx * rows
    k_relay = 2 * lax.rem(c, 2) + d
    relays = (k_relay, lax.rem(k_relay + 2, fs))
    gain_terms = jnp.zeros((1, D), wide_t)
    for slot in (2, 3, 0, 1):
        heads = inner(mixed[:, :, :, :, slot * LANES : (slot + 1) * LANES].reshape(every, LANES), normed[...].reshape(every, D))
        grad_heads[slot] = heads[:HD].astype(low)
        weights = wide[slot * LANES : slot * LANES + HD, :].astype(wide_t)
        gain_terms += jnp.sum(heads[:HD] * weights, axis=0, keepdims=True)
        if slot < 2:
            push(grad_heads.at[slot], q_land, head_send.at[slot], head_recv.at[0], 0, 2 * d + slot)
        else:
            push(grad_heads.at[slot], kv_land.at[slot - 2], head_send.at[slot], head_recv.at[slot - 1], d, relays[slot - 2])

    gain = gains_ref[0:1, :]
    gain_vec[0:1, :] = gain_terms / gain
    gain_vec[1:2, :] = gain_two_ref[0:1, :]
    each = D // n
    for index in range(n):
        gain_stage[index, :, 0:each] = gain_vec[:, index * each : (index + 1) * each]
    gain_land[me] = gain_stage[me]

    def gain_to(step, carry):
        other = lax.rem(me + step, n)
        remote(
            gain_stage.at[other], gain_land.at[me], g_send.at[other], g_recv.at[me],
            at_device(other // (ctx * fs), lax.rem(other // fs, ctx), lax.rem(other, fs)),
        ).start()
        return carry

    lax.fori_loop(1, n, gain_to, 0)

    for source in range(fs):
        arrived(proj_land.at[source], proj_recv.at[source], here)
    proj_sum[...] = sum_of(proj_land).astype(low)
    move(1, proj_sum, proj_last)

    def middle_step(step, carry):
        in_sum.step(towards(c, step, ctx))
        return carry

    lax.fori_loop(jnp.where(ends, ctx - 2, 0), ctx - 1, middle_step, 0)

    def kv_route(slot):
        owner, owner_f = slot * 2 + c // 2, k_relay
        return owner, owner_f, jnp.logical_or(jnp.logical_or(d != 1, owner != c), owner_f != f)

    for slot in range(2):
        owner, owner_f, away = kv_route(slot)

        @pl.when(f == relays[slot])
        def _():
            for source in range(fs):
                arrived(kv_land.at[slot, source], head_recv.at[1 + slot, source], here)
            kv_sum[slot] = sum_of(kv_land.at[slot]).astype(low)

            @pl.when(away)
            def _():
                remote(kv_sum.at[slot], kv_last, move_send.at[2 + slot], move_recv.at[2], at_device(1, owner, owner_f)).start()

            @pl.when(jnp.logical_not(away))
            def _():
                pltpu.make_async_copy(kv_sum.at[slot], kv_last, move_recv.at[2]).start()

    loads[5].wait()
    up_sum[...] = sum_of(up_land)
    up_copy = pltpu.make_async_copy(up_sum, up_out, up_sem)
    up_copy.start()
    @pl.when(d == 0)
    def _():
        for source in range(fs):
            arrived(q_land.at[source], head_recv.at[0, source], here)
        qkv_out[...] = sum_of(q_land)

    for slot in range(fs):
        pushed(proj_ref.at[slot], proj_send.at[slot], d, slot)
    for slot in range(2):
        pushed(grad_heads.at[slot], head_send.at[slot], 0, 2 * d + slot)
        pushed(grad_heads.at[2 + slot], head_send.at[2 + slot], d, relays[slot])

    for at in range(ctx):
        for to in range(fs):

            @pl.when(to != f)
            def _():
                left(stage.at[at, to], u_send.at[at, to], here)

    def gain_from(step, carry):
        other = lax.rem(me + step, n)
        arrived(gain_land.at[other], g_recv.at[other], here)
        return carry

    lax.fori_loop(1, n, gain_from, 0)
    total = gain_land[0]
    for index in range(1, n):
        total += gain_land[index]
    gains_out[...] = total

    def gain_left(step, carry):
        other = lax.rem(me + step, n)
        left(gain_stage.at[other], g_send.at[other], here)
        return carry

    lax.fori_loop(1, n, gain_left, 0)

    in_sum.step(c)

    values = x_ref[...].astype(wide_t)
    scale = lax.rsqrt(jnp.mean(values * values, axis=-1, keepdims=True) + EPS)
    incoming = in_sum.total[...]
    weighted = incoming * gain
    mean = jnp.mean(weighted * values, axis=-1, keepdims=True)
    d_x_ref[...] = (d_resid_ref[...] + scale * weighted - values * (scale * scale * scale) * mean).astype(low)

    for index, dst in enumerate((down_last, proj_last)):
        arrived(dst, move_recv.at[index], here)
    down_out[...] = down_last[...].astype(wide_t)
    proj_out[...] = proj_last[...].astype(wide_t)

    @pl.when(d == 1)
    def _():
        arrived(kv_last, move_recv.at[2], here)
        qkv_out[...] = kv_last[...].astype(wide_t)

    for slot in range(2):
        away = kv_route(slot)[2]

        @pl.when(jnp.logical_and(f == relays[slot], away))
        def _():
            left(kv_sum.at[slot], move_send.at[2 + slot], here)

        @pl.when(jnp.logical_not(stays))
        def _():
            left((down_sum, proj_sum)[slot], move_send.at[slot], here)

    in_sum.finish()
    up_copy.wait()


def last(sizes, x, gains, tables, d_resid, gain_two, grad_proj, unit, d_unit, normed, wide, up_land, down_land):
    dp, ctx, fs = sizes
    n = dp * ctx * fs
    rows = x.shape[0]
    span = rows // 2
    low, wide_t = jnp.bfloat16, jnp.float32
    dma = pltpu.SemaphoreType.DMA
    any_spec, vm_spec = pl.BlockSpec(memory_space=ANY), pl.BlockSpec(memory_space=VM)
    down_rows, proj_rows, half = down_land.shape[1], grad_proj.shape[1], up_land.shape[2]
    shapes = (
        jax.ShapeDtypeStruct((rows, D), low),
        jax.ShapeDtypeStruct((8, LANES), wide_t),
        jax.ShapeDtypeStruct((HD, D), wide_t),
        jax.ShapeDtypeStruct((proj_rows, D), wide_t),
        jax.ShapeDtypeStruct((D, half), wide_t),
        jax.ShapeDtypeStruct((down_rows, D), wide_t),
    )
    return pl.pallas_call(
        functools.partial(last_kernel, sizes),
        name="last",
        out_shape=shapes,
        in_specs=[vm_spec] * 7 + [any_spec] * 6,
        out_specs=[vm_spec] * 4 + [any_spec, vm_spec],
        scratch_shapes=[
            VM(unit.shape, low),
            VM(d_unit.shape, low),
            VM((ctx * fs * span, LANES), wide_t),
            VM((ctx * fs * span, LANES), wide_t),
            VM((ctx, fs, span, 4 * LANES), low),
            VM((dp, ctx, 2, span, 4 * LANES), low),
            VM(normed.shape, low),
            VM(wide.shape, low),
            VM((4, HD, D), low),
            VM(up_land.shape, low),
            VM((fs, down_rows, D), low),
            VM((fs, proj_rows, D), low),
            VM((fs, HD, D), low),
            VM((2, fs, HD, D), low),
            VM((down_rows, D), low),
            VM((proj_rows, D), low),
            VM((2, HD, D), low),
            VM((down_rows, D), low),
            VM((proj_rows, D), low),
            VM((HD, D), low),
            VM((8, D), wide_t),
            VM((n, 8, LANES), wide_t),
            VM((n, 8, LANES), wide_t),
            VM((D, half), wide_t),
            dma((6,)), dma((fs,)), dma((fs,)),
            dma((4,)), dma((3, fs)), dma((4,)), dma((3,)),
            dma((ctx, fs)), dma((fs, ctx)), dma((n,)), dma((n,)), dma,
        ] + LineSum.scratch(ctx, rows),
        compiler_params=pltpu.CompilerParams(collective_id=3, has_side_effects=True, vmem_limit_bytes=63 * 1024 * 1024),
    )(x, gains, *tables, d_resid, gain_two, grad_proj, unit, d_unit, normed, wide, up_land, down_land)


def emit_kernel(count, gains_ref, *refs):
    sources, outs, one_ref, two_ref = refs[:count], refs[count : 2 * count], refs[2 * count], refs[2 * count + 1]
    held, in_sem, out_sem = refs[2 * count + 2 : 3 * count + 2], refs[-2], refs[-1]
    loads = [pltpu.make_async_copy(sources[i], held[i], in_sem.at[i]) for i in range(count)]
    stores = [pltpu.make_async_copy(held[i], outs[i], out_sem.at[i]) for i in range(count)]
    for load in loads:
        load.start()
    each = one_ref.shape[0]
    one_ref[...] = gains_ref[0, :each]
    two_ref[...] = gains_ref[1, :each]
    for load, store in zip(loads, stores):
        load.wait()
        store.start()
    for store in stores:
        store.wait()


def emit(each, gains, *arrays):
    count = len(arrays)
    any_spec, vm_spec = pl.BlockSpec(memory_space=ANY), pl.BlockSpec(memory_space=VM)
    gain = jax.ShapeDtypeStruct((each,), jnp.float32)
    return pl.pallas_call(
        functools.partial(emit_kernel, count),
        name="emit",
        out_shape=[jax.ShapeDtypeStruct(a.shape, a.dtype) for a in arrays] + [gain, gain],
        in_specs=[vm_spec] + [any_spec] * count,
        out_specs=[any_spec] * count + [vm_spec] * 2,
        scratch_shapes=[VM(a.shape, a.dtype) for a in arrays] + [pltpu.SemaphoreType.DMA((count,))] * 2,
        compiler_params=pltpu.CompilerParams(vmem_limit_bytes=63 * 1024 * 1024),
    )(gains, *arrays)


def on_device(tokens, cotangent, attn_gain, w_qkv, w_out, mlp_gain, w_gate_up, w_down):
    dp, ctx, fs = where = tuple(lax.axis_size(name) for name in ("dp", "ctx", "fsdp"))
    mb, _, span, _ = tokens.shape
    rows = mb * span
    x = tokens.reshape(rows, D)
    dy = cotangent.reshape(rows, D)
    each = attn_gain.shape[0]
    block_out, d_resid, grad_two, *tables, normed, unit, qkv, gains, d_unit, grad_proj, up_land, down_land = front(
        where, 4, x, attn_gain, mlp_gain, w_qkv.T, dy, w_out, w_down, w_gate_up
    )
    grad_tokens, gain_grads, grad_qkv, grad_out, grad_gate_up, grad_down = last(
        where, x, gains, tables, d_resid, grad_two, grad_proj, unit, d_unit, normed, qkv, up_land, down_land
    )
    block_out, grad_tokens, grad_qkv, grad_out, grad_gate_up, grad_down, grad_one, grad_two = emit(
        each, gain_grads, block_out, grad_tokens, grad_qkv, grad_out, grad_gate_up, grad_down
    )
    return (
        block_out.reshape(tokens.shape),
        grad_tokens.reshape(tokens.shape),
        grad_one,
        grad_qkv.T,
        grad_out,
        grad_two,
        grad_gate_up,
        grad_down,
    )


def fits(mesh):
    return mesh.shape["dp"] == 2 and mesh.shape["ctx"] == 4 and mesh.shape["fsdp"] == 4


def solution(mesh):
    placed = (
        P(None, "dp", ("ctx", "fsdp"), None),
        P(None, "dp", ("ctx", "fsdp"), None),
        P(("dp", "ctx", "fsdp")),
        P(None, ("dp", "ctx", "fsdp")),
        P(("dp", "ctx", "fsdp"), None),
        P(("dp", "ctx", "fsdp")),
        P(None, ("dp", "ctx", "fsdp")),
        P(("dp", "ctx", "fsdp"), None),
    )
    return jax.shard_map(
        on_device if fits(mesh) else on_device_gathered,
        mesh=mesh,
        in_specs=placed,
        out_specs=(
            P(None, "dp", ("ctx", "fsdp"), None),
            P(None, "dp", ("ctx", "fsdp"), None),
            P(("dp", "ctx", "fsdp")),
            P(None, ("dp", "ctx", "fsdp")),
            P(("dp", "ctx", "fsdp"), None),
            P(("dp", "ctx", "fsdp")),
            P(None, ("dp", "ctx", "fsdp")),
            P(("dp", "ctx", "fsdp"), None),
        ),
        check_vma=False,
    )
```

```python
import functools
import math

import jax
import jax.numpy as jnp
from jax import lax
from jax.experimental import pallas as pl
from jax.experimental.pallas import tpu as pltpu
from jax.sharding import PartitionSpec as P

D = 1536
H = 16
KVH = 8
HD = 96
FF = 4096


EPS = 1e-05
THETA = 100000.0
NEG = -1e30


def in_blocks(value, dim, length):
    lengths = value.shape
    pieces = value.reshape(*lengths[:dim], length, lengths[dim] // length, *lengths[dim + 1 :])
    return jnp.moveaxis(pieces, dim, 0)


def sum_at_owner(value, axis, dim):
    pieces = in_blocks(value, dim, lax.axis_size(axis))
    arrived = lax.all_to_all(pieces, axis, split_axis=0, concat_axis=0, tiled=True)
    return arrived.astype(jnp.float32).sum(axis=0)


def side_by_side(arrays, axis, dim, along):
    both = jnp.concatenate(arrays, axis=along)
    whole, at, finished = (sum_at_owner(both, axis, dim), 0, [])
    for a in arrays:
        finished.append(lax.slice_in_dim(whole, at, at + a.shape[along], axis=along))
        at += a.shape[along]
    return tuple(finished)


def rms_norm(values, gain_vec):
    return values * lax.rsqrt(jnp.mean(values * values, axis=-1, keepdims=True) + EPS) * gain_vec


def tables(start, length, width):
    half_width = width // 2
    frequency = THETA ** (-(jnp.arange(half_width, dtype=jnp.float32) * 2.0) / width)
    angles = (start + jnp.arange(length, dtype=jnp.int32)).astype(jnp.float32)[:, None] * frequency[
        None, :
    ]
    return (jnp.cos(angles), jnp.sin(angles))


def rotate(values, cosine, sine_table):
    half_width = values.shape[-1] // 2
    first_half = values[..., :half_width]
    second_half = values[..., half_width:]
    cos_b = cosine[:, None, :]
    sin_b = sine_table[:, None, :]
    return jnp.concatenate(
        [first_half * cos_b - second_half * sin_b, second_half * cos_b + first_half * sin_b],
        axis=-1,
    )


def swiglu(both):
    return jax.nn.silu(both[:, :FF]) * both[:, FF:]


def inner(left, right):
    return lax.dot_general(
        left, right, (((0,), (0,)), ((), ())), preferred_element_type=jnp.float32
    )


def outer(left, right):
    return lax.dot_general(
        left, right, (((1,), (1,)), ((), ())), preferred_element_type=jnp.float32
    )


def unchanged(state):
    return state


def on_device_gathered(tokens, cotangent, attn_gain, w_qkv, w_out, mlp_gain, w_gate_up, w_down):
    tok_count = tokens.shape[2]
    groups = H // KVH
    factor = HD ** (-0.5)
    seq_length = tok_count * lax.axis_size(("ctx", "fsdp"))
    pos_first = lax.axis_index(("ctx", "fsdp")) * tok_count
    positions = pos_first + jnp.arange(tok_count, dtype=jnp.int32)
    pos_last = pos_first + tok_count - 1
    cosine, sine_table = tables(pos_first, tok_count, HD)
    sums = [
        jnp.zeros((D,), jnp.float32),
        jnp.zeros((D, (H + 2 * KVH) * HD), jnp.float32),
        jnp.zeros((H * HD, D), jnp.float32),
        jnp.zeros((D,), jnp.float32),
        jnp.zeros((D, 2 * FF), jnp.float32),
        jnp.zeros((FF, D), jnp.float32),
    ]
    outputs = []
    in_grads = []
    whole = (
        lax.all_gather(attn_gain, ("dp", "ctx", "fsdp"), axis=0, tiled=True),
        lax.all_gather(w_qkv, ("dp", "ctx", "fsdp"), axis=1, tiled=True),
        lax.all_gather(w_out, ("dp", "ctx", "fsdp"), axis=0, tiled=True),
        lax.all_gather(mlp_gain, ("dp", "ctx", "fsdp"), axis=0, tiled=True),
        lax.all_gather(w_gate_up, ("dp", "ctx", "fsdp"), axis=1, tiled=True),
        lax.all_gather(w_down, ("dp", "ctx", "fsdp"), axis=0, tiled=True),
    )
    for step_index in range(tokens.shape[0]):
        gain_one, mix_qkv, mix_out, gain_two, mix_gate_up, mix_down = whole
        inputs = tokens[step_index, 0].astype(jnp.float32)
        normed = rms_norm(inputs, gain_one.astype(jnp.float32)).astype(jnp.bfloat16)
        mixed = jnp.dot(normed, mix_qkv, preferred_element_type=jnp.float32)
        queries = rotate(mixed[:, : H * HD].reshape(tok_count, H, HD), cosine, sine_table).astype(
            jnp.bfloat16
        )
        key_rows = rotate(
            mixed[:, H * HD : (H + KVH) * HD].reshape(tok_count, KVH, HD), cosine, sine_table
        )
        key_rows = key_rows.astype(jnp.bfloat16).reshape(tok_count, KVH * HD)
        value_rows = mixed[:, (H + KVH) * HD :].astype(jnp.bfloat16)
        grouped = queries.reshape(tok_count, KVH, groups, HD)
        start_state = (
            jnp.full((KVH, groups, tok_count), NEG, jnp.float32),
            jnp.zeros((KVH, groups, tok_count), jnp.float32),
            jnp.zeros((KVH, groups, tok_count, HD), jnp.float32),
        )
        piece = (
            lax.all_gather(key_rows, ("ctx", "fsdp"), axis=0, tiled=True),
            lax.all_gather(value_rows, ("ctx", "fsdp"), axis=0, tiled=True),
        )

        def work(state):
            best, total, summed = state
            key_count = piece[0].shape[0]
            keys = piece[0].reshape(key_count, KVH, HD)
            values = piece[1].reshape(key_count, KVH, HD)
            scores = (
                jnp.einsum("qkgd,tkd->kgqt", grouped, keys, preferred_element_type=jnp.float32)
                * factor
            )
            allowed = jnp.arange(key_count, dtype=jnp.int32)[None, :] <= positions[:, None]
            scores = jnp.where(allowed, scores, NEG)
            new_best = jnp.maximum(best, jnp.max(scores, axis=-1))
            weights = jnp.where(allowed, jnp.exp(scores - new_best[..., None]), 0.0)
            total = jnp.sum(weights, axis=-1)
            summed = jnp.einsum(
                "kgqt,tkd->kgqd",
                weights.astype(jnp.bfloat16),
                values,
                preferred_element_type=jnp.float32,
            )
            return (new_best, total, summed)

        best, total, summed = lax.cond(jnp.int32(0) <= pos_last, work, unchanged, start_state)
        head_out = summed / total[..., None]
        log_total = best + jnp.log(total)
        attended = (
            jnp.transpose(head_out, (2, 0, 1, 3)).reshape(tok_count, H * HD).astype(jnp.bfloat16)
        )
        resid = inputs + jnp.dot(attended, mix_out, preferred_element_type=jnp.float32)
        normed_two = rms_norm(resid, gain_two.astype(jnp.float32)).astype(jnp.bfloat16)
        both = jnp.dot(normed_two, mix_gate_up, preferred_element_type=jnp.float32)
        acted = swiglu(both).astype(jnp.bfloat16)
        result = resid + jnp.dot(acted, mix_down, preferred_element_type=jnp.float32)
        outputs.append(result.astype(jnp.bfloat16))
        gain_one, mix_qkv, mix_out, gain_two, mix_gate_up, mix_down = whole
        up_low = cotangent[step_index, 0]
        upstream = up_low.astype(jnp.float32)
        sums[5] = sums[5] + inner(acted, up_low)
        d_act = outer(up_low, mix_down)
        _, pull_glu = jax.vjp(swiglu, both)
        d_both = pull_glu(d_act)[0].astype(jnp.bfloat16)
        sums[4] = sums[4] + inner(normed_two, d_both)
        d_normed_two = outer(d_both, mix_gate_up)
        _, pull_two = jax.vjp(rms_norm, resid, gain_two.astype(jnp.float32))
        d_resid_norm, d_gain_two = pull_two(d_normed_two)
        sums[3] = sums[3] + d_gain_two
        d_resid = upstream + d_resid_norm
        d_resid_low = d_resid.astype(jnp.bfloat16)
        sums[2] = sums[2] + inner(attended, d_resid_low)
        d_attended = outer(d_resid_low, mix_out).astype(jnp.bfloat16)
        d_grouped = d_attended.reshape(tok_count, KVH, groups, HD)
        delta = jnp.einsum("qkgd,kgqd->kgq", d_grouped.astype(jnp.float32), head_out)
        zero_q = jnp.zeros((tok_count, KVH, groups, HD), jnp.float32)
        back_state = (
            zero_q,
            jnp.zeros((seq_length, KVH * HD), jnp.float32),
            jnp.zeros((seq_length, KVH * HD), jnp.float32),
        )
        attend_piece = (
            lax.all_gather(key_rows, ("ctx", "fsdp"), axis=0, tiled=True),
            lax.all_gather(value_rows, ("ctx", "fsdp"), axis=0, tiled=True),
        )

        def attend_work(state):
            key_count = attend_piece[0].shape[0]
            keys = attend_piece[0].reshape(key_count, KVH, HD)
            values = attend_piece[1].reshape(key_count, KVH, HD)
            scores = (
                jnp.einsum("qkgd,tkd->kgqt", grouped, keys, preferred_element_type=jnp.float32)
                * factor
            )
            allowed = jnp.arange(key_count, dtype=jnp.int32)[None, :] <= positions[:, None]
            scores = jnp.where(allowed, scores, NEG)
            probs = jnp.where(allowed, jnp.exp(scores - log_total[..., None]), 0.0)
            d_probs = jnp.einsum(
                "qkgd,tkd->kgqt", d_grouped, values, preferred_element_type=jnp.float32
            )
            d_scores = (probs * (d_probs - delta[..., None])).astype(jnp.bfloat16)
            grad_q = jnp.einsum(
                "kgqt,tkd->qkgd", d_scores, keys, preferred_element_type=jnp.float32
            )
            piece_k = (
                jnp.einsum("kgqt,qkgd->tkd", d_scores, grouped, preferred_element_type=jnp.float32)
                * factor
            )
            piece_v = jnp.einsum(
                "kgqt,qkgd->tkd",
                probs.astype(jnp.bfloat16),
                d_grouped,
                preferred_element_type=jnp.float32,
            )
            grad_k = piece_k.reshape(key_count, KVH * HD)
            grad_v = piece_v.reshape(key_count, KVH * HD)
            return (grad_q, grad_k, grad_v)

        back_result = lax.cond(jnp.int32(0) <= pos_last, attend_work, unchanged, back_state)
        grad_q = back_result[0]
        summed_k, summed_v = side_by_side(
            (back_result[1].astype(jnp.bfloat16), back_result[2].astype(jnp.bfloat16)),
            ("ctx", "fsdp"),
            0,
            1,
        )
        d_q_raw = rotate(grad_q.reshape(tok_count, H, HD) * factor, cosine, -sine_table).reshape(
            tok_count, H * HD
        )
        d_k_raw = rotate(summed_k.reshape(tok_count, KVH, HD), cosine, -sine_table).reshape(
            tok_count, KVH * HD
        )
        d_mixed = jnp.concatenate([d_q_raw, d_k_raw, summed_v], axis=1).astype(jnp.bfloat16)
        sums[1] = sums[1] + inner(normed, d_mixed)
        d_normed = outer(d_mixed, mix_qkv)
        _, pull_one = jax.vjp(rms_norm, inputs, gain_one.astype(jnp.float32))
        d_inputs_norm, d_gain_one = pull_one(d_normed)
        sums[0] = sums[0] + d_gain_one
        in_grads.append((d_resid + d_inputs_norm).astype(jnp.bfloat16))
    grad_gain_one, grad_qkv, grad_out, grad_gain_two, grad_gate_up, grad_down = (
        lax.psum_scatter(sums[0], ("dp", "ctx", "fsdp"), scatter_dimension=0, tiled=True),
        lax.psum_scatter(sums[1], ("dp", "ctx", "fsdp"), scatter_dimension=1, tiled=True),
        lax.psum_scatter(sums[2], ("dp", "ctx", "fsdp"), scatter_dimension=0, tiled=True),
        lax.psum_scatter(sums[3], ("dp", "ctx", "fsdp"), scatter_dimension=0, tiled=True),
        lax.psum_scatter(sums[4], ("dp", "ctx", "fsdp"), scatter_dimension=1, tiled=True),
        lax.psum_scatter(sums[5], ("dp", "ctx", "fsdp"), scatter_dimension=0, tiled=True),
    )
    block_out = jnp.stack(outputs)[:, None]
    grad_tokens = jnp.stack(in_grads)[:, None]
    return (
        block_out,
        grad_tokens,
        grad_gain_one,
        grad_qkv,
        grad_out,
        grad_gain_two,
        grad_gate_up,
        grad_down,
    )


MESH = pl.DeviceIdType.MESH
VM = pltpu.VMEM
ANY = pl.ANY


def place():
    return lax.axis_index("dp"), lax.axis_index("ctx"), lax.axis_index("fsdp")


def at_device(dp, ctx, fs):
    return {"dp": dp, "ctx": ctx, "fsdp": fs}


def remote(src, dst, send, recv, device):
    return pltpu.make_async_remote_copy(
        src_ref=src, dst_ref=dst, send_sem=send, recv_sem=recv, device_id=device, device_id_type=MESH
    )


def arrived(dst, recv, device):
    remote(dst, dst, recv, recv, device).wait_recv()


def left(src, send, device):
    remote(src, src, send, send, device).wait_send()


def tell_all(sizes):
    dp, ctx, fs = sizes
    n = dp * ctx * fs
    d, c, f = place()
    me = (d * ctx + c) * fs + f
    barrier = pltpu.get_barrier_semaphore()

    def tell(step, carry):
        other = lax.rem(me + step, n)
        pl.semaphore_signal(
            barrier,
            inc=1,
            device_id=at_device(other // (ctx * fs), lax.rem(other // fs, ctx), lax.rem(other, fs)),
            device_id_type=MESH,
        )
        return carry

    lax.fori_loop(1, n, tell, 0)


def hear_all(sizes):
    dp, ctx, fs = sizes
    pl.semaphore_wait(pltpu.get_barrier_semaphore(), dp * ctx * fs - 1)


HALVES = 2


def part_of(ref, index):
    rows = ref.shape[-2] // HALVES
    return ref.at[index * rows : (index + 1) * rows]


def near_or_inner(c, at, n):
    ends = jnp.logical_or(c == 0, c == n - 1)
    return jnp.logical_or(jnp.logical_not(ends), jnp.abs(at - c) <= 1)


class LineGather:
    def __init__(self, n, own, whole, send, recv, local, short=False):
        self.n, self.own, self.whole, self.send, self.recv, self.local = n, own, whole, send, recv, local
        self.short = short
        self.d, self.c, self.f = place()
        self.here = at_device(self.d, self.c, self.f)

    def slot(self, at):
        return self.whole.at[self.d, at]

    def held(self, at):
        valid = jnp.logical_and(at >= 0, at < self.n)
        return jnp.logical_and(valid, near_or_inner(self.c, at, self.n)) if self.short else valid

    def passes(self, way, at):
        ahead = self.n - 2 - self.c if way == 0 else self.c - 1
        inside = at <= self.c if way == 0 else at >= self.c
        goes = jnp.logical_and(inside, ahead >= 0)
        return jnp.logical_and(goes, jnp.logical_or(at == self.c, ahead > 0)) if self.short else goes

    def along(self, way, block, at, part):
        to = (at_device(self.d, self.c + 1, self.f), at_device(self.d, self.c - 1, self.f), at_device(1 - self.d, self.c, self.f))[way]
        return remote(part_of(block, part), part_of(self.slot(at), part), self.send.at[way, at, part], self.recv.at[self.d, at, part], to)

    def start(self):
        c = self.c
        for part in range(HALVES):

            @pl.when(c < self.n - 1)
            def _():
                self.along(0, self.own, c, part).start()

            @pl.when(c > 0)
            def _():
                self.along(1, self.own, c, part).start()

        for part in range(HALVES):
            self.along(2, self.own, c, part).start()
        pltpu.make_async_copy(self.own, self.slot(c), self.local).start()

    def forward(self, k):
        for part in range(HALVES):
            for way, at in enumerate((self.c - k, self.c + k)):

                @pl.when(self.held(at))
                def _():
                    arrived(part_of(self.slot(at), part), self.recv.at[self.d, at, part], self.here)

                    @pl.when(self.passes(way, at))
                    def _():
                        self.along(way, self.slot(at), at, part).start()

                    self.along(2, self.slot(at), at, part).start()

    def reach(self, step):
        now = jnp.abs(ordered(self.c, step, self.n) - self.c)
        before = jnp.abs(ordered(self.c, step - 1, self.n) - self.c)

        @pl.when(jnp.logical_and(step > 0, now != before))
        def _():
            self.forward(now)

    def other(self, at):
        @pl.when(self.held(at))
        def _():
            for part in range(HALVES):
                arrived(part_of(self.whole.at[1 - self.d, at], part), self.recv.at[1 - self.d, at, part], self.here)

    def finish_sends(self):
        for at in range(self.n):
            for part in range(HALVES):
                block = part_of(self.slot(at), part)
                for way in range(3):

                    @pl.when(self.passes(way, at) if way < 2 else self.held(at))
                    def _():
                        left(block, self.send.at[way, at, part], self.here)

    def finish(self):
        self.finish_sends()
        pltpu.make_async_copy(self.own, self.slot(self.c), self.local).wait()


FACTOR = HD ** (-0.5)
LANES = 128


def ordered(c, step, n):
    at = jnp.int32(0)
    for here in range(n):
        near = sorted(range(n), key=lambda place_: (abs(place_ - here), place_))
        for index, value in enumerate(near):
            at = jnp.where(jnp.logical_and(c == here, step == index), value, at)
    return at


def towards(c, step, n):
    at = c
    for here in range(n):
        due = []
        for to in range(n):
            if to != here:
                hops = here if to > here else n - 1 - here
                due.append((hops + (n - 1 - to if to > here else to), -hops, to))
        for index, (_, _, to) in enumerate(sorted(due)):
            at = jnp.where(jnp.logical_and(c == here, step == index), to, at)
    return at


class LineSum:
    def __init__(self, n, mine, out_core, in_core, out_line, in_line, total, sems):
        self.n, self.mine, self.out_core, self.in_core = n, mine, out_core, in_core
        self.out_line, self.in_line, self.total = out_line, in_line, total
        self.core_send, self.core_recv, self.line_send, self.line_recv = sems
        self.d, self.c, self.f = place()
        self.here = at_device(self.d, self.c, self.f)

    def give(self, at, both):
        self.keep(at, both)
        self.hand(at)

    def keep(self, at, both):
        d = self.d
        low = both.astype(jnp.bfloat16)

        @pl.when(d == 0)
        def _():
            self.mine[at] = low[0]
            self.out_core[at] = low[1]

        @pl.when(d != 0)
        def _():
            self.mine[at] = low[1]
            self.out_core[at] = low[0]

    def hand(self, at):
        remote(
            self.out_core.at[at], self.in_core.at[at], self.core_send.at[at], self.core_recv.at[at], at_device(1 - self.d, self.c, self.f)
        ).start()

    def step(self, at):
        n, d, c, f = self.n, self.d, self.c, self.f
        arrived(self.in_core.at[at], self.core_recv.at[at], self.here)
        rows = self.total.shape[0] // HALVES
        for part in range(HALVES):
            own = slice(part * rows, (part + 1) * rows)
            self.total[own] = self.mine[at, own].astype(jnp.float32) + self.in_core[at, own].astype(jnp.float32)
            for way, comes in enumerate((jnp.logical_and(at <= c, c < n - 1), jnp.logical_and(at >= c, c > 0))):

                @pl.when(comes)
                def _():
                    arrived(self.in_line.at[way, at, own], self.line_recv.at[way, at, part], self.here)
                    self.total[own] += self.in_line[way, at, own].astype(jnp.float32)

            @pl.when(at != c)
            def _():
                self.out_line[at, own] = self.total[own].astype(jnp.bfloat16)

            for way, (goes, to) in enumerate(((at < c, c - 1), (at > c, c + 1))):

                @pl.when(goes)
                def _():
                    remote(
                        self.out_line.at[at, own], self.in_line.at[way, at, own],
                        self.line_send.at[at, part], self.line_recv.at[way, at, part], at_device(d, to, f),
                    ).start()

    def finish(self):
        rows = self.total.shape[0] // HALVES
        for at in range(self.n):
            left(self.out_core.at[at], self.core_send.at[at], self.here)

            @pl.when(at != self.c)
            def _():
                for part in range(HALVES):
                    left(self.out_line.at[at, part * rows : (part + 1) * rows], self.line_send.at[at, part], self.here)

    @staticmethod
    def scratch(ctx, rows):
        low = jnp.bfloat16
        dma = pltpu.SemaphoreType.DMA
        return [
            VM((ctx, rows, D), low), VM((ctx, rows, D), low), VM((ctx, rows, D), low), VM((ctx, rows, D), low),
            VM((2, ctx, rows, D), low), VM((rows, D), jnp.float32),
            dma((ctx,)), dma((ctx,)), dma((ctx, HALVES)), dma((2, ctx, HALVES)),
        ]


def down_route(d, c):
    return (lax.rem(c, 2), 2 * d + c // 2), (c // 2, 2 * lax.rem(c, 2) + d)


def front_kernel(
    sizes, hidden, parts, x_ref, one_ref, two_ref, w_ref, dy_ref, proj_ref, down_ref, gate_up_ref,
    out_ref, d_resid_out, gain_out, block_ref, step_ref, normed_out, qkv_out, wide_out, gains_out, unit_out, grad_proj_out, up_land, down_land,
    x_all, wide, normed, stage, qkv_unit, att_stage, att, gain_all, gain_vec,
    dy_all, proj, down_mid, down, gate_up, resid, own_two, normed_two, act, d_both, own_d, d_stage, unit,
    grad_up, grad_down, grad_proj, grad_proj_low, gains_ref, d_resid_held,
    line_send, line_recv, line_local, w_send, w_recv, w_pass, g_send, g_recv, q_send, q_recv, a_send, a_recv, out_sem,
    dy_send, dy_recv, dy_local, m_send, m_recv, m_pass, down_send, down_recv, d_recv, d_pass, gu_send, gu_recv,
    two_send, two_recv, two_local, dr_send, dr_recv, dr_local, u_send, u_recv, gup_send, gup_recv, gdn_send, gdn_recv,
    *sums,
):
    d_resid_all = x_all
    dp, ctx, fs = sizes
    n = dp * ctx * fs
    d, c, f = place()
    here = at_device(d, c, f)
    span = stage.shape[2]
    tell_all(sizes)
    fill_tables(block_ref, step_ref)
    gains_ref[0:1, 0 : D // n] = one_ref[...].astype(jnp.float32).reshape(1, D // n)
    gains_ref[1:2, 0 : D // n] = two_ref[...].astype(jnp.float32).reshape(1, D // n)
    for slot in range(4):
        wide[slot * LANES + HD : (slot + 1) * LANES, :] = jnp.zeros((LANES - HD, D), jnp.bfloat16)
    each_proj = proj_ref.shape[0]
    for start in range(2 * each_proj, 2 * LANES, LANES):
        proj[start : start + LANES - 2 * each_proj, :] = jnp.zeros((LANES - 2 * each_proj, D), jnp.bfloat16)
    hear_all(sizes)

    def proj_rows(slot):
        start = slot // 2 * LANES + lax.rem(slot, 2) * each_proj
        return proj.at[pl.ds(pl.multiple_of(start, 16), each_proj)]

    def head_rows(slot):
        return wide.at[pl.ds(pl.multiple_of(slot * LANES, LANES), HD)]

    q_core = f // 2
    kv_slot = 2 + c // 2
    kv_ctx = 2 * lax.rem(c, 2) + f // 2
    kv_core = lax.rem(f, 2)
    kv_f = lax.rem(f + 2 * (c // 2), fs)
    kv_away = jnp.logical_or(jnp.logical_or(kv_core != d, kv_ctx != c), kv_f != f)
    relay_of = {slot: f == lax.rem(2 * lax.rem(c, 2) + d + 2 * (slot - 2), fs) for slot in (2, 3)}

    me = (d * ctx + c) * fs + f

    def gain_to(step, carry):
        other = lax.rem(me + step, n)
        remote(
            gains_ref, gain_all.at[me], g_send.at[other], g_recv.at[me],
            at_device(other // (ctx * fs), lax.rem(other // fs, ctx), lax.rem(other, fs)),
        ).start()
        return carry

    lax.fori_loop(1, n, gain_to, 0)
    gain_all[me] = gains_ref[...]

    @pl.when(jnp.logical_and(d == 1, kv_away))
    def _():
        remote(w_ref, head_rows(kv_slot), w_send.at[0], w_recv.at[kv_slot], at_device(kv_core, kv_ctx, kv_f)).start()

    @pl.when(jnp.logical_and(d == 1, jnp.logical_not(kv_away)))
    def _():
        pltpu.make_async_copy(w_ref, head_rows(kv_slot), w_recv.at[kv_slot]).start()

    x_line = LineGather(ctx, x_ref, x_all, line_send, line_recv, line_local)
    x_line.start()

    @pl.when(d == 0)
    def _():
        slot = lax.rem(f, 2)
        for to in range(fs):

            @pl.when(jnp.logical_or(q_core != 0, to != f))
            def _():
                remote(w_ref, head_rows(slot), w_send.at[to], w_recv.at[slot], at_device(q_core, c, to)).start()

            @pl.when(jnp.logical_and(q_core == 0, to == f))
            def _():
                pltpu.make_async_copy(w_ref, head_rows(slot), w_recv.at[slot]).start()

    for slot in (2, 3):

        @pl.when(relay_of[slot])
        def _():
            arrived(head_rows(slot), w_recv.at[slot], here)
            for step in range(1, fs):
                to = lax.rem(f + step, fs)
                remote(head_rows(slot), head_rows(slot), w_pass.at[slot - 2, step], w_recv.at[slot], at_device(d, c, to)).start()

    gu_core = f // 2
    gu_slot = 2 * d + lax.rem(f, 2)
    part_rows = gate_up_ref.shape[0] // parts

    def push_part(part):
        first_row = part * part_rows
        src = gate_up_ref.at[first_row : first_row + part_rows]
        dst = gate_up.at[gu_slot, first_row : first_row + part_rows]
        for to in range(fs):
            own_place = jnp.logical_and(gu_core == d, f == to)

            @pl.when(jnp.logical_not(own_place))
            def _():
                remote(src, dst, gu_send.at[part, to], gu_recv.at[part, gu_slot], at_device(gu_core, c, to)).start()

            @pl.when(own_place)
            def _():
                pltpu.make_async_copy(src, dst, gu_recv.at[part, gu_slot]).start()

    def gain_from(step, carry):
        other = lax.rem(me + step, n)
        arrived(gain_all.at[other], g_recv.at[other], here)
        return carry

    lax.fori_loop(1, n, gain_from, 0)
    each = D // n
    for index in range(n):
        gain_vec[:, index * each : (index + 1) * each] = gain_all[index][:, :each]
    gain = gain_vec[0:1, :]

    for k in range(1, ctx - 1):
        x_line.forward(k)
    to_core, to_ctx = lax.rem(c, 2), 2 * d + c // 2
    stays = jnp.logical_and(to_core == d, to_ctx == c)

    @pl.when(jnp.logical_not(stays))
    def _():
        remote(proj_ref, proj_rows(f), m_send, m_recv.at[f], at_device(to_core, to_ctx, f)).start()

    @pl.when(stays)
    def _():
        pltpu.make_async_copy(proj_ref, proj_rows(f), m_recv.at[f]).start()

    dy_line = LineGather(ctx, dy_ref, dy_all, dy_send, dy_recv, dy_local)
    dy_line.start()
    for slot in range(4):
        if slot < 2:
            arrived(head_rows(slot), w_recv.at[slot], here)
        else:

            @pl.when(jnp.logical_not(relay_of[slot]))
            def _():
                arrived(head_rows(slot), w_recv.at[slot], here)

    push_part(0)
    pltpu.make_async_copy(x_line.own, x_line.slot(c), x_line.local).wait()

    def block(step, carry):
        at = ordered(c, step, ctx)

        x_line.other(at)
        values = x_all[:, at].reshape(dp * 2 * span, D).astype(jnp.float32)
        scale = lax.rsqrt(jnp.mean(values * values, axis=-1, keepdims=True) + EPS)
        low = (values * scale * gain).astype(jnp.bfloat16)
        normed[:, at] = low.reshape(dp, 2 * span, D)
        heads = outer(low, wide[...])
        cosine, sine_up, sine_down = turns(block_ref, step_ref, at * fs + f)
        for slot in range(4):
            head = heads[:, slot * LANES : (slot + 1) * LANES]
            if slot < 3:
                turned_up = pltpu.roll(head, HD // 2, 1).reshape(2 * dp, span, LANES)
                turned_down = pltpu.roll(head, LANES - HD // 2, 1).reshape(2 * dp, span, LANES)
                head = head.reshape(2 * dp, span, LANES)
                head = head * cosine[None] + turned_up * sine_up[None] + turned_down * sine_down[None]
            else:
                head = head.reshape(2 * dp, span, LANES)
            stage[at, :, :, slot * LANES : (slot + 1) * LANES] = head.astype(jnp.bfloat16)
        for to in range(2 * dp):

            @pl.when(to != f)
            def _():
                remote(stage.at[at, to], qkv_unit.at[at, f], q_send.at[at, to], q_recv.at[at, f], at_device(d, c, to)).start()

            @pl.when(to == f)
            def _():
                qkv_unit[at, f] = stage[at, to]

        return carry

    def near(step, carry):
        @pl.when(step == ctx - 1)
        def _():
            x_line.forward(ctx - 1)

        return block(step, carry)

    lax.fori_loop(0, ctx, near, 0)
    normed_copy = pltpu.make_async_copy(normed, normed_out, out_sem.at[3])
    wide_copy = pltpu.make_async_copy(wide, wide_out, out_sem.at[4])
    gains_copy = pltpu.make_async_copy(gain_vec, gains_out, out_sem.at[5])
    normed_copy.start()
    wide_copy.start()
    gains_copy.start()

    @pl.when(jnp.logical_not(stays))
    def _():
        remote(down_ref, down_mid, down_send, down_recv, at_device(to_core, to_ctx, f)).start()

    @pl.when(stays)
    def _():
        pltpu.make_async_copy(down_ref, down_mid, down_recv).start()

    arrived(proj_rows(f), m_recv.at[f], here)
    for step in range(1, fs):
        to = lax.rem(f + step, fs)
        remote(proj_rows(f), proj_rows(f), m_pass.at[step], m_recv.at[f], at_device(d, c, to)).start()

    ends = jnp.logical_or(c == 0, c == ctx - 1)

    @pl.when(jnp.logical_not(ends))
    def _():
        dy_line.forward(1)


    for at in range(ctx):
        for step in range(1, fs):
            other = lax.rem(f + step, fs)
            arrived(qkv_unit.at[at, other], q_recv.at[at, other], here)
    qkv_copy = pltpu.make_async_copy(qkv_unit, qkv_out, out_sem.at[0])
    qkv_copy.start()

    block_rows = fs * span
    for at in (0, ctx - 1, *range(1, ctx - 1)):
        keys = block_rows * (at + 1)
        k_rows = qkv_unit[0 : at + 1, :, :, 2 * LANES : 3 * LANES].reshape(keys, LANES)
        v_rows = qkv_unit[0 : at + 1, :, :, 3 * LANES : 4 * LANES].reshape(keys, LANES)
        allowed = lax.broadcasted_iota(jnp.int32, (block_rows, keys), 1) <= block_rows * at + lax.broadcasted_iota(
            jnp.int32, (block_rows, keys), 0
        )
        for head in range(2):
            q_rows = qkv_unit[at, :, :, head * LANES : (head + 1) * LANES].reshape(block_rows, LANES)
            scores = outer(q_rows, k_rows) * FACTOR
            scores = jnp.where(allowed, scores, NEG)
            best = jnp.max(scores, axis=-1, keepdims=True)
            weights = jnp.exp(scores - best)
            probs = weights / jnp.sum(weights, axis=-1, keepdims=True)
            mixed = jnp.dot(probs.astype(jnp.bfloat16), v_rows, preferred_element_type=jnp.float32)
            att_stage[at, :, :, head * LANES : (head + 1) * LANES] = mixed.astype(jnp.bfloat16).reshape(fs, span, LANES)
        for to in range(fs):

            @pl.when(to != f)
            def _():
                remote(
                    att_stage.at[at, to], att.at[f // 2, at, lax.rem(f, 2)], a_send.at[at, to], a_recv.at[f, at], at_device(d, c, to)
                ).start()

            @pl.when(to == f)
            def _():
                att[f // 2, at, lax.rem(f, 2)] = att_stage[at, to]


    ends = jnp.logical_or(c == 0, c == ctx - 1)

    @pl.when(jnp.logical_not(ends))
    def _():
        dy_line.forward(2)

    for step in range(1, fs):
        other = lax.rem(f + step, fs)
        arrived(proj_rows(other), m_recv.at[other], here)
    rows = x_ref.shape[0]
    both_rows = dp * rows
    half = hidden // 2
    line_sum = LineSum(ctx, *sums[:6], sums[6:10])
    second_sum = LineSum(ctx, *sums[10:16], sums[16:20])
    out_sum = line_sum

    def project(step, carry):
        at = towards(c, step, ctx)
        for move in range(1, fs):
            other = lax.rem(f + move, fs)
            arrived(att.at[other // 2, at, lax.rem(other, 2)], a_recv.at[other, at], here)
        terms = jnp.dot(att[:, at].reshape(both_rows, 2 * LANES), proj[...], preferred_element_type=jnp.float32)
        line_sum.give(at, terms.reshape(dp, rows, D))

        @pl.when(jnp.logical_and(ends, step > 0))
        def _():
            line_sum.step(towards(c, step - 1, ctx))

        return carry

    lax.fori_loop(0, ctx, project, 0)

    arrived(down_mid, down_recv, here)
    pltpu.make_async_copy(down_mid, down.at[f], d_recv.at[f]).start()
    for step in range(1, fs):
        to = lax.rem(f + step, fs)
        remote(down_mid, down.at[f], d_pass.at[step], d_recv.at[f], at_device(d, c, to)).start()
    for part in range(1, parts):
        push_part(part)

    def sum_step(step, carry):
        line_sum.step(towards(c, step, ctx))
        return carry

    lax.fori_loop(jnp.where(ends, ctx - 1, 0), ctx - 1, sum_step, 0)

    @pl.when(ends)
    def _():
        for k in range(1, ctx):
            dy_line.forward(k)

    line_sum.step(c)
    gain = gain_vec[1:2, :]
    values = x_ref[...].astype(jnp.float32) + line_sum.total[...]
    resid[...] = values
    scale = lax.rsqrt(jnp.mean(values * values, axis=-1, keepdims=True) + EPS)
    own_two[...] = (values * scale * gain).astype(jnp.bfloat16)
    line = LineGather(ctx, own_two, normed_two, two_send, two_recv, two_local)
    line.start()
    line.forward(1)
    line_sum.finish()
    x_line.finish_sends()
    for part in range(parts):
        for slot in range(4):
            arrived(gate_up.at[slot, part * part_rows : (part + 1) * part_rows], gu_recv.at[part, slot], here)
    for slot in range(fs):
        arrived(down.at[slot], d_recv.at[slot], here)
    pltpu.make_async_copy(dy_line.own, dy_line.slot(c), dy_line.local).wait()
    for part in range(parts):
        src = gate_up_ref.at[part * part_rows : (part + 1) * part_rows]
        for to in range(fs):

            @pl.when(jnp.logical_not(jnp.logical_and(gu_core == d, f == to)))
            def _():
                left(src, gu_send.at[part, to], here)

    for at in range(ctx):

        for to in range(fs):

            @pl.when(to != f)
            def _():
                left(stage.at[at, to], q_send.at[at, to], here)
                left(att_stage.at[at, to], a_send.at[at, to], here)

    @pl.when(jnp.logical_and(d == 1, kv_away))
    def _():
        left(w_ref, w_send.at[0], here)

    @pl.when(d == 0)
    def _():
        for to in range(fs):

            @pl.when(jnp.logical_or(q_core != 0, to != f))
            def _():
                left(w_ref, w_send.at[to], here)

    for slot in (2, 3):

        @pl.when(relay_of[slot])
        def _():
            for step in range(1, fs):
                left(head_rows(slot), w_pass.at[slot - 2, step], here)

    def gain_left(step, carry):
        other = lax.rem(me + step, n)
        left(gains_ref, g_send.at[other], here)
        return carry

    lax.fori_loop(1, n, gain_left, 0)
    for copy in (normed_copy, wide_copy, gains_copy, qkv_copy):
        copy.wait()
    for step in range(1, fs):
        left(down_mid, d_pass.at[step], here)
        left(proj_rows(f), m_pass.at[step], here)

    @pl.when(jnp.logical_not(stays))
    def _():
        left(proj_ref, m_send, here)
        left(down_ref, down_send, here)

    dy_line.finish_sends()
    pltpu.make_async_copy(line.own, line.slot(c), line.local).wait()

    def mlp(step, carry):
        at = ordered(c, step, ctx)


        @pl.when(lax.rem(step, 2) == 1)
        def _():
            line.forward(2 + step // 2)

        line.other(at)
        dy_line.other(at)
        inputs = normed_two[:, at].reshape(both_rows, D)
        dy_rows = dy_all[:, at].reshape(both_rows, D)
        for part in range(2):
            cols = slice(part * half, (part + 1) * half)
            gate = jnp.dot(inputs, gate_up[part], preferred_element_type=jnp.float32)
            up = jnp.dot(inputs, gate_up[2 + part], preferred_element_type=jnp.float32)
            d_act = outer(dy_rows, down[2 * part : 2 * part + 2].reshape(half, D))
            sig = 1.0 / (1.0 + jnp.exp(-gate))
            silu = gate * sig
            act[:, at, :, cols] = (silu * up).astype(jnp.bfloat16).reshape(dp, rows, half)
            d_gate = d_act * up * (sig * (1.0 + gate * (1.0 - sig)))
            d_both[:, at, :, cols] = d_gate.astype(jnp.bfloat16).reshape(dp, rows, half)
            d_both[:, at, :, hidden + part * half : hidden + (part + 1) * half] = (
                (d_act * silu).astype(jnp.bfloat16).reshape(dp, rows, half)
            )
        terms = outer(d_both[:, at, :, 0:half].reshape(both_rows, half), gate_up[0])
        for part in range(1, 4):
            terms += outer(d_both[:, at, :, part * half : (part + 1) * half].reshape(both_rows, half), gate_up[part])
        second_sum.give(at, terms.reshape(dp, rows, D))
        return carry

    lax.fori_loop(0, ctx, mlp, 0)

    wide_rows = D // ctx

    def push(src, dst, send, recv, core, to):
        to_self = jnp.logical_and(core == d, to == f)

        @pl.when(jnp.logical_not(to_self))
        def _():
            remote(src, dst, send, recv, at_device(core, c, to)).start()

        @pl.when(to_self)
        def _():
            pltpu.make_async_copy(src, dst, recv).start()

    def grads(step):
        first = pl.multiple_of(step * wide_rows, LANES)
        left_rows = normed_two[:, :, :, pl.ds(first, wide_rows)].reshape(dp * ctx * rows, wide_rows)
        for part in range(2):
            cols = slice(part * hidden, (part + 1) * hidden)
            terms = inner(left_rows, d_both[:, :, :, cols].reshape(dp * ctx * rows, hidden)).astype(jnp.bfloat16)
            grad_up[2 * part, pl.ds(first, wide_rows), :] = terms[:, :half]
            grad_up[2 * part + 1, pl.ds(first, wide_rows), :] = terms[:, half:]
        dy_cols = dy_all[:, :, :, pl.ds(first, wide_rows)].reshape(dp * ctx * rows, wide_rows)
        terms = inner(act[...].reshape(dp * ctx * rows, hidden), dy_cols).astype(jnp.bfloat16)
        grad_down[:, :, pl.ds(first, wide_rows)] = terms.reshape(fs, hidden // fs, wide_rows)
        for slot in range(4):
            push(
                grad_up.at[slot, pl.ds(first, wide_rows)], up_land.at[f, pl.ds(first, wide_rows)],
                gup_send.at[slot, step], gup_recv.at[f, step], slot // 2, 2 * d + slot % 2,
            )
            push(
                grad_down.at[slot, :, pl.ds(first, wide_rows)], down_land.at[f, :, pl.ds(first, wide_rows)],
                gdn_send.at[slot, step], gdn_recv.at[f, step], d, slot,
            )

    def out_terms(step):
        at = towards(c, step, ctx)
        terms = jnp.dot(act[:, at].reshape(both_rows, hidden), down[...].reshape(hidden, D), preferred_element_type=jnp.float32)
        out_sum.give(at, terms.reshape(dp, rows, D))

    def second_steps():
        def body(step, carry):
            second_sum.step(towards(c, step, ctx))
            return carry

        lax.fori_loop(0, ctx - 1, body, 0)

    def local_terms(step, carry):
        grads(step)
        out_terms(step)
        return carry

    pl.when(ends)(second_steps)
    lax.fori_loop(0, ctx - 1, local_terms, 0)
    pl.when(jnp.logical_not(ends))(second_steps)
    local_terms(ctx - 1, 0)
    second_sum.step(c)
    values = resid[...]
    scale = lax.rsqrt(jnp.mean(values * values, axis=-1, keepdims=True) + EPS)
    incoming = second_sum.total[...]
    weighted = incoming * gain
    mean = jnp.mean(weighted * values, axis=-1, keepdims=True)
    d_resid = dy_ref[...].astype(jnp.float32) + scale * weighted - values * (scale * scale * scale) * mean
    own_d[...] = d_resid.astype(jnp.bfloat16)
    d_resid_held[...] = d_resid
    d_resid_copy = pltpu.make_async_copy(d_resid_held, d_resid_out, out_sem.at[6])
    d_resid_copy.start()
    gain_out[...] = jnp.broadcast_to(jnp.sum(incoming * values * scale, axis=0, keepdims=True), gain_out.shape)
    d_line = LineGather(ctx, own_d, d_resid_all, dr_send, dr_recv, dr_local)
    d_line.start()
    def out_step(step, carry):
        out_sum.step(towards(c, step, ctx))
        return carry

    @pl.when(ends)
    def _():
        lax.fori_loop(0, ctx - 1, out_step, 0)

    line.finish_sends()
    second_sum.finish()
    pltpu.make_async_copy(d_line.own, d_line.slot(c), d_line.local).wait()
    grad_proj[...] = jnp.zeros_like(grad_proj)

    def back(step, carry):
        at = ordered(c, step, ctx)

        d_line.reach(step)
        d_line.other(at)
        incoming = d_resid_all[:, at].reshape(both_rows, D)
        d_att = outer(incoming, proj[...]).astype(jnp.bfloat16)
        d_stage[at] = d_att.reshape(2 * dp, span, 2 * LANES)
        for to in range(2 * dp):

            @pl.when(to != f)
            def _():
                remote(d_stage.at[at, to], unit.at[at, f], u_send.at[at, to], u_recv.at[at, f], at_device(d, c, to)).start()

            @pl.when(to == f)
            def _():
                unit[at, f] = d_stage[at, to]

        grad_proj[...] += inner(att[:, at].reshape(both_rows, 2 * LANES), incoming)

        @pl.when(jnp.logical_and(jnp.logical_not(ends), step == ctx - 2))
        def _():
            out_sum.step(towards(c, 0, ctx))

        return carry

    lax.fori_loop(0, ctx, back, 0)

    @pl.when(jnp.logical_not(ends))
    def _():
        lax.fori_loop(1, ctx - 1, out_step, 0)

    for slot in range(fs):
        start = slot // 2 * LANES + slot % 2 * each_proj
        grad_proj_low[slot] = grad_proj[start : start + each_proj, :].astype(jnp.bfloat16)
    grad_proj_copy = pltpu.make_async_copy(grad_proj_low, grad_proj_out, out_sem.at[1])
    grad_proj_copy.start()
    for at in range(ctx):
        for step in range(1, fs):
            other = lax.rem(f + step, fs)
            arrived(unit.at[at, other], u_recv.at[at, other], here)
    unit_copy = pltpu.make_async_copy(unit, unit_out, out_sem.at[2])
    unit_copy.start()
    d_line.finish_sends()
    for at in range(ctx):
        for to in range(fs):

            @pl.when(to != f)
            def _():
                left(d_stage.at[at, to], u_send.at[at, to], here)

    def settle_up(step, carry):
        first = pl.multiple_of(step * wide_rows, LANES)
        for slot in range(4):
            arrived(up_land.at[slot, pl.ds(first, wide_rows)], gup_recv.at[slot, step], here)

            @pl.when(jnp.logical_or(slot // 2 != d, 2 * d + slot % 2 != f))
            def _():
                left(grad_up.at[slot, pl.ds(first, wide_rows)], gup_send.at[slot, step], here)

        return carry

    def settle_down(step, carry):
        first = pl.multiple_of(step * wide_rows, LANES)
        for slot in range(4):
            arrived(down_land.at[slot, :, pl.ds(first, wide_rows)], gdn_recv.at[slot, step], here)

            @pl.when(slot != f)
            def _():
                left(grad_down.at[slot, :, pl.ds(first, wide_rows)], gdn_send.at[slot, step], here)

        return carry

    lax.fori_loop(0, ctx, settle_up, 0)
    lax.fori_loop(0, ctx, settle_down, 0)
    out_step(ctx - 1, 0)
    out_ref[...] = (resid[...] + out_sum.total[...]).astype(jnp.bfloat16)
    out_sum.finish()
    for copy in (d_resid_copy, grad_proj_copy, unit_copy):
        copy.wait()

def front(sizes, parts, x, attn_gain, mlp_gain, w_qkv, dy, w_out, w_down, w_gate_up):
    dp, ctx, fs = sizes
    n = dp * ctx * fs
    rows = x.shape[0]
    span = rows // 2
    hidden = FF // (dp * ctx)
    low, wide_t = jnp.bfloat16, jnp.float32
    dma = pltpu.SemaphoreType.DMA
    any_spec, vm_spec = pl.BlockSpec(memory_space=ANY), pl.BlockSpec(memory_space=VM)
    line_sems = [dma((3, ctx, HALVES)), dma((dp, ctx, HALVES)), dma]
    shapes = (
        jax.ShapeDtypeStruct((rows, D), low),
        jax.ShapeDtypeStruct((rows, D), wide_t),
        jax.ShapeDtypeStruct((8, D), wide_t),
        jax.ShapeDtypeStruct((2, ctx * fs, LANES), wide_t),
        jax.ShapeDtypeStruct((2, span, LANES), wide_t),
        jax.ShapeDtypeStruct((dp, ctx, rows, D), low),
        jax.ShapeDtypeStruct((ctx, fs, span, 4 * LANES), low),
        jax.ShapeDtypeStruct((4 * LANES, D), low),
        jax.ShapeDtypeStruct((8, D), wide_t),
        jax.ShapeDtypeStruct((ctx, fs, span, 2 * LANES), low),
        jax.ShapeDtypeStruct((fs,) + w_out.shape, low),
        jax.ShapeDtypeStruct((fs, D, hidden // 2), low),
        jax.ShapeDtypeStruct((fs, hidden // fs, D), low),
    )
    return pl.pallas_call(
        functools.partial(front_kernel, sizes, hidden, parts),
        name="front",
        out_shape=shapes,
        in_specs=[vm_spec] * 3 + [any_spec] + [vm_spec] * 4,
        out_specs=[vm_spec, any_spec] + [vm_spec] * 3 + [any_spec] * 8,
        scratch_shapes=[
            VM((dp, ctx, rows, D), low),
            VM((4 * LANES, D), low),
            VM((dp, ctx, rows, D), low),
            VM((ctx, 2 * dp, span, 4 * LANES), low),
            VM((ctx, fs, span, 4 * LANES), low),
            VM((ctx, fs, span, 2 * LANES), low),
            VM((dp, ctx, 2, span, 2 * LANES), low),
            VM((n, 8, LANES), wide_t),
            VM((8, D), wide_t),
            VM((dp, ctx, rows, D), low),
            VM((2 * LANES, D), low),
            VM(w_down.shape, low),
            VM((fs, hidden // fs, D), low),
            VM((4, D, hidden // 2), low),
            VM((rows, D), wide_t),
            VM((rows, D), low),
            VM((dp, ctx, rows, D), low),
            VM((dp, ctx, rows, hidden), low),
            VM((dp, ctx, rows, 2 * hidden), low),
            VM((rows, D), low),
            VM((ctx, 2 * dp, span, 2 * LANES), low),
            VM((ctx, fs, span, 2 * LANES), low),
            VM((4, D, hidden // 2), low),
            VM((fs, hidden // fs, D), low),
            VM((2 * LANES, D), wide_t),
            VM((fs,) + w_out.shape, low),
            VM((8, LANES), wide_t),
            VM((rows, D), wide_t),
            *line_sems,
            dma((fs,)), dma((4,)), dma((2, fs)), dma((n,)), dma((n,)),
            dma((ctx, 2 * dp)), dma((ctx, fs)), dma((ctx, fs)), dma((fs, ctx)), dma((7,)),
            *line_sems,
            dma, dma((fs,)), dma((fs,)), dma, dma, dma((fs,)), dma((fs,)), dma((parts, fs)), dma((parts, 4)),
            *line_sems,
            *line_sems,
            dma((ctx, 2 * dp)), dma((ctx, fs)),
            dma((4, ctx)), dma((fs, ctx)), dma((fs, ctx)), dma((fs, ctx)),
        ] + LineSum.scratch(ctx, rows) * 2,
        compiler_params=pltpu.CompilerParams(collective_id=1, has_side_effects=True, vmem_limit_bytes=67043328),
    )(x, attn_gain, mlp_gain, w_qkv, dy, w_out, w_down, w_gate_up)


def fill_tables(block_ref, step_ref):
    span = step_ref.shape[1]
    for ref, scale in ((block_ref, span), (step_ref, 1)):
        shape = ref.shape[1:]
        lane = lax.broadcasted_iota(jnp.int32, shape, 1)
        pair = jnp.where(lane >= HD // 2, lane - HD // 2, lane).astype(jnp.float32)
        frequency = jnp.exp(pair * (-2.0 * math.log(THETA) / HD))
        angles = (lax.broadcasted_iota(jnp.int32, shape, 0) * scale).astype(jnp.float32) * frequency
        ref[0] = jnp.cos(angles)
        ref[1] = jnp.sin(angles)


def turns(block_ref, step_ref, block):
    cos_b, sin_b = block_ref[0, pl.ds(block, 1)], block_ref[1, pl.ds(block, 1)]
    cos_s, sin_s = step_ref[0], step_ref[1]
    cosine = cos_b * cos_s - sin_b * sin_s
    sine = sin_b * cos_s + cos_b * sin_s
    lane = lax.broadcasted_iota(jnp.int32, sine.shape, 1)
    first_half = lane < HD // 2
    sine_up = jnp.where(jnp.logical_and(lane >= HD // 2, lane < HD), sine, 0.0)
    return cosine, sine_up, jnp.where(first_half, -sine, 0.0)


def last_kernel(
    sizes, x_ref, gains_ref, block_ref, step_ref, gain_two_ref, proj_ref,
    d_resid_in, unit_ref, d_unit_ref, normed_ref, wide_ref, up_land_ref, down_land_ref,
    d_x_ref, gains_out, qkv_out, proj_out, up_out, down_out,
    unit, d_unit, d_k, d_v, stage, mixed, packed, normed, wide, grad_heads,
    up_land, down_land, proj_land, q_land, kv_land, down_sum, proj_sum, kv_sum, down_last, proj_last, kv_last, gain_vec, gain_stage, gain_land, up_sum, d_resid_ref,
    in_sem, proj_send, proj_recv, head_send, head_recv, move_send, move_recv,
    u_send, u_recv, g_send, g_recv, up_sem, wide_sem,
    *sums,
):
    dp, ctx, fs = sizes
    n = dp * ctx * fs
    d, c, f = place()
    here = at_device(d, c, f)
    me = (d * ctx + c) * fs + f
    rows = x_ref.shape[0]
    span = rows // 2
    both_rows = dp * rows
    low, wide_t = jnp.bfloat16, jnp.float32
    loads = [
        pltpu.make_async_copy(src, dst, in_sem.at[index])
        for index, (src, dst) in enumerate((
            (unit_ref, unit), (d_unit_ref, d_unit), (normed_ref, normed), (d_resid_in, d_resid_ref), (down_land_ref, down_land), (up_land_ref, up_land),
        ))
    ]
    wide_loads = [
        pltpu.make_async_copy(
            wide_ref.at[slot * LANES : slot * LANES + HD], wide.at[slot * HD : (slot + 1) * HD], wide_sem.at[slot]
        )
        for slot in range(4)
    ]
    tell_all(sizes)
    for load in loads + wide_loads:
        load.start()
    in_sum = LineSum(ctx, *sums[:6], sums[6:10])
    d_k[...] = jnp.zeros_like(d_k)
    d_v[...] = jnp.zeros_like(d_v)

    def push(src, land, send, recv, core, fs_to):
        to_self = jnp.logical_and(core == d, fs_to == f)

        @pl.when(jnp.logical_not(to_self))
        def _():
            remote(src, land.at[f], send, recv.at[f], at_device(core, c, fs_to)).start()

        @pl.when(to_self)
        def _():
            pltpu.make_async_copy(src, land.at[f], recv.at[f]).start()

    def pushed(src, send, core, fs_to):
        @pl.when(jnp.logical_not(jnp.logical_and(core == d, fs_to == f)))
        def _():
            left(src, send, here)

    def sum_of(land):
        total = land[0].astype(wide_t)
        for source in range(1, fs):
            total += land[source].astype(wide_t)
        return total

    _, (own_core, own_ctx) = down_route(d, c)
    stays = jnp.logical_and(own_core == d, own_ctx == c)

    def move(index, src, dst):
        @pl.when(jnp.logical_not(stays))
        def _():
            remote(src, dst, move_send.at[index], move_recv.at[index], at_device(own_core, own_ctx, f)).start()

        @pl.when(stays)
        def _():
            pltpu.make_async_copy(src, dst, move_recv.at[index]).start()

    loads[0].wait()
    loads[1].wait()
    block = fs * span

    def unturn(values, at):
        up = pltpu.roll(values, HD // 2, 1)
        down = pltpu.roll(values, LANES - HD // 2, 1)
        pieces = []
        for index in range(fs):
            own = slice(index * span, (index + 1) * span)
            cosine, sine_up, sine_down = turns(block_ref, step_ref, at * fs + index)
            pieces.append(values[own] * cosine - up[own] * sine_up - down[own] * sine_down)
        return jnp.concatenate(pieces, axis=0)

    for at in reversed(range(ctx)):
        keys = block * (at + 1)
        k_rows = unit[0 : at + 1, :, :, 2 * LANES : 3 * LANES].reshape(keys, LANES)
        v_rows = unit[0 : at + 1, :, :, 3 * LANES : 4 * LANES].reshape(keys, LANES)
        allowed = lax.broadcasted_iota(jnp.int32, (block, keys), 1) <= block * at + lax.broadcasted_iota(
            jnp.int32, (block, keys), 0
        )
        for head in range(2):
            lanes = slice(head * LANES, (head + 1) * LANES)
            q_rows = unit[at, :, :, lanes].reshape(block, LANES)
            d_rows = d_unit[at, :, :, lanes].reshape(block, LANES)
            scores = jnp.where(allowed, outer(q_rows, k_rows) * FACTOR, NEG)
            weights = jnp.exp(scores - jnp.max(scores, axis=-1, keepdims=True))
            probs = weights / jnp.sum(weights, axis=-1, keepdims=True)
            d_probs = outer(d_rows, v_rows)
            delta = jnp.sum(probs * d_probs, axis=-1, keepdims=True)
            d_scores = (probs * (d_probs - delta)).astype(low)
            d_q = jnp.dot(d_scores, k_rows, preferred_element_type=wide_t) * FACTOR
            packed[:, head * HD : (head + 1) * HD] = unturn(d_q, at)[:, :HD]
            d_k[0:keys, :] += inner(d_scores, q_rows) * FACTOR
            d_v[0:keys, :] += inner(probs.astype(low), d_rows)
        packed[:, 2 * HD : 3 * HD] = unturn(d_k[block * at : keys, :], at)[:, :HD]
        packed[:, 3 * HD : 4 * HD] = d_v[block * at : keys, :HD]
        stage[at] = packed[...].astype(low).reshape(fs, span, 4 * HD)
        if at == ctx - 1:
            hear_all(sizes)
        for to in range(fs):

            @pl.when(to != f)
            def _():
                remote(
                    stage.at[at, to], mixed.at[f // 2, at, lax.rem(f, 2)], u_send.at[at, to], u_recv.at[f, at], at_device(d, c, to)
                ).start()

            @pl.when(to == f)
            def _():
                mixed[f // 2, at, lax.rem(f, 2)] = stage[at, to]

        if at == ctx - 1:
            loads[4].wait()
            down_sum[...] = sum_of(down_land).astype(low)
            move(0, down_sum, down_last)
    loads[2].wait()
    for load in wide_loads:
        load.wait()

    ends = jnp.logical_or(c == 0, c == ctx - 1)

    def give(step, carry):
        at = towards(c, step, ctx)
        for move_ in range(1, fs):
            other = lax.rem(f + move_, fs)
            arrived(mixed.at[other // 2, at, lax.rem(other, 2)], u_recv.at[other, at], here)
        terms = jnp.dot(mixed[:, at].reshape(both_rows, 4 * HD), wide[...], preferred_element_type=wide_t)
        in_sum.give(at, terms.reshape(dp, rows, D))

        @pl.when(jnp.logical_and(ends, jnp.logical_and(step > 0, step < ctx - 1)))
        def _():
            in_sum.step(towards(c, step - 1, ctx))

        return carry

    lax.fori_loop(0, ctx, give, 0)

    every = dp * ctx * rows
    k_relay = 2 * lax.rem(c, 2) + d
    relays = (k_relay, lax.rem(k_relay + 2, fs))
    gain_terms = jnp.zeros((1, D), wide_t)
    for slot in (2, 3, 0, 1):
        if slot % 2 == 0:
            both_heads = inner(
                mixed[...].reshape(every, 4 * HD)[:, slot * HD : (slot + 2) * HD], normed[...].reshape(every, D)
            )
        heads = both_heads[slot % 2 * HD : (slot % 2 + 1) * HD]
        grad_heads[slot] = heads.astype(low)
        weights = wide[slot * HD : (slot + 1) * HD, :].astype(wide_t)
        gain_terms += jnp.sum(heads * weights, axis=0, keepdims=True)
        if slot < 2:
            push(grad_heads.at[slot], q_land, head_send.at[slot], head_recv.at[0], 0, 2 * d + slot)
        else:
            push(grad_heads.at[slot], kv_land.at[slot - 2], head_send.at[slot], head_recv.at[slot - 1], d, relays[slot - 2])

    for slot in range(fs):
        push(proj_ref.at[slot], proj_land, proj_send.at[slot], proj_recv, d, slot)

    gain = gains_ref[0:1, :]
    gain_vec[0:1, :] = gain_terms / gain
    gain_vec[1:2, :] = gain_two_ref[0:1, :]
    each = D // n
    for index in range(n):
        gain_stage[index, :, 0:each] = gain_vec[:, index * each : (index + 1) * each]
    gain_land[me] = gain_stage[me]

    def gain_to(step, carry):
        other = lax.rem(me + step, n)
        remote(
            gain_stage.at[other], gain_land.at[me], g_send.at[other], g_recv.at[me],
            at_device(other // (ctx * fs), lax.rem(other // fs, ctx), lax.rem(other, fs)),
        ).start()
        return carry

    lax.fori_loop(1, n, gain_to, 0)

    def middle_step(step, carry):
        in_sum.step(towards(c, step, ctx))
        return carry

    lax.fori_loop(jnp.where(ends, ctx - 2, 0), ctx - 1, middle_step, 0)

    def kv_route(slot):
        owner, owner_f = slot * 2 + c // 2, k_relay
        return owner, owner_f, jnp.logical_or(jnp.logical_or(d != 1, owner != c), owner_f != f)

    for slot in range(2):
        owner, owner_f, away = kv_route(slot)

        @pl.when(f == relays[slot])
        def _():
            for source in range(fs):
                arrived(kv_land.at[slot, source], head_recv.at[1 + slot, source], here)
            kv_sum[slot] = sum_of(kv_land.at[slot]).astype(low)

            @pl.when(away)
            def _():
                remote(kv_sum.at[slot], kv_last, move_send.at[2 + slot], move_recv.at[2], at_device(1, owner, owner_f)).start()

            @pl.when(jnp.logical_not(away))
            def _():
                pltpu.make_async_copy(kv_sum.at[slot], kv_last, move_recv.at[2]).start()

    for source in range(fs):
        arrived(proj_land.at[source], proj_recv.at[source], here)
    proj_sum[...] = sum_of(proj_land).astype(low)
    move(1, proj_sum, proj_last)

    loads[5].wait()
    up_sum[...] = sum_of(up_land)
    up_copy = pltpu.make_async_copy(up_sum, up_out, up_sem)
    up_copy.start()
    @pl.when(d == 0)
    def _():
        for source in range(fs):
            arrived(q_land.at[source], head_recv.at[0, source], here)
        qkv_out[...] = sum_of(q_land)

    for slot in range(fs):
        pushed(proj_ref.at[slot], proj_send.at[slot], d, slot)
    for slot in range(2):
        pushed(grad_heads.at[slot], head_send.at[slot], 0, 2 * d + slot)
        pushed(grad_heads.at[2 + slot], head_send.at[2 + slot], d, relays[slot])

    for at in range(ctx):
        for to in range(fs):

            @pl.when(to != f)
            def _():
                left(stage.at[at, to], u_send.at[at, to], here)

    def gain_from(step, carry):
        other = lax.rem(me + step, n)
        arrived(gain_land.at[other], g_recv.at[other], here)
        return carry

    lax.fori_loop(1, n, gain_from, 0)
    total = gain_land[0]
    for index in range(1, n):
        total += gain_land[index]
    gains_out[...] = total

    def gain_left(step, carry):
        other = lax.rem(me + step, n)
        left(gain_stage.at[other], g_send.at[other], here)
        return carry

    lax.fori_loop(1, n, gain_left, 0)

    loads[3].wait()
    in_sum.step(c)

    values = x_ref[...].astype(wide_t)
    scale = lax.rsqrt(jnp.mean(values * values, axis=-1, keepdims=True) + EPS)
    incoming = in_sum.total[...]
    weighted = incoming * gain
    mean = jnp.mean(weighted * values, axis=-1, keepdims=True)
    d_x_ref[...] = (d_resid_ref[...] + scale * weighted - values * (scale * scale * scale) * mean).astype(low)

    for index, dst in enumerate((down_last, proj_last)):
        arrived(dst, move_recv.at[index], here)
    down_out[...] = down_last[...].astype(wide_t)
    proj_out[...] = proj_last[...].astype(wide_t)

    @pl.when(d == 1)
    def _():
        arrived(kv_last, move_recv.at[2], here)
        qkv_out[...] = kv_last[...].astype(wide_t)

    for slot in range(2):
        away = kv_route(slot)[2]

        @pl.when(jnp.logical_and(f == relays[slot], away))
        def _():
            left(kv_sum.at[slot], move_send.at[2 + slot], here)

        @pl.when(jnp.logical_not(stays))
        def _():
            left((down_sum, proj_sum)[slot], move_send.at[slot], here)

    in_sum.finish()
    up_copy.wait()


def last(sizes, x, gains, tables, d_resid, gain_two, grad_proj, unit, d_unit, normed, wide, up_land, down_land):
    dp, ctx, fs = sizes
    n = dp * ctx * fs
    rows = x.shape[0]
    span = rows // 2
    low, wide_t = jnp.bfloat16, jnp.float32
    dma = pltpu.SemaphoreType.DMA
    any_spec, vm_spec = pl.BlockSpec(memory_space=ANY), pl.BlockSpec(memory_space=VM)
    down_rows, proj_rows, half = down_land.shape[1], grad_proj.shape[1], up_land.shape[2]
    shapes = (
        jax.ShapeDtypeStruct((rows, D), low),
        jax.ShapeDtypeStruct((8, LANES), wide_t),
        jax.ShapeDtypeStruct((HD, D), wide_t),
        jax.ShapeDtypeStruct((proj_rows, D), wide_t),
        jax.ShapeDtypeStruct((D, half), wide_t),
        jax.ShapeDtypeStruct((down_rows, D), wide_t),
    )
    return pl.pallas_call(
        functools.partial(last_kernel, sizes),
        name="last",
        out_shape=shapes,
        in_specs=[vm_spec] * 6 + [any_spec] * 7,
        out_specs=[vm_spec] * 4 + [any_spec, vm_spec],
        scratch_shapes=[
            VM(unit.shape, low),
            VM(d_unit.shape, low),
            VM((ctx * fs * span, LANES), wide_t),
            VM((ctx * fs * span, LANES), wide_t),
            VM((ctx, fs, span, 4 * HD), low),
            VM((dp, ctx, 2, span, 4 * HD), low),
            VM((fs * span, 4 * HD), wide_t),
            VM(normed.shape, low),
            VM((4 * HD, D), low),
            VM((4, HD, D), low),
            VM(up_land.shape, low),
            VM((fs, down_rows, D), low),
            VM((fs, proj_rows, D), low),
            VM((fs, HD, D), low),
            VM((2, fs, HD, D), low),
            VM((down_rows, D), low),
            VM((proj_rows, D), low),
            VM((2, HD, D), low),
            VM((down_rows, D), low),
            VM((proj_rows, D), low),
            VM((HD, D), low),
            VM((8, D), wide_t),
            VM((n, 8, LANES), wide_t),
            VM((n, 8, LANES), wide_t),
            VM((D, half), wide_t),
            VM((rows, D), wide_t),
            dma((6,)), dma((fs,)), dma((fs,)),
            dma((4,)), dma((3, fs)), dma((4,)), dma((3,)),
            dma((ctx, fs)), dma((fs, ctx)), dma((n,)), dma((n,)), dma, dma((4,)),
        ] + LineSum.scratch(ctx, rows),
        compiler_params=pltpu.CompilerParams(collective_id=3, has_side_effects=True, vmem_limit_bytes=63 * 1024 * 1024),
    )(x, gains, *tables, gain_two, grad_proj, d_resid, unit, d_unit, normed, wide, up_land, down_land)


def emit_kernel(count, gains_ref, *refs):
    sources, outs, one_ref, two_ref = refs[:count], refs[count : 2 * count], refs[2 * count], refs[2 * count + 1]
    held, in_sem, out_sem = refs[2 * count + 2 : 3 * count + 2], refs[-2], refs[-1]
    loads = [pltpu.make_async_copy(sources[i], held[i], in_sem.at[i]) for i in range(count)]
    stores = [pltpu.make_async_copy(held[i], outs[i], out_sem.at[i]) for i in range(count)]
    for load in loads:
        load.start()
    each = one_ref.shape[0]
    one_ref[...] = gains_ref[0, :each]
    two_ref[...] = gains_ref[1, :each]
    for load, store in zip(loads, stores):
        load.wait()
        store.start()
    for store in stores:
        store.wait()


def emit(each, gains, *arrays):
    count = len(arrays)
    any_spec, vm_spec = pl.BlockSpec(memory_space=ANY), pl.BlockSpec(memory_space=VM)
    gain = jax.ShapeDtypeStruct((each,), jnp.float32)
    return pl.pallas_call(
        functools.partial(emit_kernel, count),
        name="emit",
        out_shape=[jax.ShapeDtypeStruct(a.shape, a.dtype) for a in arrays] + [gain, gain],
        in_specs=[vm_spec] + [any_spec] * count,
        out_specs=[any_spec] * count + [vm_spec] * 2,
        scratch_shapes=[VM(a.shape, a.dtype) for a in arrays] + [pltpu.SemaphoreType.DMA((count,))] * 2,
        compiler_params=pltpu.CompilerParams(vmem_limit_bytes=63 * 1024 * 1024),
    )(gains, *arrays)


def on_device(tokens, cotangent, attn_gain, w_qkv, w_out, mlp_gain, w_gate_up, w_down):
    dp, ctx, fs = where = tuple(lax.axis_size(name) for name in ("dp", "ctx", "fsdp"))
    mb, _, span, _ = tokens.shape
    rows = mb * span
    x = tokens.reshape(rows, D)
    dy = cotangent.reshape(rows, D)
    each = attn_gain.shape[0]
    block_out, d_resid, grad_two, *tables, normed, unit, qkv, gains, d_unit, grad_proj, up_land, down_land = front(
        where, 8, x, attn_gain, mlp_gain, w_qkv.T, dy, w_out, w_down, w_gate_up
    )
    grad_tokens, gain_grads, grad_qkv, grad_out, grad_gate_up, grad_down = last(
        where, x, gains, tables, d_resid, grad_two, grad_proj, unit, d_unit, normed, qkv, up_land, down_land
    )
    block_out, grad_tokens, grad_qkv, grad_out, grad_gate_up, grad_down, grad_one, grad_two = emit(
        each, gain_grads, block_out, grad_tokens, grad_qkv, grad_out, grad_gate_up, grad_down
    )
    return (
        block_out.reshape(tokens.shape),
        grad_tokens.reshape(tokens.shape),
        grad_one,
        grad_qkv.T,
        grad_out,
        grad_two,
        grad_gate_up,
        grad_down,
    )


def fits(mesh):
    return mesh.shape["dp"] == 2 and mesh.shape["ctx"] == 4 and mesh.shape["fsdp"] == 4


def solution(mesh):
    placed = (
        P(None, "dp", ("ctx", "fsdp"), None),
        P(None, "dp", ("ctx", "fsdp"), None),
        P(("dp", "ctx", "fsdp")),
        P(None, ("dp", "ctx", "fsdp")),
        P(("dp", "ctx", "fsdp"), None),
        P(("dp", "ctx", "fsdp")),
        P(None, ("dp", "ctx", "fsdp")),
        P(("dp", "ctx", "fsdp"), None),
    )
    return jax.shard_map(
        on_device if fits(mesh) else on_device_gathered,
        mesh=mesh,
        in_specs=placed,
        out_specs=(
            P(None, "dp", ("ctx", "fsdp"), None),
            P(None, "dp", ("ctx", "fsdp"), None),
            P(("dp", "ctx", "fsdp")),
            P(None, ("dp", "ctx", "fsdp")),
            P(("dp", "ctx", "fsdp"), None),
            P(("dp", "ctx", "fsdp")),
            P(None, ("dp", "ctx", "fsdp")),
            P(("dp", "ctx", "fsdp"), None),
        ),
        check_vma=False,
    )
```

```python
import functools
import math

import jax
import jax.numpy as jnp
from jax import lax
from jax.experimental import pallas as pl
from jax.experimental.pallas import tpu as pltpu
from jax.sharding import PartitionSpec as P

D = 1536
H = 16
KVH = 8
HD = 96
FF = 4096


EPS = 1e-05
THETA = 100000.0
NEG = -1e30


def in_blocks(value, dim, length):
    lengths = value.shape
    pieces = value.reshape(*lengths[:dim], length, lengths[dim] // length, *lengths[dim + 1 :])
    return jnp.moveaxis(pieces, dim, 0)


def sum_at_owner(value, axis, dim):
    pieces = in_blocks(value, dim, lax.axis_size(axis))
    arrived = lax.all_to_all(pieces, axis, split_axis=0, concat_axis=0, tiled=True)
    return arrived.astype(jnp.float32).sum(axis=0)


def side_by_side(arrays, axis, dim, along):
    both = jnp.concatenate(arrays, axis=along)
    whole, at, finished = (sum_at_owner(both, axis, dim), 0, [])
    for a in arrays:
        finished.append(lax.slice_in_dim(whole, at, at + a.shape[along], axis=along))
        at += a.shape[along]
    return tuple(finished)


def rms_norm(values, gain_vec):
    return values * lax.rsqrt(jnp.mean(values * values, axis=-1, keepdims=True) + EPS) * gain_vec


def tables(start, length, width):
    half_width = width // 2
    frequency = THETA ** (-(jnp.arange(half_width, dtype=jnp.float32) * 2.0) / width)
    angles = (start + jnp.arange(length, dtype=jnp.int32)).astype(jnp.float32)[:, None] * frequency[
        None, :
    ]
    return (jnp.cos(angles), jnp.sin(angles))


def rotate(values, cosine, sine_table):
    half_width = values.shape[-1] // 2
    first_half = values[..., :half_width]
    second_half = values[..., half_width:]
    cos_b = cosine[:, None, :]
    sin_b = sine_table[:, None, :]
    return jnp.concatenate(
        [first_half * cos_b - second_half * sin_b, second_half * cos_b + first_half * sin_b],
        axis=-1,
    )


def swiglu(both):
    return jax.nn.silu(both[:, :FF]) * both[:, FF:]


def inner(left, right):
    return lax.dot_general(
        left, right, (((0,), (0,)), ((), ())), preferred_element_type=jnp.float32
    )


def outer(left, right):
    return lax.dot_general(
        left, right, (((1,), (1,)), ((), ())), preferred_element_type=jnp.float32
    )


def unchanged(state):
    return state


def on_device_gathered(tokens, cotangent, attn_gain, w_qkv, w_out, mlp_gain, w_gate_up, w_down):
    tok_count = tokens.shape[2]
    groups = H // KVH
    factor = HD ** (-0.5)
    seq_length = tok_count * lax.axis_size(("ctx", "fsdp"))
    pos_first = lax.axis_index(("ctx", "fsdp")) * tok_count
    positions = pos_first + jnp.arange(tok_count, dtype=jnp.int32)
    pos_last = pos_first + tok_count - 1
    cosine, sine_table = tables(pos_first, tok_count, HD)
    sums = [
        jnp.zeros((D,), jnp.float32),
        jnp.zeros((D, (H + 2 * KVH) * HD), jnp.float32),
        jnp.zeros((H * HD, D), jnp.float32),
        jnp.zeros((D,), jnp.float32),
        jnp.zeros((D, 2 * FF), jnp.float32),
        jnp.zeros((FF, D), jnp.float32),
    ]
    outputs = []
    in_grads = []
    whole = (
        lax.all_gather(attn_gain, ("dp", "ctx", "fsdp"), axis=0, tiled=True),
        lax.all_gather(w_qkv, ("dp", "ctx", "fsdp"), axis=1, tiled=True),
        lax.all_gather(w_out, ("dp", "ctx", "fsdp"), axis=0, tiled=True),
        lax.all_gather(mlp_gain, ("dp", "ctx", "fsdp"), axis=0, tiled=True),
        lax.all_gather(w_gate_up, ("dp", "ctx", "fsdp"), axis=1, tiled=True),
        lax.all_gather(w_down, ("dp", "ctx", "fsdp"), axis=0, tiled=True),
    )
    for step_index in range(tokens.shape[0]):
        gain_one, mix_qkv, mix_out, gain_two, mix_gate_up, mix_down = whole
        inputs = tokens[step_index, 0].astype(jnp.float32)
        normed = rms_norm(inputs, gain_one.astype(jnp.float32)).astype(jnp.bfloat16)
        mixed = jnp.dot(normed, mix_qkv, preferred_element_type=jnp.float32)
        queries = rotate(mixed[:, : H * HD].reshape(tok_count, H, HD), cosine, sine_table).astype(
            jnp.bfloat16
        )
        key_rows = rotate(
            mixed[:, H * HD : (H + KVH) * HD].reshape(tok_count, KVH, HD), cosine, sine_table
        )
        key_rows = key_rows.astype(jnp.bfloat16).reshape(tok_count, KVH * HD)
        value_rows = mixed[:, (H + KVH) * HD :].astype(jnp.bfloat16)
        grouped = queries.reshape(tok_count, KVH, groups, HD)
        start_state = (
            jnp.full((KVH, groups, tok_count), NEG, jnp.float32),
            jnp.zeros((KVH, groups, tok_count), jnp.float32),
            jnp.zeros((KVH, groups, tok_count, HD), jnp.float32),
        )
        piece = (
            lax.all_gather(key_rows, ("ctx", "fsdp"), axis=0, tiled=True),
            lax.all_gather(value_rows, ("ctx", "fsdp"), axis=0, tiled=True),
        )

        def work(state):
            best, total, summed = state
            key_count = piece[0].shape[0]
            keys = piece[0].reshape(key_count, KVH, HD)
            values = piece[1].reshape(key_count, KVH, HD)
            scores = (
                jnp.einsum("qkgd,tkd->kgqt", grouped, keys, preferred_element_type=jnp.float32)
                * factor
            )
            allowed = jnp.arange(key_count, dtype=jnp.int32)[None, :] <= positions[:, None]
            scores = jnp.where(allowed, scores, NEG)
            new_best = jnp.maximum(best, jnp.max(scores, axis=-1))
            weights = jnp.where(allowed, jnp.exp(scores - new_best[..., None]), 0.0)
            total = jnp.sum(weights, axis=-1)
            summed = jnp.einsum(
                "kgqt,tkd->kgqd",
                weights.astype(jnp.bfloat16),
                values,
                preferred_element_type=jnp.float32,
            )
            return (new_best, total, summed)

        best, total, summed = lax.cond(jnp.int32(0) <= pos_last, work, unchanged, start_state)
        head_out = summed / total[..., None]
        log_total = best + jnp.log(total)
        attended = (
            jnp.transpose(head_out, (2, 0, 1, 3)).reshape(tok_count, H * HD).astype(jnp.bfloat16)
        )
        resid = inputs + jnp.dot(attended, mix_out, preferred_element_type=jnp.float32)
        normed_two = rms_norm(resid, gain_two.astype(jnp.float32)).astype(jnp.bfloat16)
        both = jnp.dot(normed_two, mix_gate_up, preferred_element_type=jnp.float32)
        acted = swiglu(both).astype(jnp.bfloat16)
        result = resid + jnp.dot(acted, mix_down, preferred_element_type=jnp.float32)
        outputs.append(result.astype(jnp.bfloat16))
        gain_one, mix_qkv, mix_out, gain_two, mix_gate_up, mix_down = whole
        up_low = cotangent[step_index, 0]
        upstream = up_low.astype(jnp.float32)
        sums[5] = sums[5] + inner(acted, up_low)
        d_act = outer(up_low, mix_down)
        _, pull_glu = jax.vjp(swiglu, both)
        d_both = pull_glu(d_act)[0].astype(jnp.bfloat16)
        sums[4] = sums[4] + inner(normed_two, d_both)
        d_normed_two = outer(d_both, mix_gate_up)
        _, pull_two = jax.vjp(rms_norm, resid, gain_two.astype(jnp.float32))
        d_resid_norm, d_gain_two = pull_two(d_normed_two)
        sums[3] = sums[3] + d_gain_two
        d_resid = upstream + d_resid_norm
        d_resid_low = d_resid.astype(jnp.bfloat16)
        sums[2] = sums[2] + inner(attended, d_resid_low)
        d_attended = outer(d_resid_low, mix_out).astype(jnp.bfloat16)
        d_grouped = d_attended.reshape(tok_count, KVH, groups, HD)
        delta = jnp.einsum("qkgd,kgqd->kgq", d_grouped.astype(jnp.float32), head_out)
        zero_q = jnp.zeros((tok_count, KVH, groups, HD), jnp.float32)
        back_state = (
            zero_q,
            jnp.zeros((seq_length, KVH * HD), jnp.float32),
            jnp.zeros((seq_length, KVH * HD), jnp.float32),
        )
        attend_piece = (
            lax.all_gather(key_rows, ("ctx", "fsdp"), axis=0, tiled=True),
            lax.all_gather(value_rows, ("ctx", "fsdp"), axis=0, tiled=True),
        )

        def attend_work(state):
            key_count = attend_piece[0].shape[0]
            keys = attend_piece[0].reshape(key_count, KVH, HD)
            values = attend_piece[1].reshape(key_count, KVH, HD)
            scores = (
                jnp.einsum("qkgd,tkd->kgqt", grouped, keys, preferred_element_type=jnp.float32)
                * factor
            )
            allowed = jnp.arange(key_count, dtype=jnp.int32)[None, :] <= positions[:, None]
            scores = jnp.where(allowed, scores, NEG)
            probs = jnp.where(allowed, jnp.exp(scores - log_total[..., None]), 0.0)
            d_probs = jnp.einsum(
                "qkgd,tkd->kgqt", d_grouped, values, preferred_element_type=jnp.float32
            )
            d_scores = (probs * (d_probs - delta[..., None])).astype(jnp.bfloat16)
            grad_q = jnp.einsum(
                "kgqt,tkd->qkgd", d_scores, keys, preferred_element_type=jnp.float32
            )
            piece_k = (
                jnp.einsum("kgqt,qkgd->tkd", d_scores, grouped, preferred_element_type=jnp.float32)
                * factor
            )
            piece_v = jnp.einsum(
                "kgqt,qkgd->tkd",
                probs.astype(jnp.bfloat16),
                d_grouped,
                preferred_element_type=jnp.float32,
            )
            grad_k = piece_k.reshape(key_count, KVH * HD)
            grad_v = piece_v.reshape(key_count, KVH * HD)
            return (grad_q, grad_k, grad_v)

        back_result = lax.cond(jnp.int32(0) <= pos_last, attend_work, unchanged, back_state)
        grad_q = back_result[0]
        summed_k, summed_v = side_by_side(
            (back_result[1].astype(jnp.bfloat16), back_result[2].astype(jnp.bfloat16)),
            ("ctx", "fsdp"),
            0,
            1,
        )
        d_q_raw = rotate(grad_q.reshape(tok_count, H, HD) * factor, cosine, -sine_table).reshape(
            tok_count, H * HD
        )
        d_k_raw = rotate(summed_k.reshape(tok_count, KVH, HD), cosine, -sine_table).reshape(
            tok_count, KVH * HD
        )
        d_mixed = jnp.concatenate([d_q_raw, d_k_raw, summed_v], axis=1).astype(jnp.bfloat16)
        sums[1] = sums[1] + inner(normed, d_mixed)
        d_normed = outer(d_mixed, mix_qkv)
        _, pull_one = jax.vjp(rms_norm, inputs, gain_one.astype(jnp.float32))
        d_inputs_norm, d_gain_one = pull_one(d_normed)
        sums[0] = sums[0] + d_gain_one
        in_grads.append((d_resid + d_inputs_norm).astype(jnp.bfloat16))
    grad_gain_one, grad_qkv, grad_out, grad_gain_two, grad_gate_up, grad_down = (
        lax.psum_scatter(sums[0], ("dp", "ctx", "fsdp"), scatter_dimension=0, tiled=True),
        lax.psum_scatter(sums[1], ("dp", "ctx", "fsdp"), scatter_dimension=1, tiled=True),
        lax.psum_scatter(sums[2], ("dp", "ctx", "fsdp"), scatter_dimension=0, tiled=True),
        lax.psum_scatter(sums[3], ("dp", "ctx", "fsdp"), scatter_dimension=0, tiled=True),
        lax.psum_scatter(sums[4], ("dp", "ctx", "fsdp"), scatter_dimension=1, tiled=True),
        lax.psum_scatter(sums[5], ("dp", "ctx", "fsdp"), scatter_dimension=0, tiled=True),
    )
    block_out = jnp.stack(outputs)[:, None]
    grad_tokens = jnp.stack(in_grads)[:, None]
    return (
        block_out,
        grad_tokens,
        grad_gain_one,
        grad_qkv,
        grad_out,
        grad_gain_two,
        grad_gate_up,
        grad_down,
    )


MESH = pl.DeviceIdType.MESH
VM = pltpu.VMEM
ANY = pl.ANY


def place():
    return lax.axis_index("dp"), lax.axis_index("ctx"), lax.axis_index("fsdp")


def at_device(dp, ctx, fs):
    return {"dp": dp, "ctx": ctx, "fsdp": fs}


def remote(src, dst, send, recv, device):
    return pltpu.make_async_remote_copy(
        src_ref=src, dst_ref=dst, send_sem=send, recv_sem=recv, device_id=device, device_id_type=MESH
    )


def arrived(dst, recv, device):
    remote(dst, dst, recv, recv, device).wait_recv()


def left(src, send, device):
    remote(src, src, send, send, device).wait_send()


def tell_all(sizes):
    dp, ctx, fs = sizes
    n = dp * ctx * fs
    d, c, f = place()
    me = (d * ctx + c) * fs + f
    barrier = pltpu.get_barrier_semaphore()

    def tell(step, carry):
        other = lax.rem(me + step, n)
        pl.semaphore_signal(
            barrier,
            inc=1,
            device_id=at_device(other // (ctx * fs), lax.rem(other // fs, ctx), lax.rem(other, fs)),
            device_id_type=MESH,
        )
        return carry

    lax.fori_loop(1, n, tell, 0)


def hear_all(sizes):
    dp, ctx, fs = sizes
    pl.semaphore_wait(pltpu.get_barrier_semaphore(), dp * ctx * fs - 1)


HALVES = 2


def part_of(ref, index):
    rows = ref.shape[-2] // HALVES
    return ref.at[index * rows : (index + 1) * rows]


def near_or_inner(c, at, n):
    ends = jnp.logical_or(c == 0, c == n - 1)
    return jnp.logical_or(jnp.logical_not(ends), jnp.abs(at - c) <= 1)


class LineGather:
    def __init__(self, n, own, whole, send, recv, local, short=False):
        self.n, self.own, self.whole, self.send, self.recv, self.local = n, own, whole, send, recv, local
        self.short = short
        self.d, self.c, self.f = place()
        self.here = at_device(self.d, self.c, self.f)

    def slot(self, at):
        return self.whole.at[self.d, at]

    def held(self, at):
        valid = jnp.logical_and(at >= 0, at < self.n)
        return jnp.logical_and(valid, near_or_inner(self.c, at, self.n)) if self.short else valid

    def passes(self, way, at):
        ahead = self.n - 2 - self.c if way == 0 else self.c - 1
        inside = at <= self.c if way == 0 else at >= self.c
        goes = jnp.logical_and(inside, ahead >= 0)
        return jnp.logical_and(goes, jnp.logical_or(at == self.c, ahead > 0)) if self.short else goes

    def along(self, way, block, at, part):
        to = (at_device(self.d, self.c + 1, self.f), at_device(self.d, self.c - 1, self.f), at_device(1 - self.d, self.c, self.f))[way]
        return remote(part_of(block, part), part_of(self.slot(at), part), self.send.at[way, at, part], self.recv.at[self.d, at, part], to)

    def start(self):
        c = self.c
        for part in range(HALVES):

            @pl.when(c < self.n - 1)
            def _():
                self.along(0, self.own, c, part).start()

            @pl.when(c > 0)
            def _():
                self.along(1, self.own, c, part).start()

        for part in range(HALVES):
            self.along(2, self.own, c, part).start()
        pltpu.make_async_copy(self.own, self.slot(c), self.local).start()

    def forward(self, k):
        for part in range(HALVES):
            for way, at in enumerate((self.c - k, self.c + k)):

                @pl.when(self.held(at))
                def _():
                    arrived(part_of(self.slot(at), part), self.recv.at[self.d, at, part], self.here)

                    @pl.when(self.passes(way, at))
                    def _():
                        self.along(way, self.slot(at), at, part).start()

                    self.along(2, self.slot(at), at, part).start()

    def reach(self, step):
        now = jnp.abs(ordered(self.c, step, self.n) - self.c)
        before = jnp.abs(ordered(self.c, step - 1, self.n) - self.c)

        @pl.when(jnp.logical_and(step > 0, now != before))
        def _():
            self.forward(now)

    def other(self, at):
        @pl.when(self.held(at))
        def _():
            for part in range(HALVES):
                arrived(part_of(self.whole.at[1 - self.d, at], part), self.recv.at[1 - self.d, at, part], self.here)

    def finish_sends(self):
        for at in range(self.n):
            for part in range(HALVES):
                block = part_of(self.slot(at), part)
                for way in range(3):

                    @pl.when(self.passes(way, at) if way < 2 else self.held(at))
                    def _():
                        left(block, self.send.at[way, at, part], self.here)

    def finish(self):
        self.finish_sends()
        pltpu.make_async_copy(self.own, self.slot(self.c), self.local).wait()


FACTOR = HD ** (-0.5)
LANES = 128


def ordered(c, step, n):
    at = jnp.int32(0)
    for here in range(n):
        near = sorted(range(n), key=lambda place_: (abs(place_ - here), place_))
        for index, value in enumerate(near):
            at = jnp.where(jnp.logical_and(c == here, step == index), value, at)
    return at


def towards(c, step, n):
    at = c
    for here in range(n):
        due = []
        for to in range(n):
            if to != here:
                hops = here if to > here else n - 1 - here
                due.append((hops + (n - 1 - to if to > here else to), -hops, to))
        for index, (_, _, to) in enumerate(sorted(due)):
            at = jnp.where(jnp.logical_and(c == here, step == index), to, at)
    return at


class LineSum:
    def __init__(self, n, mine, out_core, in_core, out_line, in_line, total, sems):
        self.n, self.mine, self.out_core, self.in_core = n, mine, out_core, in_core
        self.out_line, self.in_line, self.total = out_line, in_line, total
        self.core_send, self.core_recv, self.line_send, self.line_recv = sems
        self.d, self.c, self.f = place()
        self.here = at_device(self.d, self.c, self.f)

    def give(self, at, both):
        self.keep(at, both)
        self.hand(at)

    def keep(self, at, both):
        d = self.d
        low = both.astype(jnp.bfloat16)

        @pl.when(d == 0)
        def _():
            self.mine[at] = low[0]
            self.out_core[at] = low[1]

        @pl.when(d != 0)
        def _():
            self.mine[at] = low[1]
            self.out_core[at] = low[0]

    def hand(self, at):
        remote(
            self.out_core.at[at], self.in_core.at[at], self.core_send.at[at], self.core_recv.at[at], at_device(1 - self.d, self.c, self.f)
        ).start()

    def step(self, at):
        n, d, c, f = self.n, self.d, self.c, self.f
        arrived(self.in_core.at[at], self.core_recv.at[at], self.here)
        rows = self.total.shape[0] // HALVES
        for part in range(HALVES):
            own = slice(part * rows, (part + 1) * rows)
            self.total[own] = self.mine[at, own].astype(jnp.float32) + self.in_core[at, own].astype(jnp.float32)
            for way, comes in enumerate((jnp.logical_and(at <= c, c < n - 1), jnp.logical_and(at >= c, c > 0))):

                @pl.when(comes)
                def _():
                    arrived(self.in_line.at[way, at, own], self.line_recv.at[way, at, part], self.here)
                    self.total[own] += self.in_line[way, at, own].astype(jnp.float32)

            @pl.when(at != c)
            def _():
                self.out_line[at, own] = self.total[own].astype(jnp.bfloat16)

            for way, (goes, to) in enumerate(((at < c, c - 1), (at > c, c + 1))):

                @pl.when(goes)
                def _():
                    remote(
                        self.out_line.at[at, own], self.in_line.at[way, at, own],
                        self.line_send.at[at, part], self.line_recv.at[way, at, part], at_device(d, to, f),
                    ).start()

    def finish(self):
        rows = self.total.shape[0] // HALVES
        for at in range(self.n):
            left(self.out_core.at[at], self.core_send.at[at], self.here)

            @pl.when(at != self.c)
            def _():
                for part in range(HALVES):
                    left(self.out_line.at[at, part * rows : (part + 1) * rows], self.line_send.at[at, part], self.here)

    @staticmethod
    def scratch(ctx, rows):
        low = jnp.bfloat16
        dma = pltpu.SemaphoreType.DMA
        return [
            VM((ctx, rows, D), low), VM((ctx, rows, D), low), VM((ctx, rows, D), low), VM((ctx, rows, D), low),
            VM((2, ctx, rows, D), low), VM((rows, D), jnp.float32),
            dma((ctx,)), dma((ctx,)), dma((ctx, HALVES)), dma((2, ctx, HALVES)),
        ]


def down_route(d, c):
    return (lax.rem(c, 2), 2 * d + c // 2), (c // 2, 2 * lax.rem(c, 2) + d)


def front_kernel(
    sizes, hidden, parts, x_ref, one_ref, two_ref, w_ref, dy_ref, proj_ref, down_ref, gate_up_ref,
    out_ref, d_resid_out, gain_out, block_ref, step_ref, normed_out, qkv_out, wide_out, gains_out, unit_out, grad_proj_out, up_land, down_land,
    x_all, wide, normed, stage, qkv_unit, att_stage, att, gain_all, gain_vec,
    dy_all, proj, down_mid, down, gate_up, resid, own_two, normed_two, act, d_both, own_d, d_stage, unit,
    grad_up, grad_down, grad_proj, grad_proj_low, gains_ref, d_resid_held,
    line_send, line_recv, line_local, w_send, w_recv, w_pass, g_send, g_recv, q_send, q_recv, a_send, a_recv, out_sem,
    dy_send, dy_recv, dy_local, m_send, m_recv, m_pass, down_send, down_recv, d_recv, d_pass, gu_send, gu_recv,
    two_send, two_recv, two_local, dr_send, dr_recv, dr_local, u_send, u_recv, gup_send, gup_recv, gdn_send, gdn_recv,
    *sums,
):
    d_resid_all = x_all
    dp, ctx, fs = sizes
    n = dp * ctx * fs
    d, c, f = place()
    here = at_device(d, c, f)
    span = stage.shape[2]
    tell_all(sizes)
    fill_tables(block_ref, step_ref)
    gains_ref[0:1, 0 : D // n] = one_ref[...].astype(jnp.float32).reshape(1, D // n)
    gains_ref[1:2, 0 : D // n] = two_ref[...].astype(jnp.float32).reshape(1, D // n)
    for slot in range(4):
        wide[slot * LANES + HD : (slot + 1) * LANES, :] = jnp.zeros((LANES - HD, D), jnp.bfloat16)
    each_proj = proj_ref.shape[0]
    for start in range(2 * each_proj, 2 * LANES, LANES):
        proj[start : start + LANES - 2 * each_proj, :] = jnp.zeros((LANES - 2 * each_proj, D), jnp.bfloat16)
    hear_all(sizes)

    def proj_rows(slot):
        start = slot // 2 * LANES + lax.rem(slot, 2) * each_proj
        return proj.at[pl.ds(pl.multiple_of(start, 16), each_proj)]

    def head_rows(slot):
        return wide.at[pl.ds(pl.multiple_of(slot * LANES, LANES), HD)]

    q_core = f // 2
    kv_slot = 2 + c // 2
    kv_ctx = 2 * lax.rem(c, 2) + f // 2
    kv_core = lax.rem(f, 2)
    kv_f = lax.rem(f + 2 * (c // 2), fs)
    kv_away = jnp.logical_or(jnp.logical_or(kv_core != d, kv_ctx != c), kv_f != f)
    relay_of = {slot: f == lax.rem(2 * lax.rem(c, 2) + d + 2 * (slot - 2), fs) for slot in (2, 3)}

    me = (d * ctx + c) * fs + f

    def gain_to(step, carry):
        other = lax.rem(me + step, n)
        remote(
            gains_ref, gain_all.at[me], g_send.at[other], g_recv.at[me],
            at_device(other // (ctx * fs), lax.rem(other // fs, ctx), lax.rem(other, fs)),
        ).start()
        return carry

    lax.fori_loop(1, n, gain_to, 0)
    gain_all[me] = gains_ref[...]

    @pl.when(jnp.logical_and(d == 1, kv_away))
    def _():
        remote(w_ref, head_rows(kv_slot), w_send.at[0], w_recv.at[kv_slot], at_device(kv_core, kv_ctx, kv_f)).start()

    @pl.when(jnp.logical_and(d == 1, jnp.logical_not(kv_away)))
    def _():
        pltpu.make_async_copy(w_ref, head_rows(kv_slot), w_recv.at[kv_slot]).start()

    x_line = LineGather(ctx, x_ref, x_all, line_send, line_recv, line_local)
    x_line.start()

    @pl.when(d == 0)
    def _():
        slot = lax.rem(f, 2)
        for to in range(fs):

            @pl.when(jnp.logical_or(q_core != 0, to != f))
            def _():
                remote(w_ref, head_rows(slot), w_send.at[to], w_recv.at[slot], at_device(q_core, c, to)).start()

            @pl.when(jnp.logical_and(q_core == 0, to == f))
            def _():
                pltpu.make_async_copy(w_ref, head_rows(slot), w_recv.at[slot]).start()

    for slot in (2, 3):

        @pl.when(relay_of[slot])
        def _():
            arrived(head_rows(slot), w_recv.at[slot], here)
            for step in range(1, fs):
                to = lax.rem(f + step, fs)
                remote(head_rows(slot), head_rows(slot), w_pass.at[slot - 2, step], w_recv.at[slot], at_device(d, c, to)).start()

    gu_core = f // 2
    gu_slot = 2 * d + lax.rem(f, 2)
    part_rows = gate_up_ref.shape[0] // parts

    def push_part(part):
        first_row = part * part_rows
        src = gate_up_ref.at[first_row : first_row + part_rows]
        dst = gate_up.at[gu_slot, first_row : first_row + part_rows]
        for to in range(fs):
            own_place = jnp.logical_and(gu_core == d, f == to)

            @pl.when(jnp.logical_not(own_place))
            def _():
                remote(src, dst, gu_send.at[part, to], gu_recv.at[part, gu_slot], at_device(gu_core, c, to)).start()

            @pl.when(own_place)
            def _():
                pltpu.make_async_copy(src, dst, gu_recv.at[part, gu_slot]).start()

    def gain_from(step, carry):
        other = lax.rem(me + step, n)
        arrived(gain_all.at[other], g_recv.at[other], here)
        return carry

    lax.fori_loop(1, n, gain_from, 0)
    each = D // n
    for index in range(n):
        gain_vec[:, index * each : (index + 1) * each] = gain_all[index][:, :each]
    gain = gain_vec[0:1, :]

    for k in range(1, ctx - 1):
        x_line.forward(k)
    to_core, to_ctx = lax.rem(c, 2), 2 * d + c // 2
    stays = jnp.logical_and(to_core == d, to_ctx == c)

    @pl.when(jnp.logical_not(stays))
    def _():
        remote(proj_ref, proj_rows(f), m_send, m_recv.at[f], at_device(to_core, to_ctx, f)).start()

    @pl.when(stays)
    def _():
        pltpu.make_async_copy(proj_ref, proj_rows(f), m_recv.at[f]).start()

    dy_line = LineGather(ctx, dy_ref, dy_all, dy_send, dy_recv, dy_local)
    dy_line.start()
    for slot in range(4):
        if slot < 2:
            arrived(head_rows(slot), w_recv.at[slot], here)
        else:

            @pl.when(jnp.logical_not(relay_of[slot]))
            def _():
                arrived(head_rows(slot), w_recv.at[slot], here)

    push_part(0)
    pltpu.make_async_copy(x_line.own, x_line.slot(c), x_line.local).wait()

    def block(step, carry):
        at = ordered(c, step, ctx)

        x_line.other(at)
        values = x_all[:, at].reshape(dp * 2 * span, D).astype(jnp.float32)
        scale = lax.rsqrt(jnp.mean(values * values, axis=-1, keepdims=True) + EPS)
        low = (values * scale * gain).astype(jnp.bfloat16)
        normed[:, at] = low.reshape(dp, 2 * span, D)
        heads = outer(low, wide[...])
        cosine, sine_up, sine_down = turns(block_ref, step_ref, at * fs + f)
        for slot in range(4):
            head = heads[:, slot * LANES : (slot + 1) * LANES]
            if slot < 3:
                turned_up = pltpu.roll(head, HD // 2, 1).reshape(2 * dp, span, LANES)
                turned_down = pltpu.roll(head, LANES - HD // 2, 1).reshape(2 * dp, span, LANES)
                head = head.reshape(2 * dp, span, LANES)
                head = head * cosine[None] + turned_up * sine_up[None] + turned_down * sine_down[None]
            else:
                head = head.reshape(2 * dp, span, LANES)
            stage[at, :, :, slot * LANES : (slot + 1) * LANES] = head.astype(jnp.bfloat16)
        for to in range(2 * dp):

            @pl.when(to != f)
            def _():
                remote(stage.at[at, to], qkv_unit.at[at, f], q_send.at[at, to], q_recv.at[at, f], at_device(d, c, to)).start()

            @pl.when(to == f)
            def _():
                qkv_unit[at, f] = stage[at, to]

        return carry

    def near(step, carry):
        @pl.when(step == ctx - 1)
        def _():
            x_line.forward(ctx - 1)

        return block(step, carry)

    lax.fori_loop(0, ctx, near, 0)
    normed_copy = pltpu.make_async_copy(normed, normed_out, out_sem.at[3])
    wide_copy = pltpu.make_async_copy(wide, wide_out, out_sem.at[4])
    gains_copy = pltpu.make_async_copy(gain_vec, gains_out, out_sem.at[5])
    normed_copy.start()
    wide_copy.start()
    gains_copy.start()

    @pl.when(jnp.logical_not(stays))
    def _():
        remote(down_ref, down_mid, down_send, down_recv, at_device(to_core, to_ctx, f)).start()

    @pl.when(stays)
    def _():
        pltpu.make_async_copy(down_ref, down_mid, down_recv).start()

    arrived(proj_rows(f), m_recv.at[f], here)
    for step in range(1, fs):
        to = lax.rem(f + step, fs)
        remote(proj_rows(f), proj_rows(f), m_pass.at[step], m_recv.at[f], at_device(d, c, to)).start()

    ends = jnp.logical_or(c == 0, c == ctx - 1)

    @pl.when(jnp.logical_not(ends))
    def _():
        dy_line.forward(1)


    for at in range(ctx):
        for step in range(1, fs):
            other = lax.rem(f + step, fs)
            arrived(qkv_unit.at[at, other], q_recv.at[at, other], here)
    qkv_copy = pltpu.make_async_copy(qkv_unit, qkv_out, out_sem.at[0])
    qkv_copy.start()

    block_rows = fs * span
    for at in (0, ctx - 1, *range(1, ctx - 1)):
        keys = block_rows * (at + 1)
        k_rows = qkv_unit[0 : at + 1, :, :, 2 * LANES : 3 * LANES].reshape(keys, LANES)
        v_rows = qkv_unit[0 : at + 1, :, :, 3 * LANES : 4 * LANES].reshape(keys, LANES)
        allowed = lax.broadcasted_iota(jnp.int32, (block_rows, keys), 1) <= block_rows * at + lax.broadcasted_iota(
            jnp.int32, (block_rows, keys), 0
        )
        for head in range(2):
            q_rows = qkv_unit[at, :, :, head * LANES : (head + 1) * LANES].reshape(block_rows, LANES)
            scores = outer(q_rows, k_rows) * FACTOR
            scores = jnp.where(allowed, scores, NEG)
            best = jnp.max(scores, axis=-1, keepdims=True)
            weights = jnp.exp(scores - best)
            probs = weights / jnp.sum(weights, axis=-1, keepdims=True)
            mixed = jnp.dot(probs.astype(jnp.bfloat16), v_rows, preferred_element_type=jnp.float32)
            att_stage[at, :, :, head * LANES : (head + 1) * LANES] = mixed.astype(jnp.bfloat16).reshape(fs, span, LANES)
        for to in range(fs):

            @pl.when(to != f)
            def _():
                remote(
                    att_stage.at[at, to], att.at[f // 2, at, lax.rem(f, 2)], a_send.at[at, to], a_recv.at[f, at], at_device(d, c, to)
                ).start()

            @pl.when(to == f)
            def _():
                att[f // 2, at, lax.rem(f, 2)] = att_stage[at, to]


    ends = jnp.logical_or(c == 0, c == ctx - 1)

    @pl.when(jnp.logical_not(ends))
    def _():
        dy_line.forward(2)

    for step in range(1, fs):
        other = lax.rem(f + step, fs)
        arrived(proj_rows(other), m_recv.at[other], here)
    rows = x_ref.shape[0]
    both_rows = dp * rows
    half = hidden // 2
    line_sum = LineSum(ctx, *sums[:6], sums[6:10])
    second_sum = LineSum(ctx, *sums[10:16], sums[16:20])
    out_sum = line_sum

    def project(step, carry):
        at = towards(c, step, ctx)
        for move in range(1, fs):
            other = lax.rem(f + move, fs)
            arrived(att.at[other // 2, at, lax.rem(other, 2)], a_recv.at[other, at], here)
        terms = jnp.dot(att[:, at].reshape(both_rows, 2 * LANES), proj[...], preferred_element_type=jnp.float32)
        line_sum.give(at, terms.reshape(dp, rows, D))

        @pl.when(jnp.logical_and(ends, step > 0))
        def _():
            line_sum.step(towards(c, step - 1, ctx))

        return carry

    lax.fori_loop(0, ctx, project, 0)

    arrived(down_mid, down_recv, here)
    pltpu.make_async_copy(down_mid, down.at[f], d_recv.at[f]).start()
    for step in range(1, fs):
        to = lax.rem(f + step, fs)
        remote(down_mid, down.at[f], d_pass.at[step], d_recv.at[f], at_device(d, c, to)).start()
    for part in range(1, parts):
        push_part(part)

    def sum_step(step, carry):
        line_sum.step(towards(c, step, ctx))
        return carry

    lax.fori_loop(jnp.where(ends, ctx - 1, 0), ctx - 1, sum_step, 0)

    @pl.when(ends)
    def _():
        for k in range(1, ctx):
            dy_line.forward(k)

    line_sum.step(c)
    gain = gain_vec[1:2, :]
    values = x_ref[...].astype(jnp.float32) + line_sum.total[...]
    resid[...] = values
    scale = lax.rsqrt(jnp.mean(values * values, axis=-1, keepdims=True) + EPS)
    own_two[...] = (values * scale * gain).astype(jnp.bfloat16)
    line = LineGather(ctx, own_two, normed_two, two_send, two_recv, two_local)
    line.start()
    line.forward(1)
    line_sum.finish()
    x_line.finish_sends()
    for part in range(parts):
        for slot in range(4):
            arrived(gate_up.at[slot, part * part_rows : (part + 1) * part_rows], gu_recv.at[part, slot], here)
    for slot in range(fs):
        arrived(down.at[slot], d_recv.at[slot], here)
    pltpu.make_async_copy(dy_line.own, dy_line.slot(c), dy_line.local).wait()
    for part in range(parts):
        src = gate_up_ref.at[part * part_rows : (part + 1) * part_rows]
        for to in range(fs):

            @pl.when(jnp.logical_not(jnp.logical_and(gu_core == d, f == to)))
            def _():
                left(src, gu_send.at[part, to], here)

    for at in range(ctx):

        for to in range(fs):

            @pl.when(to != f)
            def _():
                left(stage.at[at, to], q_send.at[at, to], here)
                left(att_stage.at[at, to], a_send.at[at, to], here)

    @pl.when(jnp.logical_and(d == 1, kv_away))
    def _():
        left(w_ref, w_send.at[0], here)

    @pl.when(d == 0)
    def _():
        for to in range(fs):

            @pl.when(jnp.logical_or(q_core != 0, to != f))
            def _():
                left(w_ref, w_send.at[to], here)

    for slot in (2, 3):

        @pl.when(relay_of[slot])
        def _():
            for step in range(1, fs):
                left(head_rows(slot), w_pass.at[slot - 2, step], here)

    def gain_left(step, carry):
        other = lax.rem(me + step, n)
        left(gains_ref, g_send.at[other], here)
        return carry

    lax.fori_loop(1, n, gain_left, 0)
    for copy in (normed_copy, wide_copy, gains_copy, qkv_copy):
        copy.wait()
    for step in range(1, fs):
        left(down_mid, d_pass.at[step], here)
        left(proj_rows(f), m_pass.at[step], here)

    @pl.when(jnp.logical_not(stays))
    def _():
        left(proj_ref, m_send, here)
        left(down_ref, down_send, here)

    dy_line.finish_sends()
    pltpu.make_async_copy(line.own, line.slot(c), line.local).wait()

    def mlp(step, carry):
        at = ordered(c, step, ctx)


        @pl.when(lax.rem(step, 2) == 1)
        def _():
            line.forward(2 + step // 2)

        line.other(at)
        dy_line.other(at)
        inputs = normed_two[:, at].reshape(both_rows, D)
        dy_rows = dy_all[:, at].reshape(both_rows, D)
        for part in range(2):
            cols = slice(part * half, (part + 1) * half)
            gate = jnp.dot(inputs, gate_up[part], preferred_element_type=jnp.float32)
            up = jnp.dot(inputs, gate_up[2 + part], preferred_element_type=jnp.float32)
            d_act = outer(dy_rows, down[2 * part : 2 * part + 2].reshape(half, D))
            sig = 1.0 / (1.0 + jnp.exp(-gate))
            silu = gate * sig
            act[:, at, :, cols] = (silu * up).astype(jnp.bfloat16).reshape(dp, rows, half)
            d_gate = d_act * up * (sig * (1.0 + gate * (1.0 - sig)))
            d_both[:, at, :, cols] = d_gate.astype(jnp.bfloat16).reshape(dp, rows, half)
            d_both[:, at, :, hidden + part * half : hidden + (part + 1) * half] = (
                (d_act * silu).astype(jnp.bfloat16).reshape(dp, rows, half)
            )
        terms = outer(d_both[:, at, :, 0:half].reshape(both_rows, half), gate_up[0])
        for part in range(1, 4):
            terms += outer(d_both[:, at, :, part * half : (part + 1) * half].reshape(both_rows, half), gate_up[part])
        second_sum.give(at, terms.reshape(dp, rows, D))
        return carry

    lax.fori_loop(0, ctx, mlp, 0)

    wide_rows = D // ctx

    def push(src, dst, send, recv, core, to):
        to_self = jnp.logical_and(core == d, to == f)

        @pl.when(jnp.logical_not(to_self))
        def _():
            remote(src, dst, send, recv, at_device(core, c, to)).start()

        @pl.when(to_self)
        def _():
            pltpu.make_async_copy(src, dst, recv).start()

    def grads(step):
        first = pl.multiple_of(step * wide_rows, LANES)
        left_rows = normed_two[:, :, :, pl.ds(first, wide_rows)].reshape(dp * ctx * rows, wide_rows)
        for part in range(2):
            cols = slice(part * hidden, (part + 1) * hidden)
            terms = inner(left_rows, d_both[:, :, :, cols].reshape(dp * ctx * rows, hidden)).astype(jnp.bfloat16)
            grad_up[2 * part, pl.ds(first, wide_rows), :] = terms[:, :half]
            grad_up[2 * part + 1, pl.ds(first, wide_rows), :] = terms[:, half:]
        dy_cols = dy_all[:, :, :, pl.ds(first, wide_rows)].reshape(dp * ctx * rows, wide_rows)
        terms = inner(act[...].reshape(dp * ctx * rows, hidden), dy_cols).astype(jnp.bfloat16)
        grad_down[:, :, pl.ds(first, wide_rows)] = terms.reshape(fs, hidden // fs, wide_rows)
        for slot in range(4):
            push(
                grad_up.at[slot, pl.ds(first, wide_rows)], up_land.at[f, pl.ds(first, wide_rows)],
                gup_send.at[slot, step], gup_recv.at[f, step], slot // 2, 2 * d + slot % 2,
            )
            push(
                grad_down.at[slot, :, pl.ds(first, wide_rows)], down_land.at[f, :, pl.ds(first, wide_rows)],
                gdn_send.at[slot, step], gdn_recv.at[f, step], d, slot,
            )

    def out_terms(step):
        at = towards(c, step, ctx)
        terms = jnp.dot(act[:, at].reshape(both_rows, hidden), down[...].reshape(hidden, D), preferred_element_type=jnp.float32)
        out_sum.give(at, terms.reshape(dp, rows, D))

    def second_steps():
        def body(step, carry):
            second_sum.step(towards(c, step, ctx))
            return carry

        lax.fori_loop(0, ctx - 1, body, 0)

    def local_terms(step, carry):
        grads(step)
        out_terms(step)
        return carry

    pl.when(ends)(second_steps)
    lax.fori_loop(0, ctx - 1, local_terms, 0)
    pl.when(jnp.logical_not(ends))(second_steps)
    local_terms(ctx - 1, 0)
    second_sum.step(c)
    values = resid[...]
    scale = lax.rsqrt(jnp.mean(values * values, axis=-1, keepdims=True) + EPS)
    incoming = second_sum.total[...]
    weighted = incoming * gain
    mean = jnp.mean(weighted * values, axis=-1, keepdims=True)
    d_resid = dy_ref[...].astype(jnp.float32) + scale * weighted - values * (scale * scale * scale) * mean
    own_d[...] = d_resid.astype(jnp.bfloat16)
    d_resid_held[...] = d_resid
    d_resid_copy = pltpu.make_async_copy(d_resid_held, d_resid_out, out_sem.at[6])
    d_resid_copy.start()
    gain_out[...] = jnp.broadcast_to(jnp.sum(incoming * values * scale, axis=0, keepdims=True), gain_out.shape)
    d_line = LineGather(ctx, own_d, d_resid_all, dr_send, dr_recv, dr_local)
    d_line.start()
    def out_step(step, carry):
        out_sum.step(towards(c, step, ctx))
        return carry

    @pl.when(ends)
    def _():
        lax.fori_loop(0, ctx - 1, out_step, 0)

    line.finish_sends()
    second_sum.finish()
    pltpu.make_async_copy(d_line.own, d_line.slot(c), d_line.local).wait()
    grad_proj[...] = jnp.zeros_like(grad_proj)

    def back(step, carry):
        at = ordered(c, step, ctx)

        d_line.reach(step)
        d_line.other(at)
        incoming = d_resid_all[:, at].reshape(both_rows, D)
        d_att = outer(incoming, proj[...]).astype(jnp.bfloat16)
        d_stage[at] = d_att.reshape(2 * dp, span, 2 * LANES)
        for to in range(2 * dp):

            @pl.when(to != f)
            def _():
                remote(d_stage.at[at, to], unit.at[at, f], u_send.at[at, to], u_recv.at[at, f], at_device(d, c, to)).start()

            @pl.when(to == f)
            def _():
                unit[at, f] = d_stage[at, to]

        grad_proj[...] += inner(att[:, at].reshape(both_rows, 2 * LANES), incoming)

        @pl.when(jnp.logical_and(jnp.logical_not(ends), step == ctx - 2))
        def _():
            out_sum.step(towards(c, 0, ctx))

        return carry

    lax.fori_loop(0, ctx, back, 0)

    @pl.when(jnp.logical_not(ends))
    def _():
        lax.fori_loop(1, ctx - 1, out_step, 0)

    for slot in range(fs):
        start = slot // 2 * LANES + slot % 2 * each_proj
        grad_proj_low[slot] = grad_proj[start : start + each_proj, :].astype(jnp.bfloat16)
    grad_proj_copy = pltpu.make_async_copy(grad_proj_low, grad_proj_out, out_sem.at[1])
    grad_proj_copy.start()
    for at in range(ctx):
        for step in range(1, fs):
            other = lax.rem(f + step, fs)
            arrived(unit.at[at, other], u_recv.at[at, other], here)
    unit_copy = pltpu.make_async_copy(unit, unit_out, out_sem.at[2])
    unit_copy.start()
    d_line.finish_sends()
    for at in range(ctx):
        for to in range(fs):

            @pl.when(to != f)
            def _():
                left(d_stage.at[at, to], u_send.at[at, to], here)

    def settle_up(step, carry):
        first = pl.multiple_of(step * wide_rows, LANES)
        for slot in range(4):
            arrived(up_land.at[slot, pl.ds(first, wide_rows)], gup_recv.at[slot, step], here)

            @pl.when(jnp.logical_or(slot // 2 != d, 2 * d + slot % 2 != f))
            def _():
                left(grad_up.at[slot, pl.ds(first, wide_rows)], gup_send.at[slot, step], here)

        return carry

    def settle_down(step, carry):
        first = pl.multiple_of(step * wide_rows, LANES)
        for slot in range(4):
            arrived(down_land.at[slot, :, pl.ds(first, wide_rows)], gdn_recv.at[slot, step], here)

            @pl.when(slot != f)
            def _():
                left(grad_down.at[slot, :, pl.ds(first, wide_rows)], gdn_send.at[slot, step], here)

        return carry

    lax.fori_loop(0, ctx, settle_up, 0)
    lax.fori_loop(0, ctx, settle_down, 0)
    out_step(ctx - 1, 0)
    out_ref[...] = (resid[...] + out_sum.total[...]).astype(jnp.bfloat16)
    out_sum.finish()
    for copy in (d_resid_copy, grad_proj_copy, unit_copy):
        copy.wait()

def front(sizes, parts, x, attn_gain, mlp_gain, w_qkv, dy, w_out, w_down, w_gate_up):
    dp, ctx, fs = sizes
    n = dp * ctx * fs
    rows = x.shape[0]
    span = rows // 2
    hidden = FF // (dp * ctx)
    low, wide_t = jnp.bfloat16, jnp.float32
    dma = pltpu.SemaphoreType.DMA
    any_spec, vm_spec = pl.BlockSpec(memory_space=ANY), pl.BlockSpec(memory_space=VM)
    line_sems = [dma((3, ctx, HALVES)), dma((dp, ctx, HALVES)), dma]
    shapes = (
        jax.ShapeDtypeStruct((rows, D), low),
        jax.ShapeDtypeStruct((rows, D), wide_t),
        jax.ShapeDtypeStruct((8, D), wide_t),
        jax.ShapeDtypeStruct((2, ctx * fs, LANES), wide_t),
        jax.ShapeDtypeStruct((2, span, LANES), wide_t),
        jax.ShapeDtypeStruct((dp, ctx, rows, D), low),
        jax.ShapeDtypeStruct((ctx, fs, span, 4 * LANES), low),
        jax.ShapeDtypeStruct((4 * LANES, D), low),
        jax.ShapeDtypeStruct((8, D), wide_t),
        jax.ShapeDtypeStruct((ctx, fs, span, 2 * LANES), low),
        jax.ShapeDtypeStruct((fs,) + w_out.shape, low),
        jax.ShapeDtypeStruct((fs, D, hidden // 2), low),
        jax.ShapeDtypeStruct((fs, hidden // fs, D), low),
    )
    return pl.pallas_call(
        functools.partial(front_kernel, sizes, hidden, parts),
        name="front",
        out_shape=shapes,
        in_specs=[vm_spec] * 3 + [any_spec, vm_spec] + [any_spec] * 3,
        out_specs=[vm_spec, any_spec] + [vm_spec] * 3 + [any_spec] * 8,
        scratch_shapes=[
            VM((dp, ctx, rows, D), low),
            VM((4 * LANES, D), low),
            VM((dp, ctx, rows, D), low),
            VM((ctx, 2 * dp, span, 4 * LANES), low),
            VM((ctx, fs, span, 4 * LANES), low),
            VM((ctx, fs, span, 2 * LANES), low),
            VM((dp, ctx, 2, span, 2 * LANES), low),
            VM((n, 8, LANES), wide_t),
            VM((8, D), wide_t),
            VM((dp, ctx, rows, D), low),
            VM((2 * LANES, D), low),
            VM(w_down.shape, low),
            VM((fs, hidden // fs, D), low),
            VM((4, D, hidden // 2), low),
            VM((rows, D), wide_t),
            VM((rows, D), low),
            VM((dp, ctx, rows, D), low),
            VM((dp, ctx, rows, hidden), low),
            VM((dp, ctx, rows, 2 * hidden), low),
            VM((rows, D), low),
            VM((ctx, 2 * dp, span, 2 * LANES), low),
            VM((ctx, fs, span, 2 * LANES), low),
            VM((4, D, hidden // 2), low),
            VM((fs, hidden // fs, D), low),
            VM((2 * LANES, D), wide_t),
            VM((fs,) + w_out.shape, low),
            VM((8, LANES), wide_t),
            VM((rows, D), wide_t),
            *line_sems,
            dma((fs,)), dma((4,)), dma((2, fs)), dma((n,)), dma((n,)),
            dma((ctx, 2 * dp)), dma((ctx, fs)), dma((ctx, fs)), dma((fs, ctx)), dma((7,)),
            *line_sems,
            dma, dma((fs,)), dma((fs,)), dma, dma, dma((fs,)), dma((fs,)), dma((parts, fs)), dma((parts, 4)),
            *line_sems,
            *line_sems,
            dma((ctx, 2 * dp)), dma((ctx, fs)),
            dma((4, ctx)), dma((fs, ctx)), dma((fs, ctx)), dma((fs, ctx)),
        ] + LineSum.scratch(ctx, rows) * 2,
        compiler_params=pltpu.CompilerParams(collective_id=1, has_side_effects=True, vmem_limit_bytes=67043328),
    )(x, attn_gain, mlp_gain, w_qkv, dy, w_out, w_down, w_gate_up)


def fill_tables(block_ref, step_ref):
    span = step_ref.shape[1]
    for ref, scale in ((block_ref, span), (step_ref, 1)):
        shape = ref.shape[1:]
        lane = lax.broadcasted_iota(jnp.int32, shape, 1)
        pair = jnp.where(lane >= HD // 2, lane - HD // 2, lane).astype(jnp.float32)
        frequency = jnp.exp(pair * (-2.0 * math.log(THETA) / HD))
        angles = (lax.broadcasted_iota(jnp.int32, shape, 0) * scale).astype(jnp.float32) * frequency
        ref[0] = jnp.cos(angles)
        ref[1] = jnp.sin(angles)


def turns(block_ref, step_ref, block):
    cos_b, sin_b = block_ref[0, pl.ds(block, 1)], block_ref[1, pl.ds(block, 1)]
    cos_s, sin_s = step_ref[0], step_ref[1]
    cosine = cos_b * cos_s - sin_b * sin_s
    sine = sin_b * cos_s + cos_b * sin_s
    lane = lax.broadcasted_iota(jnp.int32, sine.shape, 1)
    first_half = lane < HD // 2
    sine_up = jnp.where(jnp.logical_and(lane >= HD // 2, lane < HD), sine, 0.0)
    return cosine, sine_up, jnp.where(first_half, -sine, 0.0)


def last_kernel(
    sizes, x_ref, gains_ref, block_ref, step_ref, gain_two_ref, proj_ref,
    d_resid_in, unit_ref, d_unit_ref, normed_ref, wide_ref, up_land_ref, down_land_ref,
    d_x_ref, gains_out, qkv_out, proj_out, up_out, down_out,
    unit, d_unit, d_k, d_v, stage, mixed, packed, normed, wide, grad_heads,
    up_land, down_land, proj_land, q_land, kv_land, down_sum, proj_sum, kv_sum, down_last, proj_last, kv_last, gain_vec, gain_stage, gain_land, up_sum, d_resid_ref,
    in_sem, proj_send, proj_recv, head_send, head_recv, move_send, move_recv,
    u_send, u_recv, g_send, g_recv, up_sem, wide_sem,
    *sums,
):
    dp, ctx, fs = sizes
    n = dp * ctx * fs
    d, c, f = place()
    here = at_device(d, c, f)
    me = (d * ctx + c) * fs + f
    rows = x_ref.shape[0]
    span = rows // 2
    both_rows = dp * rows
    low, wide_t = jnp.bfloat16, jnp.float32
    loads = [
        pltpu.make_async_copy(src, dst, in_sem.at[index])
        for index, (src, dst) in enumerate((
            (unit_ref, unit), (d_unit_ref, d_unit), (normed_ref, normed), (d_resid_in, d_resid_ref), (down_land_ref, down_land), (up_land_ref, up_land),
        ))
    ]
    wide_loads = [
        pltpu.make_async_copy(
            wide_ref.at[slot * LANES : slot * LANES + HD], wide.at[slot * HD : (slot + 1) * HD], wide_sem.at[slot]
        )
        for slot in range(4)
    ]
    tell_all(sizes)
    for load in loads + wide_loads:
        load.start()
    in_sum = LineSum(ctx, *sums[:6], sums[6:10])
    d_k[...] = jnp.zeros_like(d_k)
    d_v[...] = jnp.zeros_like(d_v)

    def push(src, land, send, recv, core, fs_to):
        to_self = jnp.logical_and(core == d, fs_to == f)

        @pl.when(jnp.logical_not(to_self))
        def _():
            remote(src, land.at[f], send, recv.at[f], at_device(core, c, fs_to)).start()

        @pl.when(to_self)
        def _():
            pltpu.make_async_copy(src, land.at[f], recv.at[f]).start()

    def pushed(src, send, core, fs_to):
        @pl.when(jnp.logical_not(jnp.logical_and(core == d, fs_to == f)))
        def _():
            left(src, send, here)

    def sum_of(land):
        total = land[0].astype(wide_t)
        for source in range(1, fs):
            total += land[source].astype(wide_t)
        return total

    _, (own_core, own_ctx) = down_route(d, c)
    stays = jnp.logical_and(own_core == d, own_ctx == c)

    def move(index, src, dst):
        @pl.when(jnp.logical_not(stays))
        def _():
            remote(src, dst, move_send.at[index], move_recv.at[index], at_device(own_core, own_ctx, f)).start()

        @pl.when(stays)
        def _():
            pltpu.make_async_copy(src, dst, move_recv.at[index]).start()

    loads[0].wait()
    loads[1].wait()
    block = fs * span

    def unturn(values, at):
        up = pltpu.roll(values, HD // 2, 1)
        down = pltpu.roll(values, LANES - HD // 2, 1)
        pieces = []
        for index in range(fs):
            own = slice(index * span, (index + 1) * span)
            cosine, sine_up, sine_down = turns(block_ref, step_ref, at * fs + index)
            pieces.append(values[own] * cosine - up[own] * sine_up - down[own] * sine_down)
        return jnp.concatenate(pieces, axis=0)

    for at in reversed(range(ctx)):
        keys = block * (at + 1)
        k_rows = unit[0 : at + 1, :, :, 2 * LANES : 3 * LANES].reshape(keys, LANES)
        v_rows = unit[0 : at + 1, :, :, 3 * LANES : 4 * LANES].reshape(keys, LANES)
        allowed = lax.broadcasted_iota(jnp.int32, (block, keys), 1) <= block * at + lax.broadcasted_iota(
            jnp.int32, (block, keys), 0
        )
        for head in range(2):
            lanes = slice(head * LANES, (head + 1) * LANES)
            q_rows = unit[at, :, :, lanes].reshape(block, LANES)
            d_rows = d_unit[at, :, :, lanes].reshape(block, LANES)
            scores = jnp.where(allowed, outer(q_rows, k_rows) * FACTOR, NEG)
            weights = jnp.exp(scores - jnp.max(scores, axis=-1, keepdims=True))
            probs = weights / jnp.sum(weights, axis=-1, keepdims=True)
            d_probs = outer(d_rows, v_rows)
            delta = jnp.sum(probs * d_probs, axis=-1, keepdims=True)
            d_scores = (probs * (d_probs - delta)).astype(low)
            d_q = jnp.dot(d_scores, k_rows, preferred_element_type=wide_t) * FACTOR
            packed[:, head * HD : (head + 1) * HD] = unturn(d_q, at)[:, :HD]
            d_k[0:keys, :] += inner(d_scores, q_rows) * FACTOR
            d_v[0:keys, :] += inner(probs.astype(low), d_rows)
        packed[:, 2 * HD : 3 * HD] = unturn(d_k[block * at : keys, :], at)[:, :HD]
        packed[:, 3 * HD : 4 * HD] = d_v[block * at : keys, :HD]
        stage[at] = packed[...].astype(low).reshape(fs, span, 4 * HD)
        if at == ctx - 1:
            hear_all(sizes)
        for to in range(fs):

            @pl.when(to != f)
            def _():
                remote(
                    stage.at[at, to], mixed.at[f // 2, at, lax.rem(f, 2)], u_send.at[at, to], u_recv.at[f, at], at_device(d, c, to)
                ).start()

            @pl.when(to == f)
            def _():
                mixed[f // 2, at, lax.rem(f, 2)] = stage[at, to]

        if at == ctx - 1:
            loads[4].wait()
            down_sum[...] = sum_of(down_land).astype(low)
            move(0, down_sum, down_last)
    loads[2].wait()
    for load in wide_loads:
        load.wait()

    ends = jnp.logical_or(c == 0, c == ctx - 1)

    def give(step, carry):
        at = towards(c, step, ctx)
        for move_ in range(1, fs):
            other = lax.rem(f + move_, fs)
            arrived(mixed.at[other // 2, at, lax.rem(other, 2)], u_recv.at[other, at], here)
        terms = jnp.dot(mixed[:, at].reshape(both_rows, 4 * HD), wide[...], preferred_element_type=wide_t)
        in_sum.give(at, terms.reshape(dp, rows, D))

        @pl.when(jnp.logical_and(ends, jnp.logical_and(step > 0, step < ctx - 1)))
        def _():
            in_sum.step(towards(c, step - 1, ctx))

        return carry

    lax.fori_loop(0, ctx, give, 0)

    every = dp * ctx * rows
    k_relay = 2 * lax.rem(c, 2) + d
    relays = (k_relay, lax.rem(k_relay + 2, fs))
    gain_terms = jnp.zeros((1, D), wide_t)
    for slot in (2, 3, 0, 1):
        if slot % 2 == 0:
            both_heads = inner(
                mixed[...].reshape(every, 4 * HD)[:, slot * HD : (slot + 2) * HD], normed[...].reshape(every, D)
            )
        heads = both_heads[slot % 2 * HD : (slot % 2 + 1) * HD]
        grad_heads[slot] = heads.astype(low)
        weights = wide[slot * HD : (slot + 1) * HD, :].astype(wide_t)
        gain_terms += jnp.sum(heads * weights, axis=0, keepdims=True)
        if slot < 2:
            push(grad_heads.at[slot], q_land, head_send.at[slot], head_recv.at[0], 0, 2 * d + slot)
        else:
            push(grad_heads.at[slot], kv_land.at[slot - 2], head_send.at[slot], head_recv.at[slot - 1], d, relays[slot - 2])

    for slot in range(fs):
        push(proj_ref.at[slot], proj_land, proj_send.at[slot], proj_recv, d, slot)

    gain = gains_ref[0:1, :]
    gain_vec[0:1, :] = gain_terms / gain
    gain_vec[1:2, :] = gain_two_ref[0:1, :]
    each = D // n
    for index in range(n):
        gain_stage[index, :, 0:each] = gain_vec[:, index * each : (index + 1) * each]
    gain_land[me] = gain_stage[me]

    def gain_to(step, carry):
        other = lax.rem(me + step, n)
        remote(
            gain_stage.at[other], gain_land.at[me], g_send.at[other], g_recv.at[me],
            at_device(other // (ctx * fs), lax.rem(other // fs, ctx), lax.rem(other, fs)),
        ).start()
        return carry

    lax.fori_loop(1, n, gain_to, 0)

    def middle_step(step, carry):
        in_sum.step(towards(c, step, ctx))
        return carry

    lax.fori_loop(jnp.where(ends, ctx - 2, 0), ctx - 1, middle_step, 0)

    def kv_route(slot):
        owner, owner_f = slot * 2 + c // 2, k_relay
        return owner, owner_f, jnp.logical_or(jnp.logical_or(d != 1, owner != c), owner_f != f)

    for slot in range(2):
        owner, owner_f, away = kv_route(slot)

        @pl.when(f == relays[slot])
        def _():
            for source in range(fs):
                arrived(kv_land.at[slot, source], head_recv.at[1 + slot, source], here)
            kv_sum[slot] = sum_of(kv_land.at[slot]).astype(low)

            @pl.when(away)
            def _():
                remote(kv_sum.at[slot], kv_last, move_send.at[2 + slot], move_recv.at[2], at_device(1, owner, owner_f)).start()

            @pl.when(jnp.logical_not(away))
            def _():
                pltpu.make_async_copy(kv_sum.at[slot], kv_last, move_recv.at[2]).start()

    for source in range(fs):
        arrived(proj_land.at[source], proj_recv.at[source], here)
    proj_sum[...] = sum_of(proj_land).astype(low)
    move(1, proj_sum, proj_last)

    loads[5].wait()
    up_sum[...] = sum_of(up_land)
    up_copy = pltpu.make_async_copy(up_sum, up_out, up_sem)
    up_copy.start()
    @pl.when(d == 0)
    def _():
        for source in range(fs):
            arrived(q_land.at[source], head_recv.at[0, source], here)
        qkv_out[...] = sum_of(q_land)

    for slot in range(fs):
        pushed(proj_ref.at[slot], proj_send.at[slot], d, slot)
    for slot in range(2):
        pushed(grad_heads.at[slot], head_send.at[slot], 0, 2 * d + slot)
        pushed(grad_heads.at[2 + slot], head_send.at[2 + slot], d, relays[slot])

    for at in range(ctx):
        for to in range(fs):

            @pl.when(to != f)
            def _():
                left(stage.at[at, to], u_send.at[at, to], here)

    def gain_from(step, carry):
        other = lax.rem(me + step, n)
        arrived(gain_land.at[other], g_recv.at[other], here)
        return carry

    lax.fori_loop(1, n, gain_from, 0)
    total = gain_land[0]
    for index in range(1, n):
        total += gain_land[index]
    gains_out[...] = total

    def gain_left(step, carry):
        other = lax.rem(me + step, n)
        left(gain_stage.at[other], g_send.at[other], here)
        return carry

    lax.fori_loop(1, n, gain_left, 0)

    loads[3].wait()
    in_sum.step(c)

    values = x_ref[...].astype(wide_t)
    scale = lax.rsqrt(jnp.mean(values * values, axis=-1, keepdims=True) + EPS)
    incoming = in_sum.total[...]
    weighted = incoming * gain
    mean = jnp.mean(weighted * values, axis=-1, keepdims=True)
    d_x_ref[...] = (d_resid_ref[...] + scale * weighted - values * (scale * scale * scale) * mean).astype(low)

    for index, dst in enumerate((down_last, proj_last)):
        arrived(dst, move_recv.at[index], here)
    down_out[...] = down_last[...].astype(wide_t)
    proj_out[...] = proj_last[...].astype(wide_t)

    @pl.when(d == 1)
    def _():
        arrived(kv_last, move_recv.at[2], here)
        qkv_out[...] = kv_last[...].astype(wide_t)

    for slot in range(2):
        away = kv_route(slot)[2]

        @pl.when(jnp.logical_and(f == relays[slot], away))
        def _():
            left(kv_sum.at[slot], move_send.at[2 + slot], here)

        @pl.when(jnp.logical_not(stays))
        def _():
            left((down_sum, proj_sum)[slot], move_send.at[slot], here)

    in_sum.finish()
    up_copy.wait()


def last(sizes, x, gains, tables, d_resid, gain_two, grad_proj, unit, d_unit, normed, wide, up_land, down_land):
    dp, ctx, fs = sizes
    n = dp * ctx * fs
    rows = x.shape[0]
    span = rows // 2
    low, wide_t = jnp.bfloat16, jnp.float32
    dma = pltpu.SemaphoreType.DMA
    any_spec, vm_spec = pl.BlockSpec(memory_space=ANY), pl.BlockSpec(memory_space=VM)
    down_rows, proj_rows, half = down_land.shape[1], grad_proj.shape[1], up_land.shape[2]
    shapes = (
        jax.ShapeDtypeStruct((rows, D), low),
        jax.ShapeDtypeStruct((8, LANES), wide_t),
        jax.ShapeDtypeStruct((HD, D), wide_t),
        jax.ShapeDtypeStruct((proj_rows, D), wide_t),
        jax.ShapeDtypeStruct((D, half), wide_t),
        jax.ShapeDtypeStruct((down_rows, D), wide_t),
    )
    return pl.pallas_call(
        functools.partial(last_kernel, sizes),
        name="last",
        out_shape=shapes,
        in_specs=[vm_spec] * 5 + [any_spec] * 8,
        out_specs=[vm_spec] * 4 + [any_spec, vm_spec],
        scratch_shapes=[
            VM(unit.shape, low),
            VM(d_unit.shape, low),
            VM((ctx * fs * span, LANES), wide_t),
            VM((ctx * fs * span, LANES), wide_t),
            VM((ctx, fs, span, 4 * HD), low),
            VM((dp, ctx, 2, span, 4 * HD), low),
            VM((fs * span, 4 * HD), wide_t),
            VM(normed.shape, low),
            VM((4 * HD, D), low),
            VM((4, HD, D), low),
            VM(up_land.shape, low),
            VM((fs, down_rows, D), low),
            VM((fs, proj_rows, D), low),
            VM((fs, HD, D), low),
            VM((2, fs, HD, D), low),
            VM((down_rows, D), low),
            VM((proj_rows, D), low),
            VM((2, HD, D), low),
            VM((down_rows, D), low),
            VM((proj_rows, D), low),
            VM((HD, D), low),
            VM((8, D), wide_t),
            VM((n, 8, LANES), wide_t),
            VM((n, 8, LANES), wide_t),
            VM((D, half), wide_t),
            VM((rows, D), wide_t),
            dma((6,)), dma((fs,)), dma((fs,)),
            dma((4,)), dma((3, fs)), dma((4,)), dma((3,)),
            dma((ctx, fs)), dma((fs, ctx)), dma((n,)), dma((n,)), dma, dma((4,)),
        ] + LineSum.scratch(ctx, rows),
        compiler_params=pltpu.CompilerParams(collective_id=3, has_side_effects=True, vmem_limit_bytes=63 * 1024 * 1024),
    )(x, gains, *tables, gain_two, grad_proj, d_resid, unit, d_unit, normed, wide, up_land, down_land)


PIECES = 4


def emit_kernel(count, gains_ref, *refs):
    sources, outs, one_ref, two_ref = refs[:count], refs[count : 2 * count], refs[2 * count], refs[2 * count + 1]
    held, in_sem, out_sem = refs[2 * count + 2 : 3 * count + 2], refs[-2], refs[-1]
    loads, stores = [], []
    for index in range(count):
        rows = held[index].shape[0]
        pieces = PIECES if rows % (PIECES * 16) == 0 else 1
        for piece in range(pieces):
            own = slice(piece * rows // pieces, (piece + 1) * rows // pieces)
            loads.append(pltpu.make_async_copy(sources[index].at[own], held[index].at[own], in_sem.at[len(loads)]))
            stores.append(pltpu.make_async_copy(held[index].at[own], outs[index].at[own], out_sem.at[len(stores)]))
    for load in loads:
        load.start()
    each = one_ref.shape[0]
    one_ref[...] = gains_ref[0, :each]
    two_ref[...] = gains_ref[1, :each]
    for load, store in zip(loads, stores):
        load.wait()
        store.start()
    for store in stores:
        store.wait()


def emit(each, gains, *arrays):
    count = len(arrays)
    any_spec, vm_spec = pl.BlockSpec(memory_space=ANY), pl.BlockSpec(memory_space=VM)
    gain = jax.ShapeDtypeStruct((each,), jnp.float32)
    return pl.pallas_call(
        functools.partial(emit_kernel, count),
        name="emit",
        out_shape=[jax.ShapeDtypeStruct(a.shape, a.dtype) for a in arrays] + [gain, gain],
        in_specs=[vm_spec] + [any_spec] * count,
        out_specs=[any_spec] * count + [vm_spec] * 2,
        scratch_shapes=[VM(a.shape, a.dtype) for a in arrays] + [pltpu.SemaphoreType.DMA((count * PIECES,))] * 2,
        compiler_params=pltpu.CompilerParams(vmem_limit_bytes=63 * 1024 * 1024),
    )(gains, *arrays)


def on_device(tokens, cotangent, attn_gain, w_qkv, w_out, mlp_gain, w_gate_up, w_down):
    dp, ctx, fs = where = tuple(lax.axis_size(name) for name in ("dp", "ctx", "fsdp"))
    mb, _, span, _ = tokens.shape
    rows = mb * span
    x = tokens.reshape(rows, D)
    dy = cotangent.reshape(rows, D)
    each = attn_gain.shape[0]
    block_out, d_resid, grad_two, *tables, normed, unit, qkv, gains, d_unit, grad_proj, up_land, down_land = front(
        where, 8, x, attn_gain, mlp_gain, w_qkv.T, dy, w_out, w_down, w_gate_up
    )
    grad_tokens, gain_grads, grad_qkv, grad_out, grad_gate_up, grad_down = last(
        where, x, gains, tables, d_resid, grad_two, grad_proj, unit, d_unit, normed, qkv, up_land, down_land
    )
    block_out, grad_tokens, grad_qkv, grad_out, grad_gate_up, grad_down, grad_one, grad_two = emit(
        each, gain_grads, block_out, grad_tokens, grad_qkv, grad_out, grad_gate_up, grad_down
    )
    return (
        block_out.reshape(tokens.shape),
        grad_tokens.reshape(tokens.shape),
        grad_one,
        grad_qkv.T,
        grad_out,
        grad_two,
        grad_gate_up,
        grad_down,
    )


def fits(mesh):
    return mesh.shape["dp"] == 2 and mesh.shape["ctx"] == 4 and mesh.shape["fsdp"] == 4


def solution(mesh):
    placed = (
        P(None, "dp", ("ctx", "fsdp"), None),
        P(None, "dp", ("ctx", "fsdp"), None),
        P(("dp", "ctx", "fsdp")),
        P(None, ("dp", "ctx", "fsdp")),
        P(("dp", "ctx", "fsdp"), None),
        P(("dp", "ctx", "fsdp")),
        P(None, ("dp", "ctx", "fsdp")),
        P(("dp", "ctx", "fsdp"), None),
    )
    return jax.shard_map(
        on_device if fits(mesh) else on_device_gathered,
        mesh=mesh,
        in_specs=placed,
        out_specs=(
            P(None, "dp", ("ctx", "fsdp"), None),
            P(None, "dp", ("ctx", "fsdp"), None),
            P(("dp", "ctx", "fsdp")),
            P(None, ("dp", "ctx", "fsdp")),
            P(("dp", "ctx", "fsdp"), None),
            P(("dp", "ctx", "fsdp")),
            P(None, ("dp", "ctx", "fsdp")),
            P(("dp", "ctx", "fsdp"), None),
        ),
        check_vma=False,
    )
```

```python
import functools
import math

import jax
import jax.numpy as jnp
from jax import lax
from jax.experimental import pallas as pl
from jax.experimental.pallas import tpu as pltpu
from jax.sharding import PartitionSpec as P

D = 1536
H = 16
KVH = 8
HD = 96
FF = 4096


EPS = 1e-05
THETA = 100000.0
NEG = -1e30


def in_blocks(value, dim, length):
    lengths = value.shape
    pieces = value.reshape(*lengths[:dim], length, lengths[dim] // length, *lengths[dim + 1 :])
    return jnp.moveaxis(pieces, dim, 0)


def sum_at_owner(value, axis, dim):
    pieces = in_blocks(value, dim, lax.axis_size(axis))
    arrived = lax.all_to_all(pieces, axis, split_axis=0, concat_axis=0, tiled=True)
    return arrived.astype(jnp.float32).sum(axis=0)


def side_by_side(arrays, axis, dim, along):
    both = jnp.concatenate(arrays, axis=along)
    whole, at, finished = (sum_at_owner(both, axis, dim), 0, [])
    for a in arrays:
        finished.append(lax.slice_in_dim(whole, at, at + a.shape[along], axis=along))
        at += a.shape[along]
    return tuple(finished)


def rms_norm(values, gain_vec):
    return values * lax.rsqrt(jnp.mean(values * values, axis=-1, keepdims=True) + EPS) * gain_vec


def tables(start, length, width):
    half_width = width // 2
    frequency = THETA ** (-(jnp.arange(half_width, dtype=jnp.float32) * 2.0) / width)
    angles = (start + jnp.arange(length, dtype=jnp.int32)).astype(jnp.float32)[:, None] * frequency[
        None, :
    ]
    return (jnp.cos(angles), jnp.sin(angles))


def rotate(values, cosine, sine_table):
    half_width = values.shape[-1] // 2
    first_half = values[..., :half_width]
    second_half = values[..., half_width:]
    cos_b = cosine[:, None, :]
    sin_b = sine_table[:, None, :]
    return jnp.concatenate(
        [first_half * cos_b - second_half * sin_b, second_half * cos_b + first_half * sin_b],
        axis=-1,
    )


def swiglu(both):
    return jax.nn.silu(both[:, :FF]) * both[:, FF:]


def inner(left, right):
    return lax.dot_general(
        left, right, (((0,), (0,)), ((), ())), preferred_element_type=jnp.float32
    )


def outer(left, right):
    return lax.dot_general(
        left, right, (((1,), (1,)), ((), ())), preferred_element_type=jnp.float32
    )


def unchanged(state):
    return state


def on_device_gathered(tokens, cotangent, attn_gain, w_qkv, w_out, mlp_gain, w_gate_up, w_down):
    tok_count = tokens.shape[2]
    groups = H // KVH
    factor = HD ** (-0.5)
    seq_length = tok_count * lax.axis_size(("ctx", "fsdp"))
    pos_first = lax.axis_index(("ctx", "fsdp")) * tok_count
    positions = pos_first + jnp.arange(tok_count, dtype=jnp.int32)
    pos_last = pos_first + tok_count - 1
    cosine, sine_table = tables(pos_first, tok_count, HD)
    sums = [
        jnp.zeros((D,), jnp.float32),
        jnp.zeros((D, (H + 2 * KVH) * HD), jnp.float32),
        jnp.zeros((H * HD, D), jnp.float32),
        jnp.zeros((D,), jnp.float32),
        jnp.zeros((D, 2 * FF), jnp.float32),
        jnp.zeros((FF, D), jnp.float32),
    ]
    outputs = []
    in_grads = []
    whole = (
        lax.all_gather(attn_gain, ("dp", "ctx", "fsdp"), axis=0, tiled=True),
        lax.all_gather(w_qkv, ("dp", "ctx", "fsdp"), axis=1, tiled=True),
        lax.all_gather(w_out, ("dp", "ctx", "fsdp"), axis=0, tiled=True),
        lax.all_gather(mlp_gain, ("dp", "ctx", "fsdp"), axis=0, tiled=True),
        lax.all_gather(w_gate_up, ("dp", "ctx", "fsdp"), axis=1, tiled=True),
        lax.all_gather(w_down, ("dp", "ctx", "fsdp"), axis=0, tiled=True),
    )
    for step_index in range(tokens.shape[0]):
        gain_one, mix_qkv, mix_out, gain_two, mix_gate_up, mix_down = whole
        inputs = tokens[step_index, 0].astype(jnp.float32)
        normed = rms_norm(inputs, gain_one.astype(jnp.float32)).astype(jnp.bfloat16)
        mixed = jnp.dot(normed, mix_qkv, preferred_element_type=jnp.float32)
        queries = rotate(mixed[:, : H * HD].reshape(tok_count, H, HD), cosine, sine_table).astype(
            jnp.bfloat16
        )
        key_rows = rotate(
            mixed[:, H * HD : (H + KVH) * HD].reshape(tok_count, KVH, HD), cosine, sine_table
        )
        key_rows = key_rows.astype(jnp.bfloat16).reshape(tok_count, KVH * HD)
        value_rows = mixed[:, (H + KVH) * HD :].astype(jnp.bfloat16)
        grouped = queries.reshape(tok_count, KVH, groups, HD)
        start_state = (
            jnp.full((KVH, groups, tok_count), NEG, jnp.float32),
            jnp.zeros((KVH, groups, tok_count), jnp.float32),
            jnp.zeros((KVH, groups, tok_count, HD), jnp.float32),
        )
        piece = (
            lax.all_gather(key_rows, ("ctx", "fsdp"), axis=0, tiled=True),
            lax.all_gather(value_rows, ("ctx", "fsdp"), axis=0, tiled=True),
        )

        def work(state):
            best, total, summed = state
            key_count = piece[0].shape[0]
            keys = piece[0].reshape(key_count, KVH, HD)
            values = piece[1].reshape(key_count, KVH, HD)
            scores = (
                jnp.einsum("qkgd,tkd->kgqt", grouped, keys, preferred_element_type=jnp.float32)
                * factor
            )
            allowed = jnp.arange(key_count, dtype=jnp.int32)[None, :] <= positions[:, None]
            scores = jnp.where(allowed, scores, NEG)
            new_best = jnp.maximum(best, jnp.max(scores, axis=-1))
            weights = jnp.where(allowed, jnp.exp(scores - new_best[..., None]), 0.0)
            total = jnp.sum(weights, axis=-1)
            summed = jnp.einsum(
                "kgqt,tkd->kgqd",
                weights.astype(jnp.bfloat16),
                values,
                preferred_element_type=jnp.float32,
            )
            return (new_best, total, summed)

        best, total, summed = lax.cond(jnp.int32(0) <= pos_last, work, unchanged, start_state)
        head_out = summed / total[..., None]
        log_total = best + jnp.log(total)
        attended = (
            jnp.transpose(head_out, (2, 0, 1, 3)).reshape(tok_count, H * HD).astype(jnp.bfloat16)
        )
        resid = inputs + jnp.dot(attended, mix_out, preferred_element_type=jnp.float32)
        normed_two = rms_norm(resid, gain_two.astype(jnp.float32)).astype(jnp.bfloat16)
        both = jnp.dot(normed_two, mix_gate_up, preferred_element_type=jnp.float32)
        acted = swiglu(both).astype(jnp.bfloat16)
        result = resid + jnp.dot(acted, mix_down, preferred_element_type=jnp.float32)
        outputs.append(result.astype(jnp.bfloat16))
        gain_one, mix_qkv, mix_out, gain_two, mix_gate_up, mix_down = whole
        up_low = cotangent[step_index, 0]
        upstream = up_low.astype(jnp.float32)
        sums[5] = sums[5] + inner(acted, up_low)
        d_act = outer(up_low, mix_down)
        _, pull_glu = jax.vjp(swiglu, both)
        d_both = pull_glu(d_act)[0].astype(jnp.bfloat16)
        sums[4] = sums[4] + inner(normed_two, d_both)
        d_normed_two = outer(d_both, mix_gate_up)
        _, pull_two = jax.vjp(rms_norm, resid, gain_two.astype(jnp.float32))
        d_resid_norm, d_gain_two = pull_two(d_normed_two)
        sums[3] = sums[3] + d_gain_two
        d_resid = upstream + d_resid_norm
        d_resid_low = d_resid.astype(jnp.bfloat16)
        sums[2] = sums[2] + inner(attended, d_resid_low)
        d_attended = outer(d_resid_low, mix_out).astype(jnp.bfloat16)
        d_grouped = d_attended.reshape(tok_count, KVH, groups, HD)
        delta = jnp.einsum("qkgd,kgqd->kgq", d_grouped.astype(jnp.float32), head_out)
        zero_q = jnp.zeros((tok_count, KVH, groups, HD), jnp.float32)
        back_state = (
            zero_q,
            jnp.zeros((seq_length, KVH * HD), jnp.float32),
            jnp.zeros((seq_length, KVH * HD), jnp.float32),
        )
        attend_piece = (
            lax.all_gather(key_rows, ("ctx", "fsdp"), axis=0, tiled=True),
            lax.all_gather(value_rows, ("ctx", "fsdp"), axis=0, tiled=True),
        )

        def attend_work(state):
            key_count = attend_piece[0].shape[0]
            keys = attend_piece[0].reshape(key_count, KVH, HD)
            values = attend_piece[1].reshape(key_count, KVH, HD)
            scores = (
                jnp.einsum("qkgd,tkd->kgqt", grouped, keys, preferred_element_type=jnp.float32)
                * factor
            )
            allowed = jnp.arange(key_count, dtype=jnp.int32)[None, :] <= positions[:, None]
            scores = jnp.where(allowed, scores, NEG)
            probs = jnp.where(allowed, jnp.exp(scores - log_total[..., None]), 0.0)
            d_probs = jnp.einsum(
                "qkgd,tkd->kgqt", d_grouped, values, preferred_element_type=jnp.float32
            )
            d_scores = (probs * (d_probs - delta[..., None])).astype(jnp.bfloat16)
            grad_q = jnp.einsum(
                "kgqt,tkd->qkgd", d_scores, keys, preferred_element_type=jnp.float32
            )
            piece_k = (
                jnp.einsum("kgqt,qkgd->tkd", d_scores, grouped, preferred_element_type=jnp.float32)
                * factor
            )
            piece_v = jnp.einsum(
                "kgqt,qkgd->tkd",
                probs.astype(jnp.bfloat16),
                d_grouped,
                preferred_element_type=jnp.float32,
            )
            grad_k = piece_k.reshape(key_count, KVH * HD)
            grad_v = piece_v.reshape(key_count, KVH * HD)
            return (grad_q, grad_k, grad_v)

        back_result = lax.cond(jnp.int32(0) <= pos_last, attend_work, unchanged, back_state)
        grad_q = back_result[0]
        summed_k, summed_v = side_by_side(
            (back_result[1].astype(jnp.bfloat16), back_result[2].astype(jnp.bfloat16)),
            ("ctx", "fsdp"),
            0,
            1,
        )
        d_q_raw = rotate(grad_q.reshape(tok_count, H, HD) * factor, cosine, -sine_table).reshape(
            tok_count, H * HD
        )
        d_k_raw = rotate(summed_k.reshape(tok_count, KVH, HD), cosine, -sine_table).reshape(
            tok_count, KVH * HD
        )
        d_mixed = jnp.concatenate([d_q_raw, d_k_raw, summed_v], axis=1).astype(jnp.bfloat16)
        sums[1] = sums[1] + inner(normed, d_mixed)
        d_normed = outer(d_mixed, mix_qkv)
        _, pull_one = jax.vjp(rms_norm, inputs, gain_one.astype(jnp.float32))
        d_inputs_norm, d_gain_one = pull_one(d_normed)
        sums[0] = sums[0] + d_gain_one
        in_grads.append((d_resid + d_inputs_norm).astype(jnp.bfloat16))
    grad_gain_one, grad_qkv, grad_out, grad_gain_two, grad_gate_up, grad_down = (
        lax.psum_scatter(sums[0], ("dp", "ctx", "fsdp"), scatter_dimension=0, tiled=True),
        lax.psum_scatter(sums[1], ("dp", "ctx", "fsdp"), scatter_dimension=1, tiled=True),
        lax.psum_scatter(sums[2], ("dp", "ctx", "fsdp"), scatter_dimension=0, tiled=True),
        lax.psum_scatter(sums[3], ("dp", "ctx", "fsdp"), scatter_dimension=0, tiled=True),
        lax.psum_scatter(sums[4], ("dp", "ctx", "fsdp"), scatter_dimension=1, tiled=True),
        lax.psum_scatter(sums[5], ("dp", "ctx", "fsdp"), scatter_dimension=0, tiled=True),
    )
    block_out = jnp.stack(outputs)[:, None]
    grad_tokens = jnp.stack(in_grads)[:, None]
    return (
        block_out,
        grad_tokens,
        grad_gain_one,
        grad_qkv,
        grad_out,
        grad_gain_two,
        grad_gate_up,
        grad_down,
    )


MESH = pl.DeviceIdType.MESH
VM = pltpu.VMEM
ANY = pl.ANY


def place():
    return lax.axis_index("dp"), lax.axis_index("ctx"), lax.axis_index("fsdp")


def at_device(dp, ctx, fs):
    return {"dp": dp, "ctx": ctx, "fsdp": fs}


def remote(src, dst, send, recv, device):
    return pltpu.make_async_remote_copy(
        src_ref=src, dst_ref=dst, send_sem=send, recv_sem=recv, device_id=device, device_id_type=MESH
    )


def arrived(dst, recv, device):
    remote(dst, dst, recv, recv, device).wait_recv()


def left(src, send, device):
    remote(src, src, send, send, device).wait_send()


def tell_all(sizes):
    dp, ctx, fs = sizes
    n = dp * ctx * fs
    d, c, f = place()
    me = (d * ctx + c) * fs + f
    barrier = pltpu.get_barrier_semaphore()

    def tell(step, carry):
        other = lax.rem(me + step, n)
        pl.semaphore_signal(
            barrier,
            inc=1,
            device_id=at_device(other // (ctx * fs), lax.rem(other // fs, ctx), lax.rem(other, fs)),
            device_id_type=MESH,
        )
        return carry

    lax.fori_loop(1, n, tell, 0)


def hear_all(sizes):
    dp, ctx, fs = sizes
    pl.semaphore_wait(pltpu.get_barrier_semaphore(), dp * ctx * fs - 1)


HALVES = 2


def part_of(ref, index):
    rows = ref.shape[-2] // HALVES
    return ref.at[index * rows : (index + 1) * rows]


def near_or_inner(c, at, n):
    ends = jnp.logical_or(c == 0, c == n - 1)
    return jnp.logical_or(jnp.logical_not(ends), jnp.abs(at - c) <= 1)


class LineGather:
    def __init__(self, n, own, whole, send, recv, local, short=False):
        self.n, self.own, self.whole, self.send, self.recv, self.local = n, own, whole, send, recv, local
        self.short = short
        self.d, self.c, self.f = place()
        self.here = at_device(self.d, self.c, self.f)

    def slot(self, at):
        return self.whole.at[self.d, at]

    def held(self, at):
        valid = jnp.logical_and(at >= 0, at < self.n)
        return jnp.logical_and(valid, near_or_inner(self.c, at, self.n)) if self.short else valid

    def passes(self, way, at):
        ahead = self.n - 2 - self.c if way == 0 else self.c - 1
        inside = at <= self.c if way == 0 else at >= self.c
        goes = jnp.logical_and(inside, ahead >= 0)
        return jnp.logical_and(goes, jnp.logical_or(at == self.c, ahead > 0)) if self.short else goes

    def along(self, way, block, at, part):
        to = (at_device(self.d, self.c + 1, self.f), at_device(self.d, self.c - 1, self.f), at_device(1 - self.d, self.c, self.f))[way]
        return remote(part_of(block, part), part_of(self.slot(at), part), self.send.at[way, at, part], self.recv.at[self.d, at, part], to)

    def start(self):
        c = self.c
        for part in range(HALVES):

            @pl.when(c < self.n - 1)
            def _():
                self.along(0, self.own, c, part).start()

            @pl.when(c > 0)
            def _():
                self.along(1, self.own, c, part).start()

        for part in range(HALVES):
            self.along(2, self.own, c, part).start()
        pltpu.make_async_copy(self.own, self.slot(c), self.local).start()

    def forward(self, k):
        for part in range(HALVES):
            for way, at in enumerate((self.c - k, self.c + k)):

                @pl.when(self.held(at))
                def _():
                    arrived(part_of(self.slot(at), part), self.recv.at[self.d, at, part], self.here)

                    @pl.when(self.passes(way, at))
                    def _():
                        self.along(way, self.slot(at), at, part).start()

                    self.along(2, self.slot(at), at, part).start()

    def reach(self, step):
        now = jnp.abs(ordered(self.c, step, self.n) - self.c)
        before = jnp.abs(ordered(self.c, step - 1, self.n) - self.c)

        @pl.when(jnp.logical_and(step > 0, now != before))
        def _():
            self.forward(now)

    def other(self, at):
        @pl.when(self.held(at))
        def _():
            for part in range(HALVES):
                arrived(part_of(self.whole.at[1 - self.d, at], part), self.recv.at[1 - self.d, at, part], self.here)

    def finish_sends(self):
        for at in range(self.n):
            for part in range(HALVES):
                block = part_of(self.slot(at), part)
                for way in range(3):

                    @pl.when(self.passes(way, at) if way < 2 else self.held(at))
                    def _():
                        left(block, self.send.at[way, at, part], self.here)

    def finish(self):
        self.finish_sends()
        pltpu.make_async_copy(self.own, self.slot(self.c), self.local).wait()


FACTOR = HD ** (-0.5)
LANES = 128


def ordered(c, step, n):
    at = jnp.int32(0)
    for here in range(n):
        near = sorted(range(n), key=lambda place_: (abs(place_ - here), place_))
        for index, value in enumerate(near):
            at = jnp.where(jnp.logical_and(c == here, step == index), value, at)
    return at


def towards(c, step, n):
    at = c
    for here in range(n):
        due = []
        for to in range(n):
            if to != here:
                hops = here if to > here else n - 1 - here
                due.append((hops + (n - 1 - to if to > here else to), -hops, to))
        for index, (_, _, to) in enumerate(sorted(due)):
            at = jnp.where(jnp.logical_and(c == here, step == index), to, at)
    return at


class LineSum:
    def __init__(self, n, mine, out_core, in_core, out_line, in_line, total, sems):
        self.n, self.mine, self.out_core, self.in_core = n, mine, out_core, in_core
        self.out_line, self.in_line, self.total = out_line, in_line, total
        self.core_send, self.core_recv, self.line_send, self.line_recv = sems
        self.d, self.c, self.f = place()
        self.here = at_device(self.d, self.c, self.f)

    def give(self, at, both):
        self.keep(at, both)
        self.hand(at)

    def keep(self, at, both):
        d = self.d
        low = both.astype(jnp.bfloat16)

        @pl.when(d == 0)
        def _():
            self.mine[at] = low[0]
            self.out_core[at] = low[1]

        @pl.when(d != 0)
        def _():
            self.mine[at] = low[1]
            self.out_core[at] = low[0]

    def hand(self, at):
        remote(
            self.out_core.at[at], self.in_core.at[at], self.core_send.at[at], self.core_recv.at[at], at_device(1 - self.d, self.c, self.f)
        ).start()

    def step(self, at):
        n, d, c, f = self.n, self.d, self.c, self.f
        arrived(self.in_core.at[at], self.core_recv.at[at], self.here)
        rows = self.total.shape[0] // HALVES
        for part in range(HALVES):
            own = slice(part * rows, (part + 1) * rows)
            self.total[own] = self.mine[at, own].astype(jnp.float32) + self.in_core[at, own].astype(jnp.float32)
            for way, comes in enumerate((jnp.logical_and(at <= c, c < n - 1), jnp.logical_and(at >= c, c > 0))):

                @pl.when(comes)
                def _():
                    arrived(self.in_line.at[way, at, own], self.line_recv.at[way, at, part], self.here)
                    self.total[own] += self.in_line[way, at, own].astype(jnp.float32)

            @pl.when(at != c)
            def _():
                self.out_line[at, own] = self.total[own].astype(jnp.bfloat16)

            for way, (goes, to) in enumerate(((at < c, c - 1), (at > c, c + 1))):

                @pl.when(goes)
                def _():
                    remote(
                        self.out_line.at[at, own], self.in_line.at[way, at, own],
                        self.line_send.at[at, part], self.line_recv.at[way, at, part], at_device(d, to, f),
                    ).start()

    def finish(self):
        rows = self.total.shape[0] // HALVES
        for at in range(self.n):
            left(self.out_core.at[at], self.core_send.at[at], self.here)

            @pl.when(at != self.c)
            def _():
                for part in range(HALVES):
                    left(self.out_line.at[at, part * rows : (part + 1) * rows], self.line_send.at[at, part], self.here)

    @staticmethod
    def scratch(ctx, rows):
        low = jnp.bfloat16
        dma = pltpu.SemaphoreType.DMA
        return [
            VM((ctx, rows, D), low), VM((ctx, rows, D), low), VM((ctx, rows, D), low), VM((ctx, rows, D), low),
            VM((2, ctx, rows, D), low), VM((rows, D), jnp.float32),
            dma((ctx,)), dma((ctx,)), dma((ctx, HALVES)), dma((2, ctx, HALVES)),
        ]


def down_route(d, c):
    return (lax.rem(c, 2), 2 * d + c // 2), (c // 2, 2 * lax.rem(c, 2) + d)


def front_kernel(
    sizes, hidden, parts, x_ref, one_ref, two_ref, w_ref, dy_ref, proj_ref, down_ref, gate_up_ref,
    out_ref, d_resid_out, gain_out, block_ref, step_ref, normed_out, qkv_out, wide_out, gains_out, unit_out, grad_proj_out, up_land, down_land,
    x_all, wide, normed, stage, qkv_unit, att_stage, att, gain_all, gain_vec,
    dy_all, proj, down_mid, down, gate_up, resid, own_two, normed_two, act, d_both, own_d, d_stage, unit,
    grad_up, grad_down, grad_proj, grad_proj_low, gains_ref, d_resid_held,
    line_send, line_recv, line_local, w_send, w_recv, w_pass, g_send, g_recv, q_send, q_recv, a_send, a_recv, out_sem,
    dy_send, dy_recv, dy_local, m_send, m_recv, m_pass, down_send, down_recv, d_recv, d_pass, gu_send, gu_recv,
    two_send, two_recv, two_local, dr_send, dr_recv, dr_local, u_send, u_recv, gup_send, gup_recv, gdn_send, gdn_recv,
    *sums,
):
    d_resid_all = x_all
    dp, ctx, fs = sizes
    n = dp * ctx * fs
    d, c, f = place()
    here = at_device(d, c, f)
    span = stage.shape[2]
    tell_all(sizes)
    fill_tables(block_ref, step_ref)
    gains_ref[0:1, 0 : D // n] = one_ref[...].astype(jnp.float32).reshape(1, D // n)
    gains_ref[1:2, 0 : D // n] = two_ref[...].astype(jnp.float32).reshape(1, D // n)
    for slot in range(4):
        wide[slot * LANES + HD : (slot + 1) * LANES, :] = jnp.zeros((LANES - HD, D), jnp.bfloat16)
    each_proj = proj_ref.shape[0]
    for start in range(2 * each_proj, 2 * LANES, LANES):
        proj[start : start + LANES - 2 * each_proj, :] = jnp.zeros((LANES - 2 * each_proj, D), jnp.bfloat16)
    hear_all(sizes)

    def proj_rows(slot):
        start = slot // 2 * LANES + lax.rem(slot, 2) * each_proj
        return proj.at[pl.ds(pl.multiple_of(start, 16), each_proj)]

    def head_rows(slot):
        return wide.at[pl.ds(pl.multiple_of(slot * LANES, LANES), HD)]

    q_core = f // 2
    kv_slot = 2 + c // 2
    kv_ctx = 2 * lax.rem(c, 2) + f // 2
    kv_core = lax.rem(f, 2)
    kv_f = lax.rem(f + 2 * (c // 2), fs)
    kv_away = jnp.logical_or(jnp.logical_or(kv_core != d, kv_ctx != c), kv_f != f)
    relay_of = {slot: f == lax.rem(2 * lax.rem(c, 2) + d + 2 * (slot - 2), fs) for slot in (2, 3)}

    me = (d * ctx + c) * fs + f

    def gain_to(step, carry):
        other = lax.rem(me + step, n)
        remote(
            gains_ref, gain_all.at[me], g_send.at[other], g_recv.at[me],
            at_device(other // (ctx * fs), lax.rem(other // fs, ctx), lax.rem(other, fs)),
        ).start()
        return carry

    lax.fori_loop(1, n, gain_to, 0)
    gain_all[me] = gains_ref[...]

    @pl.when(jnp.logical_and(d == 1, kv_away))
    def _():
        remote(w_ref, head_rows(kv_slot), w_send.at[0], w_recv.at[kv_slot], at_device(kv_core, kv_ctx, kv_f)).start()

    @pl.when(jnp.logical_and(d == 1, jnp.logical_not(kv_away)))
    def _():
        pltpu.make_async_copy(w_ref, head_rows(kv_slot), w_recv.at[kv_slot]).start()

    x_line = LineGather(ctx, x_ref, x_all, line_send, line_recv, line_local)
    x_line.start()

    @pl.when(d == 0)
    def _():
        slot = lax.rem(f, 2)
        for to in range(fs):

            @pl.when(jnp.logical_or(q_core != 0, to != f))
            def _():
                remote(w_ref, head_rows(slot), w_send.at[to], w_recv.at[slot], at_device(q_core, c, to)).start()

            @pl.when(jnp.logical_and(q_core == 0, to == f))
            def _():
                pltpu.make_async_copy(w_ref, head_rows(slot), w_recv.at[slot]).start()

    for slot in (2, 3):

        @pl.when(relay_of[slot])
        def _():
            arrived(head_rows(slot), w_recv.at[slot], here)
            for step in range(1, fs):
                to = lax.rem(f + step, fs)
                remote(head_rows(slot), head_rows(slot), w_pass.at[slot - 2, step], w_recv.at[slot], at_device(d, c, to)).start()

    gu_core = f // 2
    gu_slot = 2 * d + lax.rem(f, 2)
    part_rows = gate_up_ref.shape[0] // parts

    def push_part(part):
        first_row = part * part_rows
        src = gate_up_ref.at[first_row : first_row + part_rows]
        dst = gate_up.at[gu_slot, first_row : first_row + part_rows]
        for to in range(fs):
            own_place = jnp.logical_and(gu_core == d, f == to)

            @pl.when(jnp.logical_not(own_place))
            def _():
                remote(src, dst, gu_send.at[part, to], gu_recv.at[part, gu_slot], at_device(gu_core, c, to)).start()

            @pl.when(own_place)
            def _():
                pltpu.make_async_copy(src, dst, gu_recv.at[part, gu_slot]).start()

    def gain_from(step, carry):
        other = lax.rem(me + step, n)
        arrived(gain_all.at[other], g_recv.at[other], here)
        return carry

    lax.fori_loop(1, n, gain_from, 0)
    each = D // n
    for index in range(n):
        gain_vec[:, index * each : (index + 1) * each] = gain_all[index][:, :each]
    gain = gain_vec[0:1, :]

    for k in range(1, ctx - 1):
        x_line.forward(k)
    to_core, to_ctx = lax.rem(c, 2), 2 * d + c // 2
    stays = jnp.logical_and(to_core == d, to_ctx == c)

    @pl.when(jnp.logical_not(stays))
    def _():
        remote(proj_ref, proj_rows(f), m_send, m_recv.at[f], at_device(to_core, to_ctx, f)).start()

    @pl.when(stays)
    def _():
        pltpu.make_async_copy(proj_ref, proj_rows(f), m_recv.at[f]).start()

    dy_line = LineGather(ctx, dy_ref, dy_all, dy_send, dy_recv, dy_local)
    dy_line.start()
    for slot in range(4):
        if slot < 2:
            arrived(head_rows(slot), w_recv.at[slot], here)
        else:

            @pl.when(jnp.logical_not(relay_of[slot]))
            def _():
                arrived(head_rows(slot), w_recv.at[slot], here)

    push_part(0)
    pltpu.make_async_copy(x_line.own, x_line.slot(c), x_line.local).wait()

    def block(step, carry):
        at = ordered(c, step, ctx)

        x_line.other(at)
        values = x_all[:, at].reshape(dp * 2 * span, D).astype(jnp.float32)
        scale = lax.rsqrt(jnp.mean(values * values, axis=-1, keepdims=True) + EPS)
        low = (values * scale * gain).astype(jnp.bfloat16)
        normed[:, at] = low.reshape(dp, 2 * span, D)
        heads = outer(low, wide[...])
        cosine, sine_up, sine_down = turns(block_ref, step_ref, at * fs + f)
        for slot in range(4):
            head = heads[:, slot * LANES : (slot + 1) * LANES]
            if slot < 3:
                turned_up = pltpu.roll(head, HD // 2, 1).reshape(2 * dp, span, LANES)
                turned_down = pltpu.roll(head, LANES - HD // 2, 1).reshape(2 * dp, span, LANES)
                head = head.reshape(2 * dp, span, LANES)
                head = head * cosine[None] + turned_up * sine_up[None] + turned_down * sine_down[None]
            else:
                head = head.reshape(2 * dp, span, LANES)
            stage[at, :, :, slot * LANES : (slot + 1) * LANES] = head.astype(jnp.bfloat16)
        for to in range(2 * dp):

            @pl.when(to != f)
            def _():
                remote(stage.at[at, to], qkv_unit.at[at, f], q_send.at[at, to], q_recv.at[at, f], at_device(d, c, to)).start()

            @pl.when(to == f)
            def _():
                qkv_unit[at, f] = stage[at, to]

        return carry

    def near(step, carry):
        @pl.when(step == ctx - 1)
        def _():
            x_line.forward(ctx - 1)

        return block(step, carry)

    lax.fori_loop(0, ctx, near, 0)
    normed_copy = pltpu.make_async_copy(normed, normed_out, out_sem.at[3])
    wide_copy = pltpu.make_async_copy(wide, wide_out, out_sem.at[4])
    gains_copy = pltpu.make_async_copy(gain_vec, gains_out, out_sem.at[5])
    normed_copy.start()
    wide_copy.start()
    gains_copy.start()

    @pl.when(jnp.logical_not(stays))
    def _():
        remote(down_ref, down_mid, down_send, down_recv, at_device(to_core, to_ctx, f)).start()

    @pl.when(stays)
    def _():
        pltpu.make_async_copy(down_ref, down_mid, down_recv).start()

    arrived(proj_rows(f), m_recv.at[f], here)
    for step in range(1, fs):
        to = lax.rem(f + step, fs)
        remote(proj_rows(f), proj_rows(f), m_pass.at[step], m_recv.at[f], at_device(d, c, to)).start()

    ends = jnp.logical_or(c == 0, c == ctx - 1)

    @pl.when(jnp.logical_not(ends))
    def _():
        dy_line.forward(1)


    for at in range(ctx):
        for step in range(1, fs):
            other = lax.rem(f + step, fs)
            arrived(qkv_unit.at[at, other], q_recv.at[at, other], here)
    qkv_copy = pltpu.make_async_copy(qkv_unit, qkv_out, out_sem.at[0])
    qkv_copy.start()

    block_rows = fs * span
    for at in (0, ctx - 1, *range(1, ctx - 1)):
        keys = block_rows * (at + 1)
        k_rows = qkv_unit[0 : at + 1, :, :, 2 * LANES : 3 * LANES].reshape(keys, LANES)
        v_rows = qkv_unit[0 : at + 1, :, :, 3 * LANES : 4 * LANES].reshape(keys, LANES)
        allowed = lax.broadcasted_iota(jnp.int32, (block_rows, keys), 1) <= block_rows * at + lax.broadcasted_iota(
            jnp.int32, (block_rows, keys), 0
        )
        for head in range(2):
            q_rows = qkv_unit[at, :, :, head * LANES : (head + 1) * LANES].reshape(block_rows, LANES)
            scores = outer(q_rows, k_rows) * FACTOR
            scores = jnp.where(allowed, scores, NEG)
            best = jnp.max(scores, axis=-1, keepdims=True)
            weights = jnp.exp(scores - best)
            probs = weights / jnp.sum(weights, axis=-1, keepdims=True)
            mixed = jnp.dot(probs.astype(jnp.bfloat16), v_rows, preferred_element_type=jnp.float32)
            att_stage[at, :, :, head * LANES : (head + 1) * LANES] = mixed.astype(jnp.bfloat16).reshape(fs, span, LANES)
        for to in range(fs):

            @pl.when(to != f)
            def _():
                remote(
                    att_stage.at[at, to], att.at[f // 2, at, lax.rem(f, 2)], a_send.at[at, to], a_recv.at[f, at], at_device(d, c, to)
                ).start()

            @pl.when(to == f)
            def _():
                att[f // 2, at, lax.rem(f, 2)] = att_stage[at, to]


    ends = jnp.logical_or(c == 0, c == ctx - 1)

    @pl.when(jnp.logical_not(ends))
    def _():
        dy_line.forward(2)

    for step in range(1, fs):
        other = lax.rem(f + step, fs)
        arrived(proj_rows(other), m_recv.at[other], here)
    rows = x_ref.shape[0]
    both_rows = dp * rows
    half = hidden // 2
    line_sum = LineSum(ctx, *sums[:6], sums[6:10])
    second_sum = LineSum(ctx, *sums[10:16], sums[16:20])
    out_sum = line_sum

    def project(step, carry):
        at = towards(c, step, ctx)
        for move in range(1, fs):
            other = lax.rem(f + move, fs)
            arrived(att.at[other // 2, at, lax.rem(other, 2)], a_recv.at[other, at], here)
        terms = jnp.dot(att[:, at].reshape(both_rows, 2 * LANES), proj[...], preferred_element_type=jnp.float32)
        line_sum.give(at, terms.reshape(dp, rows, D))

        @pl.when(jnp.logical_and(ends, step > 0))
        def _():
            line_sum.step(towards(c, step - 1, ctx))

        return carry

    lax.fori_loop(0, ctx, project, 0)

    arrived(down_mid, down_recv, here)
    pltpu.make_async_copy(down_mid, down.at[f], d_recv.at[f]).start()
    for step in range(1, fs):
        to = lax.rem(f + step, fs)
        remote(down_mid, down.at[f], d_pass.at[step], d_recv.at[f], at_device(d, c, to)).start()
    for part in range(1, parts):
        push_part(part)

    def sum_step(step, carry):
        line_sum.step(towards(c, step, ctx))
        return carry

    lax.fori_loop(jnp.where(ends, ctx - 1, 0), ctx - 1, sum_step, 0)

    @pl.when(ends)
    def _():
        for k in range(1, ctx):
            dy_line.forward(k)

    line_sum.step(c)
    gain = gain_vec[1:2, :]
    values = x_ref[...].astype(jnp.float32) + line_sum.total[...]
    resid[...] = values
    scale = lax.rsqrt(jnp.mean(values * values, axis=-1, keepdims=True) + EPS)
    own_two[...] = (values * scale * gain).astype(jnp.bfloat16)
    line = LineGather(ctx, own_two, normed_two, two_send, two_recv, two_local)
    line.start()
    line.forward(1)
    line_sum.finish()
    x_line.finish_sends()
    for part in range(parts):
        for slot in range(4):
            arrived(gate_up.at[slot, part * part_rows : (part + 1) * part_rows], gu_recv.at[part, slot], here)
    for slot in range(fs):
        arrived(down.at[slot], d_recv.at[slot], here)
    pltpu.make_async_copy(dy_line.own, dy_line.slot(c), dy_line.local).wait()
    for part in range(parts):
        src = gate_up_ref.at[part * part_rows : (part + 1) * part_rows]
        for to in range(fs):

            @pl.when(jnp.logical_not(jnp.logical_and(gu_core == d, f == to)))
            def _():
                left(src, gu_send.at[part, to], here)

    for at in range(ctx):

        for to in range(fs):

            @pl.when(to != f)
            def _():
                left(stage.at[at, to], q_send.at[at, to], here)
                left(att_stage.at[at, to], a_send.at[at, to], here)

    @pl.when(jnp.logical_and(d == 1, kv_away))
    def _():
        left(w_ref, w_send.at[0], here)

    @pl.when(d == 0)
    def _():
        for to in range(fs):

            @pl.when(jnp.logical_or(q_core != 0, to != f))
            def _():
                left(w_ref, w_send.at[to], here)

    for slot in (2, 3):

        @pl.when(relay_of[slot])
        def _():
            for step in range(1, fs):
                left(head_rows(slot), w_pass.at[slot - 2, step], here)

    def gain_left(step, carry):
        other = lax.rem(me + step, n)
        left(gains_ref, g_send.at[other], here)
        return carry

    lax.fori_loop(1, n, gain_left, 0)
    for copy in (normed_copy, wide_copy, gains_copy, qkv_copy):
        copy.wait()
    for step in range(1, fs):
        left(down_mid, d_pass.at[step], here)
        left(proj_rows(f), m_pass.at[step], here)

    @pl.when(jnp.logical_not(stays))
    def _():
        left(proj_ref, m_send, here)
        left(down_ref, down_send, here)

    dy_line.finish_sends()
    pltpu.make_async_copy(line.own, line.slot(c), line.local).wait()

    def mlp(step, carry):
        at = ordered(c, step, ctx)


        @pl.when(lax.rem(step, 2) == 1)
        def _():
            line.forward(2 + step // 2)

        line.other(at)
        dy_line.other(at)
        inputs = normed_two[:, at].reshape(both_rows, D)
        dy_rows = dy_all[:, at].reshape(both_rows, D)
        for part in range(2):
            cols = slice(part * half, (part + 1) * half)
            gate = jnp.dot(inputs, gate_up[part], preferred_element_type=jnp.float32)
            up = jnp.dot(inputs, gate_up[2 + part], preferred_element_type=jnp.float32)
            d_act = outer(dy_rows, down[2 * part : 2 * part + 2].reshape(half, D))
            sig = 1.0 / (1.0 + jnp.exp(-gate))
            silu = gate * sig
            act[:, at, :, cols] = (silu * up).astype(jnp.bfloat16).reshape(dp, rows, half)
            d_gate = d_act * up * (sig * (1.0 + gate * (1.0 - sig)))
            d_both[:, at, :, cols] = d_gate.astype(jnp.bfloat16).reshape(dp, rows, half)
            d_both[:, at, :, hidden + part * half : hidden + (part + 1) * half] = (
                (d_act * silu).astype(jnp.bfloat16).reshape(dp, rows, half)
            )
        terms = outer(d_both[:, at, :, 0:half].reshape(both_rows, half), gate_up[0])
        for part in range(1, 4):
            terms += outer(d_both[:, at, :, part * half : (part + 1) * half].reshape(both_rows, half), gate_up[part])
        second_sum.give(at, terms.reshape(dp, rows, D))
        return carry

    lax.fori_loop(0, ctx, mlp, 0)

    wide_rows = D // ctx

    def push(src, dst, send, recv, core, to):
        to_self = jnp.logical_and(core == d, to == f)

        @pl.when(jnp.logical_not(to_self))
        def _():
            remote(src, dst, send, recv, at_device(core, c, to)).start()

        @pl.when(to_self)
        def _():
            pltpu.make_async_copy(src, dst, recv).start()

    def grads(step):
        first = pl.multiple_of(step * wide_rows, LANES)
        left_rows = normed_two[:, :, :, pl.ds(first, wide_rows)].reshape(dp * ctx * rows, wide_rows)
        for part in range(2):
            cols = slice(part * hidden, (part + 1) * hidden)
            terms = inner(left_rows, d_both[:, :, :, cols].reshape(dp * ctx * rows, hidden)).astype(jnp.bfloat16)
            grad_up[2 * part, pl.ds(first, wide_rows), :] = terms[:, :half]
            grad_up[2 * part + 1, pl.ds(first, wide_rows), :] = terms[:, half:]
        dy_cols = dy_all[:, :, :, pl.ds(first, wide_rows)].reshape(dp * ctx * rows, wide_rows)
        terms = inner(act[...].reshape(dp * ctx * rows, hidden), dy_cols).astype(jnp.bfloat16)
        grad_down[:, :, pl.ds(first, wide_rows)] = terms.reshape(fs, hidden // fs, wide_rows)
        for slot in range(4):
            push(
                grad_up.at[slot, pl.ds(first, wide_rows)], up_land.at[f, pl.ds(first, wide_rows)],
                gup_send.at[slot, step], gup_recv.at[f, step], slot // 2, 2 * d + slot % 2,
            )
            push(
                grad_down.at[slot, :, pl.ds(first, wide_rows)], down_land.at[f, :, pl.ds(first, wide_rows)],
                gdn_send.at[slot, step], gdn_recv.at[f, step], d, slot,
            )

    def out_terms(step):
        at = towards(c, step, ctx)
        terms = jnp.dot(act[:, at].reshape(both_rows, hidden), down[...].reshape(hidden, D), preferred_element_type=jnp.float32)
        out_sum.give(at, terms.reshape(dp, rows, D))

    def second_steps():
        def body(step, carry):
            second_sum.step(towards(c, step, ctx))
            return carry

        lax.fori_loop(0, ctx - 1, body, 0)

    def local_terms(step, carry):
        grads(step)
        out_terms(step)
        return carry

    pl.when(ends)(second_steps)
    lax.fori_loop(0, ctx - 1, local_terms, 0)
    pl.when(jnp.logical_not(ends))(second_steps)
    local_terms(ctx - 1, 0)
    second_sum.step(c)
    values = resid[...]
    scale = lax.rsqrt(jnp.mean(values * values, axis=-1, keepdims=True) + EPS)
    incoming = second_sum.total[...]
    weighted = incoming * gain
    mean = jnp.mean(weighted * values, axis=-1, keepdims=True)
    d_resid = dy_ref[...].astype(jnp.float32) + scale * weighted - values * (scale * scale * scale) * mean
    own_d[...] = d_resid.astype(jnp.bfloat16)
    d_resid_held[...] = d_resid
    d_resid_copy = pltpu.make_async_copy(d_resid_held, d_resid_out, out_sem.at[6])
    d_resid_copy.start()
    gain_out[...] = jnp.broadcast_to(jnp.sum(incoming * values * scale, axis=0, keepdims=True), gain_out.shape)
    d_line = LineGather(ctx, own_d, d_resid_all, dr_send, dr_recv, dr_local)
    d_line.start()
    def out_step(step, carry):
        out_sum.step(towards(c, step, ctx))
        return carry

    @pl.when(ends)
    def _():
        lax.fori_loop(0, ctx - 1, out_step, 0)

    line.finish_sends()
    second_sum.finish()
    pltpu.make_async_copy(d_line.own, d_line.slot(c), d_line.local).wait()
    grad_proj[...] = jnp.zeros_like(grad_proj)

    def back(step, carry):
        at = ordered(c, step, ctx)

        d_line.reach(step)
        d_line.other(at)
        incoming = d_resid_all[:, at].reshape(both_rows, D)
        d_att = outer(incoming, proj[...]).astype(jnp.bfloat16)
        d_stage[at] = d_att.reshape(2 * dp, span, 2 * LANES)
        for to in range(2 * dp):

            @pl.when(to != f)
            def _():
                remote(d_stage.at[at, to], unit.at[at, f], u_send.at[at, to], u_recv.at[at, f], at_device(d, c, to)).start()

            @pl.when(to == f)
            def _():
                unit[at, f] = d_stage[at, to]

        grad_proj[...] += inner(att[:, at].reshape(both_rows, 2 * LANES), incoming)

        @pl.when(jnp.logical_and(jnp.logical_not(ends), step == ctx - 2))
        def _():
            out_sum.step(towards(c, 0, ctx))

        return carry

    lax.fori_loop(0, ctx, back, 0)

    @pl.when(jnp.logical_not(ends))
    def _():
        lax.fori_loop(1, ctx - 1, out_step, 0)

    for slot in range(fs):
        start = slot // 2 * LANES + slot % 2 * each_proj
        grad_proj_low[slot] = grad_proj[start : start + each_proj, :].astype(jnp.bfloat16)
    grad_proj_copy = pltpu.make_async_copy(grad_proj_low, grad_proj_out, out_sem.at[1])
    grad_proj_copy.start()
    for at in range(ctx):
        for step in range(1, fs):
            other = lax.rem(f + step, fs)
            arrived(unit.at[at, other], u_recv.at[at, other], here)
    unit_copy = pltpu.make_async_copy(unit, unit_out, out_sem.at[2])
    unit_copy.start()
    d_line.finish_sends()
    for at in range(ctx):
        for to in range(fs):

            @pl.when(to != f)
            def _():
                left(d_stage.at[at, to], u_send.at[at, to], here)

    def settle_up(step, carry):
        first = pl.multiple_of(step * wide_rows, LANES)
        for slot in range(4):
            arrived(up_land.at[slot, pl.ds(first, wide_rows)], gup_recv.at[slot, step], here)

            @pl.when(jnp.logical_or(slot // 2 != d, 2 * d + slot % 2 != f))
            def _():
                left(grad_up.at[slot, pl.ds(first, wide_rows)], gup_send.at[slot, step], here)

        return carry

    def settle_down(step, carry):
        first = pl.multiple_of(step * wide_rows, LANES)
        for slot in range(4):
            arrived(down_land.at[slot, :, pl.ds(first, wide_rows)], gdn_recv.at[slot, step], here)

            @pl.when(slot != f)
            def _():
                left(grad_down.at[slot, :, pl.ds(first, wide_rows)], gdn_send.at[slot, step], here)

        return carry

    lax.fori_loop(0, ctx, settle_up, 0)
    lax.fori_loop(0, ctx, settle_down, 0)
    out_step(ctx - 1, 0)
    out_ref[...] = (resid[...] + out_sum.total[...]).astype(jnp.bfloat16)
    out_sum.finish()
    for copy in (d_resid_copy, grad_proj_copy, unit_copy):
        copy.wait()

def front(sizes, parts, x, attn_gain, mlp_gain, w_qkv, dy, w_out, w_down, w_gate_up):
    dp, ctx, fs = sizes
    n = dp * ctx * fs
    rows = x.shape[0]
    span = rows // 2
    hidden = FF // (dp * ctx)
    low, wide_t = jnp.bfloat16, jnp.float32
    dma = pltpu.SemaphoreType.DMA
    any_spec, vm_spec = pl.BlockSpec(memory_space=ANY), pl.BlockSpec(memory_space=VM)
    line_sems = [dma((3, ctx, HALVES)), dma((dp, ctx, HALVES)), dma]
    shapes = (
        jax.ShapeDtypeStruct((rows, D), low),
        jax.ShapeDtypeStruct((rows, D), wide_t),
        jax.ShapeDtypeStruct((8, D), wide_t),
        jax.ShapeDtypeStruct((2, ctx * fs, LANES), wide_t),
        jax.ShapeDtypeStruct((2, span, LANES), wide_t),
        jax.ShapeDtypeStruct((dp, ctx, rows, D), low),
        jax.ShapeDtypeStruct((ctx, fs, span, 4 * LANES), low),
        jax.ShapeDtypeStruct((4 * LANES, D), low),
        jax.ShapeDtypeStruct((8, D), wide_t),
        jax.ShapeDtypeStruct((ctx, fs, span, 2 * LANES), low),
        jax.ShapeDtypeStruct((fs,) + w_out.shape, low),
        jax.ShapeDtypeStruct((fs, D, hidden // 2), low),
        jax.ShapeDtypeStruct((fs, hidden // fs, D), low),
    )
    return pl.pallas_call(
        functools.partial(front_kernel, sizes, hidden, parts),
        name="front",
        out_shape=shapes,
        in_specs=[vm_spec] * 3 + [any_spec, vm_spec] + [any_spec] * 3,
        out_specs=[vm_spec, any_spec] + [vm_spec] * 3 + [any_spec] * 8,
        scratch_shapes=[
            VM((dp, ctx, rows, D), low),
            VM((4 * LANES, D), low),
            VM((dp, ctx, rows, D), low),
            VM((ctx, 2 * dp, span, 4 * LANES), low),
            VM((ctx, fs, span, 4 * LANES), low),
            VM((ctx, fs, span, 2 * LANES), low),
            VM((dp, ctx, 2, span, 2 * LANES), low),
            VM((n, 8, LANES), wide_t),
            VM((8, D), wide_t),
            VM((dp, ctx, rows, D), low),
            VM((2 * LANES, D), low),
            VM(w_down.shape, low),
            VM((fs, hidden // fs, D), low),
            VM((4, D, hidden // 2), low),
            VM((rows, D), wide_t),
            VM((rows, D), low),
            VM((dp, ctx, rows, D), low),
            VM((dp, ctx, rows, hidden), low),
            VM((dp, ctx, rows, 2 * hidden), low),
            VM((rows, D), low),
            VM((ctx, 2 * dp, span, 2 * LANES), low),
            VM((ctx, fs, span, 2 * LANES), low),
            VM((4, D, hidden // 2), low),
            VM((fs, hidden // fs, D), low),
            VM((2 * LANES, D), wide_t),
            VM((fs,) + w_out.shape, low),
            VM((8, LANES), wide_t),
            VM((rows, D), wide_t),
            *line_sems,
            dma((fs,)), dma((4,)), dma((2, fs)), dma((n,)), dma((n,)),
            dma((ctx, 2 * dp)), dma((ctx, fs)), dma((ctx, fs)), dma((fs, ctx)), dma((7,)),
            *line_sems,
            dma, dma((fs,)), dma((fs,)), dma, dma, dma((fs,)), dma((fs,)), dma((parts, fs)), dma((parts, 4)),
            *line_sems,
            *line_sems,
            dma((ctx, 2 * dp)), dma((ctx, fs)),
            dma((4, ctx)), dma((fs, ctx)), dma((fs, ctx)), dma((fs, ctx)),
        ] + LineSum.scratch(ctx, rows) * 2,
        compiler_params=pltpu.CompilerParams(collective_id=1, has_side_effects=True, vmem_limit_bytes=67043328),
    )(x, attn_gain, mlp_gain, w_qkv, dy, w_out, w_down, w_gate_up)


def fill_tables(block_ref, step_ref):
    span = step_ref.shape[1]
    for ref, scale in ((block_ref, span), (step_ref, 1)):
        shape = ref.shape[1:]
        lane = lax.broadcasted_iota(jnp.int32, shape, 1)
        pair = jnp.where(lane >= HD // 2, lane - HD // 2, lane).astype(jnp.float32)
        frequency = jnp.exp(pair * (-2.0 * math.log(THETA) / HD))
        angles = (lax.broadcasted_iota(jnp.int32, shape, 0) * scale).astype(jnp.float32) * frequency
        ref[0] = jnp.cos(angles)
        ref[1] = jnp.sin(angles)


def turns(block_ref, step_ref, block):
    cos_b, sin_b = block_ref[0, pl.ds(block, 1)], block_ref[1, pl.ds(block, 1)]
    cos_s, sin_s = step_ref[0], step_ref[1]
    cosine = cos_b * cos_s - sin_b * sin_s
    sine = sin_b * cos_s + cos_b * sin_s
    lane = lax.broadcasted_iota(jnp.int32, sine.shape, 1)
    first_half = lane < HD // 2
    sine_up = jnp.where(jnp.logical_and(lane >= HD // 2, lane < HD), sine, 0.0)
    return cosine, sine_up, jnp.where(first_half, -sine, 0.0)


def last_kernel(
    sizes, x_ref, gains_ref, block_ref, step_ref, gain_two_ref, proj_ref,
    d_resid_in, unit_ref, d_unit_ref, normed_ref, wide_ref, up_land_ref, down_land_ref,
    d_x_ref, gains_out, qkv_out, proj_out, up_out, down_out,
    unit, d_unit, d_k, d_v, stage, mixed, packed, normed, wide, grad_heads,
    up_land, down_land, proj_land, q_land, kv_land, down_sum, proj_sum, kv_sum, down_last, proj_last, kv_last, gain_vec, gain_stage, gain_land, up_sum, d_resid_ref,
    in_sem, proj_send, proj_recv, head_send, head_recv, move_send, move_recv,
    u_send, u_recv, g_send, g_recv, up_sem, wide_sem,
    *sums,
):
    dp, ctx, fs = sizes
    n = dp * ctx * fs
    d, c, f = place()
    here = at_device(d, c, f)
    me = (d * ctx + c) * fs + f
    rows = x_ref.shape[0]
    span = rows // 2
    both_rows = dp * rows
    low, wide_t = jnp.bfloat16, jnp.float32
    loads = [
        pltpu.make_async_copy(src, dst, in_sem.at[index])
        for index, (src, dst) in enumerate((
            (unit_ref, unit), (d_unit_ref, d_unit), (normed_ref, normed), (d_resid_in, d_resid_ref), (down_land_ref, down_land), (up_land_ref, up_land),
        ))
    ]
    wide_loads = [
        pltpu.make_async_copy(
            wide_ref.at[slot * LANES : slot * LANES + HD], wide.at[slot * HD : (slot + 1) * HD], wide_sem.at[slot]
        )
        for slot in range(4)
    ]
    tell_all(sizes)
    for load in loads + wide_loads:
        load.start()
    in_sum = LineSum(ctx, *sums[:6], sums[6:10])
    d_k[...] = jnp.zeros_like(d_k)
    d_v[...] = jnp.zeros_like(d_v)

    def push(src, land, send, recv, core, fs_to):
        to_self = jnp.logical_and(core == d, fs_to == f)

        @pl.when(jnp.logical_not(to_self))
        def _():
            remote(src, land.at[f], send, recv.at[f], at_device(core, c, fs_to)).start()

        @pl.when(to_self)
        def _():
            pltpu.make_async_copy(src, land.at[f], recv.at[f]).start()

    def pushed(src, send, core, fs_to):
        @pl.when(jnp.logical_not(jnp.logical_and(core == d, fs_to == f)))
        def _():
            left(src, send, here)

    def sum_of(land):
        total = land[0].astype(wide_t)
        for source in range(1, fs):
            total += land[source].astype(wide_t)
        return total

    _, (own_core, own_ctx) = down_route(d, c)
    stays = jnp.logical_and(own_core == d, own_ctx == c)

    def move(index, src, dst):
        @pl.when(jnp.logical_not(stays))
        def _():
            remote(src, dst, move_send.at[index], move_recv.at[index], at_device(own_core, own_ctx, f)).start()

        @pl.when(stays)
        def _():
            pltpu.make_async_copy(src, dst, move_recv.at[index]).start()

    loads[0].wait()
    loads[1].wait()
    block = fs * span

    def unturn(values, at):
        up = pltpu.roll(values, HD // 2, 1)
        down = pltpu.roll(values, LANES - HD // 2, 1)
        pieces = []
        for index in range(fs):
            own = slice(index * span, (index + 1) * span)
            cosine, sine_up, sine_down = turns(block_ref, step_ref, at * fs + index)
            pieces.append(values[own] * cosine - up[own] * sine_up - down[own] * sine_down)
        return jnp.concatenate(pieces, axis=0)

    for at in reversed(range(ctx)):
        keys = block * (at + 1)
        k_rows = unit[0 : at + 1, :, :, 2 * LANES : 3 * LANES].reshape(keys, LANES)
        v_rows = unit[0 : at + 1, :, :, 3 * LANES : 4 * LANES].reshape(keys, LANES)
        allowed = lax.broadcasted_iota(jnp.int32, (block, keys), 1) <= block * at + lax.broadcasted_iota(
            jnp.int32, (block, keys), 0
        )
        for head in range(2):
            lanes = slice(head * LANES, (head + 1) * LANES)
            q_rows = unit[at, :, :, lanes].reshape(block, LANES)
            d_rows = d_unit[at, :, :, lanes].reshape(block, LANES)
            scores = jnp.where(allowed, outer(q_rows, k_rows) * FACTOR, NEG)
            weights = jnp.exp(scores - jnp.max(scores, axis=-1, keepdims=True))
            probs = weights / jnp.sum(weights, axis=-1, keepdims=True)
            d_probs = outer(d_rows, v_rows)
            delta = jnp.sum(probs * d_probs, axis=-1, keepdims=True)
            d_scores = (probs * (d_probs - delta)).astype(low)
            d_q = jnp.dot(d_scores, k_rows, preferred_element_type=wide_t) * FACTOR
            packed[:, head * HD : (head + 1) * HD] = unturn(d_q, at)[:, :HD]
            d_k[0:keys, :] += inner(d_scores, q_rows) * FACTOR
            d_v[0:keys, :] += inner(probs.astype(low), d_rows)
        packed[:, 2 * HD : 3 * HD] = unturn(d_k[block * at : keys, :], at)[:, :HD]
        packed[:, 3 * HD : 4 * HD] = d_v[block * at : keys, :HD]
        stage[at] = packed[...].astype(low).reshape(fs, span, 4 * HD)
        if at == ctx - 1:
            hear_all(sizes)
        for to in range(fs):

            @pl.when(to != f)
            def _():
                remote(
                    stage.at[at, to], mixed.at[f // 2, at, lax.rem(f, 2)], u_send.at[at, to], u_recv.at[f, at], at_device(d, c, to)
                ).start()

            @pl.when(to == f)
            def _():
                mixed[f // 2, at, lax.rem(f, 2)] = stage[at, to]

        if at == ctx - 1:
            loads[4].wait()
            down_sum[...] = sum_of(down_land).astype(low)
            move(0, down_sum, down_last)
    loads[2].wait()
    for load in wide_loads:
        load.wait()

    ends = jnp.logical_or(c == 0, c == ctx - 1)

    def give(step, carry):
        at = towards(c, step, ctx)
        for move_ in range(1, fs):
            other = lax.rem(f + move_, fs)
            arrived(mixed.at[other // 2, at, lax.rem(other, 2)], u_recv.at[other, at], here)
        terms = jnp.dot(mixed[:, at].reshape(both_rows, 4 * HD), wide[...], preferred_element_type=wide_t)
        in_sum.give(at, terms.reshape(dp, rows, D))

        @pl.when(jnp.logical_and(ends, jnp.logical_and(step > 0, step < ctx - 1)))
        def _():
            in_sum.step(towards(c, step - 1, ctx))

        return carry

    lax.fori_loop(0, ctx, give, 0)

    every = dp * ctx * rows
    k_relay = 2 * lax.rem(c, 2) + d
    relays = (k_relay, lax.rem(k_relay + 2, fs))
    gain_terms = jnp.zeros((1, D), wide_t)
    for slot in (2, 3, 0, 1):
        if slot % 2 == 0:
            both_heads = inner(
                mixed[...].reshape(every, 4 * HD)[:, slot * HD : (slot + 2) * HD], normed[...].reshape(every, D)
            )
        heads = both_heads[slot % 2 * HD : (slot % 2 + 1) * HD]
        grad_heads[slot] = heads.astype(low)
        weights = wide[slot * HD : (slot + 1) * HD, :].astype(wide_t)
        gain_terms += jnp.sum(heads * weights, axis=0, keepdims=True)
        if slot < 2:
            push(grad_heads.at[slot], q_land, head_send.at[slot], head_recv.at[0], 0, 2 * d + slot)
        else:
            push(grad_heads.at[slot], kv_land.at[slot - 2], head_send.at[slot], head_recv.at[slot - 1], d, relays[slot - 2])

    for slot in range(fs):
        push(proj_ref.at[slot], proj_land, proj_send.at[slot], proj_recv, d, slot)

    gain = gains_ref[0:1, :]
    gain_vec[0:1, :] = gain_terms / gain
    gain_vec[1:2, :] = gain_two_ref[0:1, :]
    each = D // n
    for index in range(n):
        gain_stage[index, :, 0:each] = gain_vec[:, index * each : (index + 1) * each]
    gain_land[me] = gain_stage[me]

    def gain_to(step, carry):
        other = lax.rem(me + step, n)
        remote(
            gain_stage.at[other], gain_land.at[me], g_send.at[other], g_recv.at[me],
            at_device(other // (ctx * fs), lax.rem(other // fs, ctx), lax.rem(other, fs)),
        ).start()
        return carry

    lax.fori_loop(1, n, gain_to, 0)

    def middle_step(step, carry):
        in_sum.step(towards(c, step, ctx))
        return carry

    lax.fori_loop(jnp.where(ends, ctx - 2, 0), ctx - 1, middle_step, 0)

    def kv_route(slot):
        owner, owner_f = slot * 2 + c // 2, k_relay
        return owner, owner_f, jnp.logical_or(jnp.logical_or(d != 1, owner != c), owner_f != f)

    for slot in range(2):
        owner, owner_f, away = kv_route(slot)

        @pl.when(f == relays[slot])
        def _():
            for source in range(fs):
                arrived(kv_land.at[slot, source], head_recv.at[1 + slot, source], here)
            kv_sum[slot] = sum_of(kv_land.at[slot]).astype(low)

            @pl.when(away)
            def _():
                remote(kv_sum.at[slot], kv_last, move_send.at[2 + slot], move_recv.at[2], at_device(1, owner, owner_f)).start()

            @pl.when(jnp.logical_not(away))
            def _():
                pltpu.make_async_copy(kv_sum.at[slot], kv_last, move_recv.at[2]).start()

    for source in range(fs):
        arrived(proj_land.at[source], proj_recv.at[source], here)
    proj_sum[...] = sum_of(proj_land).astype(low)
    move(1, proj_sum, proj_last)

    loads[5].wait()
    up_sum[...] = sum_of(up_land)
    up_copy = pltpu.make_async_copy(up_sum, up_out, up_sem)
    up_copy.start()
    @pl.when(d == 0)
    def _():
        for source in range(fs):
            arrived(q_land.at[source], head_recv.at[0, source], here)
        qkv_out[...] = sum_of(q_land)

    for slot in range(fs):
        pushed(proj_ref.at[slot], proj_send.at[slot], d, slot)
    for slot in range(2):
        pushed(grad_heads.at[slot], head_send.at[slot], 0, 2 * d + slot)
        pushed(grad_heads.at[2 + slot], head_send.at[2 + slot], d, relays[slot])

    for at in range(ctx):
        for to in range(fs):

            @pl.when(to != f)
            def _():
                left(stage.at[at, to], u_send.at[at, to], here)

    def gain_from(step, carry):
        other = lax.rem(me + step, n)
        arrived(gain_land.at[other], g_recv.at[other], here)
        return carry

    lax.fori_loop(1, n, gain_from, 0)
    total = gain_land[0]
    for index in range(1, n):
        total += gain_land[index]
    gains_out[...] = total

    def gain_left(step, carry):
        other = lax.rem(me + step, n)
        left(gain_stage.at[other], g_send.at[other], here)
        return carry

    lax.fori_loop(1, n, gain_left, 0)

    loads[3].wait()
    arrived(down_last, move_recv.at[0], here)
    down_out[...] = down_last[...].astype(wide_t)
    values = x_ref[...].astype(wide_t)
    scale = lax.rsqrt(jnp.mean(values * values, axis=-1, keepdims=True) + EPS)
    in_sum.step(c)

    incoming = in_sum.total[...]
    weighted = incoming * gain
    mean = jnp.mean(weighted * values, axis=-1, keepdims=True)
    d_x_ref[...] = (d_resid_ref[...] + scale * weighted - values * (scale * scale * scale) * mean).astype(low)

    arrived(proj_last, move_recv.at[1], here)
    proj_out[...] = proj_last[...].astype(wide_t)

    @pl.when(d == 1)
    def _():
        arrived(kv_last, move_recv.at[2], here)
        qkv_out[...] = kv_last[...].astype(wide_t)

    for slot in range(2):
        away = kv_route(slot)[2]

        @pl.when(jnp.logical_and(f == relays[slot], away))
        def _():
            left(kv_sum.at[slot], move_send.at[2 + slot], here)

        @pl.when(jnp.logical_not(stays))
        def _():
            left((down_sum, proj_sum)[slot], move_send.at[slot], here)

    in_sum.finish()
    up_copy.wait()


def last(sizes, x, gains, tables, d_resid, gain_two, grad_proj, unit, d_unit, normed, wide, up_land, down_land):
    dp, ctx, fs = sizes
    n = dp * ctx * fs
    rows = x.shape[0]
    span = rows // 2
    low, wide_t = jnp.bfloat16, jnp.float32
    dma = pltpu.SemaphoreType.DMA
    any_spec, vm_spec = pl.BlockSpec(memory_space=ANY), pl.BlockSpec(memory_space=VM)
    down_rows, proj_rows, half = down_land.shape[1], grad_proj.shape[1], up_land.shape[2]
    shapes = (
        jax.ShapeDtypeStruct((rows, D), low),
        jax.ShapeDtypeStruct((8, LANES), wide_t),
        jax.ShapeDtypeStruct((HD, D), wide_t),
        jax.ShapeDtypeStruct((proj_rows, D), wide_t),
        jax.ShapeDtypeStruct((D, half), wide_t),
        jax.ShapeDtypeStruct((down_rows, D), wide_t),
    )
    return pl.pallas_call(
        functools.partial(last_kernel, sizes),
        name="last",
        out_shape=shapes,
        in_specs=[vm_spec] * 5 + [any_spec] * 8,
        out_specs=[vm_spec] * 4 + [any_spec, vm_spec],
        scratch_shapes=[
            VM(unit.shape, low),
            VM(d_unit.shape, low),
            VM((ctx * fs * span, LANES), wide_t),
            VM((ctx * fs * span, LANES), wide_t),
            VM((ctx, fs, span, 4 * HD), low),
            VM((dp, ctx, 2, span, 4 * HD), low),
            VM((fs * span, 4 * HD), wide_t),
            VM(normed.shape, low),
            VM((4 * HD, D), low),
            VM((4, HD, D), low),
            VM(up_land.shape, low),
            VM((fs, down_rows, D), low),
            VM((fs, proj_rows, D), low),
            VM((fs, HD, D), low),
            VM((2, fs, HD, D), low),
            VM((down_rows, D), low),
            VM((proj_rows, D), low),
            VM((2, HD, D), low),
            VM((down_rows, D), low),
            VM((proj_rows, D), low),
            VM((HD, D), low),
            VM((8, D), wide_t),
            VM((n, 8, LANES), wide_t),
            VM((n, 8, LANES), wide_t),
            VM((D, half), wide_t),
            VM((rows, D), wide_t),
            dma((6,)), dma((fs,)), dma((fs,)),
            dma((4,)), dma((3, fs)), dma((4,)), dma((3,)),
            dma((ctx, fs)), dma((fs, ctx)), dma((n,)), dma((n,)), dma, dma((4,)),
        ] + LineSum.scratch(ctx, rows),
        compiler_params=pltpu.CompilerParams(collective_id=3, has_side_effects=True, vmem_limit_bytes=63 * 1024 * 1024),
    )(x, gains, *tables, gain_two, grad_proj, d_resid, unit, d_unit, normed, wide, up_land, down_land)


PIECES = 4


def emit_kernel(count, gains_ref, *refs):
    sources, outs, one_ref, two_ref = refs[:count], refs[count : 2 * count], refs[2 * count], refs[2 * count + 1]
    held, in_sem, out_sem = refs[2 * count + 2 : 3 * count + 2], refs[-2], refs[-1]
    loads, stores = [], []
    for index in range(count):
        rows = held[index].shape[0]
        pieces = PIECES if rows % (PIECES * 16) == 0 else 1
        for piece in range(pieces):
            own = slice(piece * rows // pieces, (piece + 1) * rows // pieces)
            loads.append(pltpu.make_async_copy(sources[index].at[own], held[index].at[own], in_sem.at[len(loads)]))
            stores.append(pltpu.make_async_copy(held[index].at[own], outs[index].at[own], out_sem.at[len(stores)]))
    for load in loads:
        load.start()
    each = one_ref.shape[0]
    one_ref[...] = gains_ref[0, :each]
    two_ref[...] = gains_ref[1, :each]
    for load, store in zip(loads, stores):
        load.wait()
        store.start()
    for store in stores:
        store.wait()


def emit(each, gains, *arrays):
    count = len(arrays)
    any_spec, vm_spec = pl.BlockSpec(memory_space=ANY), pl.BlockSpec(memory_space=VM)
    gain = jax.ShapeDtypeStruct((each,), jnp.float32)
    return pl.pallas_call(
        functools.partial(emit_kernel, count),
        name="emit",
        out_shape=[jax.ShapeDtypeStruct(a.shape, a.dtype) for a in arrays] + [gain, gain],
        in_specs=[vm_spec] + [any_spec] * count,
        out_specs=[any_spec] * count + [vm_spec] * 2,
        scratch_shapes=[VM(a.shape, a.dtype) for a in arrays] + [pltpu.SemaphoreType.DMA((count * PIECES,))] * 2,
        compiler_params=pltpu.CompilerParams(vmem_limit_bytes=63 * 1024 * 1024),
    )(gains, *arrays)


def on_device(tokens, cotangent, attn_gain, w_qkv, w_out, mlp_gain, w_gate_up, w_down):
    dp, ctx, fs = where = tuple(lax.axis_size(name) for name in ("dp", "ctx", "fsdp"))
    mb, _, span, _ = tokens.shape
    rows = mb * span
    x = tokens.reshape(rows, D)
    dy = cotangent.reshape(rows, D)
    each = attn_gain.shape[0]
    block_out, d_resid, grad_two, *tables, normed, unit, qkv, gains, d_unit, grad_proj, up_land, down_land = front(
        where, 8, x, attn_gain, mlp_gain, w_qkv.T, dy, w_out, w_down, w_gate_up
    )
    grad_tokens, gain_grads, grad_qkv, grad_out, grad_gate_up, grad_down = last(
        where, x, gains, tables, d_resid, grad_two, grad_proj, unit, d_unit, normed, qkv, up_land, down_land
    )
    block_out, grad_tokens, grad_qkv, grad_out, grad_gate_up, grad_down, grad_one, grad_two = emit(
        each, gain_grads, block_out, grad_tokens, grad_qkv, grad_out, grad_gate_up, grad_down
    )
    return (
        block_out.reshape(tokens.shape),
        grad_tokens.reshape(tokens.shape),
        grad_one,
        grad_qkv.T,
        grad_out,
        grad_two,
        grad_gate_up,
        grad_down,
    )


def fits(mesh):
    return mesh.shape["dp"] == 2 and mesh.shape["ctx"] == 4 and mesh.shape["fsdp"] == 4


def solution(mesh):
    placed = (
        P(None, "dp", ("ctx", "fsdp"), None),
        P(None, "dp", ("ctx", "fsdp"), None),
        P(("dp", "ctx", "fsdp")),
        P(None, ("dp", "ctx", "fsdp")),
        P(("dp", "ctx", "fsdp"), None),
        P(("dp", "ctx", "fsdp")),
        P(None, ("dp", "ctx", "fsdp")),
        P(("dp", "ctx", "fsdp"), None),
    )
    return jax.shard_map(
        on_device if fits(mesh) else on_device_gathered,
        mesh=mesh,
        in_specs=placed,
        out_specs=(
            P(None, "dp", ("ctx", "fsdp"), None),
            P(None, "dp", ("ctx", "fsdp"), None),
            P(("dp", "ctx", "fsdp")),
            P(None, ("dp", "ctx", "fsdp")),
            P(("dp", "ctx", "fsdp"), None),
            P(("dp", "ctx", "fsdp")),
            P(None, ("dp", "ctx", "fsdp")),
            P(("dp", "ctx", "fsdp"), None),
        ),
        check_vma=False,
    )
```
